32 devices in a mesh: rep: 4 (over y, x), shard: 8 (over z, core).
Axes of the slice: x: 2, y: 2, z: 4, core: 2. Of those that a mesh axis runs over, the one named last changes fastest.
Arguments:
- inputs: bfloat16 [8192, 768], P(('rep', 'shard')), may hold values from -6 to 6
- cotangent: bfloat16 [8192, 768], P(('rep', 'shard')), may hold values from -6 to 6
- lengths: int32 [4, 4], P('rep'), may hold values from 1 to 1024, 2048 in all within a row
- dealing: int32 [4, 2048], P('rep', 'shard'), may hold values from 0 to 2047, each once within a row
- key_mask: int32 [4, 2048], P('rep', 'shard'), may hold values 0 or 1
- entry_weight: float32 [2, 768, 2304], P(None, 'shard'), may hold values from -0.21875 to 0.21875
- exit_weight: float32 [2, 768, 768], P(None, 'shard'), may hold values from -6 to 6
- expand_weight: float32 [2, 768, 3072], P(None, 'shard'), may hold values from -0.21875 to 0.21875
- shrink_weight: float32 [2, 3072, 768], P(None, 'shard'), may hold values from -0.109375 to 0.109375
- vectors: float32 [2, 9216], P(None, 'shard'), may hold values from -1.2 to 1.4, as said below
Outputs:
- output: bfloat16 [8192, 768], P(('rep', 'shard'))
- input_grad: float32 [8192, 768], P(('rep', 'shard'))
- entry_grad: float32 [2, 768, 2304], P(None, 'shard')
- exit_grad: float32 [2, 768, 768], P(None, 'shard')
- expand_grad: float32 [2, 768, 3072], P(None, 'shard')
- shrink_grad: float32 [2, 3072, 768], P(None, 'shard')
- vector_grad: float32 [2, 9216], P(None, 'shard')
The draws below stay inside these ranges and needn't reach their ends.
Inputs may be any that keep to these rules, and one draw needn't show every extreme that they name: The 4 lengths of a group sum to 2048; the longest of each group is exactly 1024. `dealing`: each row is a permutation of 0 to 2047. `vectors`: the norm gains lie in 0.6 to 1.4.
All inputs are finite; a program needn't handle non-finite values. No bound on the sum of `key_mask` on one device may be relied on, other than what follows from the above.
Results may differ from the reference program's by a relative error of at most 0.04.
Values may be sent and summed in bfloat16 or wider, within the bound.
No kernel may reach another device: no remote copies, remote signals or barrier semaphores. Data moves between devices by JAX's collectives and lax.ppermute only.
A program may use at most 192 MiB of HBM per device.

```python
import math
import jax
import jax.numpy as jnp
import numpy as np
from jax import lax

D = 768
HEADS = 12
HEAD_DIM = 64
FF = 3072
LAYERS = 2
SEQS = 4
GROUPS = 4
GROUP_TOK = 2048
TOKENS = 8192
MOST = 1024


def draw_vectors(key, part):
    first_key = jax.random.fold_in(key, 11)
    second_key = jax.random.fold_in(key, 23)
    total = 8 * D + FF
    column = jnp.arange(total, dtype=jnp.int32)[None, :]
    biases = 0.4 * jax.random.truncated_normal(first_key, -3.0, 3.0, (LAYERS, total), jnp.float32)
    gains = jax.random.uniform(second_key, (LAYERS, total), jnp.float32, 0.6, 1.4)
    is_gain = (column >= 3 * D) & (column < 4 * D) | (column >= 6 * D) & (column < 7 * D)
    return jnp.where(is_gain, gains, biases)


def plant(values, rng, low, top_value):
    shape = values.shape
    spot = [jax.random.randint(jax.random.fold_in(rng, axis), (), 0, shape[axis]) for axis in range(len(shape))]
    values = values.at[tuple(spot)].set(low)
    longest = shape.index(max(shape))
    spot[longest] = (spot[longest] + 1) % shape[longest]
    return values.at[tuple(spot)].set(top_value)


def shard_levels(key, dims, cuts, smallest, top_value):
    def one(axis_at, shards_of):
        draws = jax.random.uniform(jax.random.fold_in(jax.random.fold_in(key, 6), axis_at), (shards_of,), jnp.float32, smallest / len(cuts), top_value / len(cuts))
        return jnp.repeat(jnp.exp(draws), dims[axis_at] // shards_of).reshape((-1,) + (1,) * (len(dims) - axis_at - 1))

    factor_of = one(*cuts[0])
    for cut in cuts[1:]:
        factor_of = factor_of * one(*cut)
    return factor_of


def split_up(number_of, total, bound, slope):
    portions = [(1 << 20) // math.isqrt(grade ** slope) + 1 for grade in range(2, number_of + 1)]
    rest, counts = total - bound - (number_of - 1), [1] * (number_of - 1)
    while rest > 0:
        candidates = [i for i in range(number_of - 1) if counts[i] < bound]
        whole, budget = sum([portions[i] for i in candidates]), rest
        for i in candidates:
            extra = min(bound - counts[i], max(1, budget * portions[i] // whole), rest)
            counts[i] = counts[i] + extra
            rest = rest - extra
    return np.array([bound] + counts)


def ragged_sizes(own_key, count, total, most, slope):
    if count == 2:
        one = jax.random.randint(own_key, (), max(1, total - most), min(most, total - 1) + 1)
        return jnp.stack([one, total - one])
    tallies = jnp.asarray(split_up(count, total, most, slope), jnp.int32)
    pairs = (count - 1) // 2
    source_of, taker = tallies[1:1 + 2 * pairs:2], tallies[2:2 + 2 * pairs:2]
    room = jnp.minimum(source_of - 1, most - taker)
    moved = jax.random.randint(jax.random.fold_in(own_key, 1), (pairs,), 0, 1 << 20) % (room + 1)
    tallies = tallies.at[1:1 + 2 * pairs:2].set(source_of - moved).at[2:2 + 2 * pairs:2].set(taker + moved)
    return tallies[jax.random.permutation(jax.random.fold_in(own_key, 2), count)]


def noise(stream_key, dims, scale, reach, cuts=(), kind=jnp.bfloat16):
    loudness = shard_levels(stream_key, dims, cuts, -0.22, 0.18) if cuts else 1.0
    array = jax.random.normal(stream_key, dims, jnp.float32) * scale * loudness
    return jnp.minimum(jnp.maximum(array, -reach), reach).astype(kind)


def setup_inputs(seed: int = 0) -> dict:
    splits = jax.random.split(jax.random.key(seed), 11)
    inputs = noise(splits[0], (TOKENS, D), 1.0, 6.0, ((0, 32),))
    cotangent = noise(splits[1], (TOKENS, D), 1.0, 6.0, ((0, 32),))
    lengths = jax.vmap(lambda own: ragged_sizes(own, SEQS, GROUP_TOK, MOST, 2))(jax.random.split(splits[2], GROUPS)).reshape((GROUPS, SEQS)).astype(jnp.int32)
    dealing = jax.vmap(lambda own: jax.random.permutation(own, GROUP_TOK))(jax.random.split(splits[3], GROUPS)).reshape((GROUPS, GROUP_TOK)).astype(jnp.int32)
    key_mask = plant((jax.random.randint(splits[4], (GROUPS, GROUP_TOK), 0, 8) < 7).astype(jnp.int32), jax.random.fold_in(splits[4], 1), 0, 1)
    entry_weight = noise(splits[5], (LAYERS, D, 3 * D), D ** -0.5, 0.21875, ((1, 8),), jnp.float32)
    exit_weight = noise(splits[6], (LAYERS, D, D), 1 ** -0.5, 6.0, ((1, 8),), jnp.float32)
    expand_weight = noise(splits[7], (LAYERS, D, FF), D ** -0.5, 0.21875, ((1, 8),), jnp.float32)
    shrink_weight = noise(splits[8], (LAYERS, FF, D), FF ** -0.5, 0.109375, ((1, 8),), jnp.float32)
    vectors = draw_vectors(jax.random.fold_in(splits[10], 71), 0)
    return {"inputs": inputs, "cotangent": cotangent, "lengths": lengths, "dealing": dealing, "key_mask": key_mask, "entry_weight": entry_weight, "exit_weight": exit_weight, "expand_weight": expand_weight, "shrink_weight": shrink_weight, "vectors": vectors}


@jax.custom_vjp
def low(v):
    return lax.optimization_barrier(v.astype(jnp.bfloat16)).astype(jnp.float32)

@jax.custom_vjp
def low_back(v):
    return v

def low_keep(v):
    return (low(v), None)

def low_pass(kept, grad):
    return (grad,)

def back_keep(v):
    return (v, None)

def back_low(kept, grad):
    return (low(grad),)
low.defvjp(low_keep, low_pass)
low_back.defvjp(back_keep, back_low)
HIGHEST = lax.Precision.HIGHEST
NEG_FILL = -1e+30

def layer_norm(resid, gain, shift):
    center = lax.optimization_barrier(jnp.mean(resid, axis=-1, keepdims=True))
    offsets = resid - center
    spread = lax.optimization_barrier(jnp.mean(offsets * offsets, axis=-1, keepdims=True))
    return offsets * lax.rsqrt(spread + 1e-05) * gain + shift

def sequence_ids(lengths):
    ending = jnp.cumsum(lengths).astype(jnp.int32)
    opening = (ending - lengths).astype(jnp.int32)
    places = jnp.arange(GROUP_TOK, dtype=jnp.int32)
    member = lax.optimization_barrier(jnp.sum((places[:, None] >= ending[None, :]).astype(jnp.int32), axis=1)).astype(jnp.int32)
    leading = jnp.any(places[:, None] == opening[None, :], axis=1)
    return (member, leading)

def attention(queries, keys, values, member, usable):
    block_rows = min(512, GROUP_TOK)
    query_heads = queries.reshape(GROUP_TOK // block_rows, block_rows, HEADS, HEAD_DIM)
    query_member = member.reshape(GROUP_TOK // block_rows, block_rows)
    key_heads = keys.reshape(GROUP_TOK, HEADS, HEAD_DIM)
    value_heads = values.reshape(GROUP_TOK, HEADS, HEAD_DIM)

    def one_block(items):
        block_queries, block_member = items
        scores = jnp.einsum('qhd,khd->hqk', block_queries, key_heads, precision=HIGHEST) * HEAD_DIM ** (-0.5)
        scores = low_back(scores)
        allowed = ((block_member[:, None] == member[None, :]) & usable[None, :])[None]
        scores = jnp.where(allowed, scores, NEG_FILL)
        largest = lax.optimization_barrier(jnp.max(scores, axis=-1, keepdims=True))
        expos = jnp.where(allowed, jnp.exp(scores - largest), 0.0)
        probs = low(expos / lax.optimization_barrier(jnp.sum(expos, axis=-1, keepdims=True)))
        mixed = jnp.einsum('hqk,khd->qhd', probs, value_heads, precision=HIGHEST)
        return mixed.reshape(block_rows, HEADS * HEAD_DIM)
    blocks = lax.map(jax.checkpoint(one_block), (query_heads, query_member))
    return blocks.reshape(GROUP_TOK, HEADS * HEAD_DIM)

def encoder_layer(hidden, entry, leaving, expand, shrink, vector, member, usable):
    entry = low(entry)
    leaving = low(leaving)
    expand = low(expand)
    shrink = low(shrink)
    vector = low(vector)
    pieces = [vector[index * D:(index + 1) * D] for index in range(8)]
    bias_up = vector[8 * D:]
    flat = low(hidden)
    mixed = jnp.dot(flat, entry, precision=HIGHEST)
    queries = low(low_back(mixed[:, 0:D] + pieces[0]))
    keys = low(low_back(mixed[:, D:2 * D]))
    values = low(low_back(mixed[:, 2 * D:3 * D] + pieces[1]))
    attended = low(low_back(attention(queries, keys, values, member, usable)))
    branch = low_back(jnp.dot(attended, leaving, precision=HIGHEST) + pieces[2])
    middle = layer_norm(hidden + branch, pieces[3], pieces[4])
    inner = low_back(jnp.dot(low(middle), expand, precision=HIGHEST) + bias_up)
    active = low(jax.nn.gelu(inner, approximate=False))
    branch_two = low_back(jnp.dot(active, shrink, precision=HIGHEST) + pieces[5])
    return layer_norm(middle + branch_two, pieces[6], pieces[7])

def group_forward(params, rows_group, dealt, lengths, mask_row):
    member, leading = sequence_ids(lengths)
    usable = (mask_row == 1) | leading
    inverse = jnp.zeros((GROUP_TOK,), jnp.int32).at[dealt].set(jnp.arange(GROUP_TOK, dtype=jnp.int32))
    hidden = jnp.take(rows_group, dealt, axis=0)
    entry_all, exit_all, expand_all, shrink_all, vector_all = params
    for layer_index in range(LAYERS):
        hidden = encoder_layer(hidden, entry_all[layer_index], exit_all[layer_index], expand_all[layer_index], shrink_all[layer_index], vector_all[layer_index], member, usable)
    return jnp.take(hidden, inverse, axis=0)

def reference(inputs, cotangent, lengths, dealing, key_mask, entry_weight, exit_weight, expand_weight, shrink_weight, vectors):
    params = (entry_weight.astype(jnp.float32), exit_weight.astype(jnp.float32), expand_weight.astype(jnp.float32), shrink_weight.astype(jnp.float32), vectors.astype(jnp.float32))
    rows_all = inputs.astype(jnp.float32).reshape(GROUPS, GROUP_TOK, D)
    grads_all = cotangent.astype(jnp.float32).reshape(GROUPS, GROUP_TOK, D)

    def one_group(totals, items):
        rows_group, grad_group, lengths_group, dealt, mask_row = items

        def forward(weights, rows_in):
            return group_forward(weights, rows_in, dealt, lengths_group, mask_row)
        result, pullback = jax.vjp(forward, params, rows_group)
        weight_grads, rows_grad = pullback(grad_group)
        totals = jax.tree.map(jnp.add, totals, weight_grads)
        return (totals, (result, rows_grad))
    zeros = jax.tree.map(jnp.zeros_like, params)
    totals, outputs = lax.scan(one_group, zeros, (rows_all, grads_all, lengths, dealing, key_mask))
    results, rows_grads = outputs
    return (results.reshape(TOKENS, D).astype(jnp.bfloat16), rows_grads.reshape(TOKENS, D), totals[0], totals[1], totals[2], totals[3], totals[4])
```

```python
import functools

import jax
import jax.numpy as jnp
from jax import lax
from jax.experimental import pallas as pl
from jax.experimental.pallas import tpu as pltpu
from jax.sharding import PartitionSpec as P

HEADS = 12
HEAD_DIM = 64


NEG_FILL = -1e30


def norm_forward(resid, gain, shift):
    center = jnp.mean(resid, axis=-1, keepdims=True)
    offsets = resid - center
    spread = jnp.mean(offsets * offsets, axis=-1, keepdims=True)
    factor = lax.rsqrt(spread + 1e-05)
    normed = offsets * factor
    return (normed * gain + shift, normed, factor)


def norm_backward(incoming, normed, factor, gain):
    scaled = incoming * gain
    resid_grad = factor * (
        scaled
        - jnp.mean(scaled, axis=-1, keepdims=True)
        - normed * jnp.mean(scaled * normed, axis=-1, keepdims=True)
    )
    return (resid_grad, jnp.sum(incoming * normed, axis=0), jnp.sum(incoming, axis=0))


def inner_rows(left, right):
    return lax.dot_general(
        left, right, (((0,), (0,)), ((), ())), preferred_element_type=jnp.float32
    )


def times_trans(left, right):
    return lax.dot_general(
        left, right, (((1,), (1,)), ((), ())), preferred_element_type=jnp.float32
    )


def gelu_exact(value):
    return jax.nn.gelu(value, approximate=False)


def sequence_ids(lengths, group_rows):
    ending = jnp.cumsum(lengths)
    opening = ending - lengths
    places = jnp.arange(group_rows, dtype=jnp.int32)
    member = jnp.sum((places[:, None] >= ending[None, :]).astype(jnp.int32), axis=1)
    leading = jnp.any(places[:, None] == opening[None, :], axis=1)
    return (member, leading)


def split_vector(vector, model_width):
    pieces = [vector[index * model_width : (index + 1) * model_width] for index in range(8)]
    pieces.append(vector[8 * model_width :])
    return pieces


def fetch_forward(entry_weight, exit_weight, expand_weight, shrink_weight, vectors, layer_index):
    return (
        lax.all_gather(entry_weight[layer_index].astype(jnp.bfloat16), "shard", axis=0, tiled=True),
        lax.all_gather(exit_weight[layer_index].astype(jnp.bfloat16), "shard", axis=0, tiled=True),
        lax.all_gather(
            expand_weight[layer_index].astype(jnp.bfloat16), "shard", axis=0, tiled=True
        ),
        lax.all_gather(
            shrink_weight[layer_index].astype(jnp.bfloat16), "shard", axis=0, tiled=True
        ),
        lax.all_gather(vectors[layer_index].astype(jnp.bfloat16), "shard", axis=0, tiled=True),
    )


def fetch_backward(entry_weight, exit_weight, expand_weight, shrink_weight, vectors, layer_index):
    return (
        lax.all_gather(entry_weight[layer_index].astype(jnp.bfloat16), "shard", axis=0, tiled=True),
        lax.all_gather(exit_weight[layer_index].astype(jnp.bfloat16), "shard", axis=0, tiled=True),
        lax.all_gather(
            expand_weight[layer_index].astype(jnp.bfloat16), "shard", axis=0, tiled=True
        ),
        lax.all_gather(
            shrink_weight[layer_index].astype(jnp.bfloat16), "shard", axis=0, tiled=True
        ),
        lax.all_gather(vectors[layer_index].astype(jnp.bfloat16), "shard", axis=0, tiled=True),
    )


def attend_forward(queries, keys, values, own_member, member, usable):
    local_rows = queries.shape[0]
    query_heads = queries.reshape(local_rows, HEADS, HEAD_DIM)
    factor_scale = HEAD_DIM ** (-0.5)
    start_state = (
        jnp.full((HEADS, local_rows), NEG_FILL, jnp.float32),
        jnp.zeros((HEADS, local_rows), jnp.float32),
        jnp.zeros((HEADS, local_rows, HEAD_DIM), jnp.float32),
    )
    key_piece = lax.all_gather(keys, "shard", axis=0, tiled=True)
    value_piece = lax.all_gather(values, "shard", axis=0, tiled=True)
    amount = key_piece.shape[0]
    block_rows = local_rows * max(1, 512 // local_rows)

    def fold_advance(block_index, running):
        running_max, running_total, weighted = running
        begin = block_index * block_rows
        key_block = lax.dynamic_slice_in_dim(key_piece, begin, block_rows, 0).reshape(
            block_rows, HEADS, HEAD_DIM
        )
        value_block = lax.dynamic_slice_in_dim(value_piece, begin, block_rows, 0).reshape(
            block_rows, HEADS, HEAD_DIM
        )
        key_member = lax.dynamic_slice_in_dim(member, begin, block_rows, 0)
        key_usable = lax.dynamic_slice_in_dim(usable, begin, block_rows, 0)
        allowed = ((own_member[:, None] == key_member[None, :]) & key_usable[None, :])[None]
        scores = (
            jnp.einsum("qhd,khd->hqk", query_heads, key_block, preferred_element_type=jnp.float32)
            * factor_scale
        )
        scores = jnp.where(allowed, scores, NEG_FILL)
        new_max = jnp.maximum(running_max, jnp.max(scores, axis=2))
        expos = jnp.where(allowed, jnp.exp(scores - new_max[:, :, None]), 0.0)
        shrink_by = jnp.exp(running_max - new_max)
        new_total = running_total * shrink_by + jnp.sum(expos, axis=2)
        new_weighted = weighted * shrink_by[:, :, None] + jnp.einsum(
            "hqk,khd->hqd",
            expos.astype(jnp.bfloat16),
            value_block,
            preferred_element_type=jnp.float32,
        )
        return (new_max, new_total, new_weighted)

    running_max, running_total, weighted = lax.fori_loop(
        0, amount // block_rows, fold_advance, start_state
    )
    attended = jnp.transpose(weighted / running_total[:, :, None], (1, 0, 2)).reshape(
        local_rows, HEADS * HEAD_DIM
    )
    return (attended, running_max + jnp.log(running_total))


def attend_backward(
    queries, attended_grad, log_total, deltas, keys_all, values_all, own_member, member, usable
):
    local_rows = queries.shape[0]
    group_rows = keys_all.shape[0]
    model_width = HEADS * HEAD_DIM
    factor_scale = HEAD_DIM ** (-0.5)
    query_heads = queries.reshape(local_rows, HEADS, HEAD_DIM)
    grad_heads = attended_grad.reshape(local_rows, HEADS, HEAD_DIM)
    block_rows = min(512, group_rows)

    def attend_advance(query_sum, block_index):
        begin = block_index * block_rows
        key_block = lax.dynamic_slice_in_dim(keys_all, begin, block_rows, 0).reshape(
            block_rows, HEADS, HEAD_DIM
        )
        value_block = lax.dynamic_slice_in_dim(values_all, begin, block_rows, 0).reshape(
            block_rows, HEADS, HEAD_DIM
        )
        key_member = lax.dynamic_slice_in_dim(member, begin, block_rows, 0)
        key_usable = lax.dynamic_slice_in_dim(usable, begin, block_rows, 0)
        allowed = ((own_member[:, None] == key_member[None, :]) & key_usable[None, :])[None]
        scores = (
            jnp.einsum("qhd,khd->hqk", query_heads, key_block, preferred_element_type=jnp.float32)
            * factor_scale
        )
        probs = jnp.where(allowed, jnp.exp(scores - log_total[:, :, None]), 0.0)
        prob_grad = jnp.einsum(
            "qhd,khd->hqk", grad_heads, value_block, preferred_element_type=jnp.float32
        )
        score_grad = (probs * (prob_grad - deltas[:, :, None])).astype(jnp.bfloat16)
        query_sum = (
            query_sum
            + jnp.einsum("hqk,khd->qhd", score_grad, key_block, preferred_element_type=jnp.float32)
            * factor_scale
        )
        key_grad = (
            jnp.einsum("hqk,qhd->khd", score_grad, query_heads, preferred_element_type=jnp.float32)
            * factor_scale
        )
        value_grad = jnp.einsum(
            "hqk,qhd->khd",
            probs.astype(jnp.bfloat16),
            grad_heads,
            preferred_element_type=jnp.float32,
        )
        joined = jnp.concatenate(
            [
                key_grad.reshape(block_rows, model_width),
                value_grad.reshape(block_rows, model_width),
            ],
            axis=1,
        )
        return (query_sum, joined)

    query_sum, key_value = lax.scan(
        attend_advance,
        jnp.zeros((local_rows, HEADS, HEAD_DIM), jnp.float32),
        jnp.arange(group_rows // block_rows, dtype=jnp.int32),
    )
    key_value = key_value.reshape(group_rows, 2 * model_width)
    return (query_sum.reshape(local_rows, model_width), key_value)


def layer_forward(hidden, weights, own_member, member, usable):
    entry, leaving, expand, shrink, vector = weights
    model_width = leaving.shape[0]
    pieces = split_vector(vector.astype(jnp.float32), model_width)
    flat = hidden.astype(jnp.bfloat16)
    mixed = jnp.dot(flat, entry, preferred_element_type=jnp.float32)
    queries = (mixed[:, 0:model_width] + pieces[0]).astype(jnp.bfloat16)
    keys = mixed[:, model_width : 2 * model_width].astype(jnp.bfloat16)
    values = (mixed[:, 2 * model_width : 3 * model_width] + pieces[1]).astype(jnp.bfloat16)
    attended, log_total = attend_forward(queries, keys, values, own_member, member, usable)
    attended_low = attended.astype(jnp.bfloat16)
    branch = jnp.dot(attended_low, leaving, preferred_element_type=jnp.float32) + pieces[2]
    middle, normed_one, factor_one = norm_forward(hidden + branch, pieces[3], pieces[4])
    middle_low = middle.astype(jnp.bfloat16)
    inner = jnp.dot(middle_low, expand, preferred_element_type=jnp.float32) + pieces[8]
    active = gelu_exact(inner).astype(jnp.bfloat16)
    branch_two = jnp.dot(active, shrink, preferred_element_type=jnp.float32) + pieces[5]
    result, normed_two, factor_two = norm_forward(middle + branch_two, pieces[6], pieces[7])
    record = (
        flat,
        queries,
        keys,
        values,
        attended,
        log_total,
        attended_low,
        normed_one,
        factor_one,
        middle_low,
        inner,
        active,
        normed_two,
        factor_two,
    )
    return (result, record)


def layer_backward(upstream, weights, record, keys_all, values_all, own_member, member, usable):
    entry, leaving, expand, shrink, vector = weights
    model_width = leaving.shape[0]
    pieces = split_vector(vector.astype(jnp.float32), model_width)
    (
        flat,
        queries,
        keys,
        values,
        attended,
        log_total,
        attended_low,
        normed_one,
        factor_one,
        middle_low,
        inner,
        active,
        normed_two,
        factor_two,
    ) = record
    local_rows = queries.shape[0]
    resid_two, gain_two_grad, shift_two_grad = norm_backward(
        upstream, normed_two, factor_two, pieces[6]
    )
    branch_two_grad = resid_two.astype(jnp.bfloat16)
    bias_down_grad = jnp.sum(branch_two_grad.astype(jnp.float32), axis=0)
    shrink_grad = inner_rows(active, branch_two_grad)
    active_grad = times_trans(branch_two_grad, shrink)
    unused_value, gelu_pull = jax.vjp(gelu_exact, inner)
    inner_grad = gelu_pull(active_grad)[0].astype(jnp.bfloat16)
    bias_up_grad = jnp.sum(inner_grad.astype(jnp.float32), axis=0)
    expand_grad = inner_rows(middle_low, inner_grad)
    middle_grad = resid_two + times_trans(inner_grad, expand)
    resid_one, gain_one_grad, shift_one_grad = norm_backward(
        middle_grad, normed_one, factor_one, pieces[3]
    )
    branch_grad = resid_one.astype(jnp.bfloat16)
    bias_out_grad = jnp.sum(branch_grad.astype(jnp.float32), axis=0)
    exit_grad = inner_rows(attended_low, branch_grad)
    attended_grad = times_trans(branch_grad, leaving).astype(jnp.bfloat16)
    deltas = jnp.sum(
        (attended_grad.astype(jnp.float32) * attended).reshape(local_rows, HEADS, HEAD_DIM), axis=2
    ).T
    query_grad, key_value_grad = attend_backward(
        queries, attended_grad, log_total, deltas, keys_all, values_all, own_member, member, usable
    )
    own_key_value = lax.psum_scatter(
        key_value_grad.astype(jnp.bfloat16), "shard", scatter_dimension=0, tiled=True
    ).astype(jnp.float32)
    mixed_grad = jnp.concatenate([query_grad, own_key_value], axis=1).astype(jnp.bfloat16)
    bias_query_grad = jnp.sum(mixed_grad[:, 0:model_width].astype(jnp.float32), axis=0)
    bias_value_grad = jnp.sum(
        mixed_grad[:, 2 * model_width : 3 * model_width].astype(jnp.float32), axis=0
    )
    entry_grad = inner_rows(flat, mixed_grad)
    hidden_grad = resid_one + times_trans(mixed_grad, entry)
    vector_grad = jnp.concatenate(
        [
            bias_query_grad,
            bias_value_grad,
            bias_out_grad,
            gain_one_grad,
            shift_one_grad,
            bias_down_grad,
            gain_two_grad,
            shift_two_grad,
            bias_up_grad,
        ]
    )
    return (hidden_grad, (entry_grad, exit_grad, expand_grad, shrink_grad, vector_grad))


def body(
    inputs,
    cotangent,
    lengths,
    dealing,
    key_mask,
    entry_weight,
    exit_weight,
    expand_weight,
    shrink_weight,
    vectors,
):
    local_rows = inputs.shape[0]
    group_rows = local_rows * lax.axis_size("shard")
    position = lax.axis_index("shard") * local_rows
    dealt_all, mask_all = (
        lax.all_gather(dealing, "shard", axis=1, tiled=True),
        lax.all_gather(key_mask, "shard", axis=1, tiled=True),
    )
    member, leading = sequence_ids(lengths[0], group_rows)
    usable = (mask_all[0] == 1) | leading
    own_member = lax.dynamic_slice_in_dim(member, position, local_rows, 0)
    inverse = (
        jnp.zeros((group_rows,), jnp.int32)
        .at[dealt_all[0]]
        .set(jnp.arange(group_rows, dtype=jnp.int32))
    )
    own_inverse = lax.dynamic_slice_in_dim(inverse, position, local_rows, 0)
    inputs_all, cotangent_all = (
        lax.all_gather(inputs, "shard", axis=0, tiled=True),
        lax.all_gather(cotangent, "shard", axis=0, tiled=True),
    )
    hidden = jnp.take(inputs_all, dealing[0], axis=0).astype(jnp.float32)
    upstream = jnp.take(cotangent_all, dealing[0], axis=0).astype(jnp.float32)
    layers = entry_weight.shape[0]
    saved = []
    kept = []
    for layer_index in range(layers):
        weights = fetch_forward(
            entry_weight, exit_weight, expand_weight, shrink_weight, vectors, layer_index
        )
        kept.append(weights)
        hidden, record = layer_forward(hidden, weights, own_member, member, usable)
        saved.append(record)
    output_all = lax.all_gather(hidden.astype(jnp.bfloat16), "shard", axis=0, tiled=True)
    output = jnp.take(output_all, own_inverse, axis=0)
    hidden_grad = upstream
    layer_grads = [None] * layers
    for layer_index in reversed(range(layers)):
        weights = fetch_backward(
            entry_weight, exit_weight, expand_weight, shrink_weight, vectors, layer_index
        )
        record = saved[layer_index]
        keys_all, values_all = (
            lax.all_gather(record[2], "shard", axis=0, tiled=True),
            lax.all_gather(record[3], "shard", axis=0, tiled=True),
        )
        hidden_grad, local_grads = layer_backward(
            hidden_grad, weights, record, keys_all, values_all, own_member, member, usable
        )
        entry_local, exit_local, expand_local, shrink_local, vector_local = local_grads
        entry_part, exit_part, expand_part, shrink_part, vector_part = (
            lax.psum_scatter(
                entry_local.astype(jnp.bfloat16), "shard", scatter_dimension=0, tiled=True
            ).astype(jnp.float32),
            lax.psum_scatter(
                exit_local.astype(jnp.bfloat16), "shard", scatter_dimension=0, tiled=True
            ).astype(jnp.float32),
            lax.psum_scatter(
                expand_local.astype(jnp.bfloat16), "shard", scatter_dimension=0, tiled=True
            ).astype(jnp.float32),
            lax.psum_scatter(
                shrink_local.astype(jnp.bfloat16), "shard", scatter_dimension=0, tiled=True
            ).astype(jnp.float32),
            lax.psum_scatter(
                vector_local.astype(jnp.bfloat16), "shard", scatter_dimension=0, tiled=True
            ).astype(jnp.float32),
        )
        entry_part, exit_part, expand_part, shrink_part, vector_part = (
            lax.psum(entry_part.astype(jnp.bfloat16), "rep").astype(jnp.float32),
            lax.psum(exit_part.astype(jnp.bfloat16), "rep").astype(jnp.float32),
            lax.psum(expand_part.astype(jnp.bfloat16), "rep").astype(jnp.float32),
            lax.psum(shrink_part.astype(jnp.bfloat16), "rep").astype(jnp.float32),
            lax.psum(vector_part.astype(jnp.bfloat16), "rep").astype(jnp.float32),
        )
        layer_grads[layer_index] = (entry_part, exit_part, expand_part, shrink_part, vector_part)
    entry_grad = jnp.stack([item[0] for item in layer_grads])
    exit_grad = jnp.stack([item[1] for item in layer_grads])
    expand_grad = jnp.stack([item[2] for item in layer_grads])
    shrink_grad = jnp.stack([item[3] for item in layer_grads])
    vector_grad = jnp.stack([item[4] for item in layer_grads])
    grads_all = lax.all_gather(
        hidden_grad.astype(jnp.bfloat16), "shard", axis=0, tiled=True
    ).astype(hidden_grad.dtype)
    input_grad = jnp.take(grads_all, own_inverse, axis=0)
    return (output, input_grad, entry_grad, exit_grad, expand_grad, shrink_grad, vector_grad)


EDGE = (0, 1, 6, 7)
CORE = (2, 3, 4, 5)
ALL = tuple(range(8))
BOTH = ("rep", "shard")


def routes(rep_flip, shard_flip, shards):
    return [
        (rep * 8 + shard, (rep ^ rep_flip) * 8 + (shard ^ shard_flip))
        for rep in range(4)
        for shard in shards
    ]


TO_X = routes(1, 0, CORE)
TO_Y = routes(2, 0, CORE)
TO_TWIN = routes(0, 1, CORE)
TO_MID = routes(0, 6, CORE)
INWARD = routes(0, 2, EDGE)
OUTWARD = routes(0, 2, CORE)
ALL_X = routes(1, 0, ALL)
ALL_Y = routes(2, 0, ALL)


def send(value, route):
    return lax.ppermute(value, BOTH, route)


def vmem(count):
    return [pl.BlockSpec(memory_space=pltpu.VMEM)] * count


LIMIT = pltpu.CompilerParams(vmem_limit_bytes=60 * 1024 * 1024)


def nt(left, right):
    return lax.dot_general(left, right, (((1,), (1,)), ((), ())), preferred_element_type=jnp.float32)


def nn(left, right):
    return lax.dot_general(left, right, (((1,), (0,)), ((), ())), preferred_element_type=jnp.float32)


def gather_kernel(count, ids_ref, want_ref, *refs):
    out_ref = refs[count]
    want = want_ref[...]
    total = None
    for index in range(count):
        ids = ids_ref[index]
        hit = (want == ids).astype(jnp.float32).astype(jnp.bfloat16)
        part = nn(hit, refs[index][0 : ids.shape[1], :])
        total = part if total is None else total + part
    out_ref[...] = total.astype(jnp.bfloat16)


def gather_rows(pieces, ids, want):
    count = len(pieces)
    return pl.pallas_call(
        functools.partial(gather_kernel, count),
        out_shape=jax.ShapeDtypeStruct((want.shape[0], pieces[0].shape[1]), jnp.bfloat16),
        in_specs=vmem(2 + count),
        out_specs=pl.BlockSpec(memory_space=pltpu.VMEM),
        compiler_params=LIMIT,
        name="gather_rows",
    )(ids, want, *pieces)


def assemble_kernel(where_ref, *refs):
    parts, out_ref, sems = refs[:10], refs[10], refs[11]
    depth, rep, twin = where_ref[0], where_ref[1], where_ref[2]
    copies = []

    def move(src, dst):
        copies.append(pltpu.make_async_copy(src, dst, sems.at[len(copies)]))

    for side in range(2):
        own, first, over_x, over_y, over_d = parts[side * 5 : side * 5 + 5]
        core = twin ^ side
        move(own, out_ref.at[depth, core])
        for slot, flip in enumerate((1, 3, 2)):
            level = depth ^ flip
            for piece, bits in ((first, 0), (over_x, 1), (over_y, 2), (over_d, 3)):
                move(piece.at[slot], out_ref.at[level, core, rep ^ bits])
    for item in copies:
        item.start()
    for item in copies:
        item.wait()


def assemble(where, parts):
    quarter = parts[0].shape
    result = pl.pallas_call(
        assemble_kernel,
        out_shape=jax.ShapeDtypeStruct((4, 2) + quarter, jnp.bfloat16),
        in_specs=[pl.BlockSpec(memory_space=pltpu.SMEM)] + [pl.BlockSpec(memory_space=pl.ANY)] * 10,
        out_specs=pl.BlockSpec(memory_space=pl.ANY),
        scratch_shapes=[pltpu.SemaphoreType.DMA((26,))],
        name="assemble",
    )(where, *parts)
    return result.reshape(8 * quarter[0] * quarter[1], quarter[2])


def spread(own, rep, x_first):
    rows, width = own.shape
    quarter = own.reshape(4, rows // 4, width)
    piece = lax.dynamic_index_in_dim(quarter, rep, 0, keepdims=False)
    near = send(piece, INWARD)
    middle = send(piece, TO_MID)
    far = send(near, TO_MID)
    first = jnp.stack([near, middle, far])
    over_x = send(first, TO_X)
    over_y = send(first, TO_Y)
    over_d = send(over_x, TO_Y) if x_first else send(over_y, TO_X)
    mine = (quarter, first, over_x, over_y, over_d)
    return mine + tuple(send(item, TO_TWIN) for item in mine)


def reduce_grad(chip_sum, rep, is_low, is_core, x_first):
    piece, width = chip_sum.shape[2:]
    axis = 2 if x_first else 1
    bit = (rep & 1) if x_first else (rep >> 1)

    def low(value):
        return value.astype(jnp.bfloat16)

    def wide(value):
        return value.astype(jnp.float32)

    view = chip_sum.reshape(4, 2, 2, piece, width)
    keep = lax.dynamic_index_in_dim(view, bit, axis, keepdims=False)
    give = lax.dynamic_index_in_dim(view, 1 - bit, axis, keepdims=False)
    got = send(give, TO_X if x_first else TO_Y)
    stage = low(wide(keep) + wide(got))
    give = jnp.where(is_low, stage[2:4], stage[0:2])
    keep = jnp.where(is_low, stage[0:2], stage[2:4])
    got = send(give, TO_MID)
    stage = low(wide(keep) + wide(got))
    outer = jnp.where(is_low, stage[0], stage[1])
    inner = jnp.where(is_low, stage[1], stage[0])
    got = send(outer, OUTWARD)
    stage = jnp.where(is_core, inner, got)
    got = send(stage, ALL_Y if x_first else ALL_X)
    stage = low(wide(stage) + wide(got))
    got = send(stage, ALL_X if x_first else ALL_Y)
    joined = jnp.where(
        bit == 0, jnp.stack([stage, got], axis - 1), jnp.stack([got, stage], axis - 1)
    )
    return joined.astype(jnp.float32).reshape(4 * piece, width)


def attend_kernel(q_ref, ka_ref, kb_ref, va_ref, vb_ref, code_ref, member_ref, o_ref, ot_ref, lse_ref, bias_ref):
    half = q_ref.shape[0]

    @pl.when(pl.program_id(0) == 0)
    def _():
        bias_ref[...] = jnp.where(code_ref[...] == member_ref[...], 0.0, NEG_FILL)

    q = q_ref[...] * jnp.bfloat16(HEAD_DIM ** (-0.5))
    lane = lax.broadcasted_iota(jnp.int32, q.shape, 1)
    keys = (ka_ref[...], kb_ref[...])
    values = (va_ref[...].T, vb_ref[...].T)
    outs = []
    for head in range(2):
        q_head = jnp.where((lane >= HEAD_DIM) == (head == 1), q, jnp.bfloat16(0))
        scores = [
            nt(keys[side], q_head) + bias_ref[side * half : (side + 1) * half, :]
            for side in range(2)
        ]
        top = jnp.maximum(
            jnp.max(scores[0], axis=0, keepdims=True), jnp.max(scores[1], axis=0, keepdims=True)
        )
        total = None
        mixed = None
        for side in range(2):
            expo = jnp.exp(scores[side] - top)
            part = jnp.sum(expo, axis=0, keepdims=True)
            value = values[side][head * HEAD_DIM : (head + 1) * HEAD_DIM, :]
            product = nn(value, expo.astype(jnp.bfloat16))
            total = part if total is None else total + part
            mixed = product if mixed is None else mixed + product
        outs.append(mixed / total)
        lse_ref[0, head : head + 1, :] = top + jnp.log(total)
    joined = jnp.concatenate(outs, axis=0)
    ot_ref[...] = joined
    o_ref[...] = joined.T.astype(jnp.bfloat16)


def attend_fast(queries, keys, values, code, member):
    half, width = queries.shape
    column = pl.BlockSpec((half, 128), lambda pair: (0, pair))
    whole = [
        pl.BlockSpec((2 * half, 1), lambda pair: (0, 0)),
        pl.BlockSpec((1, half), lambda pair: (0, 0)),
    ]
    return pl.pallas_call(
        attend_kernel,
        grid=(width // 128,),
        in_specs=[column] * 5 + whole,
        out_specs=[
            column,
            pl.BlockSpec((128, half), lambda pair: (pair, 0)),
            pl.BlockSpec((1, 2, half), lambda pair: (pair, 0, 0)),
        ],
        out_shape=[
            jax.ShapeDtypeStruct((half, width), jnp.bfloat16),
            jax.ShapeDtypeStruct((width, half), jnp.float32),
            jax.ShapeDtypeStruct((width // 128, 2, half), jnp.float32),
        ],
        scratch_shapes=[pltpu.VMEM((2 * half, half), jnp.float32)],
        compiler_params=LIMIT,
        name="attend_forward",
    )(queries, keys[0], keys[1], values[0], values[1], code, member)


def attend_back_kernel(
    q_ref, g_ref, ka_ref, kb_ref, va_ref, vb_ref, ot_ref, lse_ref, code_ref, member_ref,
    dq_ref, dka_ref, dkb_ref, dva_ref, dvb_ref, bias_ref,
):
    half = q_ref.shape[0]

    @pl.when(pl.program_id(0) == 0)
    def _():
        bias_ref[...] = jnp.where(code_ref[...] == member_ref[...], 0.0, NEG_FILL)

    scale = HEAD_DIM ** (-0.5)
    q = q_ref[...] * jnp.bfloat16(scale)
    grad = g_ref[...]
    lane = lax.broadcasted_iota(jnp.int32, q.shape, 1)
    keys = (ka_ref[...], kb_ref[...])
    turned = (ka_ref[...].T, kb_ref[...].T)
    values = (va_ref[...], vb_ref[...])
    product = ot_ref[...] * grad.astype(jnp.float32).T
    key_sums = [None, None]
    value_sums = [None, None]
    query_parts = []
    for head in range(2):
        rows = slice(head * HEAD_DIM, (head + 1) * HEAD_DIM)
        chosen = (lane >= HEAD_DIM) == (head == 1)
        q_head = jnp.where(chosen, q, jnp.bfloat16(0))
        g_head = jnp.where(chosen, grad, jnp.bfloat16(0))
        delta = jnp.sum(product[rows, :], axis=0, keepdims=True)
        level = lse_ref[0, head : head + 1, :]
        query_sum = None
        for side in range(2):
            scores = nt(keys[side], q_head) + bias_ref[side * half : (side + 1) * half, :]
            prob = jnp.exp(scores - level)
            slope = nt(values[side], g_head)
            steep = (prob * (slope - delta)).astype(jnp.bfloat16)
            value_part = nn(prob.astype(jnp.bfloat16), g_head)
            key_part = nn(steep, q_head)
            query_part = nn(turned[side][rows, :], steep)
            value_sums[side] = value_part if head == 0 else value_sums[side] + value_part
            key_sums[side] = key_part if head == 0 else key_sums[side] + key_part
            query_sum = query_part if side == 0 else query_sum + query_part
        query_parts.append(query_sum * scale)
    dq_ref[...] = jnp.concatenate(query_parts, axis=0).T.astype(jnp.bfloat16)
    dka_ref[...] = key_sums[0]
    dkb_ref[...] = key_sums[1].astype(jnp.bfloat16)
    dva_ref[...] = value_sums[0]
    dvb_ref[...] = value_sums[1].astype(jnp.bfloat16)


def attend_back_fast(queries, grad, keys, values, turned, level, code, member):
    half, width = queries.shape
    column = pl.BlockSpec((half, 128), lambda pair: (0, pair))
    wide = jax.ShapeDtypeStruct((half, width), jnp.float32)
    thin = jax.ShapeDtypeStruct((half, width), jnp.bfloat16)
    return pl.pallas_call(
        attend_back_kernel,
        grid=(width // 128,),
        in_specs=[column] * 6
        + [
            pl.BlockSpec((128, half), lambda pair: (pair, 0)),
            pl.BlockSpec((1, 2, half), lambda pair: (pair, 0, 0)),
            pl.BlockSpec((2 * half, 1), lambda pair: (0, 0)),
            pl.BlockSpec((1, half), lambda pair: (0, 0)),
        ],
        out_specs=[column] * 5,
        out_shape=[thin, wide, thin, wide, thin],
        scratch_shapes=[pltpu.VMEM((2 * half, half), jnp.float32)],
        compiler_params=LIMIT,
        name="attend_backward",
    )(queries, grad, keys[0], keys[1], values[0], values[1], turned, level, code, member)


def forward_fast(hidden, weights, pieces, code, member):
    entry, leaving, expand, shrink = weights
    width = leaving.shape[0]
    flat = hidden.astype(jnp.bfloat16)
    mixed = jnp.dot(flat, entry, preferred_element_type=jnp.float32)
    queries = (mixed[:, 0:width] + pieces[0]).astype(jnp.bfloat16)
    keys = mixed[:, width : 2 * width].astype(jnp.bfloat16)
    values = (mixed[:, 2 * width : 3 * width] + pieces[1]).astype(jnp.bfloat16)
    keys = (keys, send(keys, TO_TWIN))
    values = (values, send(values, TO_TWIN))
    attended, turned, level = attend_fast(queries, keys, values, code, member)
    branch = jnp.dot(attended, leaving, preferred_element_type=jnp.float32) + pieces[2]
    middle, normed_one, factor_one = norm_forward(hidden + branch, pieces[3], pieces[4])
    middle_low = middle.astype(jnp.bfloat16)
    inner = jnp.dot(middle_low, expand, preferred_element_type=jnp.float32) + pieces[8]
    active = gelu_exact(inner).astype(jnp.bfloat16)
    branch_two = jnp.dot(active, shrink, preferred_element_type=jnp.float32) + pieces[5]
    result, normed_two, factor_two = norm_forward(middle + branch_two, pieces[6], pieces[7])
    record = (
        flat, queries, keys, values, attended, turned, level,
        normed_one, factor_one, middle_low, inner, active, normed_two, factor_two,
    )
    return (result, record)


def backward_fast(upstream, weights, pieces, record, code, member, twin, finish):
    entry, leaving, expand, shrink = weights
    width = leaving.shape[0]
    (
        flat, queries, keys, values, attended, turned, level,
        normed_one, factor_one, middle_low, inner, active, normed_two, factor_two,
    ) = record
    rows = queries.shape[0]
    block = jnp.arange(width, dtype=jnp.int32)
    place = jnp.arange(width // 2, dtype=jnp.int32)
    unit = width // 8

    def halves(left):
        if left.shape[1] == width:
            source = (place // unit) * (2 * unit) + place % unit

            def pick(core):
                chosen = (block[:, None] == (source + core * unit)[None, :]).astype(jnp.bfloat16)
                return jnp.dot(left, chosen, preferred_element_type=jnp.float32).astype(jnp.bfloat16)
        else:
            view = left.reshape(rows, 4, 2, left.shape[1] // 8)

            def pick(core):
                taken = lax.dynamic_index_in_dim(view, core, 2, keepdims=False)
                return taken.reshape(rows, left.shape[1] // 2)

        return pick(twin), pick(1 - twin)

    def weight_grad(left, right):
        mine, theirs = halves(left)
        left_all = jnp.concatenate([mine, send(theirs, TO_TWIN)], axis=0)
        right_all = jnp.concatenate([right, send(right, TO_TWIN)], axis=0)
        product = inner_rows(left_all, right_all).astype(jnp.bfloat16)
        return finish(product)

    resid_two, gain_two_grad, shift_two_grad = norm_backward(
        upstream, normed_two, factor_two, pieces[6]
    )
    branch_two_grad = resid_two.astype(jnp.bfloat16)
    bias_down_grad = jnp.sum(branch_two_grad.astype(jnp.float32), axis=0)
    shrink_grad = weight_grad(active, branch_two_grad)
    active_grad = times_trans(branch_two_grad, shrink)
    unused_value, gelu_pull = jax.vjp(gelu_exact, inner)
    inner_grad = gelu_pull(active_grad)[0].astype(jnp.bfloat16)
    bias_up_grad = jnp.sum(inner_grad.astype(jnp.float32), axis=0)
    expand_grad = weight_grad(middle_low, inner_grad)
    middle_grad = resid_two + times_trans(inner_grad, expand)
    resid_one, gain_one_grad, shift_one_grad = norm_backward(
        middle_grad, normed_one, factor_one, pieces[3]
    )
    branch_grad = resid_one.astype(jnp.bfloat16)
    bias_out_grad = jnp.sum(branch_grad.astype(jnp.float32), axis=0)
    exit_grad = weight_grad(attended, branch_grad)
    attended_grad = times_trans(branch_grad, leaving).astype(jnp.bfloat16)
    query_grad, key_own, key_twin, value_own, value_twin = attend_back_fast(
        queries, attended_grad, keys, values, turned, level, code, member
    )
    key_grad = (key_own + send(key_twin, TO_TWIN).astype(jnp.float32)).astype(jnp.bfloat16)
    value_grad = (value_own + send(value_twin, TO_TWIN).astype(jnp.float32)).astype(jnp.bfloat16)
    mixed_grad = jnp.concatenate([query_grad, key_grad, value_grad], axis=1)
    bias_query_grad = jnp.sum(query_grad.astype(jnp.float32), axis=0)
    bias_value_grad = jnp.sum(value_grad.astype(jnp.float32), axis=0)
    entry_grad = weight_grad(flat, mixed_grad)
    hidden_grad = resid_one + times_trans(mixed_grad, entry)
    vector_grad = jnp.concatenate(
        [
            bias_query_grad, bias_value_grad, bias_out_grad, gain_one_grad, shift_one_grad,
            bias_down_grad, gain_two_grad, shift_two_grad, bias_up_grad,
        ]
    )
    return (hidden_grad, (entry_grad, exit_grad, expand_grad, shrink_grad, vector_grad))


def body_fast(
    inputs, cotangent, lengths, dealing, key_mask,
    entry_weight, exit_weight, expand_weight, shrink_weight, vectors,
):
    rows, width = inputs.shape
    layers = entry_weight.shape[0]
    group_rows = 8 * rows
    half_rows = group_rows // 2
    core_rows = half_rows // 2
    rep = lax.axis_index("rep")
    shard = lax.axis_index("shard")
    depth, twin = shard // 2, shard % 2
    is_low = depth <= 1
    is_core = (depth == 1) | (depth == 2)
    where = jnp.stack([depth, rep, twin]).astype(jnp.int32)

    def relay(value):
        near = send(value, INWARD)
        mine = (value, near, send(value, TO_MID), send(near, TO_MID))
        return mine, tuple(send(item, TO_TWIN) for item in mine)

    def absolute(mine, theirs):
        def order(four):
            own, near, middle, far = four
            return jnp.where(
                is_low, jnp.stack([near, own, middle, far]), jnp.stack([far, middle, own, near])
            )

        one, two = order(mine), order(theirs)
        return jnp.where(twin == 0, jnp.stack([one, two], 1), jnp.stack([two, one], 1))

    flips = (0, 1, 3, 2)
    table = absolute(*relay(jnp.concatenate([dealing, key_mask], axis=0)))
    dealt_all = table[:, :, 0, :].reshape(group_rows)
    mask_all = table[:, :, 1, :].reshape(group_rows)

    extra = layers * vectors.shape[1] // width
    tail = vectors.astype(jnp.bfloat16).reshape(extra, width)
    packed = jnp.concatenate([inputs, tail, jnp.zeros((8 - extra % 8, width), jnp.bfloat16)], axis=0)
    mine, theirs = relay(packed)
    input_pieces = mine + theirs
    vector_all = absolute(
        tuple(item[rows : rows + extra] for item in mine),
        tuple(item[rows : rows + extra] for item in theirs),
    )
    vector_all = jnp.transpose(
        vector_all.reshape(8, layers, vectors.shape[1]), (1, 0, 2)
    ).reshape(layers, 8 * vectors.shape[1]).astype(jnp.float32)

    weights = []
    for layer in range(layers):
        made = []
        for index, weight in enumerate((entry_weight, exit_weight, expand_weight, shrink_weight)):
            x_first = (index != 2) == (layer == 0)
            made.append(assemble(where, spread(weight[layer].astype(jnp.bfloat16), rep, x_first)))
        weights.append(made)
    pieces = [split_vector(vector_all[layer], width) for layer in range(layers)]

    mine, theirs = relay(cotangent)
    cotangent_pieces = mine + theirs

    member, leading = sequence_ids(lengths[0], group_rows)
    usable = (mask_all == 1) | leading
    code = jnp.where(usable, member, -1)
    longest = jnp.argmax(lengths[0])
    begin = jnp.cumsum(lengths[0])[longest] - lengths[0][longest]
    spot = jnp.arange(half_rows, dtype=jnp.int32)

    def halve(values, low_side):
        inside = lax.dynamic_slice_in_dim(values, begin, half_rows, 0)
        outside = jnp.where(spot < begin, values[:half_rows], values[half_rows:])
        return jnp.where(low_side, inside, outside)

    def cores(values):
        own = lax.dynamic_slice_in_dim(values, twin * core_rows, core_rows, 0)
        other = lax.dynamic_slice_in_dim(values, (1 - twin) * core_rows, core_rows, 0)
        return own, other

    code_half = jnp.concatenate(cores(halve(code, is_low))).reshape(half_rows, 1)
    member_own = cores(halve(member, is_low))[0].reshape(1, core_rows)
    dealt_near = cores(halve(dealt_all, is_low))
    dealt_far = cores(halve(dealt_all, ~is_low))

    local = jnp.arange(rows, dtype=jnp.int32)
    bases = jnp.stack(
        [(depth ^ flip) * (2 * rows) + (twin ^ side) * rows for side in range(2) for flip in flips]
    ).astype(jnp.int32)
    source_ids = (bases[:, None] + local[None, :]).reshape(8, 1, rows)
    want_in = dealt_near[0].reshape(core_rows, 1)
    hidden = gather_rows(input_pieces, source_ids, want_in).astype(jnp.float32)
    upstream = gather_rows(cotangent_pieces, source_ids, want_in).astype(jnp.float32)

    result_ids = jnp.stack([dealt_near[0], dealt_far[0], dealt_near[1], dealt_far[1]]).reshape(
        4, 1, core_rows
    )
    want_out = jnp.concatenate([source_ids[0, 0], source_ids[1, 0]]).reshape(2 * rows, 1)

    def restore(value):
        middle = send(value, TO_MID)
        found = gather_rows(
            (value, middle, send(value, TO_TWIN), send(middle, TO_TWIN)), result_ids, want_out
        )
        outer = send(found[rows:], OUTWARD)
        return jnp.where(is_core, found[:rows], outer)

    saved = []
    for layer in range(layers):
        hidden, record = forward_fast(hidden, weights[layer], pieces[layer], code_half, member_own)
        saved.append(record)
    output = restore(hidden.astype(jnp.bfloat16))

    grad = upstream
    layer_grads = [None] * layers
    for layer in reversed(range(layers)):
        order = iter((0, 1, 1, 0) if layer == 0 else (1, 0, 0, 1))

        def finish(product):
            x_first = next(order) == 0
            return reduce_grad(
                product.reshape(4, 4, product.shape[0] // 16, product.shape[1]),
                rep, is_low, is_core, x_first,
            )

        grad, layer_grads[layer] = backward_fast(
            grad, weights[layer], pieces[layer], saved[layer], code_half, member_own, twin, finish
        )
    input_grad = restore(grad.astype(jnp.bfloat16)).astype(jnp.float32)

    joined = jnp.stack([item[4] for item in layer_grads])
    joined = jnp.transpose(joined.reshape(layers, 4, 2, vectors.shape[1]), (1, 2, 0, 3))
    keep = lax.dynamic_index_in_dim(joined, twin, 1, keepdims=False)
    give = lax.dynamic_index_in_dim(joined, 1 - twin, 1, keepdims=False)
    stage = keep + send(give, TO_TWIN)
    stage = stage + send(stage, TO_X)
    stage = stage + send(stage, TO_Y)
    give = jnp.where(is_low, stage[2:4], stage[0:2])
    keep = jnp.where(is_low, stage[0:2], stage[2:4])
    stage = keep + send(give, TO_MID)
    outer = jnp.where(is_low, stage[0], stage[1])
    inner = jnp.where(is_low, stage[1], stage[0])
    vector_grad = jnp.where(is_core, inner, send(outer, OUTWARD))
    return (
        output,
        input_grad,
        jnp.stack([item[0] for item in layer_grads]),
        jnp.stack([item[1] for item in layer_grads]),
        jnp.stack([item[2] for item in layer_grads]),
        jnp.stack([item[3] for item in layer_grads]),
        vector_grad,
    )


def solution(mesh):
    placed = (
        P(("rep", "shard"), None),
        P(("rep", "shard"), None),
        P("rep", None),
        P("rep", "shard"),
        P("rep", "shard"),
        P(None, "shard", None),
        P(None, "shard", None),
        P(None, "shard", None),
        P(None, "shard", None),
        P(None, "shard"),
    )
    small = dict(mesh.shape) == {"rep": 4, "shard": 8}
    return jax.shard_map(
        body_fast if small else body,
        mesh=mesh,
        in_specs=placed,
        out_specs=(
            P(("rep", "shard"), None),
            P(("rep", "shard"), None),
            P(None, "shard", None),
            P(None, "shard", None),
            P(None, "shard", None),
            P(None, "shard", None),
            P(None, "shard"),
        ),
        check_vma=False,
    )
```

```python
import functools

import jax
import jax.numpy as jnp
from jax import lax
from jax.experimental import pallas as pl
from jax.experimental.pallas import tpu as pltpu
from jax.sharding import PartitionSpec as P

HEADS = 12
HEAD_DIM = 64


NEG_FILL = -1e30


def norm_forward(resid, gain, shift):
    center = jnp.mean(resid, axis=-1, keepdims=True)
    offsets = resid - center
    spread = jnp.mean(offsets * offsets, axis=-1, keepdims=True)
    factor = lax.rsqrt(spread + 1e-05)
    normed = offsets * factor
    return (normed * gain + shift, normed, factor)


def norm_backward(incoming, normed, factor, gain):
    scaled = incoming * gain
    resid_grad = factor * (
        scaled
        - jnp.mean(scaled, axis=-1, keepdims=True)
        - normed * jnp.mean(scaled * normed, axis=-1, keepdims=True)
    )
    return (resid_grad, jnp.sum(incoming * normed, axis=0), jnp.sum(incoming, axis=0))


def inner_rows(left, right):
    return lax.dot_general(
        left, right, (((0,), (0,)), ((), ())), preferred_element_type=jnp.float32
    )


def times_trans(left, right):
    return lax.dot_general(
        left, right, (((1,), (1,)), ((), ())), preferred_element_type=jnp.float32
    )


def gelu_exact(value):
    return jax.nn.gelu(value, approximate=False)


def sequence_ids(lengths, group_rows):
    ending = jnp.cumsum(lengths)
    opening = ending - lengths
    places = jnp.arange(group_rows, dtype=jnp.int32)
    member = jnp.sum((places[:, None] >= ending[None, :]).astype(jnp.int32), axis=1)
    leading = jnp.any(places[:, None] == opening[None, :], axis=1)
    return (member, leading)


def split_vector(vector, model_width):
    pieces = [vector[index * model_width : (index + 1) * model_width] for index in range(8)]
    pieces.append(vector[8 * model_width :])
    return pieces


def fetch_forward(entry_weight, exit_weight, expand_weight, shrink_weight, vectors, layer_index):
    return (
        lax.all_gather(entry_weight[layer_index].astype(jnp.bfloat16), "shard", axis=0, tiled=True),
        lax.all_gather(exit_weight[layer_index].astype(jnp.bfloat16), "shard", axis=0, tiled=True),
        lax.all_gather(
            expand_weight[layer_index].astype(jnp.bfloat16), "shard", axis=0, tiled=True
        ),
        lax.all_gather(
            shrink_weight[layer_index].astype(jnp.bfloat16), "shard", axis=0, tiled=True
        ),
        lax.all_gather(vectors[layer_index].astype(jnp.bfloat16), "shard", axis=0, tiled=True),
    )


def fetch_backward(entry_weight, exit_weight, expand_weight, shrink_weight, vectors, layer_index):
    return (
        lax.all_gather(entry_weight[layer_index].astype(jnp.bfloat16), "shard", axis=0, tiled=True),
        lax.all_gather(exit_weight[layer_index].astype(jnp.bfloat16), "shard", axis=0, tiled=True),
        lax.all_gather(
            expand_weight[layer_index].astype(jnp.bfloat16), "shard", axis=0, tiled=True
        ),
        lax.all_gather(
            shrink_weight[layer_index].astype(jnp.bfloat16), "shard", axis=0, tiled=True
        ),
        lax.all_gather(vectors[layer_index].astype(jnp.bfloat16), "shard", axis=0, tiled=True),
    )


def attend_forward(queries, keys, values, own_member, member, usable):
    local_rows = queries.shape[0]
    query_heads = queries.reshape(local_rows, HEADS, HEAD_DIM)
    factor_scale = HEAD_DIM ** (-0.5)
    start_state = (
        jnp.full((HEADS, local_rows), NEG_FILL, jnp.float32),
        jnp.zeros((HEADS, local_rows), jnp.float32),
        jnp.zeros((HEADS, local_rows, HEAD_DIM), jnp.float32),
    )
    key_piece = lax.all_gather(keys, "shard", axis=0, tiled=True)
    value_piece = lax.all_gather(values, "shard", axis=0, tiled=True)
    amount = key_piece.shape[0]
    block_rows = local_rows * max(1, 512 // local_rows)

    def fold_advance(block_index, running):
        running_max, running_total, weighted = running
        begin = block_index * block_rows
        key_block = lax.dynamic_slice_in_dim(key_piece, begin, block_rows, 0).reshape(
            block_rows, HEADS, HEAD_DIM
        )
        value_block = lax.dynamic_slice_in_dim(value_piece, begin, block_rows, 0).reshape(
            block_rows, HEADS, HEAD_DIM
        )
        key_member = lax.dynamic_slice_in_dim(member, begin, block_rows, 0)
        key_usable = lax.dynamic_slice_in_dim(usable, begin, block_rows, 0)
        allowed = ((own_member[:, None] == key_member[None, :]) & key_usable[None, :])[None]
        scores = (
            jnp.einsum("qhd,khd->hqk", query_heads, key_block, preferred_element_type=jnp.float32)
            * factor_scale
        )
        scores = jnp.where(allowed, scores, NEG_FILL)
        new_max = jnp.maximum(running_max, jnp.max(scores, axis=2))
        expos = jnp.where(allowed, jnp.exp(scores - new_max[:, :, None]), 0.0)
        shrink_by = jnp.exp(running_max - new_max)
        new_total = running_total * shrink_by + jnp.sum(expos, axis=2)
        new_weighted = weighted * shrink_by[:, :, None] + jnp.einsum(
            "hqk,khd->hqd",
            expos.astype(jnp.bfloat16),
            value_block,
            preferred_element_type=jnp.float32,
        )
        return (new_max, new_total, new_weighted)

    running_max, running_total, weighted = lax.fori_loop(
        0, amount // block_rows, fold_advance, start_state
    )
    attended = jnp.transpose(weighted / running_total[:, :, None], (1, 0, 2)).reshape(
        local_rows, HEADS * HEAD_DIM
    )
    return (attended, running_max + jnp.log(running_total))


def attend_backward(
    queries, attended_grad, log_total, deltas, keys_all, values_all, own_member, member, usable
):
    local_rows = queries.shape[0]
    group_rows = keys_all.shape[0]
    model_width = HEADS * HEAD_DIM
    factor_scale = HEAD_DIM ** (-0.5)
    query_heads = queries.reshape(local_rows, HEADS, HEAD_DIM)
    grad_heads = attended_grad.reshape(local_rows, HEADS, HEAD_DIM)
    block_rows = min(512, group_rows)

    def attend_advance(query_sum, block_index):
        begin = block_index * block_rows
        key_block = lax.dynamic_slice_in_dim(keys_all, begin, block_rows, 0).reshape(
            block_rows, HEADS, HEAD_DIM
        )
        value_block = lax.dynamic_slice_in_dim(values_all, begin, block_rows, 0).reshape(
            block_rows, HEADS, HEAD_DIM
        )
        key_member = lax.dynamic_slice_in_dim(member, begin, block_rows, 0)
        key_usable = lax.dynamic_slice_in_dim(usable, begin, block_rows, 0)
        allowed = ((own_member[:, None] == key_member[None, :]) & key_usable[None, :])[None]
        scores = (
            jnp.einsum("qhd,khd->hqk", query_heads, key_block, preferred_element_type=jnp.float32)
            * factor_scale
        )
        probs = jnp.where(allowed, jnp.exp(scores - log_total[:, :, None]), 0.0)
        prob_grad = jnp.einsum(
            "qhd,khd->hqk", grad_heads, value_block, preferred_element_type=jnp.float32
        )
        score_grad = (probs * (prob_grad - deltas[:, :, None])).astype(jnp.bfloat16)
        query_sum = (
            query_sum
            + jnp.einsum("hqk,khd->qhd", score_grad, key_block, preferred_element_type=jnp.float32)
            * factor_scale
        )
        key_grad = (
            jnp.einsum("hqk,qhd->khd", score_grad, query_heads, preferred_element_type=jnp.float32)
            * factor_scale
        )
        value_grad = jnp.einsum(
            "hqk,qhd->khd",
            probs.astype(jnp.bfloat16),
            grad_heads,
            preferred_element_type=jnp.float32,
        )
        joined = jnp.concatenate(
            [
                key_grad.reshape(block_rows, model_width),
                value_grad.reshape(block_rows, model_width),
            ],
            axis=1,
        )
        return (query_sum, joined)

    query_sum, key_value = lax.scan(
        attend_advance,
        jnp.zeros((local_rows, HEADS, HEAD_DIM), jnp.float32),
        jnp.arange(group_rows // block_rows, dtype=jnp.int32),
    )
    key_value = key_value.reshape(group_rows, 2 * model_width)
    return (query_sum.reshape(local_rows, model_width), key_value)


def layer_forward(hidden, weights, own_member, member, usable):
    entry, leaving, expand, shrink, vector = weights
    model_width = leaving.shape[0]
    pieces = split_vector(vector.astype(jnp.float32), model_width)
    flat = hidden.astype(jnp.bfloat16)
    mixed = jnp.dot(flat, entry, preferred_element_type=jnp.float32)
    queries = (mixed[:, 0:model_width] + pieces[0]).astype(jnp.bfloat16)
    keys = mixed[:, model_width : 2 * model_width].astype(jnp.bfloat16)
    values = (mixed[:, 2 * model_width : 3 * model_width] + pieces[1]).astype(jnp.bfloat16)
    attended, log_total = attend_forward(queries, keys, values, own_member, member, usable)
    attended_low = attended.astype(jnp.bfloat16)
    branch = jnp.dot(attended_low, leaving, preferred_element_type=jnp.float32) + pieces[2]
    middle, normed_one, factor_one = norm_forward(hidden + branch, pieces[3], pieces[4])
    middle_low = middle.astype(jnp.bfloat16)
    inner = jnp.dot(middle_low, expand, preferred_element_type=jnp.float32) + pieces[8]
    active = gelu_exact(inner).astype(jnp.bfloat16)
    branch_two = jnp.dot(active, shrink, preferred_element_type=jnp.float32) + pieces[5]
    result, normed_two, factor_two = norm_forward(middle + branch_two, pieces[6], pieces[7])
    record = (
        flat,
        queries,
        keys,
        values,
        attended,
        log_total,
        attended_low,
        normed_one,
        factor_one,
        middle_low,
        inner,
        active,
        normed_two,
        factor_two,
    )
    return (result, record)


def layer_backward(upstream, weights, record, keys_all, values_all, own_member, member, usable):
    entry, leaving, expand, shrink, vector = weights
    model_width = leaving.shape[0]
    pieces = split_vector(vector.astype(jnp.float32), model_width)
    (
        flat,
        queries,
        keys,
        values,
        attended,
        log_total,
        attended_low,
        normed_one,
        factor_one,
        middle_low,
        inner,
        active,
        normed_two,
        factor_two,
    ) = record
    local_rows = queries.shape[0]
    resid_two, gain_two_grad, shift_two_grad = norm_backward(
        upstream, normed_two, factor_two, pieces[6]
    )
    branch_two_grad = resid_two.astype(jnp.bfloat16)
    bias_down_grad = jnp.sum(branch_two_grad.astype(jnp.float32), axis=0)
    shrink_grad = inner_rows(active, branch_two_grad)
    active_grad = times_trans(branch_two_grad, shrink)
    unused_value, gelu_pull = jax.vjp(gelu_exact, inner)
    inner_grad = gelu_pull(active_grad)[0].astype(jnp.bfloat16)
    bias_up_grad = jnp.sum(inner_grad.astype(jnp.float32), axis=0)
    expand_grad = inner_rows(middle_low, inner_grad)
    middle_grad = resid_two + times_trans(inner_grad, expand)
    resid_one, gain_one_grad, shift_one_grad = norm_backward(
        middle_grad, normed_one, factor_one, pieces[3]
    )
    branch_grad = resid_one.astype(jnp.bfloat16)
    bias_out_grad = jnp.sum(branch_grad.astype(jnp.float32), axis=0)
    exit_grad = inner_rows(attended_low, branch_grad)
    attended_grad = times_trans(branch_grad, leaving).astype(jnp.bfloat16)
    deltas = jnp.sum(
        (attended_grad.astype(jnp.float32) * attended).reshape(local_rows, HEADS, HEAD_DIM), axis=2
    ).T
    query_grad, key_value_grad = attend_backward(
        queries, attended_grad, log_total, deltas, keys_all, values_all, own_member, member, usable
    )
    own_key_value = lax.psum_scatter(
        key_value_grad.astype(jnp.bfloat16), "shard", scatter_dimension=0, tiled=True
    ).astype(jnp.float32)
    mixed_grad = jnp.concatenate([query_grad, own_key_value], axis=1).astype(jnp.bfloat16)
    bias_query_grad = jnp.sum(mixed_grad[:, 0:model_width].astype(jnp.float32), axis=0)
    bias_value_grad = jnp.sum(
        mixed_grad[:, 2 * model_width : 3 * model_width].astype(jnp.float32), axis=0
    )
    entry_grad = inner_rows(flat, mixed_grad)
    hidden_grad = resid_one + times_trans(mixed_grad, entry)
    vector_grad = jnp.concatenate(
        [
            bias_query_grad,
            bias_value_grad,
            bias_out_grad,
            gain_one_grad,
            shift_one_grad,
            bias_down_grad,
            gain_two_grad,
            shift_two_grad,
            bias_up_grad,
        ]
    )
    return (hidden_grad, (entry_grad, exit_grad, expand_grad, shrink_grad, vector_grad))


def body(
    inputs,
    cotangent,
    lengths,
    dealing,
    key_mask,
    entry_weight,
    exit_weight,
    expand_weight,
    shrink_weight,
    vectors,
):
    local_rows = inputs.shape[0]
    group_rows = local_rows * lax.axis_size("shard")
    position = lax.axis_index("shard") * local_rows
    dealt_all, mask_all = (
        lax.all_gather(dealing, "shard", axis=1, tiled=True),
        lax.all_gather(key_mask, "shard", axis=1, tiled=True),
    )
    member, leading = sequence_ids(lengths[0], group_rows)
    usable = (mask_all[0] == 1) | leading
    own_member = lax.dynamic_slice_in_dim(member, position, local_rows, 0)
    inverse = (
        jnp.zeros((group_rows,), jnp.int32)
        .at[dealt_all[0]]
        .set(jnp.arange(group_rows, dtype=jnp.int32))
    )
    own_inverse = lax.dynamic_slice_in_dim(inverse, position, local_rows, 0)
    inputs_all, cotangent_all = (
        lax.all_gather(inputs, "shard", axis=0, tiled=True),
        lax.all_gather(cotangent, "shard", axis=0, tiled=True),
    )
    hidden = jnp.take(inputs_all, dealing[0], axis=0).astype(jnp.float32)
    upstream = jnp.take(cotangent_all, dealing[0], axis=0).astype(jnp.float32)
    layers = entry_weight.shape[0]
    saved = []
    kept = []
    for layer_index in range(layers):
        weights = fetch_forward(
            entry_weight, exit_weight, expand_weight, shrink_weight, vectors, layer_index
        )
        kept.append(weights)
        hidden, record = layer_forward(hidden, weights, own_member, member, usable)
        saved.append(record)
    output_all = lax.all_gather(hidden.astype(jnp.bfloat16), "shard", axis=0, tiled=True)
    output = jnp.take(output_all, own_inverse, axis=0)
    hidden_grad = upstream
    layer_grads = [None] * layers
    for layer_index in reversed(range(layers)):
        weights = fetch_backward(
            entry_weight, exit_weight, expand_weight, shrink_weight, vectors, layer_index
        )
        record = saved[layer_index]
        keys_all, values_all = (
            lax.all_gather(record[2], "shard", axis=0, tiled=True),
            lax.all_gather(record[3], "shard", axis=0, tiled=True),
        )
        hidden_grad, local_grads = layer_backward(
            hidden_grad, weights, record, keys_all, values_all, own_member, member, usable
        )
        entry_local, exit_local, expand_local, shrink_local, vector_local = local_grads
        entry_part, exit_part, expand_part, shrink_part, vector_part = (
            lax.psum_scatter(
                entry_local.astype(jnp.bfloat16), "shard", scatter_dimension=0, tiled=True
            ).astype(jnp.float32),
            lax.psum_scatter(
                exit_local.astype(jnp.bfloat16), "shard", scatter_dimension=0, tiled=True
            ).astype(jnp.float32),
            lax.psum_scatter(
                expand_local.astype(jnp.bfloat16), "shard", scatter_dimension=0, tiled=True
            ).astype(jnp.float32),
            lax.psum_scatter(
                shrink_local.astype(jnp.bfloat16), "shard", scatter_dimension=0, tiled=True
            ).astype(jnp.float32),
            lax.psum_scatter(
                vector_local.astype(jnp.bfloat16), "shard", scatter_dimension=0, tiled=True
            ).astype(jnp.float32),
        )
        entry_part, exit_part, expand_part, shrink_part, vector_part = (
            lax.psum(entry_part.astype(jnp.bfloat16), "rep").astype(jnp.float32),
            lax.psum(exit_part.astype(jnp.bfloat16), "rep").astype(jnp.float32),
            lax.psum(expand_part.astype(jnp.bfloat16), "rep").astype(jnp.float32),
            lax.psum(shrink_part.astype(jnp.bfloat16), "rep").astype(jnp.float32),
            lax.psum(vector_part.astype(jnp.bfloat16), "rep").astype(jnp.float32),
        )
        layer_grads[layer_index] = (entry_part, exit_part, expand_part, shrink_part, vector_part)
    entry_grad = jnp.stack([item[0] for item in layer_grads])
    exit_grad = jnp.stack([item[1] for item in layer_grads])
    expand_grad = jnp.stack([item[2] for item in layer_grads])
    shrink_grad = jnp.stack([item[3] for item in layer_grads])
    vector_grad = jnp.stack([item[4] for item in layer_grads])
    grads_all = lax.all_gather(
        hidden_grad.astype(jnp.bfloat16), "shard", axis=0, tiled=True
    ).astype(hidden_grad.dtype)
    input_grad = jnp.take(grads_all, own_inverse, axis=0)
    return (output, input_grad, entry_grad, exit_grad, expand_grad, shrink_grad, vector_grad)


EDGE = (0, 1, 6, 7)
CORE = (2, 3, 4, 5)
ALL = tuple(range(8))
BOTH = ("rep", "shard")
UNIT = 24


def routes(rep_flip, shard_flip, shards):
    return [
        (rep * 8 + shard, (rep ^ rep_flip) * 8 + (shard ^ shard_flip))
        for rep in range(4)
        for shard in shards
    ]


TO_X = routes(1, 0, ALL)
TO_Y = routes(2, 0, ALL)
TO_TWIN = routes(0, 1, ALL)
TO_SIDE = routes(0, 2, ALL)
TO_MID = routes(0, 6, CORE)


def send(value, route):
    return lax.ppermute(value, BOTH, route)


def low(value):
    return value.astype(jnp.bfloat16)


def wide(value):
    return value.astype(jnp.float32)


VMEM = pl.BlockSpec(memory_space=pltpu.VMEM)
SMEM = pl.BlockSpec(memory_space=pltpu.SMEM)
LIMIT = pltpu.CompilerParams(vmem_limit_bytes=60 * 1024 * 1024)


def shaped(shape, kind=jnp.bfloat16):
    return jax.ShapeDtypeStruct(shape, kind)


def nt(left, right):
    return lax.dot_general(left, right, (((1,), (1,)), ((), ())), preferred_element_type=jnp.float32)


def nn(left, right):
    return lax.dot_general(left, right, (((1,), (0,)), ((), ())), preferred_element_type=jnp.float32)


def fixed(*shape):
    return pl.BlockSpec(shape, lambda step: (0,) * len(shape))


def gather_kernel(ids_ref, want_ref, *refs):
    out_ref = refs[-1]
    want = want_ref[...]
    total = None
    index = 0
    for piece_ref in refs[:-1]:
        for slot in range(piece_ref.shape[0]):
            ids = ids_ref[index]
            hit = low(wide(want == ids))
            part = nn(hit, piece_ref[slot, 0 : ids.shape[1], :])
            total = part if total is None else total + part
            index += 1
    out_ref[...] = low(total)


def gather_rows(pieces, ids, want):
    return pl.pallas_call(
        gather_kernel,
        out_shape=shaped((want.shape[0], pieces[0].shape[2])),
        in_specs=[VMEM] * (2 + len(pieces)),
        out_specs=VMEM,
        compiler_params=LIMIT,
        name="gather_rows",
    )(ids, want, *pieces)


def assemble_kernel(where_ref, *refs):
    out_ref = refs[10]
    depth, rep, twin = where_ref[0], where_ref[1], where_ref[2]
    for side in range(2):
        own, first, over_x, over_y, over_d = refs[side * 5 : side * 5 + 5]
        core = twin ^ side
        for row in range(4):
            out_ref[depth, core, row] = own[row]
        for slot, flip in enumerate((1, 3, 2)):
            level = depth ^ flip
            for piece, bits in ((first, 0), (over_x, 1), (over_y, 2), (over_d, 3)):
                out_ref[level, core, rep ^ bits] = piece[slot]


def assemble(where, parts, start, by_rows):
    def part_spec(part):
        return pl.BlockSpec(
            (part.shape[0], None) + part.shape[2:],
            lambda unit, where_ref: (0, start + unit, 0, 0),
        )

    width = parts[0].shape[3]
    if by_rows:
        shape = (4, 2, 4, 4, UNIT, width)
        spec = pl.BlockSpec(
            (4, 2, 4, None, UNIT, width), lambda unit, where_ref: (0, 0, 0, unit, 0, 0)
        )
    else:
        shape = (4, 4, 2, 4, UNIT, width)
        spec = pl.BlockSpec(
            (None, 4, 2, 4, UNIT, width), lambda unit, where_ref: (unit, 0, 0, 0, 0, 0)
        )
    result = pl.pallas_call(
        assemble_kernel,
        grid_spec=pltpu.PrefetchScalarGridSpec(
            num_scalar_prefetch=1,
            grid=(4,),
            in_specs=[part_spec(part) for part in parts],
            out_specs=spec,
        ),
        out_shape=shaped(shape),
        compiler_params=LIMIT,
        name="assemble",
    )(where, *parts)
    return result.reshape(4, 32 * UNIT, width)


def pack_weights(entry, leaving, expand, shrink):
    width = leaving.shape[1]

    def by_columns(weight):
        count = weight.shape[1] // width
        return low(weight).reshape(4, UNIT, count, width).transpose(0, 2, 1, 3)

    return (
        jnp.concatenate([by_columns(entry), by_columns(leaving)], axis=1),
        jnp.concatenate([by_columns(expand), low(shrink).reshape(4, 4, UNIT, width)], axis=1),
    )


def spread(own, near, middle, far):
    units = own.shape[1]
    first = jnp.stack([near, middle, far])
    over_x = send(first, TO_X)
    over_y = send(first, TO_Y)
    half = units // 2
    over_d = jnp.concatenate(
        [send(over_x[:, :half], TO_Y), send(over_y[:, half:], TO_X)], axis=1
    )
    mine = (own, first, over_x, over_y, over_d)
    return mine + tuple(send(item, TO_TWIN) for item in mine)


def project_kernel(h_ref, w_ref, vec_ref, sel_ref, q_ref, kv_ref, mine_ref, theirs_ref):
    unit = pl.program_id(0)
    product = nn(h_ref[...], w_ref[...])

    @pl.when(unit == 0)
    def _():
        q_ref[...] = low(product + vec_ref[0:1, :])
        mine_ref[...] = low(nn(h_ref[...], sel_ref[0]))
        theirs_ref[...] = low(nn(h_ref[...], sel_ref[1]))

    @pl.when(unit == 1)
    def _():
        kv_ref[...] = low(product)

    @pl.when(unit == 2)
    def _():
        kv_ref[...] = low(product + vec_ref[1:2, :])


def project(hidden, weight, vec, sel):
    rows, width = hidden.shape
    return pl.pallas_call(
        project_kernel,
        grid=(3,),
        in_specs=[
            fixed(rows, width),
            pl.BlockSpec((None, width, width), lambda unit: (unit, 0, 0)),
            fixed(12, width),
            fixed(2, width, width // 2),
        ],
        out_specs=[
            fixed(rows, width),
            pl.BlockSpec((None, rows, width), lambda unit: (jnp.maximum(unit - 1, 0), 0, 0)),
            fixed(rows, width // 2),
            fixed(rows, width // 2),
        ],
        out_shape=[
            shaped((rows, width)),
            shaped((2, rows, width)),
            shaped((rows, width // 2)),
            shaped((rows, width // 2)),
        ],
        compiler_params=LIMIT,
        name="project",
    )(hidden, weight, vec, sel)


def attend_kernel(
    q_ref, ka_ref, kb_ref, va_ref, vb_ref, code_ref, member_ref, o_ref, ot_ref, lse_ref, bias_ref
):
    half = q_ref.shape[0]

    @pl.when(pl.program_id(0) == 0)
    def _():
        bias_ref[...] = jnp.where(code_ref[...] == member_ref[...], 0.0, NEG_FILL)

    q = q_ref[...] * jnp.bfloat16(HEAD_DIM ** (-0.5))
    lane = lax.broadcasted_iota(jnp.int32, q.shape, 1)
    keys = (ka_ref[...], kb_ref[...])
    values = (va_ref[...].T, vb_ref[...].T)
    outs = []
    for head in range(2):
        q_head = jnp.where((lane >= HEAD_DIM) == (head == 1), q, jnp.bfloat16(0))
        scores = [
            nt(keys[side], q_head) + bias_ref[side * half : (side + 1) * half, :]
            for side in range(2)
        ]
        top = jnp.maximum(
            jnp.max(scores[0], axis=0, keepdims=True), jnp.max(scores[1], axis=0, keepdims=True)
        )
        total = None
        mixed = None
        for side in range(2):
            expo = jnp.exp(scores[side] - top)
            part = jnp.sum(expo, axis=0, keepdims=True)
            value = values[side][head * HEAD_DIM : (head + 1) * HEAD_DIM, :]
            product = nn(value, low(expo))
            total = part if total is None else total + part
            mixed = product if mixed is None else mixed + product
        outs.append(mixed / total)
        lse_ref[head : head + 1, :] = top + jnp.log(total)
    joined = jnp.concatenate(outs, axis=0)
    ot_ref[...] = joined
    o_ref[...] = low(joined.T)


def pair_specs(half):
    column = pl.BlockSpec((half, 128), lambda pair: (0, pair))
    key = pl.BlockSpec((None, half, 128), lambda pair: (0, 0, pair))
    value = pl.BlockSpec((None, half, 128), lambda pair: (1, 0, pair))
    turned = pl.BlockSpec((128, half), lambda pair: (pair, 0))
    level = pl.BlockSpec((None, 2, half), lambda pair: (pair, 0, 0))
    return column, key, value, turned, level


def attend_fast(queries, kv, kv_twin, code, member):
    half, width = queries.shape
    column, key, value, turned, level = pair_specs(half)
    return pl.pallas_call(
        attend_kernel,
        grid=(width // 128,),
        in_specs=[column, key, key, value, value, fixed(2 * half, 1), fixed(1, half)],
        out_specs=[column, turned, level],
        out_shape=[
            shaped((half, width)),
            shaped((width, half), jnp.float32),
            shaped((width // 128, 2, half), jnp.float32),
        ],
        scratch_shapes=[pltpu.VMEM((2 * half, half), jnp.float32)],
        compiler_params=LIMIT,
        name="attend_forward",
    )(queries, kv, kv_twin, kv, kv_twin, code, member)


def attend_back_kernel(
    q_ref, g_ref, ka_ref, kb_ref, va_ref, vb_ref, ot_ref, lse_ref, code_ref, member_ref,
    dq_ref, own_ref, twin_ref, bias_ref,
):
    half = q_ref.shape[0]

    @pl.when(pl.program_id(0) == 0)
    def _():
        bias_ref[...] = jnp.where(code_ref[...] == member_ref[...], 0.0, NEG_FILL)

    scale = HEAD_DIM ** (-0.5)
    q = q_ref[...] * jnp.bfloat16(scale)
    grad = g_ref[...]
    lane = lax.broadcasted_iota(jnp.int32, q.shape, 1)
    keys = (ka_ref[...], kb_ref[...])
    turned = (keys[0].T, keys[1].T)
    values = (va_ref[...], vb_ref[...])
    product = ot_ref[...] * wide(grad).T
    key_sums = [None, None]
    value_sums = [None, None]
    query_parts = []
    for head in range(2):
        rows = slice(head * HEAD_DIM, (head + 1) * HEAD_DIM)
        chosen = (lane >= HEAD_DIM) == (head == 1)
        q_head = jnp.where(chosen, q, jnp.bfloat16(0))
        g_head = jnp.where(chosen, grad, jnp.bfloat16(0))
        delta = jnp.sum(product[rows, :], axis=0, keepdims=True)
        level = lse_ref[head : head + 1, :]
        query_sum = None
        for side in range(2):
            scores = nt(keys[side], q_head) + bias_ref[side * half : (side + 1) * half, :]
            prob = jnp.exp(scores - level)
            slope = nt(values[side], g_head)
            steep = low(prob * (slope - delta))
            value_part = nn(low(prob), g_head)
            key_part = nn(steep, q_head)
            query_part = nn(turned[side][rows, :], steep)
            value_sums[side] = value_part if head == 0 else value_sums[side] + value_part
            key_sums[side] = key_part if head == 0 else key_sums[side] + key_part
            query_sum = query_part if side == 0 else query_sum + query_part
        query_parts.append(query_sum * scale)
    dq_ref[...] = low(jnp.concatenate(query_parts, axis=0).T)
    own_ref[0] = key_sums[0]
    own_ref[1] = value_sums[0]
    twin_ref[0] = low(key_sums[1])
    twin_ref[1] = low(value_sums[1])


def attend_back_fast(queries, grad, kv, kv_twin, ot, lse, code, member):
    half, width = queries.shape
    column, key, value, turned, level = pair_specs(half)
    both = pl.BlockSpec((2, half, 128), lambda pair: (0, 0, pair))
    return pl.pallas_call(
        attend_back_kernel,
        grid=(width // 128,),
        in_specs=[column, column, key, key, value, value, turned, level]
        + [fixed(2 * half, 1), fixed(1, half)],
        out_specs=[column, both, both],
        out_shape=[
            shaped((half, width)),
            shaped((2, half, width), jnp.float32),
            shaped((2, half, width)),
        ],
        scratch_shapes=[pltpu.VMEM((2 * half, half), jnp.float32)],
        compiler_params=LIMIT,
        name="attend_backward",
    )(queries, grad, kv, kv_twin, kv, kv_twin, ot, lse, code, member)


def normal_parts(value):
    scaled = value * 0.7071067811865476
    size = jnp.abs(scaled)
    square = size * size
    t = 1.0 / (1.0 + 0.5 * size)
    series = 0.17087277
    for factor in (
        -0.82215223, 1.48851587, -1.13520398, 0.27886807, -0.18628806,
        0.09678418, 0.37409196, 1.00002368, -1.26551223,
    ):
        series = series * t + factor
    tail = 0.5 * t * jnp.exp(series - square)
    cumulative = jnp.where(value >= 0, 1.0 - tail, tail)
    density = 0.3989422804014327 * jnp.exp(-square)
    return cumulative, density


def row_norm(resid):
    offsets = resid - jnp.mean(resid, axis=-1, keepdims=True)
    spread_of = jnp.mean(offsets * offsets, axis=-1, keepdims=True)
    factor = lax.rsqrt(spread_of + 1e-05)
    return offsets * factor, factor


def post_kernel(
    where_ref, o_ref, h_ref, wo_ref, up_ref, down_ref, vec_ref, sel_ref,
    h_out, hl_out, n1_out, t1_out, n2_out, t2_out, slope_out,
    om_out, ot_out, ym_out, yt_out, gm_out, gt_out,
    y_ref, yl_ref, f_ref,
):
    step = pl.program_id(0)
    half_width = om_out.shape[1]

    @pl.when(step == 0)
    def _():
        attended = o_ref[...]
        branch = nn(attended, wo_ref[...]) + vec_ref[2:3, :]
        normed, factor = row_norm(wide(h_ref[...]) + branch)
        middle = normed * vec_ref[3:4, :] + vec_ref[4:5, :]
        n1_out[...] = normed
        t1_out[...] = factor
        y_ref[...] = middle
        yl_ref[...] = low(middle)
        om_out[...] = low(nn(attended, sel_ref[0]))
        ot_out[...] = low(nn(attended, sel_ref[1]))
        ym_out[...] = low(nn(yl_ref[...], sel_ref[0]))
        yt_out[...] = low(nn(yl_ref[...], sel_ref[1]))

    inner = nn(yl_ref[...], up_ref[...]) + vec_ref[pl.ds(8 + step, 1), :]
    cumulative, density = normal_parts(inner)
    slope_out[...] = low(cumulative + inner * density)
    active = low(inner * cumulative)
    first, second = active[:, :half_width], active[:, half_width:]
    swap = where_ref[2] == 1
    gm_out[...] = jnp.where(swap, second, first)
    gt_out[...] = jnp.where(swap, first, second)
    part = nn(active, down_ref[...])

    @pl.when(step == 0)
    def _():
        f_ref[...] = part

    @pl.when(step > 0)
    def _():
        f_ref[...] += part

    @pl.when(step == 3)
    def _():
        normed, factor = row_norm(y_ref[...] + (f_ref[...] + vec_ref[5:6, :]))
        result = normed * vec_ref[6:7, :] + vec_ref[7:8, :]
        n2_out[...] = normed
        t2_out[...] = factor
        h_out[...] = result
        hl_out[...] = low(result)


def unit_spec(width, index):
    return pl.BlockSpec((None, width, width), lambda step: (index, 0, 0))


def step_spec(width):
    return pl.BlockSpec((None, width, width), lambda step: (step, 0, 0))


def column_spec(rows, width):
    return pl.BlockSpec((rows, width), lambda step: (0, step))


def post(where, attended, hidden, front, up, down, vec, sel):
    rows, width = attended.shape
    half = width // 2
    full = fixed(rows, width)
    thin = fixed(rows, 1)
    return pl.pallas_call(
        post_kernel,
        grid=(4,),
        in_specs=[
            SMEM, full, full, unit_spec(width, 3), step_spec(width), step_spec(width),
            fixed(12, width), fixed(2, width, half),
        ],
        out_specs=[full, full, full, thin, full, thin, column_spec(rows, width)]
        + [fixed(rows, half)] * 4
        + [column_spec(rows, half)] * 2,
        out_shape=[
            shaped((rows, width), jnp.float32),
            shaped((rows, width)),
            shaped((rows, width), jnp.float32),
            shaped((rows, 1), jnp.float32),
            shaped((rows, width), jnp.float32),
            shaped((rows, 1), jnp.float32),
            shaped((rows, 4 * width)),
        ]
        + [shaped((rows, half))] * 4
        + [shaped((rows, 4 * half))] * 2,
        scratch_shapes=[
            pltpu.VMEM((rows, width), jnp.float32),
            pltpu.VMEM((rows, width), jnp.bfloat16),
            pltpu.VMEM((rows, width), jnp.float32),
        ],
        compiler_params=LIMIT,
        name="post",
    )(where, attended, hidden, front, up, down, vec, sel)


def norm_back(incoming, normed, factor, gain):
    scaled = incoming * gain
    return factor * (
        scaled
        - jnp.mean(scaled, axis=-1, keepdims=True)
        - normed * jnp.mean(scaled * normed, axis=-1, keepdims=True)
    )


def column_sum(value):
    return jnp.sum(value, axis=0, keepdims=True)


def post_back_kernel(
    e_ref, n1_ref, t1_ref, n2_ref, t2_ref, slope_ref, wo_ref, up_ref, down_ref, vec_ref,
    df_out, dz_out, da_out, do_out, dr_out, sums_out,
    r_ref, y_ref,
):
    step = pl.program_id(0)

    @pl.when(step == 0)
    def _():
        incoming = wide(e_ref[...])
        normed = n2_ref[...]
        resid = norm_back(incoming, normed, t2_ref[...], vec_ref[6:7, :])
        r_ref[...] = resid
        rounded = low(resid)
        df_out[...] = rounded
        sums_out[0:2, :] = jnp.zeros((2, sums_out.shape[1]), jnp.float32)
        sums_out[5:6, :] = column_sum(wide(rounded))
        sums_out[6:7, :] = column_sum(incoming * normed)
        sums_out[7:8, :] = column_sum(incoming)

    steep = low(nt(df_out[...], down_ref[...]) * wide(slope_ref[...]))
    dz_out[...] = steep
    sums_out[pl.ds(8 + step, 1), :] = column_sum(wide(steep))
    part = nt(steep, up_ref[...])

    @pl.when(step == 0)
    def _():
        y_ref[...] = part

    @pl.when(step > 0)
    def _():
        y_ref[...] += part

    @pl.when(step == 3)
    def _():
        incoming = r_ref[...] + y_ref[...]
        normed = n1_ref[...]
        resid = norm_back(incoming, normed, t1_ref[...], vec_ref[3:4, :])
        dr_out[...] = resid
        rounded = low(resid)
        da_out[...] = rounded
        do_out[...] = low(nt(rounded, wo_ref[...]))
        sums_out[2:3, :] = column_sum(wide(rounded))
        sums_out[3:4, :] = column_sum(incoming * normed)
        sums_out[4:5, :] = column_sum(incoming)


def post_back(upstream, n1, t1, n2, t2, slope, front, up, down, vec):
    rows, width = upstream.shape
    full = fixed(rows, width)
    thin = fixed(rows, 1)
    return pl.pallas_call(
        post_back_kernel,
        grid=(4,),
        in_specs=[
            full, full, thin, full, thin, column_spec(rows, width),
            unit_spec(width, 3), step_spec(width), step_spec(width), fixed(12, width),
        ],
        out_specs=[full, column_spec(rows, width), full, full, full, fixed(12, width)],
        out_shape=[
            shaped((rows, width)),
            shaped((rows, 4 * width)),
            shaped((rows, width)),
            shaped((rows, width)),
            shaped((rows, width), jnp.float32),
            shaped((12, width), jnp.float32),
        ],
        scratch_shapes=[
            pltpu.VMEM((rows, width), jnp.float32),
            pltpu.VMEM((rows, width), jnp.float32),
        ],
        compiler_params=LIMIT,
        name="post_back",
    )(upstream, n1, t1, n2, t2, slope, front, up, down, vec)


def project_back_kernel(
    dq_ref, own_ref, got_ref, w_ref, dr_ref, dm_out, dx_out, dxl_out, sums_out
):
    unit = pl.program_id(0)

    @pl.when(unit == 0)
    def _():
        dm_out[...] = dq_ref[...]

    @pl.when(unit > 0)
    def _():
        dm_out[...] = low(own_ref[...] + wide(got_ref[...]))

    grad = dm_out[...]
    part = nt(grad, w_ref[...])
    total = column_sum(wide(grad))

    @pl.when(unit == 0)
    def _():
        dx_out[...] = dr_ref[...] + part
        sums_out[0:1, :] = total

    @pl.when(unit > 0)
    def _():
        dx_out[...] += part
        sums_out[1:2, :] = total

    @pl.when(unit == 2)
    def _():
        dxl_out[...] = low(dx_out[...])


def project_back(dq, own, got, front, dr):
    rows, width = dq.shape
    full = fixed(rows, width)
    late = pl.BlockSpec((None, rows, width), lambda unit: (jnp.maximum(unit - 1, 0), 0, 0))
    return pl.pallas_call(
        project_back_kernel,
        grid=(3,),
        in_specs=[full, late, late, step_spec(width), full],
        out_specs=[
            pl.BlockSpec((None, rows, width), lambda unit: (unit, 0, 0)),
            full, full, fixed(2, width),
        ],
        out_shape=[
            shaped((3, rows, width)),
            shaped((rows, width), jnp.float32),
            shaped((rows, width)),
            shaped((2, width), jnp.float32),
        ],
        compiler_params=LIMIT,
        name="project_back",
    )(dq, own, got, front, dr)


def tn(left, right):
    return nn(left.T, right)


def split_store(keep_ref, give_ref, bit, x_first, piece_of, store):
    for other in range(2):
        pair = []
        for side in range(2):
            rep = (other * 2 + side) if x_first else (side * 2 + other)
            pair.append(low(piece_of(rep)))
        store(keep_ref, other, jnp.where(bit == 0, pair[0], pair[1]))
        store(give_ref, other, jnp.where(bit == 0, pair[1], pair[0]))


def front_grad_kernel(
    x_first, bit_ref, xm_ref, xt_ref, om_ref, ot_ref, dm_ref, dmt_ref, da_ref, dat_ref,
    keep_ref, give_ref,
):
    unit = pl.program_id(0)
    bit = bit_ref[0]

    def put(product):
        for level in range(4):
            base = level * 4 * UNIT

            def piece_of(rep):
                return product[base + rep * UNIT : base + (rep + 1) * UNIT, :]

            def store(ref, other, value):
                ref[level, other, unit] = value

            split_store(keep_ref, give_ref, bit, x_first, piece_of, store)

    @pl.when(unit < 3)
    def _():
        put(tn(xm_ref[...], dm_ref[...]) + tn(xt_ref[...], dmt_ref[...]))

    @pl.when(unit == 3)
    def _():
        put(tn(om_ref[...], da_ref[...]) + tn(ot_ref[...], dat_ref[...]))


def front_grad(x_first, bit, xm, xt, om, ot, dm, dmt, da, dat):
    rows, half = xm.shape
    width = da.shape[1]
    late = pl.BlockSpec((None, rows, width), lambda unit: (jnp.minimum(unit, 2), 0, 0))
    shape = (4, 2, 4, UNIT, width)
    return pl.pallas_call(
        functools.partial(front_grad_kernel, x_first),
        grid=(4,),
        in_specs=[SMEM]
        + [fixed(rows, half)] * 4
        + [late, late, fixed(rows, width), fixed(rows, width)],
        out_specs=[fixed(*shape)] * 2,
        out_shape=[shaped(shape)] * 2,
        compiler_params=LIMIT,
        name="front_grad",
    )(bit, xm, xt, om, ot, dm, dmt, da, dat)


def feed_grad_kernel(
    x_first, bit_ref, ym_ref, yt_ref, gm_ref, gt_ref, dz_ref, dzt_ref, df_ref, dft_ref,
    keep_ref, give_ref,
):
    step = pl.program_id(0)
    bit = bit_ref[0]

    @pl.when(step < 4)
    def _():
        product = tn(ym_ref[...], dz_ref[...]) + tn(yt_ref[...], dzt_ref[...])
        for level in range(4):
            base = level * 4 * UNIT

            def piece_of(rep):
                return product[base + rep * UNIT : base + (rep + 1) * UNIT, :]

            def store(ref, other, value):
                ref[level, other, step] = value

            split_store(keep_ref, give_ref, bit, x_first, piece_of, store)

    @pl.when(step >= 4)
    def _():
        product = tn(gm_ref[...], df_ref[...]) + tn(gt_ref[...], dft_ref[...])
        for sub in range(4):

            def piece_of(rep):
                base = (rep * 4 + sub) * UNIT
                return product[base : base + UNIT, :]

            def store(ref, other, value):
                ref[step - 4, other, 4 + sub] = value

            split_store(keep_ref, give_ref, bit, x_first, piece_of, store)


def feed_grad(x_first, bit, ym, yt, gm, gt, dz, dzt, df, dft):
    rows, half = ym.shape
    width = df.shape[1]
    early = pl.BlockSpec((rows, width), lambda step: (0, jnp.minimum(step, 3)))
    late = pl.BlockSpec((rows, half), lambda step: (0, jnp.maximum(step - 4, 0)))
    shape = (4, 2, 8, UNIT, width)
    return pl.pallas_call(
        functools.partial(feed_grad_kernel, x_first),
        grid=(8,),
        in_specs=[SMEM]
        + [fixed(rows, half)] * 2
        + [late, late, early, early, fixed(rows, width), fixed(rows, width)],
        out_specs=[fixed(*shape)] * 2,
        out_shape=[shaped(shape)] * 2,
        compiler_params=LIMIT,
        name="feed_grad",
    )(bit, ym, yt, gm, gt, dz, dzt, df, dft)


def reduce_grad(keep, give, bit, is_low, is_core, x_first):
    one, two = (TO_X, TO_Y) if x_first else (TO_Y, TO_X)
    got = send(give, one)
    stage = low(wide(keep) + wide(got))
    give = jnp.where(is_low, stage[2:4], stage[0:2])
    keep = jnp.where(is_low, stage[0:2], stage[2:4])
    got = send(give, TO_MID)
    stage = low(wide(keep) + wide(got))
    outer = jnp.where(is_low, stage[0], stage[1])
    inner = jnp.where(is_low, stage[1], stage[0])
    got = send(outer, TO_SIDE)
    stage = jnp.where(is_core, inner, got)
    got = send(stage, two)
    stage = low(wide(stage) + wide(got))
    got = send(stage, one)
    axis = 1 if x_first else 0
    joined = jnp.where(bit == 0, jnp.stack([stage, got], axis), jnp.stack([got, stage], axis))
    return wide(joined).reshape((4,) + stage.shape[1:])


def body_fast(
    inputs, cotangent, lengths, dealing, key_mask,
    entry_weight, exit_weight, expand_weight, shrink_weight, vectors,
):
    rows, width = inputs.shape
    layers = entry_weight.shape[0]
    group_rows = 8 * rows
    half_rows = group_rows // 2
    core_rows = half_rows // 2
    rep = lax.axis_index("rep")
    shard = lax.axis_index("shard")
    depth, twin = shard // 2, shard % 2
    is_low = depth <= 1
    is_core = (depth == 1) | (depth == 2)
    where = jnp.stack([depth, rep, twin]).astype(jnp.int32)
    bits = (rep & 1, rep >> 1)

    def order(four):
        own, near, middle, far = four
        return jnp.where(
            is_low, jnp.stack([near, own, middle, far]), jnp.stack([far, middle, own, near])
        )

    def absolute(mine, theirs):
        one, two = order(mine), order(theirs)
        return jnp.where(twin == 0, jnp.stack([one, two], 1), jnp.stack([two, one], 1))

    packs = [
        pack_weights(entry_weight[l], exit_weight[l], expand_weight[l], shrink_weight[l])
        for l in range(layers)
    ]

    def own_piece(pack):
        piece = lax.dynamic_index_in_dim(pack, rep, 0, keepdims=False)
        return piece.reshape(-1, width)

    extra = layers * vectors.shape[1] // width
    tail = low(vectors).reshape(extra, width)
    table = jnp.concatenate([dealing // 64, dealing % 64, key_mask], axis=0)
    table = low(table).reshape(1, width)
    filler = jnp.zeros((7 - extra, width), jnp.bfloat16)
    front_rows = 4 * UNIT
    zero = jnp.concatenate([inputs, tail, table, filler, own_piece(packs[0][0])], axis=0)
    near = send(zero, TO_SIDE)
    middle = send(zero, TO_MID)
    far = send(near, TO_MID)
    four = (zero, near, middle, far)
    lead = rows + 8
    mine = jnp.stack([item[:lead] for item in four])
    theirs = send(mine, TO_TWIN)

    def relay_units(pack, near, middle, far):
        shape = (pack.shape[1], UNIT, width)
        return spread(pack, *[item.reshape(shape) for item in (near, middle, far)])

    parts = relay_units(packs[0][0], *[item[lead:] for item in four[1:]])
    fronts = [assemble(where, parts, 0, False)]

    piece = own_piece(packs[0][1])
    near = send(piece, TO_SIDE)
    parts = relay_units(packs[0][1], near, send(piece, TO_MID), send(near, TO_MID))
    ups = [assemble(where, parts, 0, False)]
    downs = [assemble(where, parts, 4, True)]

    joined = jnp.concatenate([packs[1][0], packs[1][1]], axis=1)
    piece = jnp.concatenate([own_piece(joined), cotangent], axis=0)
    split = 12 * UNIT
    near = send(piece, TO_SIDE)
    four = (piece, near, send(piece, TO_MID), send(near, TO_MID))
    parts = relay_units(joined, *[item[:split] for item in four[1:]])
    fronts.append(assemble(where, parts, 0, False))
    ups.append(assemble(where, parts, 4, False))
    downs.append(assemble(where, parts, 8, True))
    cotangent_mine = jnp.stack([item[split:] for item in four])
    cotangent_theirs = send(cotangent_mine, TO_TWIN)

    header = absolute(tuple(mine[:, rows:]), tuple(theirs[:, rows:]))
    header = header.reshape(8, 8, width)
    vector_all = wide(header[:, :extra]).reshape(8, layers, vectors.shape[1])
    vector_all = jnp.transpose(vector_all, (1, 0, 2)).reshape(layers, 12, width)
    numbers = wide(header[:, extra]).reshape(8, 3, rows)
    dealt_all = (numbers[:, 0] * 64 + numbers[:, 1]).astype(jnp.int32).reshape(group_rows)
    mask_all = numbers[:, 2].reshape(group_rows)

    member, leading = sequence_ids(lengths[0], group_rows)
    usable = (mask_all == 1) | leading
    code = jnp.where(usable, member, -1)
    longest = jnp.argmax(lengths[0])
    begin = jnp.cumsum(lengths[0])[longest] - lengths[0][longest]
    spot = jnp.arange(half_rows, dtype=jnp.int32)

    def halve(values, low_side):
        inside = lax.dynamic_slice_in_dim(values, begin, half_rows, 0)
        outside = jnp.where(spot < begin, values[:half_rows], values[half_rows:])
        return jnp.where(low_side, inside, outside)

    def cores(values):
        own = lax.dynamic_slice_in_dim(values, twin * core_rows, core_rows, 0)
        other = lax.dynamic_slice_in_dim(values, (1 - twin) * core_rows, core_rows, 0)
        return own, other

    code_half = jnp.concatenate(cores(halve(code, is_low))).reshape(half_rows, 1)
    member_own = cores(halve(member, is_low))[0].reshape(1, core_rows)
    dealt_near = cores(halve(dealt_all, is_low))
    dealt_far = cores(halve(dealt_all, ~is_low))

    block = jnp.arange(width, dtype=jnp.int32)
    place = jnp.arange(width // 2, dtype=jnp.int32)
    chunk = 4 * UNIT
    source = (place // chunk) * (2 * chunk) + place % chunk
    cores_at = jnp.stack([twin, 1 - twin])
    sel = low(block[None, :, None] == (source[None, :] + cores_at[:, None] * chunk)[:, None, :])

    local = jnp.arange(rows, dtype=jnp.int32)
    bases = jnp.stack(
        [
            (depth ^ flip) * (2 * rows) + (twin ^ side) * rows
            for side in range(2)
            for flip in (0, 1, 3, 2)
        ]
    ).astype(jnp.int32)
    source_ids = (bases[:, None] + local[None, :]).reshape(8, 1, rows)
    want_in = dealt_near[0].reshape(core_rows, 1)
    hidden_low = gather_rows((mine, theirs), source_ids, want_in)
    upstream = gather_rows((cotangent_mine, cotangent_theirs), source_ids, want_in)

    result_ids = jnp.stack([dealt_near[0], dealt_far[0], dealt_near[1], dealt_far[1]]).reshape(
        4, 1, core_rows
    )
    want_out = jnp.concatenate([source_ids[0, 0], source_ids[1, 0]]).reshape(2 * rows, 1)

    def restore(value):
        pair = jnp.stack([value, send(value, TO_MID)])
        found = gather_rows((pair, send(pair, TO_TWIN)), result_ids, want_out)
        outer = send(found[rows:], TO_SIDE)
        return jnp.where(is_core, found[:rows], outer)

    saved = []
    hidden = hidden_low
    for layer in range(layers):
        vec = vector_all[layer]
        queries, kv, xm, xt = project(hidden_low, fronts[layer], vec, sel)
        kv_twin = send(kv, TO_TWIN)
        attended, ot, lse = attend_fast(queries, kv, kv_twin, code_half, member_own)
        (
            hidden, hidden_low, n1, t1, n2, t2, slope, om, oo, ym, yo, gm, go,
        ) = post(where, attended, hidden, fronts[layer], ups[layer], downs[layer], vec, sel)
        others = tuple(send(item, TO_TWIN) for item in (xt, oo, yo, go))
        saved.append((queries, kv, kv_twin, ot, lse, n1, t1, n2, t2, slope, xm, om, ym, gm, others))
    output = restore(hidden_low)

    grads = [None] * layers
    grad = upstream
    for layer in reversed(range(layers)):
        vec = vector_all[layer]
        x_first = layer == 0
        bit = bits[0] if x_first else bits[1]
        bit_word = bit.reshape(1).astype(jnp.int32)
        queries, kv, kv_twin, ot, lse, n1, t1, n2, t2, slope, xm, om, ym, gm, others = saved[layer]
        xt, oo, yo, go = others
        df, dz, da, do, dr, sums = post_back(
            grad, n1, t1, n2, t2, slope, fronts[layer], ups[layer], downs[layer], vec
        )
        keep, give = feed_grad(
            x_first, bit_word, ym, yo, gm, go, dz, send(dz, TO_TWIN), df, send(df, TO_TWIN)
        )
        feed = reduce_grad(keep, give, bit, is_low, is_core, x_first)
        dq, own, give = attend_back_fast(queries, do, kv, kv_twin, ot, lse, code_half, member_own)
        dm, grad, grad_low, head_sums = project_back(
            dq, own, send(give, TO_TWIN), fronts[layer], dr
        )
        keep, give = front_grad(
            x_first, bit_word, xm, xt, om, oo, dm, send(dm, TO_TWIN), da, send(da, TO_TWIN)
        )
        front = reduce_grad(keep, give, bit, is_low, is_core, x_first)
        grads[layer] = (front, feed, jnp.concatenate([head_sums, sums[2:]], axis=0))
    input_grad = wide(restore(grad_low))

    def columns(units):
        count = units.shape[1]
        return units.transpose(0, 2, 1, 3).reshape(4 * UNIT, count * width)

    entry_grad = jnp.stack([columns(item[0][:, 0:3]) for item in grads])
    exit_grad = jnp.stack([columns(item[0][:, 3:4]) for item in grads])
    expand_grad = jnp.stack([columns(item[1][:, 0:4]) for item in grads])
    shrink_grad = jnp.stack([item[1][:, 4:8].reshape(16 * UNIT, width) for item in grads])

    joined = jnp.stack([item[2].reshape(-1) for item in grads])
    joined = jnp.transpose(joined.reshape(layers, 4, 2, vectors.shape[1]), (1, 2, 0, 3))
    keep = lax.dynamic_index_in_dim(joined, twin, 1, keepdims=False)
    give = lax.dynamic_index_in_dim(joined, 1 - twin, 1, keepdims=False)
    stage = keep + send(give, TO_TWIN)
    stage = stage + send(stage, TO_X)
    stage = stage + send(stage, TO_Y)
    give = jnp.where(is_low, stage[2:4], stage[0:2])
    keep = jnp.where(is_low, stage[0:2], stage[2:4])
    stage = keep + send(give, TO_MID)
    outer = jnp.where(is_low, stage[0], stage[1])
    inner = jnp.where(is_low, stage[1], stage[0])
    vector_grad = jnp.where(is_core, inner, send(outer, TO_SIDE))
    return (output, input_grad, entry_grad, exit_grad, expand_grad, shrink_grad, vector_grad)


def solution(mesh):
    placed = (
        P(("rep", "shard"), None),
        P(("rep", "shard"), None),
        P("rep", None),
        P("rep", "shard"),
        P("rep", "shard"),
        P(None, "shard", None),
        P(None, "shard", None),
        P(None, "shard", None),
        P(None, "shard", None),
        P(None, "shard"),
    )
    small = dict(mesh.shape) == {"rep": 4, "shard": 8}
    return jax.shard_map(
        body_fast if small else body,
        mesh=mesh,
        in_specs=placed,
        out_specs=(
            P(("rep", "shard"), None),
            P(("rep", "shard"), None),
            P(None, "shard", None),
            P(None, "shard", None),
            P(None, "shard", None),
            P(None, "shard", None),
            P(None, "shard"),
        ),
        check_vma=False,
    )
```

```python
import functools

import jax
import jax.numpy as jnp
from jax import lax
from jax.experimental import pallas as pl
from jax.experimental.pallas import tpu as pltpu
from jax.sharding import PartitionSpec as P

HEADS = 12
HEAD_DIM = 64


NEG_FILL = -1e30


def norm_forward(resid, gain, shift):
    center = jnp.mean(resid, axis=-1, keepdims=True)
    offsets = resid - center
    spread = jnp.mean(offsets * offsets, axis=-1, keepdims=True)
    factor = lax.rsqrt(spread + 1e-05)
    normed = offsets * factor
    return (normed * gain + shift, normed, factor)


def norm_backward(incoming, normed, factor, gain):
    scaled = incoming * gain
    resid_grad = factor * (
        scaled
        - jnp.mean(scaled, axis=-1, keepdims=True)
        - normed * jnp.mean(scaled * normed, axis=-1, keepdims=True)
    )
    return (resid_grad, jnp.sum(incoming * normed, axis=0), jnp.sum(incoming, axis=0))


def inner_rows(left, right):
    return lax.dot_general(
        left, right, (((0,), (0,)), ((), ())), preferred_element_type=jnp.float32
    )


def times_trans(left, right):
    return lax.dot_general(
        left, right, (((1,), (1,)), ((), ())), preferred_element_type=jnp.float32
    )


def gelu_exact(value):
    return jax.nn.gelu(value, approximate=False)


def sequence_ids(lengths, group_rows):
    ending = jnp.cumsum(lengths)
    opening = ending - lengths
    places = jnp.arange(group_rows, dtype=jnp.int32)
    member = jnp.sum((places[:, None] >= ending[None, :]).astype(jnp.int32), axis=1)
    leading = jnp.any(places[:, None] == opening[None, :], axis=1)
    return (member, leading)


def split_vector(vector, model_width):
    pieces = [vector[index * model_width : (index + 1) * model_width] for index in range(8)]
    pieces.append(vector[8 * model_width :])
    return pieces


def fetch_forward(entry_weight, exit_weight, expand_weight, shrink_weight, vectors, layer_index):
    return (
        lax.all_gather(entry_weight[layer_index].astype(jnp.bfloat16), "shard", axis=0, tiled=True),
        lax.all_gather(exit_weight[layer_index].astype(jnp.bfloat16), "shard", axis=0, tiled=True),
        lax.all_gather(
            expand_weight[layer_index].astype(jnp.bfloat16), "shard", axis=0, tiled=True
        ),
        lax.all_gather(
            shrink_weight[layer_index].astype(jnp.bfloat16), "shard", axis=0, tiled=True
        ),
        lax.all_gather(vectors[layer_index].astype(jnp.bfloat16), "shard", axis=0, tiled=True),
    )


def fetch_backward(entry_weight, exit_weight, expand_weight, shrink_weight, vectors, layer_index):
    return (
        lax.all_gather(entry_weight[layer_index].astype(jnp.bfloat16), "shard", axis=0, tiled=True),
        lax.all_gather(exit_weight[layer_index].astype(jnp.bfloat16), "shard", axis=0, tiled=True),
        lax.all_gather(
            expand_weight[layer_index].astype(jnp.bfloat16), "shard", axis=0, tiled=True
        ),
        lax.all_gather(
            shrink_weight[layer_index].astype(jnp.bfloat16), "shard", axis=0, tiled=True
        ),
        lax.all_gather(vectors[layer_index].astype(jnp.bfloat16), "shard", axis=0, tiled=True),
    )


def attend_forward(queries, keys, values, own_member, member, usable):
    local_rows = queries.shape[0]
    query_heads = queries.reshape(local_rows, HEADS, HEAD_DIM)
    factor_scale = HEAD_DIM ** (-0.5)
    start_state = (
        jnp.full((HEADS, local_rows), NEG_FILL, jnp.float32),
        jnp.zeros((HEADS, local_rows), jnp.float32),
        jnp.zeros((HEADS, local_rows, HEAD_DIM), jnp.float32),
    )
    key_piece = lax.all_gather(keys, "shard", axis=0, tiled=True)
    value_piece = lax.all_gather(values, "shard", axis=0, tiled=True)
    amount = key_piece.shape[0]
    block_rows = local_rows * max(1, 512 // local_rows)

    def fold_advance(block_index, running):
        running_max, running_total, weighted = running
        begin = block_index * block_rows
        key_block = lax.dynamic_slice_in_dim(key_piece, begin, block_rows, 0).reshape(
            block_rows, HEADS, HEAD_DIM
        )
        value_block = lax.dynamic_slice_in_dim(value_piece, begin, block_rows, 0).reshape(
            block_rows, HEADS, HEAD_DIM
        )
        key_member = lax.dynamic_slice_in_dim(member, begin, block_rows, 0)
        key_usable = lax.dynamic_slice_in_dim(usable, begin, block_rows, 0)
        allowed = ((own_member[:, None] == key_member[None, :]) & key_usable[None, :])[None]
        scores = (
            jnp.einsum("qhd,khd->hqk", query_heads, key_block, preferred_element_type=jnp.float32)
            * factor_scale
        )
        scores = jnp.where(allowed, scores, NEG_FILL)
        new_max = jnp.maximum(running_max, jnp.max(scores, axis=2))
        expos = jnp.where(allowed, jnp.exp(scores - new_max[:, :, None]), 0.0)
        shrink_by = jnp.exp(running_max - new_max)
        new_total = running_total * shrink_by + jnp.sum(expos, axis=2)
        new_weighted = weighted * shrink_by[:, :, None] + jnp.einsum(
            "hqk,khd->hqd",
            expos.astype(jnp.bfloat16),
            value_block,
            preferred_element_type=jnp.float32,
        )
        return (new_max, new_total, new_weighted)

    running_max, running_total, weighted = lax.fori_loop(
        0, amount // block_rows, fold_advance, start_state
    )
    attended = jnp.transpose(weighted / running_total[:, :, None], (1, 0, 2)).reshape(
        local_rows, HEADS * HEAD_DIM
    )
    return (attended, running_max + jnp.log(running_total))


def attend_backward(
    queries, attended_grad, log_total, deltas, keys_all, values_all, own_member, member, usable
):
    local_rows = queries.shape[0]
    group_rows = keys_all.shape[0]
    model_width = HEADS * HEAD_DIM
    factor_scale = HEAD_DIM ** (-0.5)
    query_heads = queries.reshape(local_rows, HEADS, HEAD_DIM)
    grad_heads = attended_grad.reshape(local_rows, HEADS, HEAD_DIM)
    block_rows = min(512, group_rows)

    def attend_advance(query_sum, block_index):
        begin = block_index * block_rows
        key_block = lax.dynamic_slice_in_dim(keys_all, begin, block_rows, 0).reshape(
            block_rows, HEADS, HEAD_DIM
        )
        value_block = lax.dynamic_slice_in_dim(values_all, begin, block_rows, 0).reshape(
            block_rows, HEADS, HEAD_DIM
        )
        key_member = lax.dynamic_slice_in_dim(member, begin, block_rows, 0)
        key_usable = lax.dynamic_slice_in_dim(usable, begin, block_rows, 0)
        allowed = ((own_member[:, None] == key_member[None, :]) & key_usable[None, :])[None]
        scores = (
            jnp.einsum("qhd,khd->hqk", query_heads, key_block, preferred_element_type=jnp.float32)
            * factor_scale
        )
        probs = jnp.where(allowed, jnp.exp(scores - log_total[:, :, None]), 0.0)
        prob_grad = jnp.einsum(
            "qhd,khd->hqk", grad_heads, value_block, preferred_element_type=jnp.float32
        )
        score_grad = (probs * (prob_grad - deltas[:, :, None])).astype(jnp.bfloat16)
        query_sum = (
            query_sum
            + jnp.einsum("hqk,khd->qhd", score_grad, key_block, preferred_element_type=jnp.float32)
            * factor_scale
        )
        key_grad = (
            jnp.einsum("hqk,qhd->khd", score_grad, query_heads, preferred_element_type=jnp.float32)
            * factor_scale
        )
        value_grad = jnp.einsum(
            "hqk,qhd->khd",
            probs.astype(jnp.bfloat16),
            grad_heads,
            preferred_element_type=jnp.float32,
        )
        joined = jnp.concatenate(
            [
                key_grad.reshape(block_rows, model_width),
                value_grad.reshape(block_rows, model_width),
            ],
            axis=1,
        )
        return (query_sum, joined)

    query_sum, key_value = lax.scan(
        attend_advance,
        jnp.zeros((local_rows, HEADS, HEAD_DIM), jnp.float32),
        jnp.arange(group_rows // block_rows, dtype=jnp.int32),
    )
    key_value = key_value.reshape(group_rows, 2 * model_width)
    return (query_sum.reshape(local_rows, model_width), key_value)


def layer_forward(hidden, weights, own_member, member, usable):
    entry, leaving, expand, shrink, vector = weights
    model_width = leaving.shape[0]
    pieces = split_vector(vector.astype(jnp.float32), model_width)
    flat = hidden.astype(jnp.bfloat16)
    mixed = jnp.dot(flat, entry, preferred_element_type=jnp.float32)
    queries = (mixed[:, 0:model_width] + pieces[0]).astype(jnp.bfloat16)
    keys = mixed[:, model_width : 2 * model_width].astype(jnp.bfloat16)
    values = (mixed[:, 2 * model_width : 3 * model_width] + pieces[1]).astype(jnp.bfloat16)
    attended, log_total = attend_forward(queries, keys, values, own_member, member, usable)
    attended_low = attended.astype(jnp.bfloat16)
    branch = jnp.dot(attended_low, leaving, preferred_element_type=jnp.float32) + pieces[2]
    middle, normed_one, factor_one = norm_forward(hidden + branch, pieces[3], pieces[4])
    middle_low = middle.astype(jnp.bfloat16)
    inner = jnp.dot(middle_low, expand, preferred_element_type=jnp.float32) + pieces[8]
    active = gelu_exact(inner).astype(jnp.bfloat16)
    branch_two = jnp.dot(active, shrink, preferred_element_type=jnp.float32) + pieces[5]
    result, normed_two, factor_two = norm_forward(middle + branch_two, pieces[6], pieces[7])
    record = (
        flat,
        queries,
        keys,
        values,
        attended,
        log_total,
        attended_low,
        normed_one,
        factor_one,
        middle_low,
        inner,
        active,
        normed_two,
        factor_two,
    )
    return (result, record)


def layer_backward(upstream, weights, record, keys_all, values_all, own_member, member, usable):
    entry, leaving, expand, shrink, vector = weights
    model_width = leaving.shape[0]
    pieces = split_vector(vector.astype(jnp.float32), model_width)
    (
        flat,
        queries,
        keys,
        values,
        attended,
        log_total,
        attended_low,
        normed_one,
        factor_one,
        middle_low,
        inner,
        active,
        normed_two,
        factor_two,
    ) = record
    local_rows = queries.shape[0]
    resid_two, gain_two_grad, shift_two_grad = norm_backward(
        upstream, normed_two, factor_two, pieces[6]
    )
    branch_two_grad = resid_two.astype(jnp.bfloat16)
    bias_down_grad = jnp.sum(branch_two_grad.astype(jnp.float32), axis=0)
    shrink_grad = inner_rows(active, branch_two_grad)
    active_grad = times_trans(branch_two_grad, shrink)
    unused_value, gelu_pull = jax.vjp(gelu_exact, inner)
    inner_grad = gelu_pull(active_grad)[0].astype(jnp.bfloat16)
    bias_up_grad = jnp.sum(inner_grad.astype(jnp.float32), axis=0)
    expand_grad = inner_rows(middle_low, inner_grad)
    middle_grad = resid_two + times_trans(inner_grad, expand)
    resid_one, gain_one_grad, shift_one_grad = norm_backward(
        middle_grad, normed_one, factor_one, pieces[3]
    )
    branch_grad = resid_one.astype(jnp.bfloat16)
    bias_out_grad = jnp.sum(branch_grad.astype(jnp.float32), axis=0)
    exit_grad = inner_rows(attended_low, branch_grad)
    attended_grad = times_trans(branch_grad, leaving).astype(jnp.bfloat16)
    deltas = jnp.sum(
        (attended_grad.astype(jnp.float32) * attended).reshape(local_rows, HEADS, HEAD_DIM), axis=2
    ).T
    query_grad, key_value_grad = attend_backward(
        queries, attended_grad, log_total, deltas, keys_all, values_all, own_member, member, usable
    )
    own_key_value = lax.psum_scatter(
        key_value_grad.astype(jnp.bfloat16), "shard", scatter_dimension=0, tiled=True
    ).astype(jnp.float32)
    mixed_grad = jnp.concatenate([query_grad, own_key_value], axis=1).astype(jnp.bfloat16)
    bias_query_grad = jnp.sum(mixed_grad[:, 0:model_width].astype(jnp.float32), axis=0)
    bias_value_grad = jnp.sum(
        mixed_grad[:, 2 * model_width : 3 * model_width].astype(jnp.float32), axis=0
    )
    entry_grad = inner_rows(flat, mixed_grad)
    hidden_grad = resid_one + times_trans(mixed_grad, entry)
    vector_grad = jnp.concatenate(
        [
            bias_query_grad,
            bias_value_grad,
            bias_out_grad,
            gain_one_grad,
            shift_one_grad,
            bias_down_grad,
            gain_two_grad,
            shift_two_grad,
            bias_up_grad,
        ]
    )
    return (hidden_grad, (entry_grad, exit_grad, expand_grad, shrink_grad, vector_grad))


def body(
    inputs,
    cotangent,
    lengths,
    dealing,
    key_mask,
    entry_weight,
    exit_weight,
    expand_weight,
    shrink_weight,
    vectors,
):
    local_rows = inputs.shape[0]
    group_rows = local_rows * lax.axis_size("shard")
    position = lax.axis_index("shard") * local_rows
    dealt_all, mask_all = (
        lax.all_gather(dealing, "shard", axis=1, tiled=True),
        lax.all_gather(key_mask, "shard", axis=1, tiled=True),
    )
    member, leading = sequence_ids(lengths[0], group_rows)
    usable = (mask_all[0] == 1) | leading
    own_member = lax.dynamic_slice_in_dim(member, position, local_rows, 0)
    inverse = (
        jnp.zeros((group_rows,), jnp.int32)
        .at[dealt_all[0]]
        .set(jnp.arange(group_rows, dtype=jnp.int32))
    )
    own_inverse = lax.dynamic_slice_in_dim(inverse, position, local_rows, 0)
    inputs_all, cotangent_all = (
        lax.all_gather(inputs, "shard", axis=0, tiled=True),
        lax.all_gather(cotangent, "shard", axis=0, tiled=True),
    )
    hidden = jnp.take(inputs_all, dealing[0], axis=0).astype(jnp.float32)
    upstream = jnp.take(cotangent_all, dealing[0], axis=0).astype(jnp.float32)
    layers = entry_weight.shape[0]
    saved = []
    kept = []
    for layer_index in range(layers):
        weights = fetch_forward(
            entry_weight, exit_weight, expand_weight, shrink_weight, vectors, layer_index
        )
        kept.append(weights)
        hidden, record = layer_forward(hidden, weights, own_member, member, usable)
        saved.append(record)
    output_all = lax.all_gather(hidden.astype(jnp.bfloat16), "shard", axis=0, tiled=True)
    output = jnp.take(output_all, own_inverse, axis=0)
    hidden_grad = upstream
    layer_grads = [None] * layers
    for layer_index in reversed(range(layers)):
        weights = fetch_backward(
            entry_weight, exit_weight, expand_weight, shrink_weight, vectors, layer_index
        )
        record = saved[layer_index]
        keys_all, values_all = (
            lax.all_gather(record[2], "shard", axis=0, tiled=True),
            lax.all_gather(record[3], "shard", axis=0, tiled=True),
        )
        hidden_grad, local_grads = layer_backward(
            hidden_grad, weights, record, keys_all, values_all, own_member, member, usable
        )
        entry_local, exit_local, expand_local, shrink_local, vector_local = local_grads
        entry_part, exit_part, expand_part, shrink_part, vector_part = (
            lax.psum_scatter(
                entry_local.astype(jnp.bfloat16), "shard", scatter_dimension=0, tiled=True
            ).astype(jnp.float32),
            lax.psum_scatter(
                exit_local.astype(jnp.bfloat16), "shard", scatter_dimension=0, tiled=True
            ).astype(jnp.float32),
            lax.psum_scatter(
                expand_local.astype(jnp.bfloat16), "shard", scatter_dimension=0, tiled=True
            ).astype(jnp.float32),
            lax.psum_scatter(
                shrink_local.astype(jnp.bfloat16), "shard", scatter_dimension=0, tiled=True
            ).astype(jnp.float32),
            lax.psum_scatter(
                vector_local.astype(jnp.bfloat16), "shard", scatter_dimension=0, tiled=True
            ).astype(jnp.float32),
        )
        entry_part, exit_part, expand_part, shrink_part, vector_part = (
            lax.psum(entry_part.astype(jnp.bfloat16), "rep").astype(jnp.float32),
            lax.psum(exit_part.astype(jnp.bfloat16), "rep").astype(jnp.float32),
            lax.psum(expand_part.astype(jnp.bfloat16), "rep").astype(jnp.float32),
            lax.psum(shrink_part.astype(jnp.bfloat16), "rep").astype(jnp.float32),
            lax.psum(vector_part.astype(jnp.bfloat16), "rep").astype(jnp.float32),
        )
        layer_grads[layer_index] = (entry_part, exit_part, expand_part, shrink_part, vector_part)
    entry_grad = jnp.stack([item[0] for item in layer_grads])
    exit_grad = jnp.stack([item[1] for item in layer_grads])
    expand_grad = jnp.stack([item[2] for item in layer_grads])
    shrink_grad = jnp.stack([item[3] for item in layer_grads])
    vector_grad = jnp.stack([item[4] for item in layer_grads])
    grads_all = lax.all_gather(
        hidden_grad.astype(jnp.bfloat16), "shard", axis=0, tiled=True
    ).astype(hidden_grad.dtype)
    input_grad = jnp.take(grads_all, own_inverse, axis=0)
    return (output, input_grad, entry_grad, exit_grad, expand_grad, shrink_grad, vector_grad)


EDGE = (0, 1, 6, 7)
CORE = (2, 3, 4, 5)
ALL = tuple(range(8))
BOTH = ("rep", "shard")
UNIT = 24


def routes(rep_flip, shard_flip, shards):
    return [
        (rep * 8 + shard, (rep ^ rep_flip) * 8 + (shard ^ shard_flip))
        for rep in range(4)
        for shard in shards
    ]


TO_X = routes(1, 0, ALL)
TO_Y = routes(2, 0, ALL)
TO_TWIN = routes(0, 1, ALL)
TO_SIDE = routes(0, 2, ALL)
TO_MID = routes(0, 6, CORE)


def send(value, route):
    return lax.ppermute(value, BOTH, route)


def low(value):
    return value.astype(jnp.bfloat16)


def wide(value):
    return value.astype(jnp.float32)


VMEM = pl.BlockSpec(memory_space=pltpu.VMEM)
SMEM = pl.BlockSpec(memory_space=pltpu.SMEM)
LIMIT = pltpu.CompilerParams(vmem_limit_bytes=60 * 1024 * 1024)


def shaped(shape, kind=jnp.bfloat16):
    return jax.ShapeDtypeStruct(shape, kind)


def cost(micros):
    return pl.CostEstimate(
        flops=int(micros * 1e9), bytes_accessed=int(micros * 1e6), transcendentals=0
    )


def nt(left, right):
    return lax.dot_general(left, right, (((1,), (1,)), ((), ())), preferred_element_type=jnp.float32)


def nn(left, right):
    return lax.dot_general(left, right, (((1,), (0,)), ((), ())), preferred_element_type=jnp.float32)


def fixed(*shape):
    return pl.BlockSpec(shape, lambda step: (0,) * len(shape))


def gather_kernel(ids_ref, want_ref, *refs):
    out_ref = refs[-1]
    want = want_ref[...]
    total = None
    index = 0
    for piece_ref in refs[:-1]:
        for slot in range(piece_ref.shape[0]):
            ids = ids_ref[index]
            hit = low(wide(want == ids))
            part = nn(hit, piece_ref[slot, 0 : ids.shape[1], :])
            total = part if total is None else total + part
            index += 1
    out_ref[...] = low(total)


def gather_rows(pieces, ids, want):
    return pl.pallas_call(
        gather_kernel,
        out_shape=shaped((want.shape[0], pieces[0].shape[2])),
        in_specs=[VMEM] * (2 + len(pieces)),
        out_specs=VMEM,
        compiler_params=LIMIT,
        cost_estimate=cost(5),
        name="gather_rows",
    )(ids, want, *pieces)


def assemble_kernel(where_ref, *refs):
    out_ref = refs[10]
    depth, rep, twin = where_ref[0], where_ref[1], where_ref[2]
    for side in range(2):
        own, first, over_x, over_y, over_d = refs[side * 5 : side * 5 + 5]
        core = twin ^ side
        for row in range(4):
            out_ref[depth, core, row] = own[row]
        for slot, flip in enumerate((1, 3, 2)):
            level = depth ^ flip
            for piece, bits in ((first, 0), (over_x, 1), (over_y, 2), (over_d, 3)):
                out_ref[level, core, rep ^ bits] = piece[slot]


def assemble(where, parts, start, by_rows):
    def part_spec(part):
        return pl.BlockSpec(
            (part.shape[0], None) + part.shape[2:],
            lambda unit, where_ref: (0, start + unit, 0, 0),
        )

    width = parts[0].shape[3]
    if by_rows:
        shape = (4, 2, 4, 4, UNIT, width)
        spec = pl.BlockSpec(
            (4, 2, 4, None, UNIT, width), lambda unit, where_ref: (0, 0, 0, unit, 0, 0)
        )
    else:
        shape = (4, 4, 2, 4, UNIT, width)
        spec = pl.BlockSpec(
            (None, 4, 2, 4, UNIT, width), lambda unit, where_ref: (unit, 0, 0, 0, 0, 0)
        )
    result = pl.pallas_call(
        assemble_kernel,
        grid_spec=pltpu.PrefetchScalarGridSpec(
            num_scalar_prefetch=1,
            grid=(4,),
            in_specs=[part_spec(part) for part in parts],
            out_specs=spec,
        ),
        out_shape=shaped(shape),
        compiler_params=LIMIT,
        cost_estimate=cost(6),
        name="assemble",
    )(where, *parts)
    return result.reshape(4, 32 * UNIT, width)


def tie(value, *others):
    return lax.optimization_barrier((value,) + others)[0]


def spread(own, first, over_x, over_y, x_last):
    over_d = send(over_y, TO_X) if x_last else send(over_x, TO_Y)
    mine = (own, first, over_x, over_y, over_d)
    return mine + tuple(send(item, TO_TWIN) for item in mine)


def project_kernel(h_ref, w_ref, vec_ref, sel_ref, q_ref, kv_ref, mine_ref, theirs_ref):
    unit = pl.program_id(0)
    product = nn(h_ref[...], w_ref[...])

    @pl.when(unit == 0)
    def _():
        q_ref[...] = low(product + vec_ref[0:1, :])
        mine_ref[...] = low(nn(h_ref[...], sel_ref[0]))
        theirs_ref[...] = low(nn(h_ref[...], sel_ref[1]))

    @pl.when(unit == 1)
    def _():
        kv_ref[...] = low(product)

    @pl.when(unit == 2)
    def _():
        kv_ref[...] = low(product + vec_ref[1:2, :])


def project(hidden, weight, vec, sel):
    rows, width = hidden.shape
    return pl.pallas_call(
        project_kernel,
        grid=(3,),
        in_specs=[
            fixed(rows, width),
            pl.BlockSpec((None, width, width), lambda unit: (unit, 0, 0)),
            fixed(12, width),
            fixed(2, width, width // 2),
        ],
        out_specs=[
            fixed(rows, width),
            pl.BlockSpec((None, rows, width), lambda unit: (jnp.maximum(unit - 1, 0), 0, 0)),
            fixed(rows, width // 2),
            fixed(rows, width // 2),
        ],
        out_shape=[
            shaped((rows, width)),
            shaped((2, rows, width)),
            shaped((rows, width // 2)),
            shaped((rows, width // 2)),
        ],
        compiler_params=LIMIT,
        cost_estimate=cost(7),
        name="project",
    )(hidden, weight, vec, sel)


def attend_kernel(
    q_ref, ka_ref, kb_ref, va_ref, vb_ref, code_ref, member_ref, o_ref, ot_ref, lse_ref, bias_ref
):
    half = q_ref.shape[0]

    @pl.when(pl.program_id(0) == 0)
    def _():
        bias_ref[...] = jnp.where(code_ref[...] == member_ref[...], 0.0, NEG_FILL)

    q = q_ref[...] * jnp.bfloat16(HEAD_DIM ** (-0.5))
    lane = lax.broadcasted_iota(jnp.int32, q.shape, 1)
    keys = (ka_ref[...], kb_ref[...])
    values = (va_ref[...].T, vb_ref[...].T)
    outs = []
    for head in range(2):
        q_head = jnp.where((lane >= HEAD_DIM) == (head == 1), q, jnp.bfloat16(0))
        scores = [
            nt(keys[side], q_head) + bias_ref[side * half : (side + 1) * half, :]
            for side in range(2)
        ]
        top = jnp.maximum(
            jnp.max(scores[0], axis=0, keepdims=True), jnp.max(scores[1], axis=0, keepdims=True)
        )
        total = None
        mixed = None
        for side in range(2):
            expo = jnp.exp(scores[side] - top)
            part = jnp.sum(expo, axis=0, keepdims=True)
            value = values[side][head * HEAD_DIM : (head + 1) * HEAD_DIM, :]
            product = nn(value, low(expo))
            total = part if total is None else total + part
            mixed = product if mixed is None else mixed + product
        outs.append(mixed / total)
        lse_ref[head : head + 1, :] = top + jnp.log(total)
    joined = jnp.concatenate(outs, axis=0)
    ot_ref[...] = joined
    o_ref[...] = low(joined.T)


def pair_specs(half):
    column = pl.BlockSpec((half, 128), lambda pair: (0, pair))
    key = pl.BlockSpec((None, half, 128), lambda pair: (0, 0, pair))
    value = pl.BlockSpec((None, half, 128), lambda pair: (1, 0, pair))
    turned = pl.BlockSpec((128, half), lambda pair: (pair, 0))
    level = pl.BlockSpec((None, 2, half), lambda pair: (pair, 0, 0))
    return column, key, value, turned, level


def attend_fast(queries, kv, kv_twin, code, member):
    half, width = queries.shape
    column, key, value, turned, level = pair_specs(half)
    return pl.pallas_call(
        attend_kernel,
        grid=(width // 128,),
        in_specs=[column, key, key, value, value, fixed(2 * half, 1), fixed(1, half)],
        out_specs=[column, turned, level],
        out_shape=[
            shaped((half, width)),
            shaped((width, half), jnp.float32),
            shaped((width // 128, 2, half), jnp.float32),
        ],
        scratch_shapes=[pltpu.VMEM((2 * half, half), jnp.float32)],
        compiler_params=LIMIT,
        cost_estimate=cost(15),
        name="attend_forward",
    )(queries, kv, kv_twin, kv, kv_twin, code, member)


def attend_back_kernel(
    q_ref, g_ref, ka_ref, kb_ref, va_ref, vb_ref, ot_ref, lse_ref, code_ref, member_ref,
    dq_ref, own_ref, twin_ref, bias_ref,
):
    half = q_ref.shape[0]

    @pl.when(pl.program_id(0) == 0)
    def _():
        bias_ref[...] = jnp.where(code_ref[...] == member_ref[...], 0.0, NEG_FILL)

    scale = HEAD_DIM ** (-0.5)
    q = q_ref[...] * jnp.bfloat16(scale)
    grad = g_ref[...]
    lane = lax.broadcasted_iota(jnp.int32, q.shape, 1)
    keys = (ka_ref[...], kb_ref[...])
    turned = (keys[0].T, keys[1].T)
    values = (va_ref[...], vb_ref[...])
    product = ot_ref[...] * wide(grad).T
    key_sums = [None, None]
    value_sums = [None, None]
    query_parts = []
    for head in range(2):
        rows = slice(head * HEAD_DIM, (head + 1) * HEAD_DIM)
        chosen = (lane >= HEAD_DIM) == (head == 1)
        q_head = jnp.where(chosen, q, jnp.bfloat16(0))
        g_head = jnp.where(chosen, grad, jnp.bfloat16(0))
        delta = jnp.sum(product[rows, :], axis=0, keepdims=True)
        level = lse_ref[head : head + 1, :]
        query_sum = None
        for side in range(2):
            scores = nt(keys[side], q_head) + bias_ref[side * half : (side + 1) * half, :]
            prob = jnp.exp(scores - level)
            slope = nt(values[side], g_head)
            steep = low(prob * (slope - delta))
            value_part = nn(low(prob), g_head)
            key_part = nn(steep, q_head)
            query_part = nn(turned[side][rows, :], steep)
            value_sums[side] = value_part if head == 0 else value_sums[side] + value_part
            key_sums[side] = key_part if head == 0 else key_sums[side] + key_part
            query_sum = query_part if side == 0 else query_sum + query_part
        query_parts.append(query_sum * scale)
    dq_ref[...] = low(jnp.concatenate(query_parts, axis=0).T)
    own_ref[0] = key_sums[0]
    own_ref[1] = value_sums[0]
    twin_ref[0] = low(key_sums[1])
    twin_ref[1] = low(value_sums[1])


def attend_back_fast(queries, grad, kv, kv_twin, ot, lse, code, member):
    half, width = queries.shape
    column, key, value, turned, level = pair_specs(half)
    both = pl.BlockSpec((2, half, 128), lambda pair: (0, 0, pair))
    return pl.pallas_call(
        attend_back_kernel,
        grid=(width // 128,),
        in_specs=[column, column, key, key, value, value, turned, level]
        + [fixed(2 * half, 1), fixed(1, half)],
        out_specs=[column, both, both],
        out_shape=[
            shaped((half, width)),
            shaped((2, half, width), jnp.float32),
            shaped((2, half, width)),
        ],
        scratch_shapes=[pltpu.VMEM((2 * half, half), jnp.float32)],
        compiler_params=LIMIT,
        cost_estimate=cost(20),
        name="attend_backward",
    )(queries, grad, kv, kv_twin, kv, kv_twin, ot, lse, code, member)


def normal_parts(value):
    scaled = value * 0.7071067811865476
    size = jnp.abs(scaled)
    square = size * size
    t = 1.0 / (1.0 + 0.5 * size)
    series = 0.17087277
    for factor in (
        -0.82215223, 1.48851587, -1.13520398, 0.27886807, -0.18628806,
        0.09678418, 0.37409196, 1.00002368, -1.26551223,
    ):
        series = series * t + factor
    tail = 0.5 * t * jnp.exp(series - square)
    cumulative = jnp.where(value >= 0, 1.0 - tail, tail)
    density = 0.3989422804014327 * jnp.exp(-square)
    return cumulative, density


def row_norm(resid):
    offsets = resid - jnp.mean(resid, axis=-1, keepdims=True)
    spread_of = jnp.mean(offsets * offsets, axis=-1, keepdims=True)
    factor = lax.rsqrt(spread_of + 1e-05)
    return offsets * factor, factor


def post_kernel(
    where_ref, o_ref, h_ref, wo_ref, up_ref, down_ref, vec_ref, sel_ref,
    h_out, hl_out, n1_out, t1_out, n2_out, t2_out, slope_out, mine_out, theirs_out,
    y_ref, yl_ref, f_ref,
):
    step = pl.program_id(0)
    half_width = mine_out.shape[2]

    @pl.when(step == 0)
    def _():
        attended = o_ref[...]
        branch = nn(attended, wo_ref[...]) + vec_ref[2:3, :]
        normed, factor = row_norm(wide(h_ref[...]) + branch)
        middle = normed * vec_ref[3:4, :] + vec_ref[4:5, :]
        n1_out[...] = normed
        t1_out[...] = factor
        y_ref[...] = middle
        yl_ref[...] = low(middle)
        mine_out[4] = low(nn(yl_ref[...], sel_ref[0]))
        theirs_out[4] = low(nn(yl_ref[...], sel_ref[1]))
        mine_out[5] = low(nn(attended, sel_ref[0]))
        theirs_out[5] = low(nn(attended, sel_ref[1]))

    inner = nn(yl_ref[...], up_ref[...]) + vec_ref[pl.ds(8 + step, 1), :]
    cumulative, density = normal_parts(inner)
    slope_out[...] = low(cumulative + inner * density)
    active = low(inner * cumulative)
    first, second = active[:, :half_width], active[:, half_width:]
    swap = where_ref[2] == 1
    mine_out[step] = jnp.where(swap, second, first)
    theirs_out[step] = jnp.where(swap, first, second)
    part = nn(active, down_ref[...])

    @pl.when(step == 0)
    def _():
        f_ref[...] = part

    @pl.when(step > 0)
    def _():
        f_ref[...] += part

    @pl.when(step == 3)
    def _():
        normed, factor = row_norm(y_ref[...] + (f_ref[...] + vec_ref[5:6, :]))
        result = normed * vec_ref[6:7, :] + vec_ref[7:8, :]
        n2_out[...] = normed
        t2_out[...] = factor
        h_out[...] = result
        hl_out[...] = low(result)


def unit_spec(width, index):
    return pl.BlockSpec((None, width, width), lambda step: (index, 0, 0))


def step_spec(width):
    return pl.BlockSpec((None, width, width), lambda step: (step, 0, 0))


def column_spec(rows, width):
    return pl.BlockSpec((rows, width), lambda step: (0, step))


def post(where, attended, hidden, front, up, down, vec, sel):
    rows, width = attended.shape
    half = width // 2
    full = fixed(rows, width)
    thin = fixed(rows, 1)
    return pl.pallas_call(
        post_kernel,
        grid=(4,),
        in_specs=[
            SMEM, full, full, unit_spec(width, 3), step_spec(width), step_spec(width),
            fixed(12, width), fixed(2, width, half),
        ],
        out_specs=[full, full, full, thin, full, thin, column_spec(rows, width)]
        + [fixed(6, rows, half)] * 2,
        out_shape=[
            shaped((rows, width), jnp.float32),
            shaped((rows, width)),
            shaped((rows, width), jnp.float32),
            shaped((rows, 1), jnp.float32),
            shaped((rows, width), jnp.float32),
            shaped((rows, 1), jnp.float32),
            shaped((rows, 4 * width)),
        ]
        + [shaped((6, rows, half))] * 2,
        scratch_shapes=[
            pltpu.VMEM((rows, width), jnp.float32),
            pltpu.VMEM((rows, width), jnp.bfloat16),
            pltpu.VMEM((rows, width), jnp.float32),
        ],
        compiler_params=LIMIT,
        cost_estimate=cost(23),
        name="post",
    )(where, attended, hidden, front, up, down, vec, sel)


def norm_back(incoming, normed, factor, gain):
    scaled = incoming * gain
    return factor * (
        scaled
        - jnp.mean(scaled, axis=-1, keepdims=True)
        - normed * jnp.mean(scaled * normed, axis=-1, keepdims=True)
    )


def column_sum(value):
    return jnp.sum(value, axis=0, keepdims=True)


def post_back_kernel(
    e_ref, n1_ref, t1_ref, n2_ref, t2_ref, slope_ref, wo_ref, up_ref, down_ref, vec_ref,
    all_out, do_out, dr_out, sums_out,
    r_ref, y_ref,
):
    step = pl.program_id(0)

    @pl.when(step == 0)
    def _():
        incoming = wide(e_ref[...])
        normed = n2_ref[...]
        resid = norm_back(incoming, normed, t2_ref[...], vec_ref[6:7, :])
        r_ref[...] = resid
        rounded = low(resid)
        all_out[4] = rounded
        sums_out[0:2, :] = jnp.zeros((2, sums_out.shape[1]), jnp.float32)
        sums_out[5:6, :] = column_sum(wide(rounded))
        sums_out[6:7, :] = column_sum(incoming * normed)
        sums_out[7:8, :] = column_sum(incoming)

    steep = low(nt(all_out[4], down_ref[...]) * wide(slope_ref[...]))
    all_out[step] = steep
    sums_out[pl.ds(8 + step, 1), :] = column_sum(wide(steep))
    part = nt(steep, up_ref[...])

    @pl.when(step == 0)
    def _():
        y_ref[...] = part

    @pl.when(step > 0)
    def _():
        y_ref[...] += part

    @pl.when(step == 3)
    def _():
        incoming = r_ref[...] + y_ref[...]
        normed = n1_ref[...]
        resid = norm_back(incoming, normed, t1_ref[...], vec_ref[3:4, :])
        dr_out[...] = resid
        rounded = low(resid)
        all_out[5] = rounded
        do_out[...] = low(nt(rounded, wo_ref[...]))
        sums_out[2:3, :] = column_sum(wide(rounded))
        sums_out[3:4, :] = column_sum(incoming * normed)
        sums_out[4:5, :] = column_sum(incoming)


def post_back(upstream, n1, t1, n2, t2, slope, front, up, down, vec):
    rows, width = upstream.shape
    full = fixed(rows, width)
    thin = fixed(rows, 1)
    return pl.pallas_call(
        post_back_kernel,
        grid=(4,),
        in_specs=[
            full, full, thin, full, thin, column_spec(rows, width),
            unit_spec(width, 3), step_spec(width), step_spec(width), fixed(12, width),
        ],
        out_specs=[fixed(6, rows, width), full, full, fixed(12, width)],
        out_shape=[
            shaped((6, rows, width)),
            shaped((rows, width)),
            shaped((rows, width), jnp.float32),
            shaped((12, width), jnp.float32),
        ],
        scratch_shapes=[
            pltpu.VMEM((rows, width), jnp.float32),
            pltpu.VMEM((rows, width), jnp.float32),
        ],
        compiler_params=LIMIT,
        cost_estimate=cost(16),
        name="post_back",
    )(upstream, n1, t1, n2, t2, slope, front, up, down, vec)


def project_back_kernel(
    dq_ref, own_ref, got_ref, w_ref, dr_ref, dm_out, dx_out, dxl_out, sums_out
):
    unit = pl.program_id(0)

    @pl.when(unit == 0)
    def _():
        dm_out[...] = dq_ref[...]

    @pl.when(unit > 0)
    def _():
        dm_out[...] = low(own_ref[...] + wide(got_ref[...]))

    grad = dm_out[...]
    part = nt(grad, w_ref[...])
    total = column_sum(wide(grad))

    @pl.when(unit == 0)
    def _():
        dx_out[...] = dr_ref[...] + part
        sums_out[0:1, :] = total

    @pl.when(unit > 0)
    def _():
        dx_out[...] += part
        sums_out[1:2, :] = total

    @pl.when(unit == 2)
    def _():
        dxl_out[...] = low(dx_out[...])


def project_back(dq, own, got, front, dr):
    rows, width = dq.shape
    full = fixed(rows, width)
    late = pl.BlockSpec((None, rows, width), lambda unit: (jnp.maximum(unit - 1, 0), 0, 0))
    return pl.pallas_call(
        project_back_kernel,
        grid=(3,),
        in_specs=[full, late, late, step_spec(width), full],
        out_specs=[
            pl.BlockSpec((None, rows, width), lambda unit: (unit, 0, 0)),
            full, full, fixed(2, width),
        ],
        out_shape=[
            shaped((3, rows, width)),
            shaped((rows, width), jnp.float32),
            shaped((rows, width)),
            shaped((2, width), jnp.float32),
        ],
        compiler_params=LIMIT,
        cost_estimate=cost(9),
        name="project_back",
    )(dq, own, got, front, dr)


def tn(left, right):
    return nn(left.T, right)


def split_store(keep_ref, give_ref, bit, x_first, piece_of, store):
    for other in range(2):
        pair = []
        for side in range(2):
            rep = (other * 2 + side) if x_first else (side * 2 + other)
            pair.append(low(piece_of(rep)))
        store(keep_ref, other, jnp.where(bit == 0, pair[0], pair[1]))
        store(give_ref, other, jnp.where(bit == 0, pair[1], pair[0]))


def column_store(ref_pair, bit, x_first, product, unit):
    keep_ref, give_ref = ref_pair
    for level in range(4):
        base = level * 4 * UNIT

        def piece_of(rep):
            return product[base + rep * UNIT : base + (rep + 1) * UNIT, :]

        def store(ref, other, value):
            ref[level, other, unit] = value

        split_store(keep_ref, give_ref, bit, x_first, piece_of, store)


def front_grad_kernel(
    x_first, bit_ref, xm_ref, xt_ref, om_ref, ot_ref, dm_ref, dmt_ref, da_ref, dat_ref,
    keep_ref, give_ref,
):
    unit = pl.program_id(0)
    bit = bit_ref[0 if x_first else 1]

    @pl.when(unit < 3)
    def _():
        product = tn(xm_ref[...], dm_ref[...]) + tn(xt_ref[...], dmt_ref[...])
        column_store((keep_ref, give_ref), bit, x_first, product, unit)

    @pl.when(unit == 3)
    def _():
        product = tn(om_ref[...], da_ref[...]) + tn(ot_ref[...], dat_ref[...])
        column_store((keep_ref, give_ref), bit, x_first, product, unit)


def block_spec(rows, width, index):
    return pl.BlockSpec((None, rows, width), lambda step: (index, 0, 0))


def front_grad(x_first, bits, xm, xt, mine, theirs, dm, dmt, da, dat):
    rows, half = xm.shape
    width = da.shape[2]
    late = pl.BlockSpec((None, rows, width), lambda unit: (jnp.minimum(unit, 2), 0, 0))
    shape = (4, 2, 4, UNIT, width)
    return pl.pallas_call(
        functools.partial(front_grad_kernel, x_first),
        grid=(4,),
        in_specs=[SMEM, fixed(rows, half), fixed(rows, half)]
        + [block_spec(rows, half, 5)] * 2
        + [late, late]
        + [block_spec(rows, width, 5)] * 2,
        out_specs=[fixed(*shape)] * 2,
        out_shape=[shaped(shape)] * 2,
        compiler_params=LIMIT,
        cost_estimate=cost(7),
        name="front_grad",
    )(bits, xm, xt, mine, theirs, dm, dmt, da, dat)


def feed_grad_kernel(
    x_first, bit_ref, ym_ref, yt_ref, gm_ref, gt_ref, dz_ref, dzt_ref, df_ref, dft_ref,
    keep_up, give_up, keep_down, give_down,
):
    step = pl.program_id(0)
    up_bit = bit_ref[0 if x_first else 1]
    down_bit = bit_ref[1 if x_first else 0]

    @pl.when(step < 4)
    def _():
        product = tn(ym_ref[...], dz_ref[...]) + tn(yt_ref[...], dzt_ref[...])
        column_store((keep_up, give_up), up_bit, x_first, product, step)

    @pl.when(step >= 4)
    def _():
        product = tn(gm_ref[...], df_ref[...]) + tn(gt_ref[...], dft_ref[...])
        for sub in range(4):

            def piece_of(rep):
                base = (rep * 4 + sub) * UNIT
                return product[base : base + UNIT, :]

            def store(ref, other, value):
                ref[step - 4, other, sub] = value

            split_store(keep_down, give_down, down_bit, not x_first, piece_of, store)


def feed_grad(x_first, bits, mine, theirs, slopes, slopes_twin):
    rows, half = mine.shape[1:]
    width = slopes.shape[2]
    early = pl.BlockSpec((None, rows, width), lambda step: (jnp.minimum(step, 3), 0, 0))
    late = pl.BlockSpec((None, rows, half), lambda step: (jnp.maximum(step - 4, 0), 0, 0))
    shape = (4, 2, 4, UNIT, width)
    return pl.pallas_call(
        functools.partial(feed_grad_kernel, x_first),
        grid=(8,),
        in_specs=[SMEM]
        + [block_spec(rows, half, 4)] * 2
        + [late, late, early, early]
        + [block_spec(rows, width, 4)] * 2,
        out_specs=[fixed(*shape)] * 4,
        out_shape=[shaped(shape)] * 4,
        compiler_params=LIMIT,
        cost_estimate=cost(12),
        name="feed_grad",
    )(bits, mine, theirs, mine, theirs, slopes, slopes_twin, slopes, slopes_twin)


class Reduction:
    def __init__(self, pairs, bits, is_low, is_core):
        self.streams = pairs
        self.bits, self.is_low, self.is_core = bits, is_low, is_core
        self.got = [
            send(give, TO_X if x_first else TO_Y) for keep, give, x_first in self.streams
        ]

    def across(self):
        stage = jnp.stack(
            [low(wide(item[0]) + wide(got)) for item, got in zip(self.streams, self.got)]
        )
        give = jnp.where(self.is_low, stage[:, 2:4], stage[:, 0:2])
        self.keep = jnp.where(self.is_low, stage[:, 0:2], stage[:, 2:4])
        self.mid = send(give, TO_MID)
        return self.keep

    def outward(self):
        stage = low(wide(self.keep) + wide(self.mid))
        outer = jnp.where(self.is_low, stage[:, 0], stage[:, 1])
        self.inner = jnp.where(self.is_low, stage[:, 1], stage[:, 0])
        self.side = send(outer, TO_SIDE)
        return self.inner

    def finish(self):
        stage = jnp.where(self.is_core, self.inner, self.side)
        results = []
        for index, (keep, give, x_first) in enumerate(self.streams):
            one, two = (TO_X, TO_Y) if x_first else (TO_Y, TO_X)
            piece = stage[index]
            piece = low(wide(piece) + wide(send(piece, two)))
            got = send(piece, one)
            axis = 1 if x_first else 0
            bit = self.bits[0] if x_first else self.bits[1]
            joined = jnp.where(
                bit == 0, jnp.stack([piece, got], axis), jnp.stack([got, piece], axis)
            )
            results.append(wide(joined).reshape((4,) + piece.shape[1:]))
        return results


def body_fast(
    inputs, cotangent, lengths, dealing, key_mask,
    entry_weight, exit_weight, expand_weight, shrink_weight, vectors,
):
    rows, width = inputs.shape
    layers = entry_weight.shape[0]
    group_rows = 8 * rows
    half_rows = group_rows // 2
    core_rows = half_rows // 2
    rep = lax.axis_index("rep")
    shard = lax.axis_index("shard")
    depth, twin = shard // 2, shard % 2
    is_low = depth <= 1
    is_core = (depth == 1) | (depth == 2)
    where = jnp.stack([depth, rep, twin]).astype(jnp.int32)
    bits = (rep & 1, rep >> 1)
    bit_words = jnp.stack(bits).astype(jnp.int32)

    def order(four):
        own, near, middle, far = four
        return jnp.where(
            is_low, jnp.stack([near, own, middle, far]), jnp.stack([far, middle, own, near])
        )

    def absolute(mine, theirs):
        one, two = order(mine), order(theirs)
        return jnp.where(twin == 0, jnp.stack([one, two], 1), jnp.stack([two, one], 1))

    def own_piece(pack):
        piece = lax.dynamic_index_in_dim(pack, rep, 0, keepdims=False)
        return piece.reshape(-1, width)

    def units_of(item):
        return item.reshape(-1, UNIT, width)

    def pack_front(entry, leaving):
        return jnp.concatenate([by_columns(entry), by_columns(leaving)], axis=1)

    def pack_feed(expand, shrink):
        return jnp.concatenate([by_columns(expand), low(shrink).reshape(4, 4, UNIT, width)], axis=1)

    def by_columns(weight):
        count = weight.shape[1] // width
        return low(weight).reshape(4, UNIT, count, width).transpose(0, 2, 1, 3)

    extra = layers * vectors.shape[1] // width
    tail = low(vectors).reshape(extra, width)
    table = jnp.concatenate([dealing // 64, dealing % 64, key_mask], axis=0)
    table = low(table).reshape(1, width)
    filler = jnp.zeros((7 - extra, width), jnp.bfloat16)
    rows_in = jnp.concatenate([inputs, tail, table, filler], axis=0)

    front_zero = pack_front(entry_weight[0], exit_weight[0])
    piece = own_piece(front_zero)
    near = send(piece, TO_SIDE)
    middle = send(piece, TO_MID)
    near_in = send(rows_in, TO_SIDE)
    middle_in = send(rows_in, TO_MID)
    far = send(near, TO_MID)
    far_in = send(near_in, TO_MID)
    first = jnp.stack([units_of(item) for item in (near, middle, far)])
    over_x, over_y = send(first, TO_X), send(first, TO_Y)
    parts = spread(front_zero, first, over_x, over_y, False)
    fronts = [assemble(where, parts, 0, False)]
    mine = jnp.stack([rows_in, near_in, middle_in, far_in])
    theirs = send(mine, TO_TWIN)

    expand_late, shrink_late = lax.optimization_barrier(
        (expand_weight[0], shrink_weight[0], near, middle)
    )[:2]
    feed_zero = pack_feed(expand_late, shrink_late)
    piece = own_piece(feed_zero)
    near = send(piece, TO_SIDE)
    middle = send(piece, TO_MID)
    far = send(near, TO_MID)
    first = jnp.stack([units_of(item) for item in (near, middle, far)])
    first = tie(first, over_x, over_y)
    over_x, over_y = send(first, TO_X), send(first, TO_Y)
    parts = spread(feed_zero, first, over_x, over_y, True)
    ups = [assemble(where, parts, 0, False)]
    downs = [assemble(where, parts, 4, True)]

    entry_late, exit_late, expand_late, shrink_late, cotangent_late = lax.optimization_barrier(
        (entry_weight[1], exit_weight[1], expand_weight[1], shrink_weight[1], cotangent, near, middle)
    )[:5]
    front_one = pack_front(entry_late, exit_late)
    feed_one = pack_feed(expand_late, shrink_late)
    piece = jnp.concatenate([own_piece(front_one), own_piece(feed_one), cotangent_late], axis=0)
    near = send(piece, TO_SIDE)
    four = (piece, near, send(piece, TO_MID), send(near, TO_MID))
    first_split, split = 4 * UNIT, 12 * UNIT
    first = jnp.stack([units_of(item[:first_split]) for item in four[1:]])
    first = tie(first, over_x, over_y)
    over_x, over_y = send(first, TO_X), send(first, TO_Y)
    parts = spread(front_one, first, over_x, over_y, True)
    fronts.append(assemble(where, parts, 0, False))
    first = jnp.stack([units_of(item[first_split:split]) for item in four[1:]])
    first = tie(first, over_x, over_y)
    over_x, over_y = send(first, TO_X), send(first, TO_Y)
    parts = spread(feed_one, first, over_x, over_y, False)
    ups.append(assemble(where, parts, 0, False))
    downs.append(assemble(where, parts, 4, True))
    cotangent_mine = jnp.stack([item[split:] for item in four])
    cotangent_theirs = send(cotangent_mine, TO_TWIN)

    header = absolute(tuple(mine[:, rows:]), tuple(theirs[:, rows:]))
    header = header.reshape(8, 8, width)
    vector_all = wide(header[:, :extra]).reshape(8, layers, vectors.shape[1])
    vector_all = jnp.transpose(vector_all, (1, 0, 2)).reshape(layers, 12, width)
    numbers = wide(header[:, extra]).reshape(8, 3, rows)
    dealt_all = (numbers[:, 0] * 64 + numbers[:, 1]).astype(jnp.int32).reshape(group_rows)
    mask_all = numbers[:, 2].reshape(group_rows)

    member, leading = sequence_ids(lengths[0], group_rows)
    usable = (mask_all == 1) | leading
    code = jnp.where(usable, member, -1)
    longest = jnp.argmax(lengths[0])
    begin = jnp.cumsum(lengths[0])[longest] - lengths[0][longest]
    spot = jnp.arange(half_rows, dtype=jnp.int32)

    def halve(values, low_side):
        inside = lax.dynamic_slice_in_dim(values, begin, half_rows, 0)
        outside = jnp.where(spot < begin, values[:half_rows], values[half_rows:])
        return jnp.where(low_side, inside, outside)

    def cores(values):
        own = lax.dynamic_slice_in_dim(values, twin * core_rows, core_rows, 0)
        other = lax.dynamic_slice_in_dim(values, (1 - twin) * core_rows, core_rows, 0)
        return own, other

    code_half = jnp.concatenate(cores(halve(code, is_low))).reshape(half_rows, 1)
    member_own = cores(halve(member, is_low))[0].reshape(1, core_rows)
    dealt_near = cores(halve(dealt_all, is_low))
    dealt_far = cores(halve(dealt_all, ~is_low))

    block = jnp.arange(width, dtype=jnp.int32)
    place = jnp.arange(width // 2, dtype=jnp.int32)
    chunk = 4 * UNIT
    source = (place // chunk) * (2 * chunk) + place % chunk
    cores_at = jnp.stack([twin, 1 - twin])
    sel = low(block[None, :, None] == (source[None, :] + cores_at[:, None] * chunk)[:, None, :])

    local = jnp.arange(rows, dtype=jnp.int32)
    bases = jnp.stack(
        [
            (depth ^ flip) * (2 * rows) + (twin ^ side) * rows
            for side in range(2)
            for flip in (0, 1, 3, 2)
        ]
    ).astype(jnp.int32)
    source_ids = (bases[:, None] + local[None, :]).reshape(8, 1, rows)
    want_in = dealt_near[0].reshape(core_rows, 1)
    hidden_low = gather_rows((mine, theirs), source_ids, want_in)
    upstream = gather_rows((cotangent_mine, cotangent_theirs), source_ids, want_in)

    result_ids = jnp.stack([dealt_near[0], dealt_far[0], dealt_near[1], dealt_far[1]]).reshape(
        4, 1, core_rows
    )
    want_out = jnp.concatenate([source_ids[0, 0], source_ids[1, 0]]).reshape(2 * rows, 1)

    def collect(value):
        pair = jnp.stack([value, send(value, TO_MID)])
        return pair, send(pair, TO_TWIN)

    def deliver(pair, other):
        found = gather_rows((pair, other), result_ids, want_out)
        outer = send(found[rows:], TO_SIDE)
        return found, jnp.where(is_core, found[:rows], outer)

    saved = []
    hidden = hidden_low
    for layer in range(layers):
        vec = vector_all[layer]
        queries, kv, xm, xt = project(hidden_low, fronts[layer], vec, sel)
        kv_twin = send(kv, TO_TWIN)
        xo = send(xt, TO_TWIN)
        attended, ot, lse = attend_fast(queries, kv, kv_twin, code_half, member_own)
        hidden, hidden_low, n1, t1, n2, t2, slope, mine, theirs = post(
            where, attended, hidden, fronts[layer], ups[layer], downs[layer], vec, sel
        )
        others = send(theirs, TO_TWIN)
        saved.append((queries, kv, kv_twin, ot, lse, n1, t1, n2, t2, slope, xm, xo, mine, others))
    results = collect(hidden_low)

    def start_back(layer, grad):
        n1, t1, n2, t2, slope = saved[layer][5:10]
        slopes, do, dr, sums = post_back(
            grad, n1, t1, n2, t2, slope,
            fronts[layer], ups[layer], downs[layer], vector_all[layer],
        )
        return slopes, send(slopes, TO_TWIN), do, dr, sums

    def attention_back(layer, do):
        queries, kv, kv_twin, ot, lse = saved[layer][:5]
        return attend_back_fast(queries, do, kv, kv_twin, ot, lse, code_half, member_own)

    def feed_part(layer, x_first, slopes, slopes_twin):
        mine, others = saved[layer][12:14]
        keep_up, give_up, keep_down, give_down = feed_grad(
            x_first, bit_words, mine, others, slopes, slopes_twin
        )
        work = Reduction(
            [(keep_up, give_up, x_first), (keep_down, give_down, not x_first)],
            bits, is_low, is_core,
        )
        return work, keep_up

    def front_part(layer, x_first, slopes, slopes_twin, dm, dm_twin):
        xm, xo, mine, others = saved[layer][10:14]
        keep, give = front_grad(
            x_first, bit_words, xm, xo, mine, others, dm, dm_twin, slopes, slopes_twin
        )
        return Reduction([(keep, give, x_first)], bits, is_low, is_core), keep

    upstream = tie(upstream, saved[0][11], saved[0][13])
    slopes_b, slopes_tb, do, dr, sums_b = start_back(1, upstream)
    do = tie(do, saved[1][11], saved[1][13])
    dq, own, give = attention_back(1, do)
    got = send(give, TO_TWIN)
    slopes_late = tie(slopes_tb, dq)
    feed_b, mark = feed_part(1, True, slopes_b, slopes_late)
    found, output = deliver(*tie(results, dq))
    dr = tie(dr, mark, found)
    dm_b, grad, _, head_b = project_back(dq, own, got, fronts[1], dr)
    dm_tb = send(dm_b, TO_TWIN)
    slopes_a, slopes_ta, do, dr, sums_a = start_back(0, grad)
    front_b, mark = front_part(1, True, slopes_b, slopes_tb, dm_b, tie(dm_tb, do))
    feed_a, mark = feed_part(0, False, slopes_a, tie(slopes_ta, mark))
    do = tie(do, mark, feed_b.across())
    dq, own, give = attention_back(0, do)
    got = send(give, TO_TWIN)
    dm_a, grad, grad_low, head_a = project_back(dq, own, got, fronts[0], dr)
    dm_ta = send(dm_a, TO_TWIN)
    dm_ta = tie(dm_ta, feed_b.outward(), front_b.across())
    front_a, mark = front_part(0, False, slopes_a, slopes_ta, dm_a, dm_ta)
    found, input_grad = deliver(*collect(grad_low))
    input_grad = wide(input_grad)
    feed_a.across()
    front_b.outward()
    feed_a.outward()
    front_a.across()
    front_a.outward()
    grads = []
    for front, feed, head_sums, sums in (
        (front_a, feed_a, head_a, sums_a),
        (front_b, feed_b, head_b, sums_b),
    ):
        up_grad, down_grad = feed.finish()
        vector = jnp.concatenate([head_sums, sums[2:]], axis=0)
        grads.append((front.finish()[0], up_grad, down_grad, vector))

    def columns(units):
        count = units.shape[1]
        return units.transpose(0, 2, 1, 3).reshape(4 * UNIT, count * width)

    entry_grad = jnp.stack([columns(item[0][:, 0:3]) for item in grads])
    exit_grad = jnp.stack([columns(item[0][:, 3:4]) for item in grads])
    expand_grad = jnp.stack([columns(item[1]) for item in grads])
    shrink_grad = jnp.stack([item[2].reshape(16 * UNIT, width) for item in grads])

    joined = jnp.stack([item[3].reshape(-1) for item in grads])
    joined = jnp.transpose(joined.reshape(layers, 4, 2, vectors.shape[1]), (1, 2, 0, 3))
    keep = lax.dynamic_index_in_dim(joined, twin, 1, keepdims=False)
    give = lax.dynamic_index_in_dim(joined, 1 - twin, 1, keepdims=False)
    stage = keep + send(give, TO_TWIN)
    stage = stage + send(stage, TO_X)
    stage = stage + send(stage, TO_Y)
    give = jnp.where(is_low, stage[2:4], stage[0:2])
    keep = jnp.where(is_low, stage[0:2], stage[2:4])
    stage = keep + send(give, TO_MID)
    outer = jnp.where(is_low, stage[0], stage[1])
    inner = jnp.where(is_low, stage[1], stage[0])
    vector_grad = jnp.where(is_core, inner, send(outer, TO_SIDE))
    return (output, input_grad, entry_grad, exit_grad, expand_grad, shrink_grad, vector_grad)


def solution(mesh):
    placed = (
        P(("rep", "shard"), None),
        P(("rep", "shard"), None),
        P("rep", None),
        P("rep", "shard"),
        P("rep", "shard"),
        P(None, "shard", None),
        P(None, "shard", None),
        P(None, "shard", None),
        P(None, "shard", None),
        P(None, "shard"),
    )
    small = dict(mesh.shape) == {"rep": 4, "shard": 8}
    return jax.shard_map(
        body_fast if small else body,
        mesh=mesh,
        in_specs=placed,
        out_specs=(
            P(("rep", "shard"), None),
            P(("rep", "shard"), None),
            P(None, "shard", None),
            P(None, "shard", None),
            P(None, "shard", None),
            P(None, "shard", None),
            P(None, "shard"),
        ),
        check_vma=False,
    )
```

```python
import functools

import jax
import jax.numpy as jnp
from jax import lax
from jax.experimental import pallas as pl
from jax.experimental.pallas import tpu as pltpu
from jax.sharding import PartitionSpec as P

HEADS = 12
HEAD_DIM = 64


NEG_FILL = -1e30


def norm_forward(resid, gain, shift):
    center = jnp.mean(resid, axis=-1, keepdims=True)
    offsets = resid - center
    spread = jnp.mean(offsets * offsets, axis=-1, keepdims=True)
    factor = lax.rsqrt(spread + 1e-05)
    normed = offsets * factor
    return (normed * gain + shift, normed, factor)


def norm_backward(incoming, normed, factor, gain):
    scaled = incoming * gain
    resid_grad = factor * (
        scaled
        - jnp.mean(scaled, axis=-1, keepdims=True)
        - normed * jnp.mean(scaled * normed, axis=-1, keepdims=True)
    )
    return (resid_grad, jnp.sum(incoming * normed, axis=0), jnp.sum(incoming, axis=0))


def inner_rows(left, right):
    return lax.dot_general(
        left, right, (((0,), (0,)), ((), ())), preferred_element_type=jnp.float32
    )


def times_trans(left, right):
    return lax.dot_general(
        left, right, (((1,), (1,)), ((), ())), preferred_element_type=jnp.float32
    )


def gelu_exact(value):
    return jax.nn.gelu(value, approximate=False)


def sequence_ids(lengths, group_rows):
    ending = jnp.cumsum(lengths)
    opening = ending - lengths
    places = jnp.arange(group_rows, dtype=jnp.int32)
    member = jnp.sum((places[:, None] >= ending[None, :]).astype(jnp.int32), axis=1)
    leading = jnp.any(places[:, None] == opening[None, :], axis=1)
    return (member, leading)


def split_vector(vector, model_width):
    pieces = [vector[index * model_width : (index + 1) * model_width] for index in range(8)]
    pieces.append(vector[8 * model_width :])
    return pieces


def fetch_forward(entry_weight, exit_weight, expand_weight, shrink_weight, vectors, layer_index):
    return (
        lax.all_gather(entry_weight[layer_index].astype(jnp.bfloat16), "shard", axis=0, tiled=True),
        lax.all_gather(exit_weight[layer_index].astype(jnp.bfloat16), "shard", axis=0, tiled=True),
        lax.all_gather(
            expand_weight[layer_index].astype(jnp.bfloat16), "shard", axis=0, tiled=True
        ),
        lax.all_gather(
            shrink_weight[layer_index].astype(jnp.bfloat16), "shard", axis=0, tiled=True
        ),
        lax.all_gather(vectors[layer_index].astype(jnp.bfloat16), "shard", axis=0, tiled=True),
    )


def fetch_backward(entry_weight, exit_weight, expand_weight, shrink_weight, vectors, layer_index):
    return (
        lax.all_gather(entry_weight[layer_index].astype(jnp.bfloat16), "shard", axis=0, tiled=True),
        lax.all_gather(exit_weight[layer_index].astype(jnp.bfloat16), "shard", axis=0, tiled=True),
        lax.all_gather(
            expand_weight[layer_index].astype(jnp.bfloat16), "shard", axis=0, tiled=True
        ),
        lax.all_gather(
            shrink_weight[layer_index].astype(jnp.bfloat16), "shard", axis=0, tiled=True
        ),
        lax.all_gather(vectors[layer_index].astype(jnp.bfloat16), "shard", axis=0, tiled=True),
    )


def attend_forward(queries, keys, values, own_member, member, usable):
    local_rows = queries.shape[0]
    query_heads = queries.reshape(local_rows, HEADS, HEAD_DIM)
    factor_scale = HEAD_DIM ** (-0.5)
    start_state = (
        jnp.full((HEADS, local_rows), NEG_FILL, jnp.float32),
        jnp.zeros((HEADS, local_rows), jnp.float32),
        jnp.zeros((HEADS, local_rows, HEAD_DIM), jnp.float32),
    )
    key_piece = lax.all_gather(keys, "shard", axis=0, tiled=True)
    value_piece = lax.all_gather(values, "shard", axis=0, tiled=True)
    amount = key_piece.shape[0]
    block_rows = local_rows * max(1, 512 // local_rows)

    def fold_advance(block_index, running):
        running_max, running_total, weighted = running
        begin = block_index * block_rows
        key_block = lax.dynamic_slice_in_dim(key_piece, begin, block_rows, 0).reshape(
            block_rows, HEADS, HEAD_DIM
        )
        value_block = lax.dynamic_slice_in_dim(value_piece, begin, block_rows, 0).reshape(
            block_rows, HEADS, HEAD_DIM
        )
        key_member = lax.dynamic_slice_in_dim(member, begin, block_rows, 0)
        key_usable = lax.dynamic_slice_in_dim(usable, begin, block_rows, 0)
        allowed = ((own_member[:, None] == key_member[None, :]) & key_usable[None, :])[None]
        scores = (
            jnp.einsum("qhd,khd->hqk", query_heads, key_block, preferred_element_type=jnp.float32)
            * factor_scale
        )
        scores = jnp.where(allowed, scores, NEG_FILL)
        new_max = jnp.maximum(running_max, jnp.max(scores, axis=2))
        expos = jnp.where(allowed, jnp.exp(scores - new_max[:, :, None]), 0.0)
        shrink_by = jnp.exp(running_max - new_max)
        new_total = running_total * shrink_by + jnp.sum(expos, axis=2)
        new_weighted = weighted * shrink_by[:, :, None] + jnp.einsum(
            "hqk,khd->hqd",
            expos.astype(jnp.bfloat16),
            value_block,
            preferred_element_type=jnp.float32,
        )
        return (new_max, new_total, new_weighted)

    running_max, running_total, weighted = lax.fori_loop(
        0, amount // block_rows, fold_advance, start_state
    )
    attended = jnp.transpose(weighted / running_total[:, :, None], (1, 0, 2)).reshape(
        local_rows, HEADS * HEAD_DIM
    )
    return (attended, running_max + jnp.log(running_total))


def attend_backward(
    queries, attended_grad, log_total, deltas, keys_all, values_all, own_member, member, usable
):
    local_rows = queries.shape[0]
    group_rows = keys_all.shape[0]
    model_width = HEADS * HEAD_DIM
    factor_scale = HEAD_DIM ** (-0.5)
    query_heads = queries.reshape(local_rows, HEADS, HEAD_DIM)
    grad_heads = attended_grad.reshape(local_rows, HEADS, HEAD_DIM)
    block_rows = min(512, group_rows)

    def attend_advance(query_sum, block_index):
        begin = block_index * block_rows
        key_block = lax.dynamic_slice_in_dim(keys_all, begin, block_rows, 0).reshape(
            block_rows, HEADS, HEAD_DIM
        )
        value_block = lax.dynamic_slice_in_dim(values_all, begin, block_rows, 0).reshape(
            block_rows, HEADS, HEAD_DIM
        )
        key_member = lax.dynamic_slice_in_dim(member, begin, block_rows, 0)
        key_usable = lax.dynamic_slice_in_dim(usable, begin, block_rows, 0)
        allowed = ((own_member[:, None] == key_member[None, :]) & key_usable[None, :])[None]
        scores = (
            jnp.einsum("qhd,khd->hqk", query_heads, key_block, preferred_element_type=jnp.float32)
            * factor_scale
        )
        probs = jnp.where(allowed, jnp.exp(scores - log_total[:, :, None]), 0.0)
        prob_grad = jnp.einsum(
            "qhd,khd->hqk", grad_heads, value_block, preferred_element_type=jnp.float32
        )
        score_grad = (probs * (prob_grad - deltas[:, :, None])).astype(jnp.bfloat16)
        query_sum = (
            query_sum
            + jnp.einsum("hqk,khd->qhd", score_grad, key_block, preferred_element_type=jnp.float32)
            * factor_scale
        )
        key_grad = (
            jnp.einsum("hqk,qhd->khd", score_grad, query_heads, preferred_element_type=jnp.float32)
            * factor_scale
        )
        value_grad = jnp.einsum(
            "hqk,qhd->khd",
            probs.astype(jnp.bfloat16),
            grad_heads,
            preferred_element_type=jnp.float32,
        )
        joined = jnp.concatenate(
            [
                key_grad.reshape(block_rows, model_width),
                value_grad.reshape(block_rows, model_width),
            ],
            axis=1,
        )
        return (query_sum, joined)

    query_sum, key_value = lax.scan(
        attend_advance,
        jnp.zeros((local_rows, HEADS, HEAD_DIM), jnp.float32),
        jnp.arange(group_rows // block_rows, dtype=jnp.int32),
    )
    key_value = key_value.reshape(group_rows, 2 * model_width)
    return (query_sum.reshape(local_rows, model_width), key_value)


def layer_forward(hidden, weights, own_member, member, usable):
    entry, leaving, expand, shrink, vector = weights
    model_width = leaving.shape[0]
    pieces = split_vector(vector.astype(jnp.float32), model_width)
    flat = hidden.astype(jnp.bfloat16)
    mixed = jnp.dot(flat, entry, preferred_element_type=jnp.float32)
    queries = (mixed[:, 0:model_width] + pieces[0]).astype(jnp.bfloat16)
    keys = mixed[:, model_width : 2 * model_width].astype(jnp.bfloat16)
    values = (mixed[:, 2 * model_width : 3 * model_width] + pieces[1]).astype(jnp.bfloat16)
    attended, log_total = attend_forward(queries, keys, values, own_member, member, usable)
    attended_low = attended.astype(jnp.bfloat16)
    branch = jnp.dot(attended_low, leaving, preferred_element_type=jnp.float32) + pieces[2]
    middle, normed_one, factor_one = norm_forward(hidden + branch, pieces[3], pieces[4])
    middle_low = middle.astype(jnp.bfloat16)
    inner = jnp.dot(middle_low, expand, preferred_element_type=jnp.float32) + pieces[8]
    active = gelu_exact(inner).astype(jnp.bfloat16)
    branch_two = jnp.dot(active, shrink, preferred_element_type=jnp.float32) + pieces[5]
    result, normed_two, factor_two = norm_forward(middle + branch_two, pieces[6], pieces[7])
    record = (
        flat,
        queries,
        keys,
        values,
        attended,
        log_total,
        attended_low,
        normed_one,
        factor_one,
        middle_low,
        inner,
        active,
        normed_two,
        factor_two,
    )
    return (result, record)


def layer_backward(upstream, weights, record, keys_all, values_all, own_member, member, usable):
    entry, leaving, expand, shrink, vector = weights
    model_width = leaving.shape[0]
    pieces = split_vector(vector.astype(jnp.float32), model_width)
    (
        flat,
        queries,
        keys,
        values,
        attended,
        log_total,
        attended_low,
        normed_one,
        factor_one,
        middle_low,
        inner,
        active,
        normed_two,
        factor_two,
    ) = record
    local_rows = queries.shape[0]
    resid_two, gain_two_grad, shift_two_grad = norm_backward(
        upstream, normed_two, factor_two, pieces[6]
    )
    branch_two_grad = resid_two.astype(jnp.bfloat16)
    bias_down_grad = jnp.sum(branch_two_grad.astype(jnp.float32), axis=0)
    shrink_grad = inner_rows(active, branch_two_grad)
    active_grad = times_trans(branch_two_grad, shrink)
    unused_value, gelu_pull = jax.vjp(gelu_exact, inner)
    inner_grad = gelu_pull(active_grad)[0].astype(jnp.bfloat16)
    bias_up_grad = jnp.sum(inner_grad.astype(jnp.float32), axis=0)
    expand_grad = inner_rows(middle_low, inner_grad)
    middle_grad = resid_two + times_trans(inner_grad, expand)
    resid_one, gain_one_grad, shift_one_grad = norm_backward(
        middle_grad, normed_one, factor_one, pieces[3]
    )
    branch_grad = resid_one.astype(jnp.bfloat16)
    bias_out_grad = jnp.sum(branch_grad.astype(jnp.float32), axis=0)
    exit_grad = inner_rows(attended_low, branch_grad)
    attended_grad = times_trans(branch_grad, leaving).astype(jnp.bfloat16)
    deltas = jnp.sum(
        (attended_grad.astype(jnp.float32) * attended).reshape(local_rows, HEADS, HEAD_DIM), axis=2
    ).T
    query_grad, key_value_grad = attend_backward(
        queries, attended_grad, log_total, deltas, keys_all, values_all, own_member, member, usable
    )
    own_key_value = lax.psum_scatter(
        key_value_grad.astype(jnp.bfloat16), "shard", scatter_dimension=0, tiled=True
    ).astype(jnp.float32)
    mixed_grad = jnp.concatenate([query_grad, own_key_value], axis=1).astype(jnp.bfloat16)
    bias_query_grad = jnp.sum(mixed_grad[:, 0:model_width].astype(jnp.float32), axis=0)
    bias_value_grad = jnp.sum(
        mixed_grad[:, 2 * model_width : 3 * model_width].astype(jnp.float32), axis=0
    )
    entry_grad = inner_rows(flat, mixed_grad)
    hidden_grad = resid_one + times_trans(mixed_grad, entry)
    vector_grad = jnp.concatenate(
        [
            bias_query_grad,
            bias_value_grad,
            bias_out_grad,
            gain_one_grad,
            shift_one_grad,
            bias_down_grad,
            gain_two_grad,
            shift_two_grad,
            bias_up_grad,
        ]
    )
    return (hidden_grad, (entry_grad, exit_grad, expand_grad, shrink_grad, vector_grad))


def body(
    inputs,
    cotangent,
    lengths,
    dealing,
    key_mask,
    entry_weight,
    exit_weight,
    expand_weight,
    shrink_weight,
    vectors,
):
    local_rows = inputs.shape[0]
    group_rows = local_rows * lax.axis_size("shard")
    position = lax.axis_index("shard") * local_rows
    dealt_all, mask_all = (
        lax.all_gather(dealing, "shard", axis=1, tiled=True),
        lax.all_gather(key_mask, "shard", axis=1, tiled=True),
    )
    member, leading = sequence_ids(lengths[0], group_rows)
    usable = (mask_all[0] == 1) | leading
    own_member = lax.dynamic_slice_in_dim(member, position, local_rows, 0)
    inverse = (
        jnp.zeros((group_rows,), jnp.int32)
        .at[dealt_all[0]]
        .set(jnp.arange(group_rows, dtype=jnp.int32))
    )
    own_inverse = lax.dynamic_slice_in_dim(inverse, position, local_rows, 0)
    inputs_all, cotangent_all = (
        lax.all_gather(inputs, "shard", axis=0, tiled=True),
        lax.all_gather(cotangent, "shard", axis=0, tiled=True),
    )
    hidden = jnp.take(inputs_all, dealing[0], axis=0).astype(jnp.float32)
    upstream = jnp.take(cotangent_all, dealing[0], axis=0).astype(jnp.float32)
    layers = entry_weight.shape[0]
    saved = []
    kept = []
    for layer_index in range(layers):
        weights = fetch_forward(
            entry_weight, exit_weight, expand_weight, shrink_weight, vectors, layer_index
        )
        kept.append(weights)
        hidden, record = layer_forward(hidden, weights, own_member, member, usable)
        saved.append(record)
    output_all = lax.all_gather(hidden.astype(jnp.bfloat16), "shard", axis=0, tiled=True)
    output = jnp.take(output_all, own_inverse, axis=0)
    hidden_grad = upstream
    layer_grads = [None] * layers
    for layer_index in reversed(range(layers)):
        weights = fetch_backward(
            entry_weight, exit_weight, expand_weight, shrink_weight, vectors, layer_index
        )
        record = saved[layer_index]
        keys_all, values_all = (
            lax.all_gather(record[2], "shard", axis=0, tiled=True),
            lax.all_gather(record[3], "shard", axis=0, tiled=True),
        )
        hidden_grad, local_grads = layer_backward(
            hidden_grad, weights, record, keys_all, values_all, own_member, member, usable
        )
        entry_local, exit_local, expand_local, shrink_local, vector_local = local_grads
        entry_part, exit_part, expand_part, shrink_part, vector_part = (
            lax.psum_scatter(
                entry_local.astype(jnp.bfloat16), "shard", scatter_dimension=0, tiled=True
            ).astype(jnp.float32),
            lax.psum_scatter(
                exit_local.astype(jnp.bfloat16), "shard", scatter_dimension=0, tiled=True
            ).astype(jnp.float32),
            lax.psum_scatter(
                expand_local.astype(jnp.bfloat16), "shard", scatter_dimension=0, tiled=True
            ).astype(jnp.float32),
            lax.psum_scatter(
                shrink_local.astype(jnp.bfloat16), "shard", scatter_dimension=0, tiled=True
            ).astype(jnp.float32),
            lax.psum_scatter(
                vector_local.astype(jnp.bfloat16), "shard", scatter_dimension=0, tiled=True
            ).astype(jnp.float32),
        )
        entry_part, exit_part, expand_part, shrink_part, vector_part = (
            lax.psum(entry_part.astype(jnp.bfloat16), "rep").astype(jnp.float32),
            lax.psum(exit_part.astype(jnp.bfloat16), "rep").astype(jnp.float32),
            lax.psum(expand_part.astype(jnp.bfloat16), "rep").astype(jnp.float32),
            lax.psum(shrink_part.astype(jnp.bfloat16), "rep").astype(jnp.float32),
            lax.psum(vector_part.astype(jnp.bfloat16), "rep").astype(jnp.float32),
        )
        layer_grads[layer_index] = (entry_part, exit_part, expand_part, shrink_part, vector_part)
    entry_grad = jnp.stack([item[0] for item in layer_grads])
    exit_grad = jnp.stack([item[1] for item in layer_grads])
    expand_grad = jnp.stack([item[2] for item in layer_grads])
    shrink_grad = jnp.stack([item[3] for item in layer_grads])
    vector_grad = jnp.stack([item[4] for item in layer_grads])
    grads_all = lax.all_gather(
        hidden_grad.astype(jnp.bfloat16), "shard", axis=0, tiled=True
    ).astype(hidden_grad.dtype)
    input_grad = jnp.take(grads_all, own_inverse, axis=0)
    return (output, input_grad, entry_grad, exit_grad, expand_grad, shrink_grad, vector_grad)


EDGE = (0, 1, 6, 7)
CORE = (2, 3, 4, 5)
ALL = tuple(range(8))
BOTH = ("rep", "shard")
UNIT = 24


def routes(rep_flip, shard_flip, shards):
    return [
        (rep * 8 + shard, (rep ^ rep_flip) * 8 + (shard ^ shard_flip))
        for rep in range(4)
        for shard in shards
    ]


TO_X = routes(1, 0, ALL)
TO_Y = routes(2, 0, ALL)
TO_TWIN = routes(0, 1, ALL)
TO_SIDE = routes(0, 2, ALL)
TO_MID = routes(0, 6, CORE)


def send(value, route):
    return lax.ppermute(value, BOTH, route)


def low(value):
    return value.astype(jnp.bfloat16)


def wide(value):
    return value.astype(jnp.float32)


VMEM = pl.BlockSpec(memory_space=pltpu.VMEM)
SMEM = pl.BlockSpec(memory_space=pltpu.SMEM)
LIMIT = pltpu.CompilerParams(vmem_limit_bytes=60 * 1024 * 1024)


def shaped(shape, kind=jnp.bfloat16):
    return jax.ShapeDtypeStruct(shape, kind)


def cost(micros):
    return pl.CostEstimate(
        flops=int(micros * 1e9), bytes_accessed=int(micros * 1e6), transcendentals=0
    )


def nt(left, right):
    return lax.dot_general(left, right, (((1,), (1,)), ((), ())), preferred_element_type=jnp.float32)


def nn(left, right):
    return lax.dot_general(left, right, (((1,), (0,)), ((), ())), preferred_element_type=jnp.float32)


def fixed(*shape):
    return pl.BlockSpec(shape, lambda step: (0,) * len(shape))


def gather_kernel(ids_ref, want_ref, *refs):
    out_ref = refs[-1]
    want = want_ref[...]
    total = None
    index = 0
    for piece_ref in refs[:-1]:
        for slot in range(piece_ref.shape[0]):
            ids = ids_ref[index]
            hit = low(wide(want == ids))
            part = nn(hit, piece_ref[slot, 0 : ids.shape[1], :])
            total = part if total is None else total + part
            index += 1
    out_ref[...] = low(total)


def gather_rows(pieces, ids, want, spend):
    return pl.pallas_call(
        gather_kernel,
        out_shape=shaped((want.shape[0], pieces[0].shape[2])),
        in_specs=[VMEM] * (2 + len(pieces)),
        out_specs=VMEM,
        compiler_params=LIMIT,
        cost_estimate=cost(spend),
        name="gather_rows",
    )(ids, want, *pieces)


def assemble_kernel(where_ref, *refs):
    out_ref = refs[10]
    depth, rep, twin = where_ref[0], where_ref[1], where_ref[2]
    for side in range(2):
        own, first, over_x, over_y, over_d = refs[side * 5 : side * 5 + 5]
        core = twin ^ side
        for row in range(4):
            out_ref[depth, core, row] = own[row]
        for slot, flip in enumerate((1, 3, 2)):
            level = depth ^ flip
            for piece, bits in ((first, 0), (over_x, 1), (over_y, 2), (over_d, 3)):
                out_ref[level, core, rep ^ bits] = piece[slot]


def assemble(where, parts, start, by_rows):
    def part_spec(part):
        return pl.BlockSpec(
            (part.shape[0], None) + part.shape[2:],
            lambda unit, where_ref: (0, start + unit, 0, 0),
        )

    width = parts[0].shape[3]
    if by_rows:
        shape = (4, 2, 4, 4, UNIT, width)
        spec = pl.BlockSpec(
            (4, 2, 4, None, UNIT, width), lambda unit, where_ref: (0, 0, 0, unit, 0, 0)
        )
    else:
        shape = (4, 4, 2, 4, UNIT, width)
        spec = pl.BlockSpec(
            (None, 4, 2, 4, UNIT, width), lambda unit, where_ref: (unit, 0, 0, 0, 0, 0)
        )
    result = pl.pallas_call(
        assemble_kernel,
        grid_spec=pltpu.PrefetchScalarGridSpec(
            num_scalar_prefetch=1,
            grid=(4,),
            in_specs=[part_spec(part) for part in parts],
            out_specs=spec,
        ),
        out_shape=shaped(shape),
        compiler_params=LIMIT,
        cost_estimate=cost(6),
        name="assemble",
    )(where, *parts)
    return result.reshape(4, 32 * UNIT, width)


def tie(value, *others):
    return lax.optimization_barrier((value,) + others)[0]


def after(values, *others):
    return list(lax.optimization_barrier(tuple(values) + others)[: len(values)])


def spread(own, first, over_x, over_y, x_last):
    others = [send(own, TO_TWIN), send(first, TO_TWIN)]
    over_x, over_y = after([over_x, over_y], *others)
    over_d = send(over_y, TO_X) if x_last else send(over_x, TO_Y)
    others += [send(over_x, TO_TWIN), send(over_y, TO_TWIN)]
    over_d = after([over_d], *others)[0]
    others.append(send(over_d, TO_TWIN))
    return (own, first, over_x, over_y, over_d) + tuple(others)


def project_kernel(h_ref, w_ref, vec_ref, sel_ref, q_ref, kv_ref, mine_ref, theirs_ref):
    unit = pl.program_id(0)
    product = nn(h_ref[...], w_ref[...])

    @pl.when(unit == 0)
    def _():
        q_ref[...] = low(product + vec_ref[0:1, :])
        mine_ref[...] = low(nn(h_ref[...], sel_ref[0]))
        theirs_ref[...] = low(nn(h_ref[...], sel_ref[1]))

    @pl.when(unit == 1)
    def _():
        kv_ref[...] = low(product)

    @pl.when(unit == 2)
    def _():
        kv_ref[...] = low(product + vec_ref[1:2, :])


def project(hidden, weight, vec, sel):
    rows, width = hidden.shape
    return pl.pallas_call(
        project_kernel,
        grid=(3,),
        in_specs=[
            fixed(rows, width),
            pl.BlockSpec((None, width, width), lambda unit: (unit, 0, 0)),
            fixed(12, width),
            fixed(2, width, width // 2),
        ],
        out_specs=[
            fixed(rows, width),
            pl.BlockSpec((None, rows, width), lambda unit: (jnp.maximum(unit - 1, 0), 0, 0)),
            fixed(rows, width // 2),
            fixed(rows, width // 2),
        ],
        out_shape=[
            shaped((rows, width)),
            shaped((2, rows, width)),
            shaped((rows, width // 2)),
            shaped((rows, width // 2)),
        ],
        compiler_params=LIMIT,
        cost_estimate=cost(7),
        name="project",
    )(hidden, weight, vec, sel)


def attend_kernel(
    q_ref, ka_ref, kb_ref, va_ref, vb_ref, code_ref, member_ref, o_ref, ot_ref, lse_ref, bias_ref
):
    half = q_ref.shape[0]

    @pl.when(pl.program_id(0) == 0)
    def _():
        bias_ref[...] = jnp.where(code_ref[...] == member_ref[...], 0.0, NEG_FILL)

    q = q_ref[...] * jnp.bfloat16(HEAD_DIM ** (-0.5))
    lane = lax.broadcasted_iota(jnp.int32, q.shape, 1)
    keys = (ka_ref[...], kb_ref[...])
    values = (va_ref[...].T, vb_ref[...].T)
    outs = []
    for head in range(2):
        q_head = jnp.where((lane >= HEAD_DIM) == (head == 1), q, jnp.bfloat16(0))
        scores = [
            nt(keys[side], q_head) + bias_ref[side * half : (side + 1) * half, :]
            for side in range(2)
        ]
        top = jnp.maximum(
            jnp.max(scores[0], axis=0, keepdims=True), jnp.max(scores[1], axis=0, keepdims=True)
        )
        total = None
        mixed = None
        for side in range(2):
            expo = jnp.exp(scores[side] - top)
            part = jnp.sum(expo, axis=0, keepdims=True)
            value = values[side][head * HEAD_DIM : (head + 1) * HEAD_DIM, :]
            product = nn(value, low(expo))
            total = part if total is None else total + part
            mixed = product if mixed is None else mixed + product
        outs.append(mixed / total)
        lse_ref[head : head + 1, :] = top + jnp.log(total)
    joined = jnp.concatenate(outs, axis=0)
    ot_ref[...] = joined
    o_ref[...] = low(joined.T)


def pair_specs(half):
    column = pl.BlockSpec((half, 128), lambda pair: (0, pair))
    key = pl.BlockSpec((None, half, 128), lambda pair: (0, 0, pair))
    value = pl.BlockSpec((None, half, 128), lambda pair: (1, 0, pair))
    turned = pl.BlockSpec((128, half), lambda pair: (pair, 0))
    level = pl.BlockSpec((None, 2, half), lambda pair: (pair, 0, 0))
    return column, key, value, turned, level


def attend_fast(queries, kv, kv_twin, code, member):
    half, width = queries.shape
    column, key, value, turned, level = pair_specs(half)
    return pl.pallas_call(
        attend_kernel,
        grid=(width // 128,),
        in_specs=[column, key, key, value, value, fixed(2 * half, 1), fixed(1, half)],
        out_specs=[column, turned, level],
        out_shape=[
            shaped((half, width)),
            shaped((width, half), jnp.float32),
            shaped((width // 128, 2, half), jnp.float32),
        ],
        scratch_shapes=[pltpu.VMEM((2 * half, half), jnp.float32)],
        compiler_params=LIMIT,
        cost_estimate=cost(15),
        name="attend_forward",
    )(queries, kv, kv_twin, kv, kv_twin, code, member)


def attend_back_kernel(
    q_ref, g_ref, ka_ref, kb_ref, va_ref, vb_ref, ot_ref, lse_ref, code_ref, member_ref,
    dq_ref, own_ref, twin_ref, bias_ref,
):
    half = q_ref.shape[0]

    @pl.when(pl.program_id(0) == 0)
    def _():
        bias_ref[...] = jnp.where(code_ref[...] == member_ref[...], 0.0, NEG_FILL)

    scale = HEAD_DIM ** (-0.5)
    q = q_ref[...] * jnp.bfloat16(scale)
    grad = g_ref[...]
    lane = lax.broadcasted_iota(jnp.int32, q.shape, 1)
    keys = (ka_ref[...], kb_ref[...])
    turned = (keys[0].T, keys[1].T)
    values = (va_ref[...], vb_ref[...])
    product = ot_ref[...] * wide(grad).T
    key_sums = [None, None]
    value_sums = [None, None]
    query_parts = []
    for head in range(2):
        rows = slice(head * HEAD_DIM, (head + 1) * HEAD_DIM)
        chosen = (lane >= HEAD_DIM) == (head == 1)
        q_head = jnp.where(chosen, q, jnp.bfloat16(0))
        g_head = jnp.where(chosen, grad, jnp.bfloat16(0))
        delta = jnp.sum(product[rows, :], axis=0, keepdims=True)
        level = lse_ref[head : head + 1, :]
        query_sum = None
        for side in range(2):
            scores = nt(keys[side], q_head) + bias_ref[side * half : (side + 1) * half, :]
            prob = jnp.exp(scores - level)
            slope = nt(values[side], g_head)
            steep = low(prob * (slope - delta))
            value_part = nn(low(prob), g_head)
            key_part = nn(steep, q_head)
            query_part = nn(turned[side][rows, :], steep)
            value_sums[side] = value_part if head == 0 else value_sums[side] + value_part
            key_sums[side] = key_part if head == 0 else key_sums[side] + key_part
            query_sum = query_part if side == 0 else query_sum + query_part
        query_parts.append(query_sum * scale)
    dq_ref[...] = low(jnp.concatenate(query_parts, axis=0).T)
    own_ref[0] = key_sums[0]
    own_ref[1] = value_sums[0]
    twin_ref[0] = low(key_sums[1])
    twin_ref[1] = low(value_sums[1])


def attend_back_fast(queries, grad, kv, kv_twin, ot, lse, code, member, spend):
    half, width = queries.shape
    column, key, value, turned, level = pair_specs(half)
    both = pl.BlockSpec((2, half, 128), lambda pair: (0, 0, pair))
    return pl.pallas_call(
        attend_back_kernel,
        grid=(width // 128,),
        in_specs=[column, column, key, key, value, value, turned, level]
        + [fixed(2 * half, 1), fixed(1, half)],
        out_specs=[column, both, both],
        out_shape=[
            shaped((half, width)),
            shaped((2, half, width), jnp.float32),
            shaped((2, half, width)),
        ],
        scratch_shapes=[pltpu.VMEM((2 * half, half), jnp.float32)],
        compiler_params=LIMIT,
        cost_estimate=cost(spend),
        name="attend_backward",
    )(queries, grad, kv, kv_twin, kv, kv_twin, ot, lse, code, member)


def normal_parts(value):
    scaled = value * 0.7071067811865476
    size = jnp.abs(scaled)
    square = size * size
    t = 1.0 / (1.0 + 0.5 * size)
    series = 0.17087277
    for factor in (
        -0.82215223, 1.48851587, -1.13520398, 0.27886807, -0.18628806,
        0.09678418, 0.37409196, 1.00002368, -1.26551223,
    ):
        series = series * t + factor
    tail = 0.5 * t * jnp.exp(series - square)
    cumulative = jnp.where(value >= 0, 1.0 - tail, tail)
    density = 0.3989422804014327 * jnp.exp(-square)
    return cumulative, density


def row_norm(resid):
    offsets = resid - jnp.mean(resid, axis=-1, keepdims=True)
    spread_of = jnp.mean(offsets * offsets, axis=-1, keepdims=True)
    factor = lax.rsqrt(spread_of + 1e-05)
    return offsets * factor, factor


def post_kernel(
    where_ref, o_ref, h_ref, wo_ref, up_ref, down_ref, vec_ref, sel_ref,
    h_out, hl_out, n1_out, t1_out, n2_out, t2_out, slope_out, mine_out, theirs_out,
    y_ref, yl_ref, f_ref,
):
    step = pl.program_id(0)
    half_width = mine_out.shape[2]

    @pl.when(step == 0)
    def _():
        attended = o_ref[...]
        branch = nn(attended, wo_ref[...]) + vec_ref[2:3, :]
        normed, factor = row_norm(wide(h_ref[...]) + branch)
        middle = normed * vec_ref[3:4, :] + vec_ref[4:5, :]
        n1_out[...] = normed
        t1_out[...] = factor
        y_ref[...] = middle
        yl_ref[...] = low(middle)
        mine_out[4] = low(nn(yl_ref[...], sel_ref[0]))
        theirs_out[4] = low(nn(yl_ref[...], sel_ref[1]))
        mine_out[5] = low(nn(attended, sel_ref[0]))
        theirs_out[5] = low(nn(attended, sel_ref[1]))

    inner = nn(yl_ref[...], up_ref[...]) + vec_ref[pl.ds(8 + step, 1), :]
    cumulative, density = normal_parts(inner)
    slope_out[...] = low(cumulative + inner * density)
    active = low(inner * cumulative)
    first, second = active[:, :half_width], active[:, half_width:]
    swap = where_ref[2] == 1
    mine_out[step] = jnp.where(swap, second, first)
    theirs_out[step] = jnp.where(swap, first, second)
    part = nn(active, down_ref[...])

    @pl.when(step == 0)
    def _():
        f_ref[...] = part

    @pl.when(step > 0)
    def _():
        f_ref[...] += part

    @pl.when(step == 3)
    def _():
        normed, factor = row_norm(y_ref[...] + (f_ref[...] + vec_ref[5:6, :]))
        result = normed * vec_ref[6:7, :] + vec_ref[7:8, :]
        n2_out[...] = normed
        t2_out[...] = factor
        h_out[...] = result
        hl_out[...] = low(result)


def unit_spec(width, index):
    return pl.BlockSpec((None, width, width), lambda step: (index, 0, 0))


def step_spec(width):
    return pl.BlockSpec((None, width, width), lambda step: (step, 0, 0))


def column_spec(rows, width):
    return pl.BlockSpec((rows, width), lambda step: (0, step))


def post(where, attended, hidden, front, up, down, vec, sel):
    rows, width = attended.shape
    half = width // 2
    full = fixed(rows, width)
    thin = fixed(rows, 1)
    return pl.pallas_call(
        post_kernel,
        grid=(4,),
        in_specs=[
            SMEM, full, full, unit_spec(width, 3), step_spec(width), step_spec(width),
            fixed(12, width), fixed(2, width, half),
        ],
        out_specs=[full, full, full, thin, full, thin, column_spec(rows, width)]
        + [fixed(6, rows, half)] * 2,
        out_shape=[
            shaped((rows, width), jnp.float32),
            shaped((rows, width)),
            shaped((rows, width), jnp.float32),
            shaped((rows, 1), jnp.float32),
            shaped((rows, width), jnp.float32),
            shaped((rows, 1), jnp.float32),
            shaped((rows, 4 * width)),
        ]
        + [shaped((6, rows, half))] * 2,
        scratch_shapes=[
            pltpu.VMEM((rows, width), jnp.float32),
            pltpu.VMEM((rows, width), jnp.bfloat16),
            pltpu.VMEM((rows, width), jnp.float32),
        ],
        compiler_params=LIMIT,
        cost_estimate=cost(23),
        name="post",
    )(where, attended, hidden, front, up, down, vec, sel)


def norm_back(incoming, normed, factor, gain):
    scaled = incoming * gain
    return factor * (
        scaled
        - jnp.mean(scaled, axis=-1, keepdims=True)
        - normed * jnp.mean(scaled * normed, axis=-1, keepdims=True)
    )


def column_sum(value):
    return jnp.sum(value, axis=0, keepdims=True)


def post_back_kernel(
    e_ref, n1_ref, t1_ref, n2_ref, t2_ref, slope_ref, wo_ref, up_ref, down_ref, vec_ref,
    all_out, do_out, dr_out, sums_out,
    r_ref, y_ref,
):
    step = pl.program_id(0)

    @pl.when(step == 0)
    def _():
        incoming = wide(e_ref[...])
        normed = n2_ref[...]
        resid = norm_back(incoming, normed, t2_ref[...], vec_ref[6:7, :])
        r_ref[...] = resid
        rounded = low(resid)
        all_out[4] = rounded
        sums_out[0:2, :] = jnp.zeros((2, sums_out.shape[1]), jnp.float32)
        sums_out[5:6, :] = column_sum(wide(rounded))
        sums_out[6:7, :] = column_sum(incoming * normed)
        sums_out[7:8, :] = column_sum(incoming)

    steep = low(nt(all_out[4], down_ref[...]) * wide(slope_ref[...]))
    all_out[step] = steep
    sums_out[pl.ds(8 + step, 1), :] = column_sum(wide(steep))
    part = nt(steep, up_ref[...])

    @pl.when(step == 0)
    def _():
        y_ref[...] = part

    @pl.when(step > 0)
    def _():
        y_ref[...] += part

    @pl.when(step == 3)
    def _():
        incoming = r_ref[...] + y_ref[...]
        normed = n1_ref[...]
        resid = norm_back(incoming, normed, t1_ref[...], vec_ref[3:4, :])
        dr_out[...] = resid
        rounded = low(resid)
        all_out[5] = rounded
        do_out[...] = low(nt(rounded, wo_ref[...]))
        sums_out[2:3, :] = column_sum(wide(rounded))
        sums_out[3:4, :] = column_sum(incoming * normed)
        sums_out[4:5, :] = column_sum(incoming)


def post_back(upstream, n1, t1, n2, t2, slope, front, up, down, vec, spend):
    rows, width = upstream.shape
    full = fixed(rows, width)
    thin = fixed(rows, 1)
    return pl.pallas_call(
        post_back_kernel,
        grid=(4,),
        in_specs=[
            full, full, thin, full, thin, column_spec(rows, width),
            unit_spec(width, 3), step_spec(width), step_spec(width), fixed(12, width),
        ],
        out_specs=[fixed(6, rows, width), full, full, fixed(12, width)],
        out_shape=[
            shaped((6, rows, width)),
            shaped((rows, width)),
            shaped((rows, width), jnp.float32),
            shaped((12, width), jnp.float32),
        ],
        scratch_shapes=[
            pltpu.VMEM((rows, width), jnp.float32),
            pltpu.VMEM((rows, width), jnp.float32),
        ],
        compiler_params=LIMIT,
        cost_estimate=cost(spend),
        name="post_back",
    )(upstream, n1, t1, n2, t2, slope, front, up, down, vec)


def project_back_kernel(
    dq_ref, own_ref, got_ref, w_ref, dr_ref, dm_out, dx_out, dxl_out, sums_out
):
    unit = pl.program_id(0)

    @pl.when(unit == 0)
    def _():
        dm_out[...] = dq_ref[...]

    @pl.when(unit > 0)
    def _():
        dm_out[...] = low(own_ref[...] + wide(got_ref[...]))

    grad = dm_out[...]
    part = nt(grad, w_ref[...])
    total = column_sum(wide(grad))

    @pl.when(unit == 0)
    def _():
        dx_out[...] = dr_ref[...] + part
        sums_out[0:1, :] = total

    @pl.when(unit > 0)
    def _():
        dx_out[...] += part
        sums_out[1:2, :] = total

    @pl.when(unit == 2)
    def _():
        dxl_out[...] = low(dx_out[...])


def project_back(dq, own, got, front, dr, spend):
    rows, width = dq.shape
    full = fixed(rows, width)
    late = pl.BlockSpec((None, rows, width), lambda unit: (jnp.maximum(unit - 1, 0), 0, 0))
    return pl.pallas_call(
        project_back_kernel,
        grid=(3,),
        in_specs=[full, late, late, step_spec(width), full],
        out_specs=[
            pl.BlockSpec((None, rows, width), lambda unit: (unit, 0, 0)),
            full, full, fixed(2, width),
        ],
        out_shape=[
            shaped((3, rows, width)),
            shaped((rows, width), jnp.float32),
            shaped((rows, width)),
            shaped((2, width), jnp.float32),
        ],
        compiler_params=LIMIT,
        cost_estimate=cost(spend),
        name="project_back",
    )(dq, own, got, front, dr)


def tn(left, right):
    return nn(left.T, right)


def split_store(keep_ref, give_ref, bit, x_first, piece_of, store):
    for other in range(2):
        pair = []
        for side in range(2):
            rep = (other * 2 + side) if x_first else (side * 2 + other)
            pair.append(low(piece_of(rep)))
        store(keep_ref, other, jnp.where(bit == 0, pair[0], pair[1]))
        store(give_ref, other, jnp.where(bit == 0, pair[1], pair[0]))


def column_store(ref_pair, bit, x_first, product, unit):
    keep_ref, give_ref = ref_pair
    for level in range(4):
        base = level * 4 * UNIT

        def piece_of(rep):
            return product[base + rep * UNIT : base + (rep + 1) * UNIT, :]

        def store(ref, other, value):
            ref[level, other, unit] = value

        split_store(keep_ref, give_ref, bit, x_first, piece_of, store)


def front_grad_kernel(
    bit_ref, xm_ref, xt_ref, om_ref, ot_ref, dm_ref, dmt_ref, da_ref, dat_ref,
    keep_x, give_x, keep_y, give_y,
):
    unit = pl.program_id(0)

    def store(product, index, x_first):
        pair = (keep_x, give_x) if x_first else (keep_y, give_y)
        column_store(pair, bit_ref[0 if x_first else 1], x_first, product, index)

    @pl.when(unit < 2)
    def _():
        store(tn(xm_ref[...], dm_ref[...]) + tn(xt_ref[...], dmt_ref[...]), unit, True)

    @pl.when(unit == 2)
    def _():
        store(tn(xm_ref[...], dm_ref[...]) + tn(xt_ref[...], dmt_ref[...]), 0, False)

    @pl.when(unit == 3)
    def _():
        store(tn(om_ref[...], da_ref[...]) + tn(ot_ref[...], dat_ref[...]), 1, False)


def block_spec(rows, width, index):
    return pl.BlockSpec((None, rows, width), lambda step: (index, 0, 0))


def front_grad(bits, xm, xt, mine, theirs, dm, dmt, da, dat, spend):
    rows, half = xm.shape
    width = da.shape[2]
    late = pl.BlockSpec((None, rows, width), lambda unit: (jnp.minimum(unit, 2), 0, 0))
    shape = (4, 2, 2, UNIT, width)
    return pl.pallas_call(
        front_grad_kernel,
        grid=(4,),
        in_specs=[SMEM, fixed(rows, half), fixed(rows, half)]
        + [block_spec(rows, half, 5)] * 2
        + [late, late]
        + [block_spec(rows, width, 5)] * 2,
        out_specs=[fixed(*shape)] * 4,
        out_shape=[shaped(shape)] * 4,
        compiler_params=LIMIT,
        cost_estimate=cost(spend),
        name="front_grad",
    )(bits, xm, xt, mine, theirs, dm, dmt, da, dat)


def feed_grad_kernel(
    x_first, bit_ref, ym_ref, yt_ref, gm_ref, gt_ref, dz_ref, dzt_ref, df_ref, dft_ref,
    keep_up, give_up, keep_down, give_down,
):
    step = pl.program_id(0)
    up_bit = bit_ref[0 if x_first else 1]
    down_bit = bit_ref[1 if x_first else 0]

    @pl.when(step < 4)
    def _():
        product = tn(ym_ref[...], dz_ref[...]) + tn(yt_ref[...], dzt_ref[...])
        column_store((keep_up, give_up), up_bit, x_first, product, step)

    @pl.when(step >= 4)
    def _():
        product = tn(gm_ref[...], df_ref[...]) + tn(gt_ref[...], dft_ref[...])
        for sub in range(4):

            def piece_of(rep):
                base = (rep * 4 + sub) * UNIT
                return product[base : base + UNIT, :]

            def store(ref, other, value):
                ref[step - 4, other, sub] = value

            split_store(keep_down, give_down, down_bit, not x_first, piece_of, store)


def feed_grad(x_first, bits, mine, theirs, slopes, slopes_twin, spend):
    rows, half = mine.shape[1:]
    width = slopes.shape[2]
    early = pl.BlockSpec((None, rows, width), lambda step: (jnp.minimum(step, 3), 0, 0))
    late = pl.BlockSpec((None, rows, half), lambda step: (jnp.maximum(step - 4, 0), 0, 0))
    shape = (4, 2, 4, UNIT, width)
    return pl.pallas_call(
        functools.partial(feed_grad_kernel, x_first),
        grid=(8,),
        in_specs=[SMEM]
        + [block_spec(rows, half, 4)] * 2
        + [late, late, early, early]
        + [block_spec(rows, width, 4)] * 2,
        out_specs=[fixed(*shape)] * 4,
        out_shape=[shaped(shape)] * 4,
        compiler_params=LIMIT,
        cost_estimate=cost(spend),
        name="feed_grad",
    )(bits, mine, theirs, mine, theirs, slopes, slopes_twin, slopes, slopes_twin)


def halve_kernel(low_ref, keep_x, got_x, keep_y, got_y, keep_out, give_out):
    start = jnp.where(low_ref[0] == 1, 0, 2)
    for index, (keep, got) in enumerate(((keep_x, got_x), (keep_y, got_y))):
        for out, begin in ((keep_out, start), (give_out, 2 - start)):
            for level in range(2):
                out[index, level] = low(wide(keep[begin + level]) + wide(got[begin + level]))


def halve_sum(is_low, keeps, gots, spend):
    count, width = keeps[0].shape[2], keeps[0].shape[4]
    whole = pl.BlockSpec((4, None, count, UNIT, width), lambda other: (0, other, 0, 0, 0))
    half = pl.BlockSpec((2, 2, None, count, UNIT, width), lambda other: (0, 0, other, 0, 0, 0))
    return pl.pallas_call(
        halve_kernel,
        grid=(2,),
        in_specs=[SMEM] + [whole] * 4,
        out_specs=[half] * 2,
        out_shape=[shaped((2, 2, 2, count, UNIT, width))] * 2,
        compiler_params=LIMIT,
        cost_estimate=cost(spend),
        name="halve_sum",
    )(is_low.astype(jnp.int32).reshape(1), keeps[0], gots[0], keeps[1], gots[1])


class Reduction:
    def __init__(self, pairs, bits, is_low, is_core):
        self.keeps = [pair[0] for pair in pairs]
        self.firsts = [pair[2] for pair in pairs]
        self.bits, self.is_low, self.is_core = bits, is_low, is_core
        self.got = [send(pair[1], TO_X if pair[2] else TO_Y) for pair in pairs]

    def across(self, spend, *others):
        got = after(self.got, *others)
        self.keep, give = halve_sum(self.is_low, self.keeps, got, spend)
        self.mid = send(give, TO_MID)
        return give

    def join(self, other):
        self.keep = jnp.concatenate([self.keep, other.keep], axis=3)
        self.mid = jnp.concatenate([self.mid, other.mid], axis=3)

    def outward(self, *others):
        mid = after([self.mid], *others)[0]
        stage = low(wide(self.keep) + wide(mid))
        outer = jnp.where(self.is_low, stage[:, 0], stage[:, 1])
        self.inner = jnp.where(self.is_low, stage[:, 1], stage[:, 0])
        self.side = send(outer, TO_SIDE)
        return outer

    def turn(self, *others):
        side = after([self.side], *others)[0]
        stage = jnp.where(self.is_core, self.inner, side)
        self.pieces = [stage[index] for index in range(len(self.firsts))]
        self.over = [
            send(piece, TO_Y if first else TO_X)
            for piece, first in zip(self.pieces, self.firsts)
        ]
        return stage

    def share(self, *others):
        over = after(self.over, *others)
        self.sums = [low(wide(piece) + wide(item)) for piece, item in zip(self.pieces, over)]
        self.got = [
            send(piece, TO_X if first else TO_Y) for piece, first in zip(self.sums, self.firsts)
        ]
        return self.sums[0]

    def finish(self, *others):
        results = []
        for piece, got, first in zip(self.sums, after(self.got, *others), self.firsts):
            axis = 1 if first else 0
            bit = self.bits[0] if first else self.bits[1]
            joined = jnp.where(
                bit == 0, jnp.stack([piece, got], axis), jnp.stack([got, piece], axis)
            )
            results.append(wide(joined).reshape((4,) + piece.shape[1:]))
        return results


def body_fast(
    inputs, cotangent, lengths, dealing, key_mask,
    entry_weight, exit_weight, expand_weight, shrink_weight, vectors,
):
    rows, width = inputs.shape
    layers = entry_weight.shape[0]
    group_rows = 8 * rows
    half_rows = group_rows // 2
    core_rows = half_rows // 2
    rep = lax.axis_index("rep")
    shard = lax.axis_index("shard")
    depth, twin = shard // 2, shard % 2
    is_low = depth <= 1
    is_core = (depth == 1) | (depth == 2)
    where = jnp.stack([depth, rep, twin]).astype(jnp.int32)
    bits = (rep & 1, rep >> 1)
    bit_words = jnp.stack(bits).astype(jnp.int32)

    def order(four):
        own, near, middle, far = four
        return jnp.where(
            is_low, jnp.stack([near, own, middle, far]), jnp.stack([far, middle, own, near])
        )

    def absolute(mine, theirs):
        one, two = order(mine), order(theirs)
        return jnp.where(twin == 0, jnp.stack([one, two], 1), jnp.stack([two, one], 1))

    def own_piece(pack):
        piece = lax.dynamic_index_in_dim(pack, rep, 0, keepdims=False)
        return piece.reshape(-1, width)

    def units_of(item):
        return item.reshape(-1, UNIT, width)

    def pack_front(entry, leaving):
        return jnp.concatenate([by_columns(entry), by_columns(leaving)], axis=1)

    def pack_feed(expand, shrink):
        return jnp.concatenate([by_columns(expand), low(shrink).reshape(4, 4, UNIT, width)], axis=1)

    def by_columns(weight):
        count = weight.shape[1] // width
        return low(weight).reshape(4, UNIT, count, width).transpose(0, 2, 1, 3)

    extra = layers * vectors.shape[1] // width
    tail = low(vectors).reshape(extra, width)
    table = jnp.concatenate([dealing // 64, dealing % 64, key_mask], axis=0)
    table = low(table).reshape(1, width)
    filler = jnp.zeros((7 - extra, width), jnp.bfloat16)
    rows_in = jnp.concatenate([inputs, tail, table, filler], axis=0)

    front_zero = pack_front(entry_weight[0], exit_weight[0])
    piece = own_piece(front_zero)
    near = send(piece, TO_SIDE)
    middle = send(piece, TO_MID)
    near_in = send(rows_in, TO_SIDE)
    middle_in = send(rows_in, TO_MID)
    far = send(near, TO_MID)
    first = jnp.stack([units_of(item) for item in (near, middle, far)])
    over_x, over_y = send(first, TO_X), send(first, TO_Y)
    expand_late, shrink_late, twin_late, near_in = after(
        [expand_weight[0], shrink_weight[0], twin, near_in], first
    )
    far_in = send(near_in, TO_MID)
    parts = spread(front_zero, first, over_x, over_y, False)

    feed_zero = pack_feed(expand_late, shrink_late)
    piece = tie(own_piece(feed_zero), parts[5], parts[6])
    near = send(piece, TO_SIDE)
    middle = send(piece, TO_MID)
    mine = jnp.stack([rows_in, near_in, middle_in, far_in])
    theirs = send(mine, TO_TWIN)
    far = send(near, TO_MID)
    first = jnp.stack([units_of(item) for item in (near, middle, far)])
    first = tie(first, parts[7], parts[8], theirs)
    over_x, over_y = send(first, TO_X), send(first, TO_Y)
    feed_parts = spread(feed_zero, first, over_x, over_y, True)
    fronts = [assemble(where, parts, 0, False)]

    entry_late, exit_late, expand_late, shrink_late, cotangent_late = after(
        [entry_weight[1], exit_weight[1], expand_weight[1], shrink_weight[1], cotangent], first
    )
    front_one = pack_front(entry_late, exit_late)
    feed_one = pack_feed(expand_late, shrink_late)
    piece = jnp.concatenate([own_piece(front_one), own_piece(feed_one), cotangent_late], axis=0)
    piece = tie(piece, feed_parts[5], feed_parts[6])
    near = send(piece, TO_SIDE)
    middle = send(piece, TO_MID)
    far = send(near, TO_MID)
    four = (piece, near, middle, far)
    parts = feed_parts
    ups = [assemble(where, parts, 0, False)]
    downs = [assemble(where, parts, 4, True)]

    first_split, split = 4 * UNIT, 12 * UNIT
    first = jnp.stack([units_of(item[:first_split]) for item in four[1:]])
    first = tie(first, parts[7], parts[8])
    over_x, over_y = send(first, TO_X), send(first, TO_Y)
    parts = spread(front_one, first, over_x, over_y, True)
    fronts.append(assemble(where, parts, 0, False))
    first = jnp.stack([units_of(item[first_split:split]) for item in four[1:]])
    first = tie(first, parts[7], parts[8])
    over_x, over_y = send(first, TO_X), send(first, TO_Y)
    parts = spread(feed_one, first, over_x, over_y, False)
    ups.append(assemble(where, parts, 0, False))
    downs.append(assemble(where, parts, 4, True))
    cotangent_mine = jnp.stack([item[split:] for item in four])
    cotangent_theirs = send(cotangent_mine, TO_TWIN)

    header = absolute(tuple(mine[:, rows:]), tuple(theirs[:, rows:]))
    header = header.reshape(8, 8, width)
    vector_all = wide(header[:, :extra]).reshape(8, layers, vectors.shape[1])
    vector_all = jnp.transpose(vector_all, (1, 0, 2)).reshape(layers, 12, width)
    numbers = wide(header[:, extra]).reshape(8, 3, rows)
    dealt_all = (numbers[:, 0] * 64 + numbers[:, 1]).astype(jnp.int32).reshape(group_rows)
    mask_all = numbers[:, 2].reshape(group_rows)

    member, leading = sequence_ids(lengths[0], group_rows)
    usable = (mask_all == 1) | leading
    code = jnp.where(usable, member, -1)
    longest = jnp.argmax(lengths[0])
    begin = jnp.cumsum(lengths[0])[longest] - lengths[0][longest]
    spot = jnp.arange(half_rows, dtype=jnp.int32)

    def halve(values, low_side):
        inside = lax.dynamic_slice_in_dim(values, begin, half_rows, 0)
        outside = jnp.where(spot < begin, values[:half_rows], values[half_rows:])
        return jnp.where(low_side, inside, outside)

    def cores(values):
        own = lax.dynamic_slice_in_dim(values, twin * core_rows, core_rows, 0)
        other = lax.dynamic_slice_in_dim(values, (1 - twin) * core_rows, core_rows, 0)
        return own, other

    code_half = jnp.concatenate(cores(halve(code, is_low))).reshape(half_rows, 1)
    member_own = cores(halve(member, is_low))[0].reshape(1, core_rows)
    dealt_near = cores(halve(dealt_all, is_low))
    dealt_far = cores(halve(dealt_all, ~is_low))

    block = jnp.arange(width, dtype=jnp.int32)
    place = jnp.arange(width // 2, dtype=jnp.int32)
    chunk = 4 * UNIT
    source = (place // chunk) * (2 * chunk) + place % chunk
    cores_at = jnp.stack([twin_late, 1 - twin_late])
    sel = low(block[None, :, None] == (source[None, :] + cores_at[:, None] * chunk)[:, None, :])

    local = jnp.arange(rows, dtype=jnp.int32)
    bases = jnp.stack(
        [
            (depth ^ flip) * (2 * rows) + (twin ^ side) * rows
            for side in range(2)
            for flip in (0, 1, 3, 2)
        ]
    ).astype(jnp.int32)
    source_ids = (bases[:, None] + local[None, :]).reshape(8, 1, rows)
    want_in = dealt_near[0].reshape(core_rows, 1)
    hidden_low = gather_rows((mine, theirs), source_ids, want_in, 5)
    upstream = gather_rows((cotangent_mine, cotangent_theirs), source_ids, want_in, 5)

    result_ids = jnp.stack([dealt_near[0], dealt_far[0], dealt_near[1], dealt_far[1]]).reshape(
        4, 1, core_rows
    )
    want_out = jnp.concatenate([source_ids[0, 0], source_ids[1, 0]]).reshape(2 * rows, 1)

    def deliver(pieces, spend):
        pieces = [piece[None] for piece in pieces]
        found = gather_rows(pieces, result_ids, want_out, spend)
        return found, send(found[rows:], TO_SIDE)

    saved = []
    hidden = hidden_low
    for layer in range(layers):
        vec = vector_all[layer]
        queries, kv, xm, xt = project(hidden_low, fronts[layer], vec, sel)
        kv_twin = send(kv, TO_TWIN)
        xo = send(xt, TO_TWIN)
        attended, ot, lse = attend_fast(queries, kv, kv_twin, code_half, member_own)
        hidden, hidden_low, n1, t1, n2, t2, slope, mine, theirs = post(
            where, attended, hidden, fronts[layer], ups[layer], downs[layer], vec, sel
        )
        others = send(theirs, TO_TWIN)
        saved.append((queries, kv, kv_twin, ot, lse, n1, t1, n2, t2, slope, xm, xo, mine, others))
    result_mid = send(hidden_low, TO_MID)
    result_twin = send(hidden_low, TO_TWIN)

    def start_back(layer, grad, spend):
        n1, t1, n2, t2, slope = saved[layer][5:10]
        slopes, do, dr, sums = post_back(
            grad, n1, t1, n2, t2, slope,
            fronts[layer], ups[layer], downs[layer], vector_all[layer], spend,
        )
        return slopes, send(slopes, TO_TWIN), do, dr, sums

    def attention_back(layer, do, spend):
        queries, kv, kv_twin, ot, lse = saved[layer][:5]
        return attend_back_fast(
            queries, do, kv, kv_twin, ot, lse, code_half, member_own, spend
        )

    def feed_part(layer, x_first, slopes, slopes_twin, spend):
        mine, others = saved[layer][12:14]
        keep_up, give_up, keep_down, give_down = feed_grad(
            x_first, bit_words, mine, others, slopes, slopes_twin, spend
        )
        work = Reduction(
            [(keep_up, give_up, x_first), (keep_down, give_down, not x_first)],
            bits, is_low, is_core,
        )
        return work, keep_up

    def front_part(layer, slopes, slopes_twin, dm, dm_twin, spend):
        xm, xo, mine, others = saved[layer][10:14]
        keep_x, give_x, keep_y, give_y = front_grad(
            bit_words, xm, xo, mine, others, dm, dm_twin, slopes, slopes_twin, spend
        )
        work = Reduction(
            [(keep_x, give_x, True), (keep_y, give_y, False)], bits, is_low, is_core
        )
        return work, keep_x

    upstream = tie(upstream, saved[0][11], saved[0][13])
    slopes_b, slopes_tb, do, dr, sums_b = start_back(1, upstream, 16)
    dq, own, give = attention_back(1, do, 21)
    got = send(give, TO_TWIN)
    feed_b, mark = feed_part(1, True, slopes_b, tie(slopes_tb, dq, saved[1][11], result_twin), 12)
    pair = (hidden_low, tie(result_mid, mark))
    pair += (result_twin, send(pair[1], TO_TWIN))
    dm_b, grad, _, head_b = project_back(dq, own, got, fronts[1], tie(dr, mark, pair[1]), 0.5)
    dm_tb = send(dm_b, TO_TWIN)
    found, output_side = deliver(after(pair, head_b), 0.5)
    slopes_a, slopes_ta, do, dr, sums_a = start_back(0, tie(grad, found), 0.5)
    ready = feed_b.across(3, do)
    dq, own, give = attention_back(0, tie(do, ready), 45)
    got = send(give, TO_TWIN)
    front_b, mark = front_part(1, slopes_b, slopes_tb, dm_b, tie(dm_tb, dq), 0.5)
    feed_a, mark = feed_part(0, False, slopes_a, tie(slopes_ta, mark, output_side, feed_b.mid), 12)
    ready = front_b.across(2, mark)
    dm_a, grad, grad_low, head_a = project_back(
        dq, own, got, fronts[0], tie(dr, ready), 0.5
    )
    dm_ta = send(dm_a, TO_TWIN)
    grad_mid = send(grad_low, TO_MID)
    grad_twin = send(grad_low, TO_TWIN)

    vectors_all = [
        jnp.concatenate([head_sums, sums[2:]], axis=0)
        for head_sums, sums in ((head_a, sums_a), (head_b, sums_b))
    ]
    joined = jnp.stack([item.reshape(-1) for item in vectors_all])
    joined = jnp.transpose(joined.reshape(layers, 4, 2, vectors.shape[1]), (1, 2, 0, 3))
    vector_keep = lax.dynamic_index_in_dim(joined, twin, 1, keepdims=False)
    vector_give = lax.dynamic_index_in_dim(joined, 1 - twin, 1, keepdims=False)
    vector_twin = send(vector_give, TO_TWIN)

    ready = feed_a.across(25, grad_low, front_b.mid)
    front_a, mark = front_part(0, slopes_a, slopes_ta, dm_a, tie(dm_ta, vector_give, ready, grad_twin), 0.5)

    feed_b.join(front_b)
    ready = feed_b.outward(mark)
    vector_stage = vector_keep + tie(vector_twin, ready)
    vector_over = send(vector_stage, TO_X)
    pair = (grad_low, tie(grad_mid, vector_stage), grad_twin)
    pair += (send(pair[1], TO_TWIN),)
    found_in, input_side = deliver(pair, 0.5)
    ready = feed_b.turn(found_in)
    vector_stage = vector_stage + tie(vector_over, ready)
    vector_over = send(vector_stage, TO_Y)

    ready = front_a.across(0.5, vector_stage)
    ready = feed_b.share(ready)
    vector_stage = vector_stage + tie(vector_over, ready)
    vector_give = jnp.where(is_low, vector_stage[2:4], vector_stage[0:2])
    vector_keep = jnp.where(is_low, vector_stage[0:2], vector_stage[2:4])
    vector_mid = send(vector_give, TO_MID)
    ready = feed_a.outward(vector_give)
    done_b = feed_b.finish(ready)
    up_b, down_b = (item[:, :4] for item in done_b)
    front_grad_b = jnp.concatenate([item[:, 4:] for item in done_b], axis=1)

    ready = front_a.outward(up_b, down_b, front_grad_b)
    vector_stage = vector_keep + tie(vector_mid, ready)
    vector_outer = jnp.where(is_low, vector_stage[0], vector_stage[1])
    vector_inner = jnp.where(is_low, vector_stage[1], vector_stage[0])
    vector_side = send(vector_outer, TO_SIDE)
    ready = feed_a.turn(vector_outer)
    output = jnp.where(is_core, found[:rows], output_side)
    input_grad = wide(jnp.where(is_core, found_in[:rows], tie(input_side, ready)))

    ready = front_a.turn(ready)
    ready_two = feed_a.share(ready)
    ready = front_a.share(ready_two)
    up_a, down_a = feed_a.finish(ready)
    front_grad_a = jnp.concatenate(front_a.finish(up_a, down_a), axis=1)
    vector_grad = jnp.where(is_core, vector_inner, tie(vector_side, ready))
    grads = [(front_grad_a, up_a, down_a), (front_grad_b, up_b, down_b)]

    def columns(units):
        count = units.shape[1]
        return units.transpose(0, 2, 1, 3).reshape(4 * UNIT, count * width)

    entry_grad = jnp.stack([columns(item[0][:, 0:3]) for item in grads])
    exit_grad = jnp.stack([columns(item[0][:, 3:4]) for item in grads])
    expand_grad = jnp.stack([columns(item[1]) for item in grads])
    shrink_grad = jnp.stack([item[2].reshape(16 * UNIT, width) for item in grads])
    return (output, input_grad, entry_grad, exit_grad, expand_grad, shrink_grad, vector_grad)


def solution(mesh):
    placed = (
        P(("rep", "shard"), None),
        P(("rep", "shard"), None),
        P("rep", None),
        P("rep", "shard"),
        P("rep", "shard"),
        P(None, "shard", None),
        P(None, "shard", None),
        P(None, "shard", None),
        P(None, "shard", None),
        P(None, "shard"),
    )
    small = dict(mesh.shape) == {"rep": 4, "shard": 8}
    return jax.shard_map(
        body_fast if small else body,
        mesh=mesh,
        in_specs=placed,
        out_specs=(
            P(("rep", "shard"), None),
            P(("rep", "shard"), None),
            P(None, "shard", None),
            P(None, "shard", None),
            P(None, "shard", None),
            P(None, "shard", None),
            P(None, "shard"),
        ),
        check_vma=False,
    )
```

```python
import functools

import jax
import jax.numpy as jnp
from jax import lax
from jax.experimental import pallas as pl
from jax.experimental.pallas import tpu as pltpu
from jax.sharding import PartitionSpec as P

HEADS = 12
HEAD_DIM = 64


NEG_FILL = -1e30


def norm_forward(resid, gain, shift):
    center = jnp.mean(resid, axis=-1, keepdims=True)
    offsets = resid - center
    spread = jnp.mean(offsets * offsets, axis=-1, keepdims=True)
    factor = lax.rsqrt(spread + 1e-05)
    normed = offsets * factor
    return (normed * gain + shift, normed, factor)


def norm_backward(incoming, normed, factor, gain):
    scaled = incoming * gain
    resid_grad = factor * (
        scaled
        - jnp.mean(scaled, axis=-1, keepdims=True)
        - normed * jnp.mean(scaled * normed, axis=-1, keepdims=True)
    )
    return (resid_grad, jnp.sum(incoming * normed, axis=0), jnp.sum(incoming, axis=0))


def inner_rows(left, right):
    return lax.dot_general(
        left, right, (((0,), (0,)), ((), ())), preferred_element_type=jnp.float32
    )


def times_trans(left, right):
    return lax.dot_general(
        left, right, (((1,), (1,)), ((), ())), preferred_element_type=jnp.float32
    )


def gelu_exact(value):
    return jax.nn.gelu(value, approximate=False)


def sequence_ids(lengths, group_rows):
    ending = jnp.cumsum(lengths)
    opening = ending - lengths
    places = jnp.arange(group_rows, dtype=jnp.int32)
    member = jnp.sum((places[:, None] >= ending[None, :]).astype(jnp.int32), axis=1)
    leading = jnp.any(places[:, None] == opening[None, :], axis=1)
    return (member, leading)


def split_vector(vector, model_width):
    pieces = [vector[index * model_width : (index + 1) * model_width] for index in range(8)]
    pieces.append(vector[8 * model_width :])
    return pieces


def fetch_forward(entry_weight, exit_weight, expand_weight, shrink_weight, vectors, layer_index):
    return (
        lax.all_gather(entry_weight[layer_index].astype(jnp.bfloat16), "shard", axis=0, tiled=True),
        lax.all_gather(exit_weight[layer_index].astype(jnp.bfloat16), "shard", axis=0, tiled=True),
        lax.all_gather(
            expand_weight[layer_index].astype(jnp.bfloat16), "shard", axis=0, tiled=True
        ),
        lax.all_gather(
            shrink_weight[layer_index].astype(jnp.bfloat16), "shard", axis=0, tiled=True
        ),
        lax.all_gather(vectors[layer_index].astype(jnp.bfloat16), "shard", axis=0, tiled=True),
    )


def fetch_backward(entry_weight, exit_weight, expand_weight, shrink_weight, vectors, layer_index):
    return (
        lax.all_gather(entry_weight[layer_index].astype(jnp.bfloat16), "shard", axis=0, tiled=True),
        lax.all_gather(exit_weight[layer_index].astype(jnp.bfloat16), "shard", axis=0, tiled=True),
        lax.all_gather(
            expand_weight[layer_index].astype(jnp.bfloat16), "shard", axis=0, tiled=True
        ),
        lax.all_gather(
            shrink_weight[layer_index].astype(jnp.bfloat16), "shard", axis=0, tiled=True
        ),
        lax.all_gather(vectors[layer_index].astype(jnp.bfloat16), "shard", axis=0, tiled=True),
    )


def attend_forward(queries, keys, values, own_member, member, usable):
    local_rows = queries.shape[0]
    query_heads = queries.reshape(local_rows, HEADS, HEAD_DIM)
    factor_scale = HEAD_DIM ** (-0.5)
    start_state = (
        jnp.full((HEADS, local_rows), NEG_FILL, jnp.float32),
        jnp.zeros((HEADS, local_rows), jnp.float32),
        jnp.zeros((HEADS, local_rows, HEAD_DIM), jnp.float32),
    )
    key_piece = lax.all_gather(keys, "shard", axis=0, tiled=True)
    value_piece = lax.all_gather(values, "shard", axis=0, tiled=True)
    amount = key_piece.shape[0]
    block_rows = local_rows * max(1, 512 // local_rows)

    def fold_advance(block_index, running):
        running_max, running_total, weighted = running
        begin = block_index * block_rows
        key_block = lax.dynamic_slice_in_dim(key_piece, begin, block_rows, 0).reshape(
            block_rows, HEADS, HEAD_DIM
        )
        value_block = lax.dynamic_slice_in_dim(value_piece, begin, block_rows, 0).reshape(
            block_rows, HEADS, HEAD_DIM
        )
        key_member = lax.dynamic_slice_in_dim(member, begin, block_rows, 0)
        key_usable = lax.dynamic_slice_in_dim(usable, begin, block_rows, 0)
        allowed = ((own_member[:, None] == key_member[None, :]) & key_usable[None, :])[None]
        scores = (
            jnp.einsum("qhd,khd->hqk", query_heads, key_block, preferred_element_type=jnp.float32)
            * factor_scale
        )
        scores = jnp.where(allowed, scores, NEG_FILL)
        new_max = jnp.maximum(running_max, jnp.max(scores, axis=2))
        expos = jnp.where(allowed, jnp.exp(scores - new_max[:, :, None]), 0.0)
        shrink_by = jnp.exp(running_max - new_max)
        new_total = running_total * shrink_by + jnp.sum(expos, axis=2)
        new_weighted = weighted * shrink_by[:, :, None] + jnp.einsum(
            "hqk,khd->hqd",
            expos.astype(jnp.bfloat16),
            value_block,
            preferred_element_type=jnp.float32,
        )
        return (new_max, new_total, new_weighted)

    running_max, running_total, weighted = lax.fori_loop(
        0, amount // block_rows, fold_advance, start_state
    )
    attended = jnp.transpose(weighted / running_total[:, :, None], (1, 0, 2)).reshape(
        local_rows, HEADS * HEAD_DIM
    )
    return (attended, running_max + jnp.log(running_total))


def attend_backward(
    queries, attended_grad, log_total, deltas, keys_all, values_all, own_member, member, usable
):
    local_rows = queries.shape[0]
    group_rows = keys_all.shape[0]
    model_width = HEADS * HEAD_DIM
    factor_scale = HEAD_DIM ** (-0.5)
    query_heads = queries.reshape(local_rows, HEADS, HEAD_DIM)
    grad_heads = attended_grad.reshape(local_rows, HEADS, HEAD_DIM)
    block_rows = min(512, group_rows)

    def attend_advance(query_sum, block_index):
        begin = block_index * block_rows
        key_block = lax.dynamic_slice_in_dim(keys_all, begin, block_rows, 0).reshape(
            block_rows, HEADS, HEAD_DIM
        )
        value_block = lax.dynamic_slice_in_dim(values_all, begin, block_rows, 0).reshape(
            block_rows, HEADS, HEAD_DIM
        )
        key_member = lax.dynamic_slice_in_dim(member, begin, block_rows, 0)
        key_usable = lax.dynamic_slice_in_dim(usable, begin, block_rows, 0)
        allowed = ((own_member[:, None] == key_member[None, :]) & key_usable[None, :])[None]
        scores = (
            jnp.einsum("qhd,khd->hqk", query_heads, key_block, preferred_element_type=jnp.float32)
            * factor_scale
        )
        probs = jnp.where(allowed, jnp.exp(scores - log_total[:, :, None]), 0.0)
        prob_grad = jnp.einsum(
            "qhd,khd->hqk", grad_heads, value_block, preferred_element_type=jnp.float32
        )
        score_grad = (probs * (prob_grad - deltas[:, :, None])).astype(jnp.bfloat16)
        query_sum = (
            query_sum
            + jnp.einsum("hqk,khd->qhd", score_grad, key_block, preferred_element_type=jnp.float32)
            * factor_scale
        )
        key_grad = (
            jnp.einsum("hqk,qhd->khd", score_grad, query_heads, preferred_element_type=jnp.float32)
            * factor_scale
        )
        value_grad = jnp.einsum(
            "hqk,qhd->khd",
            probs.astype(jnp.bfloat16),
            grad_heads,
            preferred_element_type=jnp.float32,
        )
        joined = jnp.concatenate(
            [
                key_grad.reshape(block_rows, model_width),
                value_grad.reshape(block_rows, model_width),
            ],
            axis=1,
        )
        return (query_sum, joined)

    query_sum, key_value = lax.scan(
        attend_advance,
        jnp.zeros((local_rows, HEADS, HEAD_DIM), jnp.float32),
        jnp.arange(group_rows // block_rows, dtype=jnp.int32),
    )
    key_value = key_value.reshape(group_rows, 2 * model_width)
    return (query_sum.reshape(local_rows, model_width), key_value)


def layer_forward(hidden, weights, own_member, member, usable):
    entry, leaving, expand, shrink, vector = weights
    model_width = leaving.shape[0]
    pieces = split_vector(vector.astype(jnp.float32), model_width)
    flat = hidden.astype(jnp.bfloat16)
    mixed = jnp.dot(flat, entry, preferred_element_type=jnp.float32)
    queries = (mixed[:, 0:model_width] + pieces[0]).astype(jnp.bfloat16)
    keys = mixed[:, model_width : 2 * model_width].astype(jnp.bfloat16)
    values = (mixed[:, 2 * model_width : 3 * model_width] + pieces[1]).astype(jnp.bfloat16)
    attended, log_total = attend_forward(queries, keys, values, own_member, member, usable)
    attended_low = attended.astype(jnp.bfloat16)
    branch = jnp.dot(attended_low, leaving, preferred_element_type=jnp.float32) + pieces[2]
    middle, normed_one, factor_one = norm_forward(hidden + branch, pieces[3], pieces[4])
    middle_low = middle.astype(jnp.bfloat16)
    inner = jnp.dot(middle_low, expand, preferred_element_type=jnp.float32) + pieces[8]
    active = gelu_exact(inner).astype(jnp.bfloat16)
    branch_two = jnp.dot(active, shrink, preferred_element_type=jnp.float32) + pieces[5]
    result, normed_two, factor_two = norm_forward(middle + branch_two, pieces[6], pieces[7])
    record = (
        flat,
        queries,
        keys,
        values,
        attended,
        log_total,
        attended_low,
        normed_one,
        factor_one,
        middle_low,
        inner,
        active,
        normed_two,
        factor_two,
    )
    return (result, record)


def layer_backward(upstream, weights, record, keys_all, values_all, own_member, member, usable):
    entry, leaving, expand, shrink, vector = weights
    model_width = leaving.shape[0]
    pieces = split_vector(vector.astype(jnp.float32), model_width)
    (
        flat,
        queries,
        keys,
        values,
        attended,
        log_total,
        attended_low,
        normed_one,
        factor_one,
        middle_low,
        inner,
        active,
        normed_two,
        factor_two,
    ) = record
    local_rows = queries.shape[0]
    resid_two, gain_two_grad, shift_two_grad = norm_backward(
        upstream, normed_two, factor_two, pieces[6]
    )
    branch_two_grad = resid_two.astype(jnp.bfloat16)
    bias_down_grad = jnp.sum(branch_two_grad.astype(jnp.float32), axis=0)
    shrink_grad = inner_rows(active, branch_two_grad)
    active_grad = times_trans(branch_two_grad, shrink)
    unused_value, gelu_pull = jax.vjp(gelu_exact, inner)
    inner_grad = gelu_pull(active_grad)[0].astype(jnp.bfloat16)
    bias_up_grad = jnp.sum(inner_grad.astype(jnp.float32), axis=0)
    expand_grad = inner_rows(middle_low, inner_grad)
    middle_grad = resid_two + times_trans(inner_grad, expand)
    resid_one, gain_one_grad, shift_one_grad = norm_backward(
        middle_grad, normed_one, factor_one, pieces[3]
    )
    branch_grad = resid_one.astype(jnp.bfloat16)
    bias_out_grad = jnp.sum(branch_grad.astype(jnp.float32), axis=0)
    exit_grad = inner_rows(attended_low, branch_grad)
    attended_grad = times_trans(branch_grad, leaving).astype(jnp.bfloat16)
    deltas = jnp.sum(
        (attended_grad.astype(jnp.float32) * attended).reshape(local_rows, HEADS, HEAD_DIM), axis=2
    ).T
    query_grad, key_value_grad = attend_backward(
        queries, attended_grad, log_total, deltas, keys_all, values_all, own_member, member, usable
    )
    own_key_value = lax.psum_scatter(
        key_value_grad.astype(jnp.bfloat16), "shard", scatter_dimension=0, tiled=True
    ).astype(jnp.float32)
    mixed_grad = jnp.concatenate([query_grad, own_key_value], axis=1).astype(jnp.bfloat16)
    bias_query_grad = jnp.sum(mixed_grad[:, 0:model_width].astype(jnp.float32), axis=0)
    bias_value_grad = jnp.sum(
        mixed_grad[:, 2 * model_width : 3 * model_width].astype(jnp.float32), axis=0
    )
    entry_grad = inner_rows(flat, mixed_grad)
    hidden_grad = resid_one + times_trans(mixed_grad, entry)
    vector_grad = jnp.concatenate(
        [
            bias_query_grad,
            bias_value_grad,
            bias_out_grad,
            gain_one_grad,
            shift_one_grad,
            bias_down_grad,
            gain_two_grad,
            shift_two_grad,
            bias_up_grad,
        ]
    )
    return (hidden_grad, (entry_grad, exit_grad, expand_grad, shrink_grad, vector_grad))


def body(
    inputs,
    cotangent,
    lengths,
    dealing,
    key_mask,
    entry_weight,
    exit_weight,
    expand_weight,
    shrink_weight,
    vectors,
):
    local_rows = inputs.shape[0]
    group_rows = local_rows * lax.axis_size("shard")
    position = lax.axis_index("shard") * local_rows
    dealt_all, mask_all = (
        lax.all_gather(dealing, "shard", axis=1, tiled=True),
        lax.all_gather(key_mask, "shard", axis=1, tiled=True),
    )
    member, leading = sequence_ids(lengths[0], group_rows)
    usable = (mask_all[0] == 1) | leading
    own_member = lax.dynamic_slice_in_dim(member, position, local_rows, 0)
    inverse = (
        jnp.zeros((group_rows,), jnp.int32)
        .at[dealt_all[0]]
        .set(jnp.arange(group_rows, dtype=jnp.int32))
    )
    own_inverse = lax.dynamic_slice_in_dim(inverse, position, local_rows, 0)
    inputs_all, cotangent_all = (
        lax.all_gather(inputs, "shard", axis=0, tiled=True),
        lax.all_gather(cotangent, "shard", axis=0, tiled=True),
    )
    hidden = jnp.take(inputs_all, dealing[0], axis=0).astype(jnp.float32)
    upstream = jnp.take(cotangent_all, dealing[0], axis=0).astype(jnp.float32)
    layers = entry_weight.shape[0]
    saved = []
    kept = []
    for layer_index in range(layers):
        weights = fetch_forward(
            entry_weight, exit_weight, expand_weight, shrink_weight, vectors, layer_index
        )
        kept.append(weights)
        hidden, record = layer_forward(hidden, weights, own_member, member, usable)
        saved.append(record)
    output_all = lax.all_gather(hidden.astype(jnp.bfloat16), "shard", axis=0, tiled=True)
    output = jnp.take(output_all, own_inverse, axis=0)
    hidden_grad = upstream
    layer_grads = [None] * layers
    for layer_index in reversed(range(layers)):
        weights = fetch_backward(
            entry_weight, exit_weight, expand_weight, shrink_weight, vectors, layer_index
        )
        record = saved[layer_index]
        keys_all, values_all = (
            lax.all_gather(record[2], "shard", axis=0, tiled=True),
            lax.all_gather(record[3], "shard", axis=0, tiled=True),
        )
        hidden_grad, local_grads = layer_backward(
            hidden_grad, weights, record, keys_all, values_all, own_member, member, usable
        )
        entry_local, exit_local, expand_local, shrink_local, vector_local = local_grads
        entry_part, exit_part, expand_part, shrink_part, vector_part = (
            lax.psum_scatter(
                entry_local.astype(jnp.bfloat16), "shard", scatter_dimension=0, tiled=True
            ).astype(jnp.float32),
            lax.psum_scatter(
                exit_local.astype(jnp.bfloat16), "shard", scatter_dimension=0, tiled=True
            ).astype(jnp.float32),
            lax.psum_scatter(
                expand_local.astype(jnp.bfloat16), "shard", scatter_dimension=0, tiled=True
            ).astype(jnp.float32),
            lax.psum_scatter(
                shrink_local.astype(jnp.bfloat16), "shard", scatter_dimension=0, tiled=True
            ).astype(jnp.float32),
            lax.psum_scatter(
                vector_local.astype(jnp.bfloat16), "shard", scatter_dimension=0, tiled=True
            ).astype(jnp.float32),
        )
        entry_part, exit_part, expand_part, shrink_part, vector_part = (
            lax.psum(entry_part.astype(jnp.bfloat16), "rep").astype(jnp.float32),
            lax.psum(exit_part.astype(jnp.bfloat16), "rep").astype(jnp.float32),
            lax.psum(expand_part.astype(jnp.bfloat16), "rep").astype(jnp.float32),
            lax.psum(shrink_part.astype(jnp.bfloat16), "rep").astype(jnp.float32),
            lax.psum(vector_part.astype(jnp.bfloat16), "rep").astype(jnp.float32),
        )
        layer_grads[layer_index] = (entry_part, exit_part, expand_part, shrink_part, vector_part)
    entry_grad = jnp.stack([item[0] for item in layer_grads])
    exit_grad = jnp.stack([item[1] for item in layer_grads])
    expand_grad = jnp.stack([item[2] for item in layer_grads])
    shrink_grad = jnp.stack([item[3] for item in layer_grads])
    vector_grad = jnp.stack([item[4] for item in layer_grads])
    grads_all = lax.all_gather(
        hidden_grad.astype(jnp.bfloat16), "shard", axis=0, tiled=True
    ).astype(hidden_grad.dtype)
    input_grad = jnp.take(grads_all, own_inverse, axis=0)
    return (output, input_grad, entry_grad, exit_grad, expand_grad, shrink_grad, vector_grad)


EDGE = (0, 1, 6, 7)
CORE = (2, 3, 4, 5)
ALL = tuple(range(8))
BOTH = ("rep", "shard")
UNIT = 24


def routes(rep_flip, shard_flip, shards):
    return [
        (rep * 8 + shard, (rep ^ rep_flip) * 8 + (shard ^ shard_flip))
        for rep in range(4)
        for shard in shards
    ]


TO_X = routes(1, 0, ALL)
TO_Y = routes(2, 0, ALL)
TO_TWIN = routes(0, 1, ALL)
TO_SIDE = routes(0, 2, ALL)
TO_MID = routes(0, 6, CORE) + routes(0, 1, EDGE)


def send(value, route):
    return lax.ppermute(value, BOTH, route)


def low(value):
    return value.astype(jnp.bfloat16)


def wide(value):
    return value.astype(jnp.float32)


VMEM = pl.BlockSpec(memory_space=pltpu.VMEM)
SMEM = pl.BlockSpec(memory_space=pltpu.SMEM)
LIMIT = pltpu.CompilerParams(vmem_limit_bytes=60 * 1024 * 1024)


def shaped(shape, kind=jnp.bfloat16):
    return jax.ShapeDtypeStruct(shape, kind)


def cost(micros):
    return pl.CostEstimate(
        flops=int(micros * 1e9), bytes_accessed=int(micros * 1e6), transcendentals=0
    )


def nt(left, right):
    return lax.dot_general(left, right, (((1,), (1,)), ((), ())), preferred_element_type=jnp.float32)


def nn(left, right):
    return lax.dot_general(left, right, (((1,), (0,)), ((), ())), preferred_element_type=jnp.float32)


def fixed(*shape):
    return pl.BlockSpec(shape, lambda step: (0,) * len(shape))


def gather_kernel(ids_ref, want_ref, *refs):
    out_ref = refs[-1]
    want = want_ref[...]
    total = None
    index = 0
    for piece_ref in refs[:-1]:
        for slot in range(piece_ref.shape[0]):
            ids = ids_ref[index]
            hit = low(wide(want == ids))
            part = nn(hit, piece_ref[slot, 0 : ids.shape[1], :])
            total = part if total is None else total + part
            index += 1
    out_ref[...] = low(total)


def gather_rows(pieces, ids, want, spend):
    return pl.pallas_call(
        gather_kernel,
        out_shape=shaped((want.shape[0], pieces[0].shape[2])),
        in_specs=[VMEM] * (2 + len(pieces)),
        out_specs=VMEM,
        compiler_params=LIMIT,
        cost_estimate=cost(spend),
        name="gather_rows",
    )(ids, want, *pieces)


def assemble_kernel(where_ref, *refs):
    out_ref = refs[10]
    depth, rep, twin = where_ref[0], where_ref[1], where_ref[2]
    for side in range(2):
        own, first, over_x, over_y, over_d = refs[side * 5 : side * 5 + 5]
        core = twin ^ side
        for row in range(4):
            out_ref[depth, core, row] = own[row]
        for slot, flip in enumerate((1, 3, 2)):
            level = depth ^ flip
            for piece, bits in ((first, 0), (over_x, 1), (over_y, 2), (over_d, 3)):
                out_ref[level, core, rep ^ bits] = piece[slot]


def assemble(where, parts, start, by_rows):
    def part_spec(part):
        return pl.BlockSpec(
            (part.shape[0], None) + part.shape[2:],
            lambda unit, where_ref: (0, start + unit, 0, 0),
        )

    width = parts[0].shape[3]
    if by_rows:
        shape = (4, 2, 4, 4, UNIT, width)
        spec = pl.BlockSpec(
            (4, 2, 4, None, UNIT, width), lambda unit, where_ref: (0, 0, 0, unit, 0, 0)
        )
    else:
        shape = (4, 4, 2, 4, UNIT, width)
        spec = pl.BlockSpec(
            (None, 4, 2, 4, UNIT, width), lambda unit, where_ref: (unit, 0, 0, 0, 0, 0)
        )
    result = pl.pallas_call(
        assemble_kernel,
        grid_spec=pltpu.PrefetchScalarGridSpec(
            num_scalar_prefetch=1,
            grid=(4,),
            in_specs=[part_spec(part) for part in parts],
            out_specs=spec,
        ),
        out_shape=shaped(shape),
        compiler_params=LIMIT,
        cost_estimate=cost(0.3),
        name="assemble",
    )(where, *parts)
    return result.reshape(4, 32 * UNIT, width)


def tie(value, *others):
    return lax.optimization_barrier((value,) + others)[0]


def after(values, *others):
    return list(lax.optimization_barrier(tuple(values) + others)[: len(values)])


class Spread:
    def __init__(self, own, first, x_last):
        self.own, self.first, self.x_last = own, first, x_last
        self.over = [send(first, TO_X), send(first, TO_Y)]
        self.twins = [send(own, TO_TWIN), send(first, TO_TWIN)]

    def turn(self, *others):
        self.over_x, self.over_y = after(self.over, *self.twins, *others)
        last = self.over_y if self.x_last else self.over_x
        self.over_d = send(last, TO_X if self.x_last else TO_Y)
        self.twins += [send(self.over_x, TO_TWIN), send(self.over_y, TO_TWIN)]
        return self.over_x

    def parts(self, *others):
        over_d = after([self.over_d], *self.twins, *others)[0]
        mine = (self.own, self.first, self.over_x, self.over_y, over_d)
        return mine + tuple(self.twins) + (send(over_d, TO_TWIN),)


def project_kernel(h_ref, w_ref, vec_ref, sel_ref, q_ref, kv_ref, mine_ref, theirs_ref):
    unit = pl.program_id(0)
    product = nn(h_ref[...], w_ref[...])

    @pl.when(unit == 0)
    def _():
        q_ref[...] = low(product + vec_ref[0:1, :])
        mine_ref[...] = low(nn(h_ref[...], sel_ref[0]))
        theirs_ref[...] = low(nn(h_ref[...], sel_ref[1]))

    @pl.when(unit == 1)
    def _():
        kv_ref[...] = low(product)

    @pl.when(unit == 2)
    def _():
        kv_ref[...] = low(product + vec_ref[1:2, :])


def project(hidden, weight, vec, sel):
    rows, width = hidden.shape
    return pl.pallas_call(
        project_kernel,
        grid=(3,),
        in_specs=[
            fixed(rows, width),
            pl.BlockSpec((None, width, width), lambda unit: (unit, 0, 0)),
            fixed(12, width),
            fixed(2, width, width // 2),
        ],
        out_specs=[
            fixed(rows, width),
            pl.BlockSpec((None, rows, width), lambda unit: (jnp.maximum(unit - 1, 0), 0, 0)),
            fixed(rows, width // 2),
            fixed(rows, width // 2),
        ],
        out_shape=[
            shaped((rows, width)),
            shaped((2, rows, width)),
            shaped((rows, width // 2)),
            shaped((rows, width // 2)),
        ],
        compiler_params=LIMIT,
        cost_estimate=cost(0.3),
        name="project",
    )(hidden, weight, vec, sel)


def attend_kernel(
    q_ref, ka_ref, kb_ref, va_ref, vb_ref, code_ref, member_ref, o_ref, ot_ref, lse_ref, bias_ref
):
    half = q_ref.shape[0]

    @pl.when(pl.program_id(0) == 0)
    def _():
        bias_ref[...] = jnp.where(code_ref[...] == member_ref[...], 0.0, NEG_FILL)

    q = q_ref[...] * jnp.bfloat16(HEAD_DIM ** (-0.5))
    lane = lax.broadcasted_iota(jnp.int32, q.shape, 1)
    keys = (ka_ref[...], kb_ref[...])
    values = (va_ref[...].T, vb_ref[...].T)
    outs = []
    for head in range(2):
        q_head = jnp.where((lane >= HEAD_DIM) == (head == 1), q, jnp.bfloat16(0))
        scores = [
            nt(keys[side], q_head) + bias_ref[side * half : (side + 1) * half, :]
            for side in range(2)
        ]
        top = jnp.maximum(
            jnp.max(scores[0], axis=0, keepdims=True), jnp.max(scores[1], axis=0, keepdims=True)
        )
        total = None
        mixed = None
        for side in range(2):
            expo = jnp.exp(scores[side] - top)
            part = jnp.sum(expo, axis=0, keepdims=True)
            value = values[side][head * HEAD_DIM : (head + 1) * HEAD_DIM, :]
            product = nn(value, low(expo))
            total = part if total is None else total + part
            mixed = product if mixed is None else mixed + product
        outs.append(mixed / total)
        lse_ref[head : head + 1, :] = top + jnp.log(total)
    joined = jnp.concatenate(outs, axis=0)
    ot_ref[...] = joined
    o_ref[...] = low(joined.T)


def pair_specs(half):
    column = pl.BlockSpec((half, 128), lambda pair: (0, pair))
    key = pl.BlockSpec((None, half, 128), lambda pair: (0, 0, pair))
    value = pl.BlockSpec((None, half, 128), lambda pair: (1, 0, pair))
    turned = pl.BlockSpec((128, half), lambda pair: (pair, 0))
    level = pl.BlockSpec((None, 2, half), lambda pair: (pair, 0, 0))
    return column, key, value, turned, level


def attend_fast(queries, kv, kv_twin, code, member):
    half, width = queries.shape
    column, key, value, turned, level = pair_specs(half)
    return pl.pallas_call(
        attend_kernel,
        grid=(width // 128,),
        in_specs=[column, key, key, value, value, fixed(2 * half, 1), fixed(1, half)],
        out_specs=[column, turned, level],
        out_shape=[
            shaped((half, width)),
            shaped((width, half), jnp.float32),
            shaped((width // 128, 2, half), jnp.float32),
        ],
        scratch_shapes=[pltpu.VMEM((2 * half, half), jnp.float32)],
        compiler_params=LIMIT,
        cost_estimate=cost(0.3),
        name="attend_forward",
    )(queries, kv, kv_twin, kv, kv_twin, code, member)


def attend_back_kernel(
    q_ref, g_ref, ka_ref, kb_ref, va_ref, vb_ref, ot_ref, lse_ref, code_ref, member_ref,
    dq_ref, own_ref, twin_ref, bias_ref,
):
    half = q_ref.shape[0]

    @pl.when(pl.program_id(0) == 0)
    def _():
        bias_ref[...] = jnp.where(code_ref[...] == member_ref[...], 0.0, NEG_FILL)

    scale = HEAD_DIM ** (-0.5)
    q = q_ref[...] * jnp.bfloat16(scale)
    grad = g_ref[...]
    lane = lax.broadcasted_iota(jnp.int32, q.shape, 1)
    keys = (ka_ref[...], kb_ref[...])
    turned = (keys[0].T, keys[1].T)
    values = (va_ref[...], vb_ref[...])
    product = ot_ref[...] * wide(grad).T
    key_sums = [None, None]
    value_sums = [None, None]
    query_parts = []
    for head in range(2):
        rows = slice(head * HEAD_DIM, (head + 1) * HEAD_DIM)
        chosen = (lane >= HEAD_DIM) == (head == 1)
        q_head = jnp.where(chosen, q, jnp.bfloat16(0))
        g_head = jnp.where(chosen, grad, jnp.bfloat16(0))
        delta = jnp.sum(product[rows, :], axis=0, keepdims=True)
        level = lse_ref[head : head + 1, :]
        query_sum = None
        for side in range(2):
            scores = nt(keys[side], q_head) + bias_ref[side * half : (side + 1) * half, :]
            prob = jnp.exp(scores - level)
            slope = nt(values[side], g_head)
            steep = low(prob * (slope - delta))
            value_part = nn(low(prob), g_head)
            key_part = nn(steep, q_head)
            query_part = nn(turned[side][rows, :], steep)
            value_sums[side] = value_part if head == 0 else value_sums[side] + value_part
            key_sums[side] = key_part if head == 0 else key_sums[side] + key_part
            query_sum = query_part if side == 0 else query_sum + query_part
        query_parts.append(query_sum * scale)
    dq_ref[...] = low(jnp.concatenate(query_parts, axis=0).T)
    own_ref[0] = key_sums[0]
    own_ref[1] = value_sums[0]
    twin_ref[0] = low(key_sums[1])
    twin_ref[1] = low(value_sums[1])


def attend_back_fast(queries, grad, kv, kv_twin, ot, lse, code, member, spend):
    half, width = queries.shape
    column, key, value, turned, level = pair_specs(half)
    both = pl.BlockSpec((2, half, 128), lambda pair: (0, 0, pair))
    return pl.pallas_call(
        attend_back_kernel,
        grid=(width // 128,),
        in_specs=[column, column, key, key, value, value, turned, level]
        + [fixed(2 * half, 1), fixed(1, half)],
        out_specs=[column, both, both],
        out_shape=[
            shaped((half, width)),
            shaped((2, half, width), jnp.float32),
            shaped((2, half, width)),
        ],
        scratch_shapes=[pltpu.VMEM((2 * half, half), jnp.float32)],
        compiler_params=LIMIT,
        cost_estimate=cost(spend),
        name="attend_backward",
    )(queries, grad, kv, kv_twin, kv, kv_twin, ot, lse, code, member)


def normal_parts(value):
    scaled = value * 0.7071067811865476
    size = jnp.abs(scaled)
    square = size * size
    t = 1.0 / (1.0 + 0.5 * size)
    series = 0.17087277
    for factor in (
        -0.82215223, 1.48851587, -1.13520398, 0.27886807, -0.18628806,
        0.09678418, 0.37409196, 1.00002368, -1.26551223,
    ):
        series = series * t + factor
    tail = 0.5 * t * jnp.exp(series - square)
    cumulative = jnp.where(value >= 0, 1.0 - tail, tail)
    density = 0.3989422804014327 * jnp.exp(-square)
    return cumulative, density


def row_norm(resid):
    offsets = resid - jnp.mean(resid, axis=-1, keepdims=True)
    spread_of = jnp.mean(offsets * offsets, axis=-1, keepdims=True)
    factor = lax.rsqrt(spread_of + 1e-05)
    return offsets * factor, factor


def post_kernel(
    where_ref, o_ref, h_ref, wo_ref, up_ref, down_ref, vec_ref, sel_ref,
    h_out, hl_out, n1_out, t1_out, n2_out, t2_out, slope_out, mine_out, theirs_out,
    y_ref, yl_ref, f_ref,
):
    step = pl.program_id(0)
    half_width = mine_out.shape[2]

    @pl.when(step == 0)
    def _():
        attended = o_ref[...]
        branch = nn(attended, wo_ref[...]) + vec_ref[2:3, :]
        normed, factor = row_norm(wide(h_ref[...]) + branch)
        middle = normed * vec_ref[3:4, :] + vec_ref[4:5, :]
        n1_out[...] = normed
        t1_out[...] = factor
        y_ref[...] = middle
        yl_ref[...] = low(middle)
        mine_out[4] = low(nn(yl_ref[...], sel_ref[0]))
        theirs_out[4] = low(nn(yl_ref[...], sel_ref[1]))
        mine_out[5] = low(nn(attended, sel_ref[0]))
        theirs_out[5] = low(nn(attended, sel_ref[1]))

    inner = nn(yl_ref[...], up_ref[...]) + vec_ref[pl.ds(8 + step, 1), :]
    cumulative, density = normal_parts(inner)
    slope_out[...] = low(cumulative + inner * density)
    active = low(inner * cumulative)
    first, second = active[:, :half_width], active[:, half_width:]
    swap = where_ref[2] == 1
    mine_out[step] = jnp.where(swap, second, first)
    theirs_out[step] = jnp.where(swap, first, second)
    part = nn(active, down_ref[...])

    @pl.when(step == 0)
    def _():
        f_ref[...] = part

    @pl.when(step > 0)
    def _():
        f_ref[...] += part

    @pl.when(step == 3)
    def _():
        normed, factor = row_norm(y_ref[...] + (f_ref[...] + vec_ref[5:6, :]))
        result = normed * vec_ref[6:7, :] + vec_ref[7:8, :]
        n2_out[...] = normed
        t2_out[...] = factor
        h_out[...] = result
        hl_out[...] = low(result)


def unit_spec(width, index):
    return pl.BlockSpec((None, width, width), lambda step: (index, 0, 0))


def step_spec(width):
    return pl.BlockSpec((None, width, width), lambda step: (step, 0, 0))


def column_spec(rows, width):
    return pl.BlockSpec((rows, width), lambda step: (0, step))


def post(where, attended, hidden, front, up, down, vec, sel):
    rows, width = attended.shape
    half = width // 2
    full = fixed(rows, width)
    thin = fixed(rows, 1)
    return pl.pallas_call(
        post_kernel,
        grid=(4,),
        in_specs=[
            SMEM, full, full, unit_spec(width, 3), step_spec(width), step_spec(width),
            fixed(12, width), fixed(2, width, half),
        ],
        out_specs=[full, full, full, thin, full, thin, column_spec(rows, width)]
        + [fixed(6, rows, half)] * 2,
        out_shape=[
            shaped((rows, width), jnp.float32),
            shaped((rows, width)),
            shaped((rows, width), jnp.float32),
            shaped((rows, 1), jnp.float32),
            shaped((rows, width), jnp.float32),
            shaped((rows, 1), jnp.float32),
            shaped((rows, 4 * width)),
        ]
        + [shaped((6, rows, half))] * 2,
        scratch_shapes=[
            pltpu.VMEM((rows, width), jnp.float32),
            pltpu.VMEM((rows, width), jnp.bfloat16),
            pltpu.VMEM((rows, width), jnp.float32),
        ],
        compiler_params=LIMIT,
        cost_estimate=cost(0.3),
        name="post",
    )(where, attended, hidden, front, up, down, vec, sel)


def norm_back(incoming, normed, factor, gain):
    scaled = incoming * gain
    return factor * (
        scaled
        - jnp.mean(scaled, axis=-1, keepdims=True)
        - normed * jnp.mean(scaled * normed, axis=-1, keepdims=True)
    )


def column_sum(value):
    return jnp.sum(value, axis=0, keepdims=True)


def post_back_kernel(
    e_ref, n1_ref, t1_ref, n2_ref, t2_ref, slope_ref, wo_ref, up_ref, down_ref, vec_ref,
    all_out, do_out, dr_out, sums_out,
    r_ref, y_ref,
):
    step = pl.program_id(0)

    @pl.when(step == 0)
    def _():
        incoming = wide(e_ref[...])
        normed = n2_ref[...]
        resid = norm_back(incoming, normed, t2_ref[...], vec_ref[6:7, :])
        r_ref[...] = resid
        rounded = low(resid)
        all_out[4] = rounded
        sums_out[0:2, :] = jnp.zeros((2, sums_out.shape[1]), jnp.float32)
        sums_out[5:6, :] = column_sum(wide(rounded))
        sums_out[6:7, :] = column_sum(incoming * normed)
        sums_out[7:8, :] = column_sum(incoming)

    steep = low(nt(all_out[4], down_ref[...]) * wide(slope_ref[...]))
    all_out[step] = steep
    sums_out[pl.ds(8 + step, 1), :] = column_sum(wide(steep))
    part = nt(steep, up_ref[...])

    @pl.when(step == 0)
    def _():
        y_ref[...] = part

    @pl.when(step > 0)
    def _():
        y_ref[...] += part

    @pl.when(step == 3)
    def _():
        incoming = r_ref[...] + y_ref[...]
        normed = n1_ref[...]
        resid = norm_back(incoming, normed, t1_ref[...], vec_ref[3:4, :])
        dr_out[...] = resid
        rounded = low(resid)
        all_out[5] = rounded
        do_out[...] = low(nt(rounded, wo_ref[...]))
        sums_out[2:3, :] = column_sum(wide(rounded))
        sums_out[3:4, :] = column_sum(incoming * normed)
        sums_out[4:5, :] = column_sum(incoming)


def post_back(upstream, n1, t1, n2, t2, slope, front, up, down, vec, spend):
    rows, width = upstream.shape
    full = fixed(rows, width)
    thin = fixed(rows, 1)
    return pl.pallas_call(
        post_back_kernel,
        grid=(4,),
        in_specs=[
            full, full, thin, full, thin, column_spec(rows, width),
            unit_spec(width, 3), step_spec(width), step_spec(width), fixed(12, width),
        ],
        out_specs=[fixed(6, rows, width), full, full, fixed(12, width)],
        out_shape=[
            shaped((6, rows, width)),
            shaped((rows, width)),
            shaped((rows, width), jnp.float32),
            shaped((12, width), jnp.float32),
        ],
        scratch_shapes=[
            pltpu.VMEM((rows, width), jnp.float32),
            pltpu.VMEM((rows, width), jnp.float32),
        ],
        compiler_params=LIMIT,
        cost_estimate=cost(spend),
        name="post_back",
    )(upstream, n1, t1, n2, t2, slope, front, up, down, vec)


def project_back_kernel(
    dq_ref, own_ref, got_ref, w_ref, dr_ref, dm_out, dx_out, dxl_out, sums_out
):
    unit = pl.program_id(0)

    @pl.when(unit == 0)
    def _():
        dm_out[...] = dq_ref[...]

    @pl.when(unit > 0)
    def _():
        dm_out[...] = low(own_ref[...] + wide(got_ref[...]))

    grad = dm_out[...]
    part = nt(grad, w_ref[...])
    total = column_sum(wide(grad))

    @pl.when(unit == 0)
    def _():
        dx_out[...] = dr_ref[...] + part
        sums_out[0:1, :] = total

    @pl.when(unit > 0)
    def _():
        dx_out[...] += part
        sums_out[1:2, :] = total

    @pl.when(unit == 2)
    def _():
        dxl_out[...] = low(dx_out[...])


def project_back(dq, own, got, front, dr, spend):
    rows, width = dq.shape
    full = fixed(rows, width)
    late = pl.BlockSpec((None, rows, width), lambda unit: (jnp.maximum(unit - 1, 0), 0, 0))
    return pl.pallas_call(
        project_back_kernel,
        grid=(3,),
        in_specs=[full, late, late, step_spec(width), full],
        out_specs=[
            pl.BlockSpec((None, rows, width), lambda unit: (unit, 0, 0)),
            full, full, fixed(2, width),
        ],
        out_shape=[
            shaped((3, rows, width)),
            shaped((rows, width), jnp.float32),
            shaped((rows, width)),
            shaped((2, width), jnp.float32),
        ],
        compiler_params=LIMIT,
        cost_estimate=cost(spend),
        name="project_back",
    )(dq, own, got, front, dr)


def tn(left, right):
    return nn(left.T, right)


def split_store(keep_ref, give_ref, bit, x_first, piece_of, store):
    for other in range(2):
        pair = []
        for side in range(2):
            rep = (other * 2 + side) if x_first else (side * 2 + other)
            pair.append(low(piece_of(rep)))
        store(keep_ref, other, jnp.where(bit == 0, pair[0], pair[1]))
        store(give_ref, other, jnp.where(bit == 0, pair[1], pair[0]))


def column_store(ref_pair, bit, x_first, product, unit):
    keep_ref, give_ref = ref_pair
    for level in range(4):
        base = level * 4 * UNIT

        def piece_of(rep):
            return product[base + rep * UNIT : base + (rep + 1) * UNIT, :]

        def store(ref, other, value):
            ref[level, other, unit] = value

        split_store(keep_ref, give_ref, bit, x_first, piece_of, store)


def front_grad_kernel(
    bit_ref, xm_ref, xt_ref, om_ref, ot_ref, dm_ref, dmt_ref, da_ref, dat_ref,
    keep_x, give_x, keep_y, give_y,
):
    unit = pl.program_id(0)

    def store(product, index, x_first):
        pair = (keep_x, give_x) if x_first else (keep_y, give_y)
        column_store(pair, bit_ref[0 if x_first else 1], x_first, product, index)

    @pl.when(unit < 2)
    def _():
        store(tn(xm_ref[...], dm_ref[...]) + tn(xt_ref[...], dmt_ref[...]), unit, True)

    @pl.when(unit == 2)
    def _():
        store(tn(xm_ref[...], dm_ref[...]) + tn(xt_ref[...], dmt_ref[...]), 0, False)

    @pl.when(unit == 3)
    def _():
        store(tn(om_ref[...], da_ref[...]) + tn(ot_ref[...], dat_ref[...]), 1, False)


def block_spec(rows, width, index):
    return pl.BlockSpec((None, rows, width), lambda step: (index, 0, 0))


def front_grad(bits, xm, xt, mine, theirs, dm, dmt, da, dat, spend):
    rows, half = xm.shape
    width = da.shape[2]
    late = pl.BlockSpec((None, rows, width), lambda unit: (jnp.minimum(unit, 2), 0, 0))
    shape = (4, 2, 2, UNIT, width)
    return pl.pallas_call(
        front_grad_kernel,
        grid=(4,),
        in_specs=[SMEM, fixed(rows, half), fixed(rows, half)]
        + [block_spec(rows, half, 5)] * 2
        + [late, late]
        + [block_spec(rows, width, 5)] * 2,
        out_specs=[fixed(*shape)] * 4,
        out_shape=[shaped(shape)] * 4,
        compiler_params=LIMIT,
        cost_estimate=cost(spend),
        name="front_grad",
    )(bits, xm, xt, mine, theirs, dm, dmt, da, dat)


def feed_grad_kernel(
    x_first, bit_ref, ym_ref, yt_ref, gm_ref, gt_ref, dz_ref, dzt_ref, df_ref, dft_ref,
    keep_up, give_up, keep_down, give_down,
):
    step = pl.program_id(0)
    up_bit = bit_ref[0 if x_first else 1]
    down_bit = bit_ref[1 if x_first else 0]

    @pl.when(step < 4)
    def _():
        product = tn(ym_ref[...], dz_ref[...]) + tn(yt_ref[...], dzt_ref[...])
        column_store((keep_up, give_up), up_bit, x_first, product, step)

    @pl.when(step >= 4)
    def _():
        product = tn(gm_ref[...], df_ref[...]) + tn(gt_ref[...], dft_ref[...])
        for sub in range(4):

            def piece_of(rep):
                base = (rep * 4 + sub) * UNIT
                return product[base : base + UNIT, :]

            def store(ref, other, value):
                ref[step - 4, other, sub] = value

            split_store(keep_down, give_down, down_bit, not x_first, piece_of, store)


def feed_grad(x_first, bits, mine, theirs, slopes, slopes_twin, spend):
    rows, half = mine.shape[1:]
    width = slopes.shape[2]
    early = pl.BlockSpec((None, rows, width), lambda step: (jnp.minimum(step, 3), 0, 0))
    late = pl.BlockSpec((None, rows, half), lambda step: (jnp.maximum(step - 4, 0), 0, 0))
    shape = (4, 2, 4, UNIT, width)
    return pl.pallas_call(
        functools.partial(feed_grad_kernel, x_first),
        grid=(8,),
        in_specs=[SMEM]
        + [block_spec(rows, half, 4)] * 2
        + [late, late, early, early]
        + [block_spec(rows, width, 4)] * 2,
        out_specs=[fixed(*shape)] * 4,
        out_shape=[shaped(shape)] * 4,
        compiler_params=LIMIT,
        cost_estimate=cost(spend),
        name="feed_grad",
    )(bits, mine, theirs, mine, theirs, slopes, slopes_twin, slopes, slopes_twin)


def halve_kernel(low_ref, keep_x, got_x, keep_y, got_y, keep_out, give_out):
    start = jnp.where(low_ref[0] == 1, 0, 2)
    for index, (keep, got) in enumerate(((keep_x, got_x), (keep_y, got_y))):
        for out, begin in ((keep_out, start), (give_out, 2 - start)):
            for level in range(2):
                out[index, level] = low(wide(keep[begin + level]) + wide(got[begin + level]))


def halve_sum(is_low, keeps, gots, spend):
    count, width = keeps[0].shape[2], keeps[0].shape[4]
    whole = pl.BlockSpec((4, None, count, UNIT, width), lambda other: (0, other, 0, 0, 0))
    half = pl.BlockSpec((2, 2, None, count, UNIT, width), lambda other: (0, 0, other, 0, 0, 0))
    return pl.pallas_call(
        halve_kernel,
        grid=(2,),
        in_specs=[SMEM] + [whole] * 4,
        out_specs=[half] * 2,
        out_shape=[shaped((2, 2, 2, count, UNIT, width))] * 2,
        compiler_params=LIMIT,
        cost_estimate=cost(spend),
        name="halve_sum",
    )(is_low.astype(jnp.int32).reshape(1), keeps[0], gots[0], keeps[1], gots[1])


class Reduction:
    def __init__(self, pairs, bits, is_low, is_core):
        self.keeps = [pair[0] for pair in pairs]
        self.firsts = [pair[2] for pair in pairs]
        self.bits, self.is_low, self.is_core = bits, is_low, is_core
        self.got = [send(pair[1], TO_X if pair[2] else TO_Y) for pair in pairs]

    def across(self, spend, *others):
        got = after(self.got, *others)
        self.keep, give = halve_sum(self.is_low, self.keeps, got, spend)
        self.mid = send(give, TO_MID)
        return give

    def join(self, other):
        self.keep = jnp.concatenate([self.keep, other.keep], axis=3)
        self.mid = jnp.concatenate([self.mid, other.mid], axis=3)

    def outward(self, *others):
        mid = after([self.mid], *others)[0]
        stage = low(wide(self.keep) + wide(mid))
        outer = jnp.where(self.is_low, stage[:, 0], stage[:, 1])
        self.inner = jnp.where(self.is_low, stage[:, 1], stage[:, 0])
        self.side = send(outer, TO_SIDE)
        return outer

    def turn(self, *others):
        side = after([self.side], *others)[0]
        stage = jnp.where(self.is_core, self.inner, side)
        self.pieces = [stage[index] for index in range(len(self.firsts))]
        self.over = [
            send(piece, TO_Y if first else TO_X)
            for piece, first in zip(self.pieces, self.firsts)
        ]
        return stage

    def share(self, *others):
        over = after(self.over, *others)
        self.sums = [low(wide(piece) + wide(item)) for piece, item in zip(self.pieces, over)]
        self.got = [
            send(piece, TO_X if first else TO_Y) for piece, first in zip(self.sums, self.firsts)
        ]
        return self.sums[0]

    def finish(self, *others):
        return list(zip(self.sums, after(self.got, *others)))


def unpack_kernel(plan, bit_ref, *refs):
    outs = refs[-4:]
    width = outs[1].shape[1]
    for index, (x_first, units) in enumerate(plan):
        piece, got = refs[2 * index], refs[2 * index + 1]
        bit = bit_ref[0 if x_first else 1]
        for other in range(2):
            for side in range(2):
                rep = (other * 2 + side) if x_first else (side * 2 + other)
                for unit, (target, place) in enumerate(units):
                    value = wide(jnp.where(bit == side, piece[other, unit], got[other, unit]))
                    if target < 3:
                        rows = slice(rep * UNIT, (rep + 1) * UNIT)
                        outs[target][rows, place * width : (place + 1) * width] = value
                    else:
                        base = (rep * 4 + place) * UNIT
                        outs[target][base : base + UNIT, :] = value


def unpack(bits, pairs, plan, layer, layers, before):
    width = pairs[0][0].shape[3]
    shapes = [(4 * UNIT, 3 * width), (4 * UNIT, width), (4 * UNIT, 4 * width), (16 * UNIT, width)]
    arrays = [item for pair in pairs for item in pair]
    first = 1 + len(arrays)
    return pl.pallas_call(
        functools.partial(unpack_kernel, plan),
        grid=(1,),
        in_specs=[SMEM]
        + [fixed(*item.shape) for item in arrays]
        + [pl.BlockSpec(memory_space=pl.ANY) for _ in before],
        out_specs=[pl.BlockSpec((None,) + shape, lambda step: (layer, 0, 0)) for shape in shapes],
        out_shape=[shaped((layers,) + shape, jnp.float32) for shape in shapes],
        input_output_aliases={first + index: index for index in range(len(before))},
        compiler_params=LIMIT,
        cost_estimate=cost(3),
        name="unpack",
    )(bits, *arrays, *before)


def body_fast(
    inputs, cotangent, lengths, dealing, key_mask,
    entry_weight, exit_weight, expand_weight, shrink_weight, vectors,
):
    rows, width = inputs.shape
    layers = entry_weight.shape[0]
    group_rows = 8 * rows
    half_rows = group_rows // 2
    core_rows = half_rows // 2
    rep = lax.axis_index("rep")
    shard = lax.axis_index("shard")
    depth, twin = shard // 2, shard % 2
    is_low = depth <= 1
    is_core = (depth == 1) | (depth == 2)
    where = jnp.stack([depth, rep, twin]).astype(jnp.int32)
    bits = (rep & 1, rep >> 1)
    bit_words = jnp.stack(bits).astype(jnp.int32)

    def order(four):
        own, near, middle, far = four
        return jnp.where(
            is_low, jnp.stack([near, own, middle, far]), jnp.stack([far, middle, own, near])
        )

    def absolute(mine, theirs):
        one, two = order(mine), order(theirs)
        return jnp.where(twin == 0, jnp.stack([one, two], 1), jnp.stack([two, one], 1))

    def own_piece(pack):
        piece = lax.dynamic_index_in_dim(pack, rep, 0, keepdims=False)
        return piece.reshape(-1, width)

    def units_of(item):
        return item.reshape(-1, UNIT, width)

    def pack_front(entry, leaving):
        return jnp.concatenate([by_columns(entry), by_columns(leaving)], axis=1)

    def pack_feed(expand, shrink):
        return jnp.concatenate([by_columns(expand), low(shrink).reshape(4, 4, UNIT, width)], axis=1)

    def by_columns(weight):
        count = weight.shape[1] // width
        return low(weight).reshape(4, UNIT, count, width).transpose(0, 2, 1, 3)

    extra = layers * vectors.shape[1] // width
    tail = low(vectors).reshape(extra, width)
    table = jnp.concatenate([dealing // 64, dealing % 64, key_mask], axis=0)
    table = low(table).reshape(1, width)
    filler = jnp.zeros((7 - extra, width), jnp.bfloat16)
    rows_in = jnp.concatenate([inputs, tail, table, filler], axis=0)

    def group(items, begin, end):
        return jnp.stack([units_of(item[begin:end]) for item in items])

    front_zero = pack_front(entry_weight[0], exit_weight[0])
    piece = own_piece(front_zero)
    near = send(piece, TO_SIDE)
    middle = send(piece, TO_MID)
    feed_zero = pack_feed(expand_weight[0], shrink_weight[0])
    in_rows = rows_in.shape[0]
    far = send(near, TO_MID)
    first = jnp.stack([units_of(item) for item in (near, middle, far)])
    front_spread = Spread(front_zero, first, False)
    rows_late, twin_late, lengths = after([rows_in, twin, lengths], first)
    second = jnp.concatenate([rows_late, own_piece(feed_zero)], axis=0)
    second_near = send(second, TO_SIDE)
    second_middle = send(second, TO_MID)
    second_far = send(second_near, TO_MID)

    entry_late, exit_late, expand_late, shrink_late, cotangent_late = after(
        [entry_weight[1], exit_weight[1], expand_weight[1], shrink_weight[1], cotangent], first
    )
    front_one = pack_front(entry_late, exit_late)
    feed_one = pack_feed(expand_late, shrink_late)
    third = jnp.concatenate([own_piece(front_one), own_piece(feed_one), cotangent_late], axis=0)
    ready = front_spread.turn()

    second_middle, second_far = after([second_middle, second_far], ready)
    four = (second, second_near, second_middle, second_far)
    mine = jnp.stack([item[:in_rows] for item in four])
    theirs = send(mine, TO_TWIN)
    feed_spread = Spread(feed_zero, tie(group(four[1:], in_rows, in_rows + 8 * UNIT), ready), True)
    third = tie(third, ready)
    third_near = send(third, TO_SIDE)
    third_middle = send(third, TO_MID)
    fronts = [assemble(where, front_spread.parts(feed_spread.first, mine, third), 0, False)]

    header = absolute(tuple(mine[:, rows:]), tuple(theirs[:, rows:]))
    header = header.reshape(8, 8, width)
    vector_all = wide(header[:, :extra]).reshape(8, layers, vectors.shape[1])
    vector_all = jnp.transpose(vector_all, (1, 0, 2)).reshape(layers, 12, width)
    numbers = wide(header[:, extra]).reshape(8, 3, rows)
    dealt_all = (numbers[:, 0] * 64 + numbers[:, 1]).astype(jnp.int32).reshape(group_rows)
    mask_all = numbers[:, 2].reshape(group_rows)

    member, leading = sequence_ids(lengths[0], group_rows)
    usable = (mask_all == 1) | leading
    code = jnp.where(usable, member, -1)
    longest = jnp.argmax(lengths[0])
    begin = jnp.cumsum(lengths[0])[longest] - lengths[0][longest]
    spot = jnp.arange(half_rows, dtype=jnp.int32)

    def halve(values, low_side):
        inside = lax.dynamic_slice_in_dim(values, begin, half_rows, 0)
        outside = jnp.where(spot < begin, values[:half_rows], values[half_rows:])
        return jnp.where(low_side, inside, outside)

    def cores(values):
        own = lax.dynamic_slice_in_dim(values, twin * core_rows, core_rows, 0)
        other = lax.dynamic_slice_in_dim(values, (1 - twin) * core_rows, core_rows, 0)
        return own, other

    code_half = jnp.concatenate(cores(halve(code, is_low))).reshape(half_rows, 1)
    member_own = cores(halve(member, is_low))[0].reshape(1, core_rows)
    dealt_near = cores(halve(dealt_all, is_low))
    dealt_far = cores(halve(dealt_all, ~is_low))

    block = jnp.arange(width, dtype=jnp.int32)
    place = jnp.arange(width // 2, dtype=jnp.int32)
    chunk = 4 * UNIT
    source = (place // chunk) * (2 * chunk) + place % chunk
    cores_at = jnp.stack([twin_late, 1 - twin_late])
    sel = low(block[None, :, None] == (source[None, :] + cores_at[:, None] * chunk)[:, None, :])

    local = jnp.arange(rows, dtype=jnp.int32)
    bases = jnp.stack(
        [
            (depth ^ flip) * (2 * rows) + (twin ^ side) * rows
            for side in range(2)
            for flip in (0, 1, 3, 2)
        ]
    ).astype(jnp.int32)
    source_ids = (bases[:, None] + local[None, :]).reshape(8, 1, rows)
    want_in = dealt_near[0].reshape(core_rows, 1)
    theirs, third_near = after([theirs, third_near], fronts[0])
    third_far = send(third_near, TO_MID)
    hidden_low = gather_rows((mine, tie(theirs, third_near)), source_ids, want_in, 0.3)

    result_ids = jnp.stack([dealt_near[0], dealt_far[0], dealt_near[1], dealt_far[1]]).reshape(
        4, 1, core_rows
    )
    want_out = jnp.concatenate([source_ids[0, 0], source_ids[1, 0]]).reshape(2 * rows, 1)

    def deliver(pieces, spend):
        pieces = [piece[None] for piece in pieces]
        found = gather_rows(pieces, result_ids, want_out, spend)
        return found, send(found[rows:], TO_SIDE)

    saved = []
    def begin(layer):
        queries, kv, xm, xt = project(hidden_low, fronts[layer], vector_all[layer], sel)
        return queries, kv, send(kv, TO_TWIN), xm, send(xt, TO_TWIN)

    def attention(queries, kv, kv_twin):
        return attend_fast(queries, kv, kv_twin, code_half, member_own)

    def complete(layer, attended):
        results = post(
            where, attended, hidden, fronts[layer], ups[layer], downs[layer],
            vector_all[layer], sel,
        )
        return results, send(results[8], TO_TWIN)

    def record(start, middle, results, others):
        queries, kv, kv_twin, xm, xo = start
        saved.append(
            (queries, kv, kv_twin) + tuple(middle[1:]) + tuple(results[2:7])
            + (xm, xo, results[7], others)
        )

    hidden = hidden_low
    ready = feed_spread.turn(fronts[0])
    hidden_low, third_middle = after([hidden_low, third_middle], ready)
    hidden_low = tie(hidden_low, third_middle)
    start = begin(0)
    middle = attention(*start[:3])
    parts = feed_spread.parts(middle[0])
    third_far = tie(third_far, middle[0])
    four = (third, third_near, third_middle, third_far)
    split = 12 * UNIT
    front_spread = Spread(front_one, group(four[1:], 0, 4 * UNIT), True)
    cotangent_mine = jnp.stack([item[split:] for item in four])
    ups = [assemble(where, parts, 0, False)]
    downs = [assemble(where, parts, 4, True)]
    ready = front_spread.turn(ups[0], downs[0])
    feed_spread = Spread(feed_one, tie(group(four[1:], 4 * UNIT, split), ready), False)
    cotangent_theirs = send(cotangent_mine, TO_TWIN)
    held = [feed_spread.first, cotangent_theirs] + front_spread.twins + feed_spread.twins
    results, others = complete(0, tie(middle[0], ready, *held))
    hidden, hidden_low = results[:2]
    record(start, middle, results, others)
    ready = feed_spread.turn(hidden_low)
    fronts.append(assemble(where, front_spread.parts(ready), 0, False))
    start = begin(1)
    upstream = gather_rows(
        (cotangent_mine, tie(cotangent_theirs, start[0])), source_ids, want_in, 0.3
    )
    middle = attention(tie(start[0], upstream), start[1], start[2])
    parts = feed_spread.parts(middle[0])
    ups.append(assemble(where, parts, 0, False))
    downs.append(assemble(where, parts, 4, True))
    results, others = complete(1, middle[0])
    hidden, hidden_low = results[:2]
    record(start, middle, results, others)
    result_mid = send(hidden_low, TO_MID)
    result_twin = send(hidden_low, TO_TWIN)

    def start_back(layer, grad, spend):
        n1, t1, n2, t2, slope = saved[layer][5:10]
        slopes, do, dr, sums = post_back(
            grad, n1, t1, n2, t2, slope,
            fronts[layer], ups[layer], downs[layer], vector_all[layer], spend,
        )
        return slopes, send(slopes, TO_TWIN), do, dr, sums

    def attention_back(layer, do, spend):
        queries, kv, kv_twin, ot, lse = saved[layer][:5]
        return attend_back_fast(
            queries, do, kv, kv_twin, ot, lse, code_half, member_own, spend
        )

    def feed_part(layer, x_first, slopes, slopes_twin, spend):
        mine, others = saved[layer][12:14]
        keep_up, give_up, keep_down, give_down = feed_grad(
            x_first, bit_words, mine, others, slopes, slopes_twin, spend
        )
        work = Reduction(
            [(keep_up, give_up, x_first), (keep_down, give_down, not x_first)],
            bits, is_low, is_core,
        )
        return work, keep_up

    def front_part(layer, slopes, slopes_twin, dm, dm_twin, spend):
        xm, xo, mine, others = saved[layer][10:14]
        keep_x, give_x, keep_y, give_y = front_grad(
            bit_words, xm, xo, mine, others, dm, dm_twin, slopes, slopes_twin, spend
        )
        work = Reduction(
            [(keep_x, give_x, True), (keep_y, give_y, False)], bits, is_low, is_core
        )
        return work, keep_x

    upstream = tie(upstream, saved[0][11], saved[0][13])
    slopes_b, slopes_tb, do, dr, sums_b = start_back(1, upstream, 16)
    dq, own, give = attention_back(1, do, 21)
    got = send(give, TO_TWIN)
    feed_b, mark = feed_part(1, True, slopes_b, tie(slopes_tb, dq, saved[1][11], result_twin), 12)
    pair = (hidden_low, tie(result_mid, mark))
    pair += (result_twin, send(pair[1], TO_TWIN))
    dm_b, grad, _, head_b = project_back(dq, own, got, fronts[1], tie(dr, mark, pair[1]), 0.5)
    dm_tb = send(dm_b, TO_TWIN)
    found, output_side = deliver(after(pair, head_b), 0.5)
    slopes_a, slopes_ta, do, dr, sums_a = start_back(0, tie(grad, found), 0.5)
    ready = feed_b.across(3, do)
    dq, own, give = attention_back(0, tie(do, ready), 45)
    got = send(give, TO_TWIN)
    front_b, mark = front_part(1, slopes_b, slopes_tb, dm_b, tie(dm_tb, dq), 0.5)
    feed_a, mark = feed_part(0, False, slopes_a, tie(slopes_ta, mark, output_side, feed_b.mid), 12)
    ready = front_b.across(2, mark)
    dm_a, grad, grad_low, head_a = project_back(
        dq, own, got, fronts[0], tie(dr, ready), 0.5
    )
    dm_ta = send(dm_a, TO_TWIN)
    grad_mid = send(grad_low, TO_MID)
    grad_twin = send(grad_low, TO_TWIN)

    vectors_all = [
        jnp.concatenate([head_sums, sums[2:]], axis=0)
        for head_sums, sums in ((head_a, sums_a), (head_b, sums_b))
    ]
    joined = jnp.stack([item.reshape(-1) for item in vectors_all])
    joined = jnp.transpose(joined.reshape(layers, 4, 2, vectors.shape[1]), (1, 2, 0, 3))
    vector_keep = lax.dynamic_index_in_dim(joined, twin, 1, keepdims=False)
    vector_give = lax.dynamic_index_in_dim(joined, 1 - twin, 1, keepdims=False)
    vector_twin = send(vector_give, TO_TWIN)

    ready = feed_a.across(25, grad_low, front_b.mid)
    front_a, mark = front_part(0, slopes_a, slopes_ta, dm_a, tie(dm_ta, vector_give, ready, grad_twin), 0.5)

    feed_b.join(front_b)
    ready = feed_b.outward(mark)
    vector_stage = vector_keep + tie(vector_twin, ready)
    vector_over = send(vector_stage, TO_X)
    pair = (grad_low, tie(grad_mid, vector_stage), grad_twin)
    pair += (send(pair[1], TO_TWIN),)
    found_in, input_side = deliver(pair, 0.5)
    ready = feed_b.turn(found_in)
    vector_stage = vector_stage + tie(vector_over, ready)
    vector_over = send(vector_stage, TO_Y)

    ready = front_a.across(0.5, vector_stage)
    ready = feed_b.share(ready)
    vector_stage = vector_stage + tie(vector_over, ready)
    vector_give = jnp.where(is_low, vector_stage[2:4], vector_stage[0:2])
    vector_keep = jnp.where(is_low, vector_stage[0:2], vector_stage[2:4])
    vector_mid = send(vector_give, TO_MID)
    ready = feed_a.outward(vector_give)
    ups_at = tuple((2, place) for place in range(4))
    downs_at = tuple((3, place) for place in range(4))
    early_at, late_at = ((0, 0), (0, 1)), ((0, 2), (1, 0))
    plan = ((True, ups_at + early_at), (False, downs_at + late_at))

    ready = front_a.outward(ready)
    grads = unpack(bit_words, feed_b.finish(ready), plan, 1, layers, ())
    vector_stage = vector_keep + tie(vector_mid, ready)
    vector_outer = jnp.where(is_low, vector_stage[0], vector_stage[1])
    vector_inner = jnp.where(is_low, vector_stage[1], vector_stage[0])
    vector_side = send(vector_outer, TO_SIDE)
    ready = feed_a.turn(vector_outer, grads[1])
    output = jnp.where(is_core, found[:rows], output_side)
    input_grad = wide(jnp.where(is_core, found_in[:rows], tie(input_side, ready)))

    ready = front_a.turn(ready)
    ready_two = feed_a.share(ready)
    ready = front_a.share(ready_two)
    pairs = feed_a.finish(ready) + front_a.finish(ready)
    plan = ((False, ups_at), (True, downs_at), (True, early_at), (False, late_at))
    entry_grad, exit_grad, expand_grad, shrink_grad = unpack(
        bit_words, pairs, plan, 0, layers, grads
    )
    vector_grad = jnp.where(is_core, vector_inner, tie(vector_side, ready))
    return (output, input_grad, entry_grad, exit_grad, expand_grad, shrink_grad, vector_grad)


def solution(mesh):
    placed = (
        P(("rep", "shard"), None),
        P(("rep", "shard"), None),
        P("rep", None),
        P("rep", "shard"),
        P("rep", "shard"),
        P(None, "shard", None),
        P(None, "shard", None),
        P(None, "shard", None),
        P(None, "shard", None),
        P(None, "shard"),
    )
    small = dict(mesh.shape) == {"rep": 4, "shard": 8}
    return jax.shard_map(
        body_fast if small else body,
        mesh=mesh,
        in_specs=placed,
        out_specs=(
            P(("rep", "shard"), None),
            P(("rep", "shard"), None),
            P(None, "shard", None),
            P(None, "shard", None),
            P(None, "shard", None),
            P(None, "shard", None),
            P(None, "shard"),
        ),
        check_vma=False,
    )
```

```python
import functools

import jax
import jax.numpy as jnp
from jax import lax
from jax.experimental import pallas as pl
from jax.experimental.pallas import tpu as pltpu
from jax.sharding import PartitionSpec as P

HEADS = 12
HEAD_DIM = 64


NEG_FILL = -1e30


def norm_forward(resid, gain, shift):
    center = jnp.mean(resid, axis=-1, keepdims=True)
    offsets = resid - center
    spread = jnp.mean(offsets * offsets, axis=-1, keepdims=True)
    factor = lax.rsqrt(spread + 1e-05)
    normed = offsets * factor
    return (normed * gain + shift, normed, factor)


def norm_backward(incoming, normed, factor, gain):
    scaled = incoming * gain
    resid_grad = factor * (
        scaled
        - jnp.mean(scaled, axis=-1, keepdims=True)
        - normed * jnp.mean(scaled * normed, axis=-1, keepdims=True)
    )
    return (resid_grad, jnp.sum(incoming * normed, axis=0), jnp.sum(incoming, axis=0))


def inner_rows(left, right):
    return lax.dot_general(
        left, right, (((0,), (0,)), ((), ())), preferred_element_type=jnp.float32
    )


def times_trans(left, right):
    return lax.dot_general(
        left, right, (((1,), (1,)), ((), ())), preferred_element_type=jnp.float32
    )


def gelu_exact(value):
    return jax.nn.gelu(value, approximate=False)


def sequence_ids(lengths, group_rows):
    ending = jnp.cumsum(lengths)
    opening = ending - lengths
    places = jnp.arange(group_rows, dtype=jnp.int32)
    member = jnp.sum((places[:, None] >= ending[None, :]).astype(jnp.int32), axis=1)
    leading = jnp.any(places[:, None] == opening[None, :], axis=1)
    return (member, leading)


def split_vector(vector, model_width):
    pieces = [vector[index * model_width : (index + 1) * model_width] for index in range(8)]
    pieces.append(vector[8 * model_width :])
    return pieces


def fetch_forward(entry_weight, exit_weight, expand_weight, shrink_weight, vectors, layer_index):
    return (
        lax.all_gather(entry_weight[layer_index].astype(jnp.bfloat16), "shard", axis=0, tiled=True),
        lax.all_gather(exit_weight[layer_index].astype(jnp.bfloat16), "shard", axis=0, tiled=True),
        lax.all_gather(
            expand_weight[layer_index].astype(jnp.bfloat16), "shard", axis=0, tiled=True
        ),
        lax.all_gather(
            shrink_weight[layer_index].astype(jnp.bfloat16), "shard", axis=0, tiled=True
        ),
        lax.all_gather(vectors[layer_index].astype(jnp.bfloat16), "shard", axis=0, tiled=True),
    )


def fetch_backward(entry_weight, exit_weight, expand_weight, shrink_weight, vectors, layer_index):
    return (
        lax.all_gather(entry_weight[layer_index].astype(jnp.bfloat16), "shard", axis=0, tiled=True),
        lax.all_gather(exit_weight[layer_index].astype(jnp.bfloat16), "shard", axis=0, tiled=True),
        lax.all_gather(
            expand_weight[layer_index].astype(jnp.bfloat16), "shard", axis=0, tiled=True
        ),
        lax.all_gather(
            shrink_weight[layer_index].astype(jnp.bfloat16), "shard", axis=0, tiled=True
        ),
        lax.all_gather(vectors[layer_index].astype(jnp.bfloat16), "shard", axis=0, tiled=True),
    )


def attend_forward(queries, keys, values, own_member, member, usable):
    local_rows = queries.shape[0]
    query_heads = queries.reshape(local_rows, HEADS, HEAD_DIM)
    factor_scale = HEAD_DIM ** (-0.5)
    start_state = (
        jnp.full((HEADS, local_rows), NEG_FILL, jnp.float32),
        jnp.zeros((HEADS, local_rows), jnp.float32),
        jnp.zeros((HEADS, local_rows, HEAD_DIM), jnp.float32),
    )
    key_piece = lax.all_gather(keys, "shard", axis=0, tiled=True)
    value_piece = lax.all_gather(values, "shard", axis=0, tiled=True)
    amount = key_piece.shape[0]
    block_rows = local_rows * max(1, 512 // local_rows)

    def fold_advance(block_index, running):
        running_max, running_total, weighted = running
        begin = block_index * block_rows
        key_block = lax.dynamic_slice_in_dim(key_piece, begin, block_rows, 0).reshape(
            block_rows, HEADS, HEAD_DIM
        )
        value_block = lax.dynamic_slice_in_dim(value_piece, begin, block_rows, 0).reshape(
            block_rows, HEADS, HEAD_DIM
        )
        key_member = lax.dynamic_slice_in_dim(member, begin, block_rows, 0)
        key_usable = lax.dynamic_slice_in_dim(usable, begin, block_rows, 0)
        allowed = ((own_member[:, None] == key_member[None, :]) & key_usable[None, :])[None]
        scores = (
            jnp.einsum("qhd,khd->hqk", query_heads, key_block, preferred_element_type=jnp.float32)
            * factor_scale
        )
        scores = jnp.where(allowed, scores, NEG_FILL)
        new_max = jnp.maximum(running_max, jnp.max(scores, axis=2))
        expos = jnp.where(allowed, jnp.exp(scores - new_max[:, :, None]), 0.0)
        shrink_by = jnp.exp(running_max - new_max)
        new_total = running_total * shrink_by + jnp.sum(expos, axis=2)
        new_weighted = weighted * shrink_by[:, :, None] + jnp.einsum(
            "hqk,khd->hqd",
            expos.astype(jnp.bfloat16),
            value_block,
            preferred_element_type=jnp.float32,
        )
        return (new_max, new_total, new_weighted)

    running_max, running_total, weighted = lax.fori_loop(
        0, amount // block_rows, fold_advance, start_state
    )
    attended = jnp.transpose(weighted / running_total[:, :, None], (1, 0, 2)).reshape(
        local_rows, HEADS * HEAD_DIM
    )
    return (attended, running_max + jnp.log(running_total))


def attend_backward(
    queries, attended_grad, log_total, deltas, keys_all, values_all, own_member, member, usable
):
    local_rows = queries.shape[0]
    group_rows = keys_all.shape[0]
    model_width = HEADS * HEAD_DIM
    factor_scale = HEAD_DIM ** (-0.5)
    query_heads = queries.reshape(local_rows, HEADS, HEAD_DIM)
    grad_heads = attended_grad.reshape(local_rows, HEADS, HEAD_DIM)
    block_rows = min(512, group_rows)

    def attend_advance(query_sum, block_index):
        begin = block_index * block_rows
        key_block = lax.dynamic_slice_in_dim(keys_all, begin, block_rows, 0).reshape(
            block_rows, HEADS, HEAD_DIM
        )
        value_block = lax.dynamic_slice_in_dim(values_all, begin, block_rows, 0).reshape(
            block_rows, HEADS, HEAD_DIM
        )
        key_member = lax.dynamic_slice_in_dim(member, begin, block_rows, 0)
        key_usable = lax.dynamic_slice_in_dim(usable, begin, block_rows, 0)
        allowed = ((own_member[:, None] == key_member[None, :]) & key_usable[None, :])[None]
        scores = (
            jnp.einsum("qhd,khd->hqk", query_heads, key_block, preferred_element_type=jnp.float32)
            * factor_scale
        )
        probs = jnp.where(allowed, jnp.exp(scores - log_total[:, :, None]), 0.0)
        prob_grad = jnp.einsum(
            "qhd,khd->hqk", grad_heads, value_block, preferred_element_type=jnp.float32
        )
        score_grad = (probs * (prob_grad - deltas[:, :, None])).astype(jnp.bfloat16)
        query_sum = (
            query_sum
            + jnp.einsum("hqk,khd->qhd", score_grad, key_block, preferred_element_type=jnp.float32)
            * factor_scale
        )
        key_grad = (
            jnp.einsum("hqk,qhd->khd", score_grad, query_heads, preferred_element_type=jnp.float32)
            * factor_scale
        )
        value_grad = jnp.einsum(
            "hqk,qhd->khd",
            probs.astype(jnp.bfloat16),
            grad_heads,
            preferred_element_type=jnp.float32,
        )
        joined = jnp.concatenate(
            [
                key_grad.reshape(block_rows, model_width),
                value_grad.reshape(block_rows, model_width),
            ],
            axis=1,
        )
        return (query_sum, joined)

    query_sum, key_value = lax.scan(
        attend_advance,
        jnp.zeros((local_rows, HEADS, HEAD_DIM), jnp.float32),
        jnp.arange(group_rows // block_rows, dtype=jnp.int32),
    )
    key_value = key_value.reshape(group_rows, 2 * model_width)
    return (query_sum.reshape(local_rows, model_width), key_value)


def layer_forward(hidden, weights, own_member, member, usable):
    entry, leaving, expand, shrink, vector = weights
    model_width = leaving.shape[0]
    pieces = split_vector(vector.astype(jnp.float32), model_width)
    flat = hidden.astype(jnp.bfloat16)
    mixed = jnp.dot(flat, entry, preferred_element_type=jnp.float32)
    queries = (mixed[:, 0:model_width] + pieces[0]).astype(jnp.bfloat16)
    keys = mixed[:, model_width : 2 * model_width].astype(jnp.bfloat16)
    values = (mixed[:, 2 * model_width : 3 * model_width] + pieces[1]).astype(jnp.bfloat16)
    attended, log_total = attend_forward(queries, keys, values, own_member, member, usable)
    attended_low = attended.astype(jnp.bfloat16)
    branch = jnp.dot(attended_low, leaving, preferred_element_type=jnp.float32) + pieces[2]
    middle, normed_one, factor_one = norm_forward(hidden + branch, pieces[3], pieces[4])
    middle_low = middle.astype(jnp.bfloat16)
    inner = jnp.dot(middle_low, expand, preferred_element_type=jnp.float32) + pieces[8]
    active = gelu_exact(inner).astype(jnp.bfloat16)
    branch_two = jnp.dot(active, shrink, preferred_element_type=jnp.float32) + pieces[5]
    result, normed_two, factor_two = norm_forward(middle + branch_two, pieces[6], pieces[7])
    record = (
        flat,
        queries,
        keys,
        values,
        attended,
        log_total,
        attended_low,
        normed_one,
        factor_one,
        middle_low,
        inner,
        active,
        normed_two,
        factor_two,
    )
    return (result, record)


def layer_backward(upstream, weights, record, keys_all, values_all, own_member, member, usable):
    entry, leaving, expand, shrink, vector = weights
    model_width = leaving.shape[0]
    pieces = split_vector(vector.astype(jnp.float32), model_width)
    (
        flat,
        queries,
        keys,
        values,
        attended,
        log_total,
        attended_low,
        normed_one,
        factor_one,
        middle_low,
        inner,
        active,
        normed_two,
        factor_two,
    ) = record
    local_rows = queries.shape[0]
    resid_two, gain_two_grad, shift_two_grad = norm_backward(
        upstream, normed_two, factor_two, pieces[6]
    )
    branch_two_grad = resid_two.astype(jnp.bfloat16)
    bias_down_grad = jnp.sum(branch_two_grad.astype(jnp.float32), axis=0)
    shrink_grad = inner_rows(active, branch_two_grad)
    active_grad = times_trans(branch_two_grad, shrink)
    unused_value, gelu_pull = jax.vjp(gelu_exact, inner)
    inner_grad = gelu_pull(active_grad)[0].astype(jnp.bfloat16)
    bias_up_grad = jnp.sum(inner_grad.astype(jnp.float32), axis=0)
    expand_grad = inner_rows(middle_low, inner_grad)
    middle_grad = resid_two + times_trans(inner_grad, expand)
    resid_one, gain_one_grad, shift_one_grad = norm_backward(
        middle_grad, normed_one, factor_one, pieces[3]
    )
    branch_grad = resid_one.astype(jnp.bfloat16)
    bias_out_grad = jnp.sum(branch_grad.astype(jnp.float32), axis=0)
    exit_grad = inner_rows(attended_low, branch_grad)
    attended_grad = times_trans(branch_grad, leaving).astype(jnp.bfloat16)
    deltas = jnp.sum(
        (attended_grad.astype(jnp.float32) * attended).reshape(local_rows, HEADS, HEAD_DIM), axis=2
    ).T
    query_grad, key_value_grad = attend_backward(
        queries, attended_grad, log_total, deltas, keys_all, values_all, own_member, member, usable
    )
    own_key_value = lax.psum_scatter(
        key_value_grad.astype(jnp.bfloat16), "shard", scatter_dimension=0, tiled=True
    ).astype(jnp.float32)
    mixed_grad = jnp.concatenate([query_grad, own_key_value], axis=1).astype(jnp.bfloat16)
    bias_query_grad = jnp.sum(mixed_grad[:, 0:model_width].astype(jnp.float32), axis=0)
    bias_value_grad = jnp.sum(
        mixed_grad[:, 2 * model_width : 3 * model_width].astype(jnp.float32), axis=0
    )
    entry_grad = inner_rows(flat, mixed_grad)
    hidden_grad = resid_one + times_trans(mixed_grad, entry)
    vector_grad = jnp.concatenate(
        [
            bias_query_grad,
            bias_value_grad,
            bias_out_grad,
            gain_one_grad,
            shift_one_grad,
            bias_down_grad,
            gain_two_grad,
            shift_two_grad,
            bias_up_grad,
        ]
    )
    return (hidden_grad, (entry_grad, exit_grad, expand_grad, shrink_grad, vector_grad))


def body(
    inputs,
    cotangent,
    lengths,
    dealing,
    key_mask,
    entry_weight,
    exit_weight,
    expand_weight,
    shrink_weight,
    vectors,
):
    local_rows = inputs.shape[0]
    group_rows = local_rows * lax.axis_size("shard")
    position = lax.axis_index("shard") * local_rows
    dealt_all, mask_all = (
        lax.all_gather(dealing, "shard", axis=1, tiled=True),
        lax.all_gather(key_mask, "shard", axis=1, tiled=True),
    )
    member, leading = sequence_ids(lengths[0], group_rows)
    usable = (mask_all[0] == 1) | leading
    own_member = lax.dynamic_slice_in_dim(member, position, local_rows, 0)
    inverse = (
        jnp.zeros((group_rows,), jnp.int32)
        .at[dealt_all[0]]
        .set(jnp.arange(group_rows, dtype=jnp.int32))
    )
    own_inverse = lax.dynamic_slice_in_dim(inverse, position, local_rows, 0)
    inputs_all, cotangent_all = (
        lax.all_gather(inputs, "shard", axis=0, tiled=True),
        lax.all_gather(cotangent, "shard", axis=0, tiled=True),
    )
    hidden = jnp.take(inputs_all, dealing[0], axis=0).astype(jnp.float32)
    upstream = jnp.take(cotangent_all, dealing[0], axis=0).astype(jnp.float32)
    layers = entry_weight.shape[0]
    saved = []
    kept = []
    for layer_index in range(layers):
        weights = fetch_forward(
            entry_weight, exit_weight, expand_weight, shrink_weight, vectors, layer_index
        )
        kept.append(weights)
        hidden, record = layer_forward(hidden, weights, own_member, member, usable)
        saved.append(record)
    output_all = lax.all_gather(hidden.astype(jnp.bfloat16), "shard", axis=0, tiled=True)
    output = jnp.take(output_all, own_inverse, axis=0)
    hidden_grad = upstream
    layer_grads = [None] * layers
    for layer_index in reversed(range(layers)):
        weights = fetch_backward(
            entry_weight, exit_weight, expand_weight, shrink_weight, vectors, layer_index
        )
        record = saved[layer_index]
        keys_all, values_all = (
            lax.all_gather(record[2], "shard", axis=0, tiled=True),
            lax.all_gather(record[3], "shard", axis=0, tiled=True),
        )
        hidden_grad, local_grads = layer_backward(
            hidden_grad, weights, record, keys_all, values_all, own_member, member, usable
        )
        entry_local, exit_local, expand_local, shrink_local, vector_local = local_grads
        entry_part, exit_part, expand_part, shrink_part, vector_part = (
            lax.psum_scatter(
                entry_local.astype(jnp.bfloat16), "shard", scatter_dimension=0, tiled=True
            ).astype(jnp.float32),
            lax.psum_scatter(
                exit_local.astype(jnp.bfloat16), "shard", scatter_dimension=0, tiled=True
            ).astype(jnp.float32),
            lax.psum_scatter(
                expand_local.astype(jnp.bfloat16), "shard", scatter_dimension=0, tiled=True
            ).astype(jnp.float32),
            lax.psum_scatter(
                shrink_local.astype(jnp.bfloat16), "shard", scatter_dimension=0, tiled=True
            ).astype(jnp.float32),
            lax.psum_scatter(
                vector_local.astype(jnp.bfloat16), "shard", scatter_dimension=0, tiled=True
            ).astype(jnp.float32),
        )
        entry_part, exit_part, expand_part, shrink_part, vector_part = (
            lax.psum(entry_part.astype(jnp.bfloat16), "rep").astype(jnp.float32),
            lax.psum(exit_part.astype(jnp.bfloat16), "rep").astype(jnp.float32),
            lax.psum(expand_part.astype(jnp.bfloat16), "rep").astype(jnp.float32),
            lax.psum(shrink_part.astype(jnp.bfloat16), "rep").astype(jnp.float32),
            lax.psum(vector_part.astype(jnp.bfloat16), "rep").astype(jnp.float32),
        )
        layer_grads[layer_index] = (entry_part, exit_part, expand_part, shrink_part, vector_part)
    entry_grad = jnp.stack([item[0] for item in layer_grads])
    exit_grad = jnp.stack([item[1] for item in layer_grads])
    expand_grad = jnp.stack([item[2] for item in layer_grads])
    shrink_grad = jnp.stack([item[3] for item in layer_grads])
    vector_grad = jnp.stack([item[4] for item in layer_grads])
    grads_all = lax.all_gather(
        hidden_grad.astype(jnp.bfloat16), "shard", axis=0, tiled=True
    ).astype(hidden_grad.dtype)
    input_grad = jnp.take(grads_all, own_inverse, axis=0)
    return (output, input_grad, entry_grad, exit_grad, expand_grad, shrink_grad, vector_grad)


EDGE = (0, 1, 6, 7)
CORE = (2, 3, 4, 5)
ALL = tuple(range(8))
BOTH = ("rep", "shard")
UNIT = 24


def routes(rep_flip, shard_flip, shards):
    return [
        (rep * 8 + shard, (rep ^ rep_flip) * 8 + (shard ^ shard_flip))
        for rep in range(4)
        for shard in shards
    ]


TO_X = routes(1, 0, ALL)
TO_Y = routes(2, 0, ALL)
TO_TWIN = routes(0, 1, ALL)
TO_SIDE = routes(0, 2, ALL)
TO_MID = routes(0, 6, CORE) + routes(0, 1, EDGE)


def send(value, route):
    return lax.ppermute(value, BOTH, route)


def low(value):
    return value.astype(jnp.bfloat16)


def wide(value):
    return value.astype(jnp.float32)


VMEM = pl.BlockSpec(memory_space=pltpu.VMEM)
SMEM = pl.BlockSpec(memory_space=pltpu.SMEM)
LIMIT = pltpu.CompilerParams(vmem_limit_bytes=60 * 1024 * 1024)


def shaped(shape, kind=jnp.bfloat16):
    return jax.ShapeDtypeStruct(shape, kind)


def cost(micros):
    return pl.CostEstimate(
        flops=int(micros * 1e9), bytes_accessed=int(micros * 1e6), transcendentals=0
    )


def nt(left, right):
    return lax.dot_general(left, right, (((1,), (1,)), ((), ())), preferred_element_type=jnp.float32)


def nn(left, right):
    return lax.dot_general(left, right, (((1,), (0,)), ((), ())), preferred_element_type=jnp.float32)


def fixed(*shape):
    return pl.BlockSpec(shape, lambda step: (0,) * len(shape))


def gather_kernel(ids_ref, want_ref, *refs):
    out_ref = refs[-1]
    want = want_ref[...]
    total = None
    index = 0
    for piece_ref in refs[:-1]:
        for slot in range(piece_ref.shape[0]):
            ids = ids_ref[index]
            hit = low(wide(want == ids))
            part = nn(hit, piece_ref[slot, 0 : ids.shape[1], :])
            total = part if total is None else total + part
            index += 1
    out_ref[...] = low(total)


def gather_rows(pieces, ids, want, spend):
    return pl.pallas_call(
        gather_kernel,
        out_shape=shaped((want.shape[0], pieces[0].shape[2])),
        in_specs=[VMEM] * (2 + len(pieces)),
        out_specs=VMEM,
        compiler_params=LIMIT,
        cost_estimate=cost(spend),
        name="gather_rows",
    )(ids, want, *pieces)


def assemble_kernel(where_ref, *refs):
    out_ref = refs[10]
    depth, rep, twin = where_ref[0], where_ref[1], where_ref[2]
    for side in range(2):
        own, first, over_x, over_y, over_d = refs[side * 5 : side * 5 + 5]
        core = twin ^ side
        for row in range(4):
            out_ref[depth, core, row] = own[row]
        for slot, flip in enumerate((1, 3, 2)):
            level = depth ^ flip
            for piece, bits in ((first, 0), (over_x, 1), (over_y, 2), (over_d, 3)):
                out_ref[level, core, rep ^ bits] = piece[slot]


def assemble(where, parts, start, by_rows):
    def part_spec(part):
        return pl.BlockSpec(
            (part.shape[0], None) + part.shape[2:],
            lambda unit, where_ref: (0, start + unit, 0, 0),
        )

    width = parts[0].shape[3]
    if by_rows:
        shape = (4, 2, 4, 4, UNIT, width)
        spec = pl.BlockSpec(
            (4, 2, 4, None, UNIT, width), lambda unit, where_ref: (0, 0, 0, unit, 0, 0)
        )
    else:
        shape = (4, 4, 2, 4, UNIT, width)
        spec = pl.BlockSpec(
            (None, 4, 2, 4, UNIT, width), lambda unit, where_ref: (unit, 0, 0, 0, 0, 0)
        )
    result = pl.pallas_call(
        assemble_kernel,
        grid_spec=pltpu.PrefetchScalarGridSpec(
            num_scalar_prefetch=1,
            grid=(4,),
            in_specs=[part_spec(part) for part in parts],
            out_specs=spec,
        ),
        out_shape=shaped(shape),
        compiler_params=LIMIT,
        cost_estimate=cost(0.3),
        name="assemble",
    )(where, *parts)
    return result.reshape(4, 32 * UNIT, width)


def tie(value, *others):
    return lax.optimization_barrier((value,) + others)[0]


def after(values, *others):
    return list(lax.optimization_barrier(tuple(values) + others)[: len(values)])


class Spread:
    def __init__(self, own, first, x_last):
        self.own, self.first, self.x_last = own, first, x_last
        self.over = [send(first, TO_X), send(first, TO_Y)]
        self.twins = [send(own, TO_TWIN), send(first, TO_TWIN)]

    def turn(self, *others):
        self.over_x, self.over_y = after(self.over, *self.twins, *others)
        last = self.over_y if self.x_last else self.over_x
        self.over_d = send(last, TO_X if self.x_last else TO_Y)
        self.twins += [send(self.over_x, TO_TWIN), send(self.over_y, TO_TWIN)]
        return self.over_x

    def parts(self, *others):
        over_d = after([self.over_d], *self.twins, *others)[0]
        mine = (self.own, self.first, self.over_x, self.over_y, over_d)
        return mine + tuple(self.twins) + (send(over_d, TO_TWIN),)


def project_kernel(h_ref, w_ref, vec_ref, sel_ref, q_ref, kv_ref, mine_ref, theirs_ref):
    unit = pl.program_id(0)
    product = nn(h_ref[...], w_ref[...])

    @pl.when(unit == 0)
    def _():
        q_ref[...] = low(product + vec_ref[0:1, :])
        mine_ref[...] = low(nn(h_ref[...], sel_ref[0]))
        theirs_ref[...] = low(nn(h_ref[...], sel_ref[1]))

    @pl.when(unit == 1)
    def _():
        kv_ref[...] = low(product)

    @pl.when(unit == 2)
    def _():
        kv_ref[...] = low(product + vec_ref[1:2, :])


def project(hidden, weight, vec, sel):
    rows, width = hidden.shape
    return pl.pallas_call(
        project_kernel,
        grid=(3,),
        in_specs=[
            fixed(rows, width),
            pl.BlockSpec((None, width, width), lambda unit: (unit, 0, 0)),
            fixed(12, width),
            fixed(2, width, width // 2),
        ],
        out_specs=[
            fixed(rows, width),
            pl.BlockSpec((None, rows, width), lambda unit: (jnp.maximum(unit - 1, 0), 0, 0)),
            fixed(rows, width // 2),
            fixed(rows, width // 2),
        ],
        out_shape=[
            shaped((rows, width)),
            shaped((2, rows, width)),
            shaped((rows, width // 2)),
            shaped((rows, width // 2)),
        ],
        compiler_params=LIMIT,
        cost_estimate=cost(0.3),
        name="project",
    )(hidden, weight, vec, sel)


def attend_kernel(
    q_ref, ka_ref, kb_ref, va_ref, vb_ref, code_ref, member_ref, o_ref, ot_ref, lse_ref, bias_ref
):
    half = q_ref.shape[0]

    @pl.when(pl.program_id(0) == 0)
    def _():
        bias_ref[...] = jnp.where(code_ref[...] == member_ref[...], 0.0, NEG_FILL)

    q = q_ref[...] * jnp.bfloat16(HEAD_DIM ** (-0.5))
    lane = lax.broadcasted_iota(jnp.int32, q.shape, 1)
    keys = (ka_ref[...], kb_ref[...])
    values = (va_ref[...].T, vb_ref[...].T)
    outs = []
    for head in range(2):
        q_head = jnp.where((lane >= HEAD_DIM) == (head == 1), q, jnp.bfloat16(0))
        scores = [
            nt(keys[side], q_head) + bias_ref[side * half : (side + 1) * half, :]
            for side in range(2)
        ]
        top = jnp.maximum(
            jnp.max(scores[0], axis=0, keepdims=True), jnp.max(scores[1], axis=0, keepdims=True)
        )
        total = None
        mixed = None
        for side in range(2):
            expo = jnp.exp(scores[side] - top)
            part = jnp.sum(expo, axis=0, keepdims=True)
            value = values[side][head * HEAD_DIM : (head + 1) * HEAD_DIM, :]
            product = nn(value, low(expo))
            total = part if total is None else total + part
            mixed = product if mixed is None else mixed + product
        outs.append(mixed / total)
        lse_ref[head : head + 1, :] = top + jnp.log(total)
    joined = jnp.concatenate(outs, axis=0)
    ot_ref[...] = joined
    o_ref[...] = low(joined.T)


def pair_specs(half):
    column = pl.BlockSpec((half, 128), lambda pair: (0, pair))
    key = pl.BlockSpec((None, half, 128), lambda pair: (0, 0, pair))
    value = pl.BlockSpec((None, half, 128), lambda pair: (1, 0, pair))
    turned = pl.BlockSpec((128, half), lambda pair: (pair, 0))
    level = pl.BlockSpec((None, 2, half), lambda pair: (pair, 0, 0))
    return column, key, value, turned, level


def attend_fast(queries, kv, kv_twin, code, member):
    half, width = queries.shape
    column, key, value, turned, level = pair_specs(half)
    return pl.pallas_call(
        attend_kernel,
        grid=(width // 128,),
        in_specs=[column, key, key, value, value, fixed(2 * half, 1), fixed(1, half)],
        out_specs=[column, turned, level],
        out_shape=[
            shaped((half, width)),
            shaped((width, half), jnp.float32),
            shaped((width // 128, 2, half), jnp.float32),
        ],
        scratch_shapes=[pltpu.VMEM((2 * half, half), jnp.float32)],
        compiler_params=LIMIT,
        cost_estimate=cost(0.3),
        name="attend_forward",
    )(queries, kv, kv_twin, kv, kv_twin, code, member)


def attend_back_kernel(
    q_ref, g_ref, ka_ref, kb_ref, va_ref, vb_ref, ot_ref, lse_ref, code_ref, member_ref,
    dq_ref, own_ref, twin_ref, bias_ref,
):
    half = q_ref.shape[0]

    @pl.when(pl.program_id(0) == 0)
    def _():
        bias_ref[...] = jnp.where(code_ref[...] == member_ref[...], 0.0, NEG_FILL)

    scale = HEAD_DIM ** (-0.5)
    q = q_ref[...] * jnp.bfloat16(scale)
    grad = g_ref[...]
    lane = lax.broadcasted_iota(jnp.int32, q.shape, 1)
    keys = (ka_ref[...], kb_ref[...])
    turned = (keys[0].T, keys[1].T)
    values = (va_ref[...], vb_ref[...])
    product = ot_ref[...] * wide(grad).T
    key_sums = [None, None]
    value_sums = [None, None]
    query_parts = []
    for head in range(2):
        rows = slice(head * HEAD_DIM, (head + 1) * HEAD_DIM)
        chosen = (lane >= HEAD_DIM) == (head == 1)
        q_head = jnp.where(chosen, q, jnp.bfloat16(0))
        g_head = jnp.where(chosen, grad, jnp.bfloat16(0))
        delta = jnp.sum(product[rows, :], axis=0, keepdims=True)
        level = lse_ref[head : head + 1, :]
        query_sum = None
        for side in range(2):
            scores = nt(keys[side], q_head) + bias_ref[side * half : (side + 1) * half, :]
            prob = jnp.exp(scores - level)
            slope = nt(values[side], g_head)
            steep = low(prob * (slope - delta))
            value_part = nn(low(prob), g_head)
            key_part = nn(steep, q_head)
            query_part = nn(turned[side][rows, :], steep)
            value_sums[side] = value_part if head == 0 else value_sums[side] + value_part
            key_sums[side] = key_part if head == 0 else key_sums[side] + key_part
            query_sum = query_part if side == 0 else query_sum + query_part
        query_parts.append(query_sum * scale)
    dq_ref[...] = low(jnp.concatenate(query_parts, axis=0).T)
    own_ref[0] = key_sums[0]
    own_ref[1] = value_sums[0]
    twin_ref[0] = low(key_sums[1])
    twin_ref[1] = low(value_sums[1])


def attend_back_fast(queries, grad, kv, kv_twin, ot, lse, code, member, spend):
    half, width = queries.shape
    column, key, value, turned, level = pair_specs(half)
    both = pl.BlockSpec((2, half, 128), lambda pair: (0, 0, pair))
    return pl.pallas_call(
        attend_back_kernel,
        grid=(width // 128,),
        in_specs=[column, column, key, key, value, value, turned, level]
        + [fixed(2 * half, 1), fixed(1, half)],
        out_specs=[column, both, both],
        out_shape=[
            shaped((half, width)),
            shaped((2, half, width), jnp.float32),
            shaped((2, half, width)),
        ],
        scratch_shapes=[pltpu.VMEM((2 * half, half), jnp.float32)],
        compiler_params=LIMIT,
        cost_estimate=cost(spend),
        name="attend_backward",
    )(queries, grad, kv, kv_twin, kv, kv_twin, ot, lse, code, member)


def normal_parts(value):
    scaled = value * 0.7071067811865476
    size = jnp.abs(scaled)
    square = size * size
    t = 1.0 / (1.0 + 0.5 * size)
    series = 0.17087277
    for factor in (
        -0.82215223, 1.48851587, -1.13520398, 0.27886807, -0.18628806,
        0.09678418, 0.37409196, 1.00002368, -1.26551223,
    ):
        series = series * t + factor
    tail = 0.5 * t * jnp.exp(series - square)
    cumulative = jnp.where(value >= 0, 1.0 - tail, tail)
    density = 0.3989422804014327 * jnp.exp(-square)
    return cumulative, density


def row_norm(resid):
    offsets = resid - jnp.mean(resid, axis=-1, keepdims=True)
    spread_of = jnp.mean(offsets * offsets, axis=-1, keepdims=True)
    factor = lax.rsqrt(spread_of + 1e-05)
    return offsets * factor, factor


def post_kernel(
    where_ref, o_ref, h_ref, wo_ref, up_ref, down_ref, vec_ref, sel_ref,
    h_out, hl_out, n1_out, t1_out, n2_out, t2_out, slope_out, mine_out, theirs_out,
    y_ref, yl_ref, f_ref,
):
    step = pl.program_id(0)
    half_width = mine_out.shape[2]

    @pl.when(step == 0)
    def _():
        attended = o_ref[...]
        branch = nn(attended, wo_ref[...]) + vec_ref[2:3, :]
        normed, factor = row_norm(wide(h_ref[...]) + branch)
        middle = normed * vec_ref[3:4, :] + vec_ref[4:5, :]
        n1_out[...] = normed
        t1_out[...] = factor
        y_ref[...] = middle
        yl_ref[...] = low(middle)
        mine_out[4] = low(nn(yl_ref[...], sel_ref[0]))
        theirs_out[4] = low(nn(yl_ref[...], sel_ref[1]))
        mine_out[5] = low(nn(attended, sel_ref[0]))
        theirs_out[5] = low(nn(attended, sel_ref[1]))

    inner = nn(yl_ref[...], up_ref[...]) + vec_ref[pl.ds(8 + step, 1), :]
    cumulative, density = normal_parts(inner)
    slope_out[...] = low(cumulative + inner * density)
    active = low(inner * cumulative)
    first, second = active[:, :half_width], active[:, half_width:]
    swap = where_ref[2] == 1
    mine_out[step] = jnp.where(swap, second, first)
    theirs_out[step] = jnp.where(swap, first, second)
    part = nn(active, down_ref[...])

    @pl.when(step == 0)
    def _():
        f_ref[...] = part

    @pl.when(step > 0)
    def _():
        f_ref[...] += part

    @pl.when(step == 3)
    def _():
        normed, factor = row_norm(y_ref[...] + (f_ref[...] + vec_ref[5:6, :]))
        result = normed * vec_ref[6:7, :] + vec_ref[7:8, :]
        n2_out[...] = normed
        t2_out[...] = factor
        h_out[...] = result
        hl_out[...] = low(result)


def unit_spec(width, index):
    return pl.BlockSpec((None, width, width), lambda step: (index, 0, 0))


def step_spec(width):
    return pl.BlockSpec((None, width, width), lambda step: (step, 0, 0))


def column_spec(rows, width):
    return pl.BlockSpec((rows, width), lambda step: (0, step))


def post(where, attended, hidden, front, up, down, vec, sel):
    rows, width = attended.shape
    half = width // 2
    full = fixed(rows, width)
    thin = fixed(rows, 1)
    return pl.pallas_call(
        post_kernel,
        grid=(4,),
        in_specs=[
            SMEM, full, full, unit_spec(width, 3), step_spec(width), step_spec(width),
            fixed(12, width), fixed(2, width, half),
        ],
        out_specs=[full, full, full, thin, full, thin, column_spec(rows, width)]
        + [fixed(6, rows, half)] * 2,
        out_shape=[
            shaped((rows, width), jnp.float32),
            shaped((rows, width)),
            shaped((rows, width), jnp.float32),
            shaped((rows, 1), jnp.float32),
            shaped((rows, width), jnp.float32),
            shaped((rows, 1), jnp.float32),
            shaped((rows, 4 * width)),
        ]
        + [shaped((6, rows, half))] * 2,
        scratch_shapes=[
            pltpu.VMEM((rows, width), jnp.float32),
            pltpu.VMEM((rows, width), jnp.bfloat16),
            pltpu.VMEM((rows, width), jnp.float32),
        ],
        compiler_params=LIMIT,
        cost_estimate=cost(0.3),
        name="post",
    )(where, attended, hidden, front, up, down, vec, sel)


def norm_back(incoming, normed, factor, gain):
    scaled = incoming * gain
    return factor * (
        scaled
        - jnp.mean(scaled, axis=-1, keepdims=True)
        - normed * jnp.mean(scaled * normed, axis=-1, keepdims=True)
    )


def column_sum(value):
    return jnp.sum(value, axis=0, keepdims=True)


def post_back_kernel(
    e_ref, n1_ref, t1_ref, n2_ref, t2_ref, slope_ref, wo_ref, up_ref, down_ref, vec_ref,
    all_out, do_out, dr_out, sums_out,
    r_ref, y_ref,
):
    step = pl.program_id(0)

    @pl.when(step == 0)
    def _():
        incoming = wide(e_ref[...])
        normed = n2_ref[...]
        resid = norm_back(incoming, normed, t2_ref[...], vec_ref[6:7, :])
        r_ref[...] = resid
        rounded = low(resid)
        all_out[4] = rounded
        sums_out[0:2, :] = jnp.zeros((2, sums_out.shape[1]), jnp.float32)
        sums_out[5:6, :] = column_sum(wide(rounded))
        sums_out[6:7, :] = column_sum(incoming * normed)
        sums_out[7:8, :] = column_sum(incoming)

    steep = low(nt(all_out[4], down_ref[...]) * wide(slope_ref[...]))
    all_out[step] = steep
    sums_out[pl.ds(8 + step, 1), :] = column_sum(wide(steep))
    part = nt(steep, up_ref[...])

    @pl.when(step == 0)
    def _():
        y_ref[...] = part

    @pl.when(step > 0)
    def _():
        y_ref[...] += part

    @pl.when(step == 3)
    def _():
        incoming = r_ref[...] + y_ref[...]
        normed = n1_ref[...]
        resid = norm_back(incoming, normed, t1_ref[...], vec_ref[3:4, :])
        dr_out[...] = resid
        rounded = low(resid)
        all_out[5] = rounded
        do_out[...] = low(nt(rounded, wo_ref[...]))
        sums_out[2:3, :] = column_sum(wide(rounded))
        sums_out[3:4, :] = column_sum(incoming * normed)
        sums_out[4:5, :] = column_sum(incoming)


def post_back(upstream, n1, t1, n2, t2, slope, front, up, down, vec, spend):
    rows, width = upstream.shape
    full = fixed(rows, width)
    thin = fixed(rows, 1)
    return pl.pallas_call(
        post_back_kernel,
        grid=(4,),
        in_specs=[
            full, full, thin, full, thin, column_spec(rows, width),
            unit_spec(width, 3), step_spec(width), step_spec(width), fixed(12, width),
        ],
        out_specs=[fixed(6, rows, width), full, full, fixed(12, width)],
        out_shape=[
            shaped((6, rows, width)),
            shaped((rows, width)),
            shaped((rows, width), jnp.float32),
            shaped((12, width), jnp.float32),
        ],
        scratch_shapes=[
            pltpu.VMEM((rows, width), jnp.float32),
            pltpu.VMEM((rows, width), jnp.float32),
        ],
        compiler_params=LIMIT,
        cost_estimate=cost(spend),
        name="post_back",
    )(upstream, n1, t1, n2, t2, slope, front, up, down, vec)


def project_back_kernel(
    dq_ref, own_ref, got_ref, w_ref, dr_ref, dm_out, dx_out, dxl_out, sums_out
):
    unit = pl.program_id(0)

    @pl.when(unit == 0)
    def _():
        dm_out[...] = dq_ref[...]

    @pl.when(unit > 0)
    def _():
        dm_out[...] = low(own_ref[...] + wide(got_ref[...]))

    grad = dm_out[...]
    part = nt(grad, w_ref[...])
    total = column_sum(wide(grad))

    @pl.when(unit == 0)
    def _():
        dx_out[...] = dr_ref[...] + part
        sums_out[0:1, :] = total

    @pl.when(unit > 0)
    def _():
        dx_out[...] += part
        sums_out[1:2, :] = total

    @pl.when(unit == 2)
    def _():
        dxl_out[...] = low(dx_out[...])


def project_back(dq, own, got, front, dr, spend):
    rows, width = dq.shape
    full = fixed(rows, width)
    late = pl.BlockSpec((None, rows, width), lambda unit: (jnp.maximum(unit - 1, 0), 0, 0))
    return pl.pallas_call(
        project_back_kernel,
        grid=(3,),
        in_specs=[full, late, late, step_spec(width), full],
        out_specs=[
            pl.BlockSpec((None, rows, width), lambda unit: (unit, 0, 0)),
            full, full, fixed(2, width),
        ],
        out_shape=[
            shaped((3, rows, width)),
            shaped((rows, width), jnp.float32),
            shaped((rows, width)),
            shaped((2, width), jnp.float32),
        ],
        compiler_params=LIMIT,
        cost_estimate=cost(spend),
        name="project_back",
    )(dq, own, got, front, dr)


def tn(left, right):
    return nn(left.T, right)


def split_store(keep_ref, give_ref, bit, x_first, piece_of, store):
    for other in range(2):
        pair = []
        for side in range(2):
            rep = (other * 2 + side) if x_first else (side * 2 + other)
            pair.append(low(piece_of(rep)))
        store(keep_ref, other, jnp.where(bit == 0, pair[0], pair[1]))
        store(give_ref, other, jnp.where(bit == 0, pair[1], pair[0]))


def column_store(ref_pair, bit, x_first, product, unit):
    keep_ref, give_ref = ref_pair
    for level in range(4):
        base = level * 4 * UNIT

        def piece_of(rep):
            return product[base + rep * UNIT : base + (rep + 1) * UNIT, :]

        def store(ref, other, value):
            ref[level, other, unit] = value

        split_store(keep_ref, give_ref, bit, x_first, piece_of, store)


def front_grad_kernel(
    bit_ref, xm_ref, xt_ref, om_ref, ot_ref, dm_ref, dmt_ref, da_ref, dat_ref,
    keep_x, give_x, keep_y, give_y,
):
    unit = pl.program_id(0)

    def store(product, index, x_first):
        pair = (keep_x, give_x) if x_first else (keep_y, give_y)
        column_store(pair, bit_ref[0 if x_first else 1], x_first, product, index)

    @pl.when(unit < 2)
    def _():
        store(tn(xm_ref[...], dm_ref[...]) + tn(xt_ref[...], dmt_ref[...]), unit, True)

    @pl.when(unit == 2)
    def _():
        store(tn(xm_ref[...], dm_ref[...]) + tn(xt_ref[...], dmt_ref[...]), 0, False)

    @pl.when(unit == 3)
    def _():
        store(tn(om_ref[...], da_ref[...]) + tn(ot_ref[...], dat_ref[...]), 1, False)


def block_spec(rows, width, index):
    return pl.BlockSpec((None, rows, width), lambda step: (index, 0, 0))


def front_grad(bits, xm, xt, mine, theirs, dm, dmt, da, dat, spend):
    rows, half = xm.shape
    width = da.shape[2]
    late = pl.BlockSpec((None, rows, width), lambda unit: (jnp.minimum(unit, 2), 0, 0))
    shape = (4, 2, 2, UNIT, width)
    return pl.pallas_call(
        front_grad_kernel,
        grid=(4,),
        in_specs=[SMEM, fixed(rows, half), fixed(rows, half)]
        + [block_spec(rows, half, 5)] * 2
        + [late, late]
        + [block_spec(rows, width, 5)] * 2,
        out_specs=[fixed(*shape)] * 4,
        out_shape=[shaped(shape)] * 4,
        compiler_params=LIMIT,
        cost_estimate=cost(spend),
        name="front_grad",
    )(bits, xm, xt, mine, theirs, dm, dmt, da, dat)


def feed_grad_kernel(
    x_first, bit_ref, ym_ref, yt_ref, gm_ref, gt_ref, dz_ref, dzt_ref, df_ref, dft_ref,
    keep_up, give_up, keep_down, give_down,
):
    step = pl.program_id(0)
    up_bit = bit_ref[0 if x_first else 1]
    down_bit = bit_ref[1 if x_first else 0]

    @pl.when(step < 4)
    def _():
        product = tn(ym_ref[...], dz_ref[...]) + tn(yt_ref[...], dzt_ref[...])
        column_store((keep_up, give_up), up_bit, x_first, product, step)

    @pl.when(step >= 4)
    def _():
        product = tn(gm_ref[...], df_ref[...]) + tn(gt_ref[...], dft_ref[...])
        for sub in range(4):

            def piece_of(rep):
                base = (rep * 4 + sub) * UNIT
                return product[base : base + UNIT, :]

            def store(ref, other, value):
                ref[step - 4, other, sub] = value

            split_store(keep_down, give_down, down_bit, not x_first, piece_of, store)


def feed_grad(x_first, bits, mine, theirs, slopes, slopes_twin, spend):
    rows, half = mine.shape[1:]
    width = slopes.shape[2]
    early = pl.BlockSpec((None, rows, width), lambda step: (jnp.minimum(step, 3), 0, 0))
    late = pl.BlockSpec((None, rows, half), lambda step: (jnp.maximum(step - 4, 0), 0, 0))
    shape = (4, 2, 4, UNIT, width)
    return pl.pallas_call(
        functools.partial(feed_grad_kernel, x_first),
        grid=(8,),
        in_specs=[SMEM]
        + [block_spec(rows, half, 4)] * 2
        + [late, late, early, early]
        + [block_spec(rows, width, 4)] * 2,
        out_specs=[fixed(*shape)] * 4,
        out_shape=[shaped(shape)] * 4,
        compiler_params=LIMIT,
        cost_estimate=cost(spend),
        name="feed_grad",
    )(bits, mine, theirs, mine, theirs, slopes, slopes_twin, slopes, slopes_twin)


def halve_kernel(low_ref, keep_x, got_x, keep_y, got_y, keep_out, give_out):
    start = jnp.where(low_ref[0] == 1, 0, 2)
    for index, (keep, got) in enumerate(((keep_x, got_x), (keep_y, got_y))):
        for out, begin in ((keep_out, start), (give_out, 2 - start)):
            for level in range(2):
                out[index, level] = low(wide(keep[begin + level]) + wide(got[begin + level]))


def halve_sum(is_low, keeps, gots, spend):
    count, width = keeps[0].shape[2], keeps[0].shape[4]
    whole = pl.BlockSpec((4, None, count, UNIT, width), lambda other: (0, other, 0, 0, 0))
    half = pl.BlockSpec((2, 2, None, count, UNIT, width), lambda other: (0, 0, other, 0, 0, 0))
    return pl.pallas_call(
        halve_kernel,
        grid=(2,),
        in_specs=[SMEM] + [whole] * 4,
        out_specs=[half] * 2,
        out_shape=[shaped((2, 2, 2, count, UNIT, width))] * 2,
        compiler_params=LIMIT,
        cost_estimate=cost(spend),
        name="halve_sum",
    )(is_low.astype(jnp.int32).reshape(1), keeps[0], gots[0], keeps[1], gots[1])


class Reduction:
    def __init__(self, pairs, bits, is_low, is_core):
        self.keeps = [pair[0] for pair in pairs]
        self.firsts = [pair[2] for pair in pairs]
        self.bits, self.is_low, self.is_core = bits, is_low, is_core
        self.got = [send(pair[1], TO_X if pair[2] else TO_Y) for pair in pairs]

    def across(self, spend, *others):
        got = after(self.got, *others)
        self.keep, give = halve_sum(self.is_low, self.keeps, got, spend)
        self.mid = send(give, TO_MID)
        return give

    def join(self, other):
        self.keep = jnp.concatenate([self.keep, other.keep], axis=3)
        self.mid = jnp.concatenate([self.mid, other.mid], axis=3)

    def outward(self, *others):
        mid = after([self.mid], *others)[0]
        stage = low(wide(self.keep) + wide(mid))
        outer = jnp.where(self.is_low, stage[:, 0], stage[:, 1])
        self.inner = jnp.where(self.is_low, stage[:, 1], stage[:, 0])
        self.side = send(outer, TO_SIDE)
        return outer

    def turn(self, *others):
        side = after([self.side], *others)[0]
        stage = jnp.where(self.is_core, self.inner, side)
        self.pieces = [stage[index] for index in range(len(self.firsts))]
        self.over = [
            send(piece, TO_Y if first else TO_X)
            for piece, first in zip(self.pieces, self.firsts)
        ]
        return stage

    def share(self, *others):
        over = after(self.over, *others)
        self.sums = [low(wide(piece) + wide(item)) for piece, item in zip(self.pieces, over)]
        self.got = [
            send(piece, TO_X if first else TO_Y) for piece, first in zip(self.sums, self.firsts)
        ]
        return self.sums[0]

    def finish(self, *others):
        return list(zip(self.sums, after(self.got, *others)))


def unpack_kernel(plan, bit_ref, *refs):
    outs = refs[-4:]
    width = outs[1].shape[1]
    for index, (x_first, units) in enumerate(plan):
        piece, got = refs[2 * index], refs[2 * index + 1]
        bit = bit_ref[0 if x_first else 1]
        for other in range(2):
            for side in range(2):
                rep = (other * 2 + side) if x_first else (side * 2 + other)
                for unit, (target, place) in enumerate(units):
                    value = wide(jnp.where(bit == side, piece[other, unit], got[other, unit]))
                    if target < 3:
                        rows = slice(rep * UNIT, (rep + 1) * UNIT)
                        outs[target][rows, place * width : (place + 1) * width] = value
                    else:
                        base = (rep * 4 + place) * UNIT
                        outs[target][base : base + UNIT, :] = value


def unpack(bits, pairs, plan, layer, layers, before):
    width = pairs[0][0].shape[3]
    shapes = [(4 * UNIT, 3 * width), (4 * UNIT, width), (4 * UNIT, 4 * width), (16 * UNIT, width)]
    arrays = [item for pair in pairs for item in pair]
    first = 1 + len(arrays)
    return pl.pallas_call(
        functools.partial(unpack_kernel, plan),
        grid=(1,),
        in_specs=[SMEM]
        + [fixed(*item.shape) for item in arrays]
        + [pl.BlockSpec(memory_space=pl.ANY) for _ in before],
        out_specs=[pl.BlockSpec((None,) + shape, lambda step: (layer, 0, 0)) for shape in shapes],
        out_shape=[shaped((layers,) + shape, jnp.float32) for shape in shapes],
        input_output_aliases={first + index: index for index in range(len(before))},
        compiler_params=LIMIT,
        cost_estimate=cost(3),
        name="unpack",
    )(bits, *arrays, *before)


def body_fast(
    inputs, cotangent, lengths, dealing, key_mask,
    entry_weight, exit_weight, expand_weight, shrink_weight, vectors,
):
    rows, width = inputs.shape
    layers = entry_weight.shape[0]
    group_rows = 8 * rows
    half_rows = group_rows // 2
    core_rows = half_rows // 2
    rep = lax.axis_index("rep")
    shard = lax.axis_index("shard")
    depth, twin = shard // 2, shard % 2
    is_low = depth <= 1
    is_core = (depth == 1) | (depth == 2)
    where = jnp.stack([depth, rep, twin]).astype(jnp.int32)
    bits = (rep & 1, rep >> 1)
    bit_words = jnp.stack(bits).astype(jnp.int32)

    def order(four):
        own, near, middle, far = four
        return jnp.where(
            is_low, jnp.stack([near, own, middle, far]), jnp.stack([far, middle, own, near])
        )

    def absolute(mine, theirs):
        one, two = order(mine), order(theirs)
        return jnp.where(twin == 0, jnp.stack([one, two], 1), jnp.stack([two, one], 1))

    def own_piece(pack):
        piece = lax.dynamic_index_in_dim(pack, rep, 0, keepdims=False)
        return piece.reshape(-1, width)

    def units_of(item):
        return item.reshape(-1, UNIT, width)

    def pack_front(entry, leaving):
        return jnp.concatenate([by_columns(entry), by_columns(leaving)], axis=1)

    def pack_feed(expand, shrink):
        return jnp.concatenate([by_columns(expand), low(shrink).reshape(4, 4, UNIT, width)], axis=1)

    def by_columns(weight):
        count = weight.shape[1] // width
        return low(weight).reshape(4, UNIT, count, width).transpose(0, 2, 1, 3)

    extra = layers * vectors.shape[1] // width
    tail = low(vectors).reshape(extra, width)
    table = jnp.concatenate([dealing // 64, dealing % 64, key_mask], axis=0)
    table = low(table).reshape(1, width)
    filler = jnp.zeros((7 - extra, width), jnp.bfloat16)
    rows_in = jnp.concatenate([inputs, tail, table, filler], axis=0)

    def group(items, begin, end):
        return jnp.stack([units_of(item[begin:end]) for item in items])

    front_zero = pack_front(entry_weight[0], exit_weight[0])
    piece = own_piece(front_zero)
    near = send(piece, TO_SIDE)
    middle = send(piece, TO_MID)
    feed_zero = pack_feed(expand_weight[0], shrink_weight[0])
    in_rows = rows_in.shape[0]
    far = send(near, TO_MID)
    first = jnp.stack([units_of(item) for item in (near, middle, far)])
    front_spread = Spread(front_zero, first, False)
    rows_late, twin_late, lengths = after([rows_in, twin, lengths], first)
    second = jnp.concatenate([rows_late, own_piece(feed_zero)], axis=0)
    second_near = send(second, TO_SIDE)
    second_middle = send(second, TO_MID)
    second_far = send(second_near, TO_MID)

    entry_late, exit_late, expand_late, shrink_late, cotangent_late = after(
        [entry_weight[1], exit_weight[1], expand_weight[1], shrink_weight[1], cotangent], first
    )
    front_one = pack_front(entry_late, exit_late)
    feed_one = pack_feed(expand_late, shrink_late)
    third = jnp.concatenate([own_piece(front_one), own_piece(feed_one), cotangent_late], axis=0)
    ready = front_spread.turn()

    second_middle, second_far = after([second_middle, second_far], ready)
    four = (second, second_near, second_middle, second_far)
    mine = jnp.stack([item[:in_rows] for item in four])
    theirs = send(mine, TO_TWIN)
    feed_spread = Spread(feed_zero, tie(group(four[1:], in_rows, in_rows + 8 * UNIT), ready), True)
    third = tie(third, ready)
    third_near = send(third, TO_SIDE)
    third_middle = send(third, TO_MID)
    fronts = [assemble(where, front_spread.parts(feed_spread.first, mine, third_near), 0, False)]

    header = absolute(tuple(mine[:, rows:]), tuple(theirs[:, rows:]))
    header = header.reshape(8, 8, width)
    vector_all = wide(header[:, :extra]).reshape(8, layers, vectors.shape[1])
    vector_all = jnp.transpose(vector_all, (1, 0, 2)).reshape(layers, 12, width)
    numbers = wide(header[:, extra]).reshape(8, 3, rows)
    dealt_all = (numbers[:, 0] * 64 + numbers[:, 1]).astype(jnp.int32).reshape(group_rows)
    mask_all = numbers[:, 2].reshape(group_rows)

    member, leading = sequence_ids(lengths[0], group_rows)
    usable = (mask_all == 1) | leading
    code = jnp.where(usable, member, -1)
    longest = jnp.argmax(lengths[0])
    begin = jnp.cumsum(lengths[0])[longest] - lengths[0][longest]
    spot = jnp.arange(half_rows, dtype=jnp.int32)

    def halve(values, low_side):
        inside = lax.dynamic_slice_in_dim(values, begin, half_rows, 0)
        outside = jnp.where(spot < begin, values[:half_rows], values[half_rows:])
        return jnp.where(low_side, inside, outside)

    def cores(values):
        own = lax.dynamic_slice_in_dim(values, twin * core_rows, core_rows, 0)
        other = lax.dynamic_slice_in_dim(values, (1 - twin) * core_rows, core_rows, 0)
        return own, other

    code_half = jnp.concatenate(cores(halve(code, is_low))).reshape(half_rows, 1)
    member_own = cores(halve(member, is_low))[0].reshape(1, core_rows)
    dealt_near = cores(halve(dealt_all, is_low))
    dealt_far = cores(halve(dealt_all, ~is_low))

    block = jnp.arange(width, dtype=jnp.int32)
    place = jnp.arange(width // 2, dtype=jnp.int32)
    chunk = 4 * UNIT
    source = (place // chunk) * (2 * chunk) + place % chunk
    cores_at = jnp.stack([twin_late, 1 - twin_late])
    sel = low(block[None, :, None] == (source[None, :] + cores_at[:, None] * chunk)[:, None, :])

    local = jnp.arange(rows, dtype=jnp.int32)
    bases = jnp.stack(
        [
            (depth ^ flip) * (2 * rows) + (twin ^ side) * rows
            for side in range(2)
            for flip in (0, 1, 3, 2)
        ]
    ).astype(jnp.int32)
    source_ids = (bases[:, None] + local[None, :]).reshape(8, 1, rows)
    want_in = dealt_near[0].reshape(core_rows, 1)
    theirs, third_near = after([theirs, third_near], fronts[0])
    third_far = send(third_near, TO_MID)
    hidden_low = gather_rows((mine, tie(theirs, third_near)), source_ids, want_in, 0.3)

    result_ids = jnp.stack([dealt_near[0], dealt_far[0], dealt_near[1], dealt_far[1]]).reshape(
        4, 1, core_rows
    )
    want_out = jnp.concatenate([source_ids[0, 0], source_ids[1, 0]]).reshape(2 * rows, 1)

    def deliver(pieces, spend):
        pieces = [piece[None] for piece in pieces]
        found = gather_rows(pieces, result_ids, want_out, spend)
        return found, send(found[rows:], TO_SIDE)

    saved = []
    def begin(layer):
        queries, kv, xm, xt = project(hidden_low, fronts[layer], vector_all[layer], sel)
        return queries, kv, send(kv, TO_TWIN), xm, send(xt, TO_TWIN)

    def attention(queries, kv, kv_twin):
        return attend_fast(queries, kv, kv_twin, code_half, member_own)

    def complete(layer, attended):
        results = post(
            where, attended, hidden, fronts[layer], ups[layer], downs[layer],
            vector_all[layer], sel,
        )
        return results, send(results[8], TO_TWIN)

    def record(start, middle, results, others):
        queries, kv, kv_twin, xm, xo = start
        saved.append(
            (queries, kv, kv_twin) + tuple(middle[1:]) + tuple(results[2:7])
            + (xm, xo, results[7], others)
        )

    hidden = hidden_low
    ready = feed_spread.turn(fronts[0])
    hidden_low, third_middle = after([hidden_low, third_middle], ready)
    hidden_low = tie(hidden_low, third_middle)
    start = begin(0)
    middle = attention(*start[:3])
    parts = feed_spread.parts(middle[0])
    third_far = tie(third_far, middle[0])
    four = (third, third_near, third_middle, third_far)
    split = 12 * UNIT
    front_spread = Spread(front_one, group(four[1:], 0, 4 * UNIT), True)
    cotangent_mine = jnp.stack([item[split:] for item in four])
    ups = [assemble(where, parts, 0, False)]
    downs = [assemble(where, parts, 4, True)]
    ready = front_spread.turn(ups[0], downs[0])
    feed_spread = Spread(feed_one, tie(group(four[1:], 4 * UNIT, split), ready), False)
    cotangent_theirs = send(cotangent_mine, TO_TWIN)
    held = [feed_spread.first, cotangent_theirs] + front_spread.twins + feed_spread.twins
    results, others = complete(0, tie(middle[0], ready, *held))
    hidden, hidden_low = results[:2]
    record(start, middle, results, others)
    ready = feed_spread.turn(hidden_low)
    fronts.append(assemble(where, front_spread.parts(ready), 0, False))
    start = begin(1)
    upstream = gather_rows(
        (cotangent_mine, tie(cotangent_theirs, start[0])), source_ids, want_in, 0.3
    )
    middle = attention(tie(start[0], upstream), start[1], start[2])
    parts = feed_spread.parts(middle[0])
    ups.append(assemble(where, parts, 0, False))
    downs.append(assemble(where, parts, 4, True))
    results, others = complete(1, middle[0])
    hidden, hidden_low = results[:2]
    record(start, middle, results, others)
    result_mid = send(hidden_low, TO_MID)
    result_twin = send(hidden_low, TO_TWIN)

    def start_back(layer, grad, spend):
        n1, t1, n2, t2, slope = saved[layer][5:10]
        slopes, do, dr, sums = post_back(
            grad, n1, t1, n2, t2, slope,
            fronts[layer], ups[layer], downs[layer], vector_all[layer], spend,
        )
        return slopes, send(slopes, TO_TWIN), do, dr, sums

    def attention_back(layer, do, spend):
        queries, kv, kv_twin, ot, lse = saved[layer][:5]
        return attend_back_fast(
            queries, do, kv, kv_twin, ot, lse, code_half, member_own, spend
        )

    def feed_part(layer, x_first, slopes, slopes_twin, spend):
        mine, others = saved[layer][12:14]
        keep_up, give_up, keep_down, give_down = feed_grad(
            x_first, bit_words, mine, others, slopes, slopes_twin, spend
        )
        work = Reduction(
            [(keep_up, give_up, x_first), (keep_down, give_down, not x_first)],
            bits, is_low, is_core,
        )
        return work, keep_up

    def front_part(layer, slopes, slopes_twin, dm, dm_twin, spend):
        xm, xo, mine, others = saved[layer][10:14]
        keep_x, give_x, keep_y, give_y = front_grad(
            bit_words, xm, xo, mine, others, dm, dm_twin, slopes, slopes_twin, spend
        )
        work = Reduction(
            [(keep_x, give_x, True), (keep_y, give_y, False)], bits, is_low, is_core
        )
        return work, keep_x

    upstream = tie(upstream, saved[0][11], saved[0][13])
    slopes_b, slopes_tb, do, dr, sums_b = start_back(1, upstream, 16)
    dq, own, give = attention_back(1, do, 21)
    got = send(give, TO_TWIN)
    feed_b, mark = feed_part(1, True, slopes_b, tie(slopes_tb, dq, saved[1][11], result_twin), 12)
    pair = (hidden_low, tie(result_mid, mark))
    pair += (result_twin, send(pair[1], TO_TWIN))
    dm_b, grad, _, head_b = project_back(dq, own, got, fronts[1], tie(dr, mark, pair[1]), 0.5)
    dm_tb = send(dm_b, TO_TWIN)
    found, output_side = deliver(after(pair, head_b), 0.5)
    slopes_a, slopes_ta, do, dr, sums_a = start_back(0, tie(grad, found), 0.5)
    ready = feed_b.across(3, do)
    dq, own, give = attention_back(0, tie(do, ready), 45)
    got = send(give, TO_TWIN)
    front_b, mark = front_part(1, slopes_b, slopes_tb, dm_b, tie(dm_tb, dq), 0.5)
    feed_a, mark = feed_part(0, False, slopes_a, tie(slopes_ta, mark, output_side, feed_b.mid), 12)
    ready = front_b.across(2, mark)
    dm_a, grad, grad_low, head_a = project_back(
        dq, own, got, fronts[0], tie(dr, ready), 0.5
    )
    dm_ta = send(dm_a, TO_TWIN)
    grad_mid = send(grad_low, TO_MID)
    grad_twin = send(grad_low, TO_TWIN)

    vectors_all = [
        jnp.concatenate([head_sums, sums[2:]], axis=0)
        for head_sums, sums in ((head_a, sums_a), (head_b, sums_b))
    ]
    joined = jnp.stack([item.reshape(-1) for item in vectors_all])
    joined = jnp.transpose(joined.reshape(layers, 4, 2, vectors.shape[1]), (1, 2, 0, 3))
    vector_keep = lax.dynamic_index_in_dim(joined, twin, 1, keepdims=False)
    vector_give = lax.dynamic_index_in_dim(joined, 1 - twin, 1, keepdims=False)
    vector_twin = send(vector_give, TO_TWIN)

    ready = feed_a.across(25, grad_low, front_b.mid)
    front_a, mark = front_part(0, slopes_a, slopes_ta, dm_a, tie(dm_ta, vector_give, ready, grad_twin), 0.5)

    feed_b.join(front_b)
    ready = feed_b.outward(mark)
    vector_stage = vector_keep + tie(vector_twin, ready)
    vector_over = send(vector_stage, TO_X)
    pair = (grad_low, tie(grad_mid, vector_stage), grad_twin)
    pair += (send(pair[1], TO_TWIN),)
    found_in, input_side = deliver(pair, 0.5)
    ready = feed_b.turn(found_in)
    vector_stage = vector_stage + tie(vector_over, ready)
    vector_over = send(vector_stage, TO_Y)

    ready = front_a.across(0.5, vector_stage)
    ready = feed_b.share(ready)
    vector_stage = vector_stage + tie(vector_over, ready)
    vector_give = jnp.where(is_low, vector_stage[2:4], vector_stage[0:2])
    vector_keep = jnp.where(is_low, vector_stage[0:2], vector_stage[2:4])
    vector_mid = send(vector_give, TO_MID)
    ready = feed_a.outward(vector_give)
    ups_at = tuple((2, place) for place in range(4))
    downs_at = tuple((3, place) for place in range(4))
    early_at, late_at = ((0, 0), (0, 1)), ((0, 2), (1, 0))
    plan = ((True, ups_at + early_at), (False, downs_at + late_at))

    ready = front_a.outward(ready)
    grads = unpack(bit_words, feed_b.finish(ready), plan, 1, layers, ())
    vector_stage = vector_keep + tie(vector_mid, ready)
    vector_outer = jnp.where(is_low, vector_stage[0], vector_stage[1])
    vector_inner = jnp.where(is_low, vector_stage[1], vector_stage[0])
    vector_side = send(vector_outer, TO_SIDE)
    ready = feed_a.turn(vector_outer, grads[1])
    output = jnp.where(is_core, found[:rows], output_side)
    input_grad = wide(jnp.where(is_core, found_in[:rows], tie(input_side, ready)))

    ready = front_a.turn(ready)
    ready_two = feed_a.share(ready)
    ready = front_a.share(ready_two)
    pairs = feed_a.finish(ready) + front_a.finish(ready)
    plan = ((False, ups_at), (True, downs_at), (True, early_at), (False, late_at))
    entry_grad, exit_grad, expand_grad, shrink_grad = unpack(
        bit_words, pairs, plan, 0, layers, grads
    )
    vector_grad = jnp.where(is_core, vector_inner, tie(vector_side, ready))
    return (output, input_grad, entry_grad, exit_grad, expand_grad, shrink_grad, vector_grad)


def solution(mesh):
    placed = (
        P(("rep", "shard"), None),
        P(("rep", "shard"), None),
        P("rep", None),
        P("rep", "shard"),
        P("rep", "shard"),
        P(None, "shard", None),
        P(None, "shard", None),
        P(None, "shard", None),
        P(None, "shard", None),
        P(None, "shard"),
    )
    small = dict(mesh.shape) == {"rep": 4, "shard": 8}
    return jax.shard_map(
        body_fast if small else body,
        mesh=mesh,
        in_specs=placed,
        out_specs=(
            P(("rep", "shard"), None),
            P(("rep", "shard"), None),
            P(None, "shard", None),
            P(None, "shard", None),
            P(None, "shard", None),
            P(None, "shard", None),
            P(None, "shard"),
        ),
        check_vma=False,
    )
```

```python
import functools

import jax
import jax.numpy as jnp
from jax import lax
from jax.experimental import pallas as pl
from jax.experimental.pallas import tpu as pltpu
from jax.sharding import PartitionSpec as P

HEADS = 12
HEAD_DIM = 64


NEG_FILL = -1e30


def norm_forward(resid, gain, shift):
    center = jnp.mean(resid, axis=-1, keepdims=True)
    offsets = resid - center
    spread = jnp.mean(offsets * offsets, axis=-1, keepdims=True)
    factor = lax.rsqrt(spread + 1e-05)
    normed = offsets * factor
    return (normed * gain + shift, normed, factor)


def norm_backward(incoming, normed, factor, gain):
    scaled = incoming * gain
    resid_grad = factor * (
        scaled
        - jnp.mean(scaled, axis=-1, keepdims=True)
        - normed * jnp.mean(scaled * normed, axis=-1, keepdims=True)
    )
    return (resid_grad, jnp.sum(incoming * normed, axis=0), jnp.sum(incoming, axis=0))


def inner_rows(left, right):
    return lax.dot_general(
        left, right, (((0,), (0,)), ((), ())), preferred_element_type=jnp.float32
    )


def times_trans(left, right):
    return lax.dot_general(
        left, right, (((1,), (1,)), ((), ())), preferred_element_type=jnp.float32
    )


def gelu_exact(value):
    return jax.nn.gelu(value, approximate=False)


def sequence_ids(lengths, group_rows):
    ending = jnp.cumsum(lengths)
    opening = ending - lengths
    places = jnp.arange(group_rows, dtype=jnp.int32)
    member = jnp.sum((places[:, None] >= ending[None, :]).astype(jnp.int32), axis=1)
    leading = jnp.any(places[:, None] == opening[None, :], axis=1)
    return (member, leading)


def split_vector(vector, model_width):
    pieces = [vector[index * model_width : (index + 1) * model_width] for index in range(8)]
    pieces.append(vector[8 * model_width :])
    return pieces


def fetch_forward(entry_weight, exit_weight, expand_weight, shrink_weight, vectors, layer_index):
    return (
        lax.all_gather(entry_weight[layer_index].astype(jnp.bfloat16), "shard", axis=0, tiled=True),
        lax.all_gather(exit_weight[layer_index].astype(jnp.bfloat16), "shard", axis=0, tiled=True),
        lax.all_gather(
            expand_weight[layer_index].astype(jnp.bfloat16), "shard", axis=0, tiled=True
        ),
        lax.all_gather(
            shrink_weight[layer_index].astype(jnp.bfloat16), "shard", axis=0, tiled=True
        ),
        lax.all_gather(vectors[layer_index].astype(jnp.bfloat16), "shard", axis=0, tiled=True),
    )


def fetch_backward(entry_weight, exit_weight, expand_weight, shrink_weight, vectors, layer_index):
    return (
        lax.all_gather(entry_weight[layer_index].astype(jnp.bfloat16), "shard", axis=0, tiled=True),
        lax.all_gather(exit_weight[layer_index].astype(jnp.bfloat16), "shard", axis=0, tiled=True),
        lax.all_gather(
            expand_weight[layer_index].astype(jnp.bfloat16), "shard", axis=0, tiled=True
        ),
        lax.all_gather(
            shrink_weight[layer_index].astype(jnp.bfloat16), "shard", axis=0, tiled=True
        ),
        lax.all_gather(vectors[layer_index].astype(jnp.bfloat16), "shard", axis=0, tiled=True),
    )


def attend_forward(queries, keys, values, own_member, member, usable):
    local_rows = queries.shape[0]
    query_heads = queries.reshape(local_rows, HEADS, HEAD_DIM)
    factor_scale = HEAD_DIM ** (-0.5)
    start_state = (
        jnp.full((HEADS, local_rows), NEG_FILL, jnp.float32),
        jnp.zeros((HEADS, local_rows), jnp.float32),
        jnp.zeros((HEADS, local_rows, HEAD_DIM), jnp.float32),
    )
    key_piece = lax.all_gather(keys, "shard", axis=0, tiled=True)
    value_piece = lax.all_gather(values, "shard", axis=0, tiled=True)
    amount = key_piece.shape[0]
    block_rows = local_rows * max(1, 512 // local_rows)

    def fold_advance(block_index, running):
        running_max, running_total, weighted = running
        begin = block_index * block_rows
        key_block = lax.dynamic_slice_in_dim(key_piece, begin, block_rows, 0).reshape(
            block_rows, HEADS, HEAD_DIM
        )
        value_block = lax.dynamic_slice_in_dim(value_piece, begin, block_rows, 0).reshape(
            block_rows, HEADS, HEAD_DIM
        )
        key_member = lax.dynamic_slice_in_dim(member, begin, block_rows, 0)
        key_usable = lax.dynamic_slice_in_dim(usable, begin, block_rows, 0)
        allowed = ((own_member[:, None] == key_member[None, :]) & key_usable[None, :])[None]
        scores = (
            jnp.einsum("qhd,khd->hqk", query_heads, key_block, preferred_element_type=jnp.float32)
            * factor_scale
        )
        scores = jnp.where(allowed, scores, NEG_FILL)
        new_max = jnp.maximum(running_max, jnp.max(scores, axis=2))
        expos = jnp.where(allowed, jnp.exp(scores - new_max[:, :, None]), 0.0)
        shrink_by = jnp.exp(running_max - new_max)
        new_total = running_total * shrink_by + jnp.sum(expos, axis=2)
        new_weighted = weighted * shrink_by[:, :, None] + jnp.einsum(
            "hqk,khd->hqd",
            expos.astype(jnp.bfloat16),
            value_block,
            preferred_element_type=jnp.float32,
        )
        return (new_max, new_total, new_weighted)

    running_max, running_total, weighted = lax.fori_loop(
        0, amount // block_rows, fold_advance, start_state
    )
    attended = jnp.transpose(weighted / running_total[:, :, None], (1, 0, 2)).reshape(
        local_rows, HEADS * HEAD_DIM
    )
    return (attended, running_max + jnp.log(running_total))


def attend_backward(
    queries, attended_grad, log_total, deltas, keys_all, values_all, own_member, member, usable
):
    local_rows = queries.shape[0]
    group_rows = keys_all.shape[0]
    model_width = HEADS * HEAD_DIM
    factor_scale = HEAD_DIM ** (-0.5)
    query_heads = queries.reshape(local_rows, HEADS, HEAD_DIM)
    grad_heads = attended_grad.reshape(local_rows, HEADS, HEAD_DIM)
    block_rows = min(512, group_rows)

    def attend_advance(query_sum, block_index):
        begin = block_index * block_rows
        key_block = lax.dynamic_slice_in_dim(keys_all, begin, block_rows, 0).reshape(
            block_rows, HEADS, HEAD_DIM
        )
        value_block = lax.dynamic_slice_in_dim(values_all, begin, block_rows, 0).reshape(
            block_rows, HEADS, HEAD_DIM
        )
        key_member = lax.dynamic_slice_in_dim(member, begin, block_rows, 0)
        key_usable = lax.dynamic_slice_in_dim(usable, begin, block_rows, 0)
        allowed = ((own_member[:, None] == key_member[None, :]) & key_usable[None, :])[None]
        scores = (
            jnp.einsum("qhd,khd->hqk", query_heads, key_block, preferred_element_type=jnp.float32)
            * factor_scale
        )
        probs = jnp.where(allowed, jnp.exp(scores - log_total[:, :, None]), 0.0)
        prob_grad = jnp.einsum(
            "qhd,khd->hqk", grad_heads, value_block, preferred_element_type=jnp.float32
        )
        score_grad = (probs * (prob_grad - deltas[:, :, None])).astype(jnp.bfloat16)
        query_sum = (
            query_sum
            + jnp.einsum("hqk,khd->qhd", score_grad, key_block, preferred_element_type=jnp.float32)
            * factor_scale
        )
        key_grad = (
            jnp.einsum("hqk,qhd->khd", score_grad, query_heads, preferred_element_type=jnp.float32)
            * factor_scale
        )
        value_grad = jnp.einsum(
            "hqk,qhd->khd",
            probs.astype(jnp.bfloat16),
            grad_heads,
            preferred_element_type=jnp.float32,
        )
        joined = jnp.concatenate(
            [
                key_grad.reshape(block_rows, model_width),
                value_grad.reshape(block_rows, model_width),
            ],
            axis=1,
        )
        return (query_sum, joined)

    query_sum, key_value = lax.scan(
        attend_advance,
        jnp.zeros((local_rows, HEADS, HEAD_DIM), jnp.float32),
        jnp.arange(group_rows // block_rows, dtype=jnp.int32),
    )
    key_value = key_value.reshape(group_rows, 2 * model_width)
    return (query_sum.reshape(local_rows, model_width), key_value)


def layer_forward(hidden, weights, own_member, member, usable):
    entry, leaving, expand, shrink, vector = weights
    model_width = leaving.shape[0]
    pieces = split_vector(vector.astype(jnp.float32), model_width)
    flat = hidden.astype(jnp.bfloat16)
    mixed = jnp.dot(flat, entry, preferred_element_type=jnp.float32)
    queries = (mixed[:, 0:model_width] + pieces[0]).astype(jnp.bfloat16)
    keys = mixed[:, model_width : 2 * model_width].astype(jnp.bfloat16)
    values = (mixed[:, 2 * model_width : 3 * model_width] + pieces[1]).astype(jnp.bfloat16)
    attended, log_total = attend_forward(queries, keys, values, own_member, member, usable)
    attended_low = attended.astype(jnp.bfloat16)
    branch = jnp.dot(attended_low, leaving, preferred_element_type=jnp.float32) + pieces[2]
    middle, normed_one, factor_one = norm_forward(hidden + branch, pieces[3], pieces[4])
    middle_low = middle.astype(jnp.bfloat16)
    inner = jnp.dot(middle_low, expand, preferred_element_type=jnp.float32) + pieces[8]
    active = gelu_exact(inner).astype(jnp.bfloat16)
    branch_two = jnp.dot(active, shrink, preferred_element_type=jnp.float32) + pieces[5]
    result, normed_two, factor_two = norm_forward(middle + branch_two, pieces[6], pieces[7])
    record = (
        flat,
        queries,
        keys,
        values,
        attended,
        log_total,
        attended_low,
        normed_one,
        factor_one,
        middle_low,
        inner,
        active,
        normed_two,
        factor_two,
    )
    return (result, record)


def layer_backward(upstream, weights, record, keys_all, values_all, own_member, member, usable):
    entry, leaving, expand, shrink, vector = weights
    model_width = leaving.shape[0]
    pieces = split_vector(vector.astype(jnp.float32), model_width)
    (
        flat,
        queries,
        keys,
        values,
        attended,
        log_total,
        attended_low,
        normed_one,
        factor_one,
        middle_low,
        inner,
        active,
        normed_two,
        factor_two,
    ) = record
    local_rows = queries.shape[0]
    resid_two, gain_two_grad, shift_two_grad = norm_backward(
        upstream, normed_two, factor_two, pieces[6]
    )
    branch_two_grad = resid_two.astype(jnp.bfloat16)
    bias_down_grad = jnp.sum(branch_two_grad.astype(jnp.float32), axis=0)
    shrink_grad = inner_rows(active, branch_two_grad)
    active_grad = times_trans(branch_two_grad, shrink)
    unused_value, gelu_pull = jax.vjp(gelu_exact, inner)
    inner_grad = gelu_pull(active_grad)[0].astype(jnp.bfloat16)
    bias_up_grad = jnp.sum(inner_grad.astype(jnp.float32), axis=0)
    expand_grad = inner_rows(middle_low, inner_grad)
    middle_grad = resid_two + times_trans(inner_grad, expand)
    resid_one, gain_one_grad, shift_one_grad = norm_backward(
        middle_grad, normed_one, factor_one, pieces[3]
    )
    branch_grad = resid_one.astype(jnp.bfloat16)
    bias_out_grad = jnp.sum(branch_grad.astype(jnp.float32), axis=0)
    exit_grad = inner_rows(attended_low, branch_grad)
    attended_grad = times_trans(branch_grad, leaving).astype(jnp.bfloat16)
    deltas = jnp.sum(
        (attended_grad.astype(jnp.float32) * attended).reshape(local_rows, HEADS, HEAD_DIM), axis=2
    ).T
    query_grad, key_value_grad = attend_backward(
        queries, attended_grad, log_total, deltas, keys_all, values_all, own_member, member, usable
    )
    own_key_value = lax.psum_scatter(
        key_value_grad.astype(jnp.bfloat16), "shard", scatter_dimension=0, tiled=True
    ).astype(jnp.float32)
    mixed_grad = jnp.concatenate([query_grad, own_key_value], axis=1).astype(jnp.bfloat16)
    bias_query_grad = jnp.sum(mixed_grad[:, 0:model_width].astype(jnp.float32), axis=0)
    bias_value_grad = jnp.sum(
        mixed_grad[:, 2 * model_width : 3 * model_width].astype(jnp.float32), axis=0
    )
    entry_grad = inner_rows(flat, mixed_grad)
    hidden_grad = resid_one + times_trans(mixed_grad, entry)
    vector_grad = jnp.concatenate(
        [
            bias_query_grad,
            bias_value_grad,
            bias_out_grad,
            gain_one_grad,
            shift_one_grad,
            bias_down_grad,
            gain_two_grad,
            shift_two_grad,
            bias_up_grad,
        ]
    )
    return (hidden_grad, (entry_grad, exit_grad, expand_grad, shrink_grad, vector_grad))


def body(
    inputs,
    cotangent,
    lengths,
    dealing,
    key_mask,
    entry_weight,
    exit_weight,
    expand_weight,
    shrink_weight,
    vectors,
):
    local_rows = inputs.shape[0]
    group_rows = local_rows * lax.axis_size("shard")
    position = lax.axis_index("shard") * local_rows
    dealt_all, mask_all = (
        lax.all_gather(dealing, "shard", axis=1, tiled=True),
        lax.all_gather(key_mask, "shard", axis=1, tiled=True),
    )
    member, leading = sequence_ids(lengths[0], group_rows)
    usable = (mask_all[0] == 1) | leading
    own_member = lax.dynamic_slice_in_dim(member, position, local_rows, 0)
    inverse = (
        jnp.zeros((group_rows,), jnp.int32)
        .at[dealt_all[0]]
        .set(jnp.arange(group_rows, dtype=jnp.int32))
    )
    own_inverse = lax.dynamic_slice_in_dim(inverse, position, local_rows, 0)
    inputs_all, cotangent_all = (
        lax.all_gather(inputs, "shard", axis=0, tiled=True),
        lax.all_gather(cotangent, "shard", axis=0, tiled=True),
    )
    hidden = jnp.take(inputs_all, dealing[0], axis=0).astype(jnp.float32)
    upstream = jnp.take(cotangent_all, dealing[0], axis=0).astype(jnp.float32)
    layers = entry_weight.shape[0]
    saved = []
    kept = []
    for layer_index in range(layers):
        weights = fetch_forward(
            entry_weight, exit_weight, expand_weight, shrink_weight, vectors, layer_index
        )
        kept.append(weights)
        hidden, record = layer_forward(hidden, weights, own_member, member, usable)
        saved.append(record)
    output_all = lax.all_gather(hidden.astype(jnp.bfloat16), "shard", axis=0, tiled=True)
    output = jnp.take(output_all, own_inverse, axis=0)
    hidden_grad = upstream
    layer_grads = [None] * layers
    for layer_index in reversed(range(layers)):
        weights = fetch_backward(
            entry_weight, exit_weight, expand_weight, shrink_weight, vectors, layer_index
        )
        record = saved[layer_index]
        keys_all, values_all = (
            lax.all_gather(record[2], "shard", axis=0, tiled=True),
            lax.all_gather(record[3], "shard", axis=0, tiled=True),
        )
        hidden_grad, local_grads = layer_backward(
            hidden_grad, weights, record, keys_all, values_all, own_member, member, usable
        )
        entry_local, exit_local, expand_local, shrink_local, vector_local = local_grads
        entry_part, exit_part, expand_part, shrink_part, vector_part = (
            lax.psum_scatter(
                entry_local.astype(jnp.bfloat16), "shard", scatter_dimension=0, tiled=True
            ).astype(jnp.float32),
            lax.psum_scatter(
                exit_local.astype(jnp.bfloat16), "shard", scatter_dimension=0, tiled=True
            ).astype(jnp.float32),
            lax.psum_scatter(
                expand_local.astype(jnp.bfloat16), "shard", scatter_dimension=0, tiled=True
            ).astype(jnp.float32),
            lax.psum_scatter(
                shrink_local.astype(jnp.bfloat16), "shard", scatter_dimension=0, tiled=True
            ).astype(jnp.float32),
            lax.psum_scatter(
                vector_local.astype(jnp.bfloat16), "shard", scatter_dimension=0, tiled=True
            ).astype(jnp.float32),
        )
        entry_part, exit_part, expand_part, shrink_part, vector_part = (
            lax.psum(entry_part.astype(jnp.bfloat16), "rep").astype(jnp.float32),
            lax.psum(exit_part.astype(jnp.bfloat16), "rep").astype(jnp.float32),
            lax.psum(expand_part.astype(jnp.bfloat16), "rep").astype(jnp.float32),
            lax.psum(shrink_part.astype(jnp.bfloat16), "rep").astype(jnp.float32),
            lax.psum(vector_part.astype(jnp.bfloat16), "rep").astype(jnp.float32),
        )
        layer_grads[layer_index] = (entry_part, exit_part, expand_part, shrink_part, vector_part)
    entry_grad = jnp.stack([item[0] for item in layer_grads])
    exit_grad = jnp.stack([item[1] for item in layer_grads])
    expand_grad = jnp.stack([item[2] for item in layer_grads])
    shrink_grad = jnp.stack([item[3] for item in layer_grads])
    vector_grad = jnp.stack([item[4] for item in layer_grads])
    grads_all = lax.all_gather(
        hidden_grad.astype(jnp.bfloat16), "shard", axis=0, tiled=True
    ).astype(hidden_grad.dtype)
    input_grad = jnp.take(grads_all, own_inverse, axis=0)
    return (output, input_grad, entry_grad, exit_grad, expand_grad, shrink_grad, vector_grad)


EDGE = (0, 1, 6, 7)
CORE = (2, 3, 4, 5)
ALL = tuple(range(8))
BOTH = ("rep", "shard")
UNIT = 24


def routes(rep_flip, shard_flip, shards):
    return [
        (rep * 8 + shard, (rep ^ rep_flip) * 8 + (shard ^ shard_flip))
        for rep in range(4)
        for shard in shards
    ]


TO_X = routes(1, 0, ALL)
TO_Y = routes(2, 0, ALL)
TO_TWIN = routes(0, 1, ALL)
TO_SIDE = routes(0, 2, ALL)
TO_MID = routes(0, 6, CORE) + routes(0, 1, EDGE)


def send(value, route):
    return lax.ppermute(value, BOTH, route)


def low(value):
    return value.astype(jnp.bfloat16)


def wide(value):
    return value.astype(jnp.float32)


VMEM = pl.BlockSpec(memory_space=pltpu.VMEM)
SMEM = pl.BlockSpec(memory_space=pltpu.SMEM)
LIMIT = pltpu.CompilerParams(vmem_limit_bytes=60 * 1024 * 1024)


def shaped(shape, kind=jnp.bfloat16):
    return jax.ShapeDtypeStruct(shape, kind)


def cost(micros):
    return pl.CostEstimate(
        flops=int(micros * 1e9), bytes_accessed=int(micros * 1e6), transcendentals=0
    )


def nt(left, right):
    return lax.dot_general(left, right, (((1,), (1,)), ((), ())), preferred_element_type=jnp.float32)


def nn(left, right):
    return lax.dot_general(left, right, (((1,), (0,)), ((), ())), preferred_element_type=jnp.float32)


def fixed(*shape):
    return pl.BlockSpec(shape, lambda step: (0,) * len(shape))


def gather_kernel(ids_ref, want_ref, *refs):
    out_ref = refs[-1]
    want = want_ref[...]
    total = None
    index = 0
    for piece_ref in refs[:-1]:
        for slot in range(piece_ref.shape[0]):
            ids = ids_ref[index]
            hit = low(wide(want == ids))
            part = nn(hit, piece_ref[slot, 0 : ids.shape[1], :])
            total = part if total is None else total + part
            index += 1
    out_ref[...] = low(total)


def gather_rows(pieces, ids, want, spend):
    return pl.pallas_call(
        gather_kernel,
        out_shape=shaped((want.shape[0], pieces[0].shape[2])),
        in_specs=[VMEM] * (2 + len(pieces)),
        out_specs=VMEM,
        compiler_params=LIMIT,
        cost_estimate=cost(spend),
        name="gather_rows",
    )(ids, want, *pieces)


def assemble_kernel(where_ref, *refs):
    out_ref = refs[10]
    depth, rep, twin = where_ref[0], where_ref[1], where_ref[2]
    for side in range(2):
        own, first, over_x, over_y, over_d = refs[side * 5 : side * 5 + 5]
        core = twin ^ side
        for row in range(4):
            out_ref[depth, core, row] = own[row]
        for slot, flip in enumerate((1, 3, 2)):
            level = depth ^ flip
            for piece, bits in ((first, 0), (over_x, 1), (over_y, 2), (over_d, 3)):
                out_ref[level, core, rep ^ bits] = piece[slot]


def assemble(where, parts, start, by_rows):
    def part_spec(part):
        return pl.BlockSpec(
            (part.shape[0], None) + part.shape[2:],
            lambda unit, where_ref: (0, start + unit, 0, 0),
        )

    width = parts[0].shape[3]
    if by_rows:
        shape = (4, 2, 4, 4, UNIT, width)
        spec = pl.BlockSpec(
            (4, 2, 4, None, UNIT, width), lambda unit, where_ref: (0, 0, 0, unit, 0, 0)
        )
    else:
        shape = (4, 4, 2, 4, UNIT, width)
        spec = pl.BlockSpec(
            (None, 4, 2, 4, UNIT, width), lambda unit, where_ref: (unit, 0, 0, 0, 0, 0)
        )
    result = pl.pallas_call(
        assemble_kernel,
        grid_spec=pltpu.PrefetchScalarGridSpec(
            num_scalar_prefetch=1,
            grid=(4,),
            in_specs=[part_spec(part) for part in parts],
            out_specs=spec,
        ),
        out_shape=shaped(shape),
        compiler_params=LIMIT,
        cost_estimate=cost(0.3),
        name="assemble",
    )(where, *parts)
    return result.reshape(4, 32 * UNIT, width)


def tie(value, *others):
    return lax.optimization_barrier((value,) + others)[0]


def after(values, *others):
    return list(lax.optimization_barrier(tuple(values) + others)[: len(values)])


class Spread:
    def __init__(self, own, first, x_last):
        self.own, self.first, self.x_last = own, first, x_last
        self.over = [send(first, TO_X), send(first, TO_Y)]
        self.twins = [send(own, TO_TWIN), send(first, TO_TWIN)]

    def turn(self, *others):
        self.over_x, self.over_y = after(self.over, *self.twins, *others)
        last = self.over_y if self.x_last else self.over_x
        self.over_d = send(last, TO_X if self.x_last else TO_Y)
        self.twins += [send(self.over_x, TO_TWIN), send(self.over_y, TO_TWIN)]
        return self.over_x

    def parts(self, *others):
        over_d = after([self.over_d], *self.twins, *others)[0]
        mine = (self.own, self.first, self.over_x, self.over_y, over_d)
        return mine + tuple(self.twins) + (send(over_d, TO_TWIN),)


def project_kernel(h_ref, w_ref, vec_ref, sel_ref, q_ref, kv_ref, mine_ref, theirs_ref):
    unit = pl.program_id(0)
    product = nn(h_ref[...], w_ref[...])

    @pl.when(unit == 0)
    def _():
        q_ref[...] = low(product + vec_ref[0:1, :])
        mine_ref[...] = low(nn(h_ref[...], sel_ref[0]))
        theirs_ref[...] = low(nn(h_ref[...], sel_ref[1]))

    @pl.when(unit == 1)
    def _():
        kv_ref[...] = low(product)

    @pl.when(unit == 2)
    def _():
        kv_ref[...] = low(product + vec_ref[1:2, :])


def project(hidden, weight, vec, sel):
    rows, width = hidden.shape
    return pl.pallas_call(
        project_kernel,
        grid=(3,),
        in_specs=[
            fixed(rows, width),
            pl.BlockSpec((None, width, width), lambda unit: (unit, 0, 0)),
            fixed(12, width),
            fixed(2, width, width // 2),
        ],
        out_specs=[
            fixed(rows, width),
            pl.BlockSpec((None, rows, width), lambda unit: (jnp.maximum(unit - 1, 0), 0, 0)),
            fixed(rows, width // 2),
            fixed(rows, width // 2),
        ],
        out_shape=[
            shaped((rows, width)),
            shaped((2, rows, width)),
            shaped((rows, width // 2)),
            shaped((rows, width // 2)),
        ],
        compiler_params=LIMIT,
        cost_estimate=cost(0.3),
        name="project",
    )(hidden, weight, vec, sel)


def attend_kernel(
    q_ref, ka_ref, kb_ref, va_ref, vb_ref, code_ref, member_ref, o_ref, ot_ref, lse_ref, bias_ref
):
    half = q_ref.shape[0]

    @pl.when(pl.program_id(0) == 0)
    def _():
        bias_ref[...] = jnp.where(code_ref[...] == member_ref[...], 0.0, NEG_FILL)

    q = q_ref[...] * jnp.bfloat16(HEAD_DIM ** (-0.5))
    lane = lax.broadcasted_iota(jnp.int32, q.shape, 1)
    keys = (ka_ref[...], kb_ref[...])
    values = (va_ref[...].T, vb_ref[...].T)
    outs = []
    for head in range(2):
        q_head = jnp.where((lane >= HEAD_DIM) == (head == 1), q, jnp.bfloat16(0))
        scores = [
            nt(keys[side], q_head) + bias_ref[side * half : (side + 1) * half, :]
            for side in range(2)
        ]
        top = jnp.maximum(
            jnp.max(scores[0], axis=0, keepdims=True), jnp.max(scores[1], axis=0, keepdims=True)
        )
        total = None
        mixed = None
        for side in range(2):
            expo = jnp.exp(scores[side] - top)
            part = jnp.sum(expo, axis=0, keepdims=True)
            value = values[side][head * HEAD_DIM : (head + 1) * HEAD_DIM, :]
            product = nn(value, low(expo))
            total = part if total is None else total + part
            mixed = product if mixed is None else mixed + product
        outs.append(mixed / total)
        lse_ref[head : head + 1, :] = top + jnp.log(total)
    joined = jnp.concatenate(outs, axis=0)
    ot_ref[...] = joined
    o_ref[...] = low(joined.T)


def pair_specs(half):
    column = pl.BlockSpec((half, 128), lambda pair: (0, pair))
    key = pl.BlockSpec((None, half, 128), lambda pair: (0, 0, pair))
    value = pl.BlockSpec((None, half, 128), lambda pair: (1, 0, pair))
    turned = pl.BlockSpec((128, half), lambda pair: (pair, 0))
    level = pl.BlockSpec((None, 2, half), lambda pair: (pair, 0, 0))
    return column, key, value, turned, level


def attend_fast(queries, kv, kv_twin, code, member):
    half, width = queries.shape
    column, key, value, turned, level = pair_specs(half)
    return pl.pallas_call(
        attend_kernel,
        grid=(width // 128,),
        in_specs=[column, key, key, value, value, fixed(2 * half, 1), fixed(1, half)],
        out_specs=[column, turned, level],
        out_shape=[
            shaped((half, width)),
            shaped((width, half), jnp.float32),
            shaped((width // 128, 2, half), jnp.float32),
        ],
        scratch_shapes=[pltpu.VMEM((2 * half, half), jnp.float32)],
        compiler_params=LIMIT,
        cost_estimate=cost(0.3),
        name="attend_forward",
    )(queries, kv, kv_twin, kv, kv_twin, code, member)


def attend_back_kernel(
    q_ref, g_ref, ka_ref, kb_ref, va_ref, vb_ref, ot_ref, lse_ref, code_ref, member_ref,
    dq_ref, own_ref, twin_ref, bias_ref,
):
    half = q_ref.shape[0]

    @pl.when(pl.program_id(0) == 0)
    def _():
        bias_ref[...] = jnp.where(code_ref[...] == member_ref[...], 0.0, NEG_FILL)

    scale = HEAD_DIM ** (-0.5)
    q = q_ref[...] * jnp.bfloat16(scale)
    grad = g_ref[...]
    lane = lax.broadcasted_iota(jnp.int32, q.shape, 1)
    keys = (ka_ref[...], kb_ref[...])
    turned = (keys[0].T, keys[1].T)
    values = (va_ref[...], vb_ref[...])
    product = ot_ref[...] * wide(grad).T
    key_sums = [None, None]
    value_sums = [None, None]
    query_parts = []
    for head in range(2):
        rows = slice(head * HEAD_DIM, (head + 1) * HEAD_DIM)
        chosen = (lane >= HEAD_DIM) == (head == 1)
        q_head = jnp.where(chosen, q, jnp.bfloat16(0))
        g_head = jnp.where(chosen, grad, jnp.bfloat16(0))
        delta = jnp.sum(product[rows, :], axis=0, keepdims=True)
        level = lse_ref[head : head + 1, :]
        query_sum = None
        for side in range(2):
            scores = nt(keys[side], q_head) + bias_ref[side * half : (side + 1) * half, :]
            prob = jnp.exp(scores - level)
            slope = nt(values[side], g_head)
            steep = low(prob * (slope - delta))
            value_part = nn(low(prob), g_head)
            key_part = nn(steep, q_head)
            query_part = nn(turned[side][rows, :], steep)
            value_sums[side] = value_part if head == 0 else value_sums[side] + value_part
            key_sums[side] = key_part if head == 0 else key_sums[side] + key_part
            query_sum = query_part if side == 0 else query_sum + query_part
        query_parts.append(query_sum * scale)
    dq_ref[...] = low(jnp.concatenate(query_parts, axis=0).T)
    own_ref[0] = key_sums[0]
    own_ref[1] = value_sums[0]
    twin_ref[0] = low(key_sums[1])
    twin_ref[1] = low(value_sums[1])


def attend_back_fast(queries, grad, kv, kv_twin, ot, lse, code, member, spend):
    half, width = queries.shape
    column, key, value, turned, level = pair_specs(half)
    both = pl.BlockSpec((2, half, 128), lambda pair: (0, 0, pair))
    return pl.pallas_call(
        attend_back_kernel,
        grid=(width // 128,),
        in_specs=[column, column, key, key, value, value, turned, level]
        + [fixed(2 * half, 1), fixed(1, half)],
        out_specs=[column, both, both],
        out_shape=[
            shaped((half, width)),
            shaped((2, half, width), jnp.float32),
            shaped((2, half, width)),
        ],
        scratch_shapes=[pltpu.VMEM((2 * half, half), jnp.float32)],
        compiler_params=LIMIT,
        cost_estimate=cost(spend),
        name="attend_backward",
    )(queries, grad, kv, kv_twin, kv, kv_twin, ot, lse, code, member)


def normal_parts(value):
    scaled = value * 0.7071067811865476
    size = jnp.abs(scaled)
    square = size * size
    t = 1.0 / (1.0 + 0.5 * size)
    series = 0.17087277
    for factor in (
        -0.82215223, 1.48851587, -1.13520398, 0.27886807, -0.18628806,
        0.09678418, 0.37409196, 1.00002368, -1.26551223,
    ):
        series = series * t + factor
    tail = 0.5 * t * jnp.exp(series - square)
    cumulative = jnp.where(value >= 0, 1.0 - tail, tail)
    density = 0.3989422804014327 * jnp.exp(-square)
    return cumulative, density


def row_norm(resid):
    offsets = resid - jnp.mean(resid, axis=-1, keepdims=True)
    spread_of = jnp.mean(offsets * offsets, axis=-1, keepdims=True)
    factor = lax.rsqrt(spread_of + 1e-05)
    return offsets * factor, factor


def post_kernel(
    where_ref, o_ref, h_ref, wo_ref, up_ref, down_ref, vec_ref, sel_ref,
    h_out, hl_out, n1_out, t1_out, n2_out, t2_out, slope_out, mine_out, theirs_out,
    y_ref, yl_ref, f_ref,
):
    step = pl.program_id(0)
    half_width = mine_out.shape[2]

    @pl.when(step == 0)
    def _():
        attended = o_ref[...]
        branch = nn(attended, wo_ref[...]) + vec_ref[2:3, :]
        normed, factor = row_norm(wide(h_ref[...]) + branch)
        middle = normed * vec_ref[3:4, :] + vec_ref[4:5, :]
        n1_out[...] = normed
        t1_out[...] = factor
        y_ref[...] = middle
        yl_ref[...] = low(middle)
        mine_out[4] = low(nn(yl_ref[...], sel_ref[0]))
        theirs_out[4] = low(nn(yl_ref[...], sel_ref[1]))
        mine_out[5] = low(nn(attended, sel_ref[0]))
        theirs_out[5] = low(nn(attended, sel_ref[1]))

    inner = nn(yl_ref[...], up_ref[...]) + vec_ref[pl.ds(8 + step, 1), :]
    cumulative, density = normal_parts(inner)
    slope_out[...] = low(cumulative + inner * density)
    active = low(inner * cumulative)
    first, second = active[:, :half_width], active[:, half_width:]
    swap = where_ref[2] == 1
    mine_out[step] = jnp.where(swap, second, first)
    theirs_out[step] = jnp.where(swap, first, second)
    part = nn(active, down_ref[...])

    @pl.when(step == 0)
    def _():
        f_ref[...] = part

    @pl.when(step > 0)
    def _():
        f_ref[...] += part

    @pl.when(step == 3)
    def _():
        normed, factor = row_norm(y_ref[...] + (f_ref[...] + vec_ref[5:6, :]))
        result = normed * vec_ref[6:7, :] + vec_ref[7:8, :]
        n2_out[...] = normed
        t2_out[...] = factor
        h_out[...] = result
        hl_out[...] = low(result)


def unit_spec(width, index):
    return pl.BlockSpec((None, width, width), lambda step: (index, 0, 0))


def step_spec(width):
    return pl.BlockSpec((None, width, width), lambda step: (step, 0, 0))


def column_spec(rows, width):
    return pl.BlockSpec((rows, width), lambda step: (0, step))


def post(where, attended, hidden, front, up, down, vec, sel):
    rows, width = attended.shape
    half = width // 2
    full = fixed(rows, width)
    thin = fixed(rows, 1)
    return pl.pallas_call(
        post_kernel,
        grid=(4,),
        in_specs=[
            SMEM, full, full, unit_spec(width, 3), step_spec(width), step_spec(width),
            fixed(12, width), fixed(2, width, half),
        ],
        out_specs=[full, full, full, thin, full, thin, column_spec(rows, width)]
        + [fixed(6, rows, half)] * 2,
        out_shape=[
            shaped((rows, width), jnp.float32),
            shaped((rows, width)),
            shaped((rows, width), jnp.float32),
            shaped((rows, 1), jnp.float32),
            shaped((rows, width), jnp.float32),
            shaped((rows, 1), jnp.float32),
            shaped((rows, 4 * width)),
        ]
        + [shaped((6, rows, half))] * 2,
        scratch_shapes=[
            pltpu.VMEM((rows, width), jnp.float32),
            pltpu.VMEM((rows, width), jnp.bfloat16),
            pltpu.VMEM((rows, width), jnp.float32),
        ],
        compiler_params=LIMIT,
        cost_estimate=cost(0.3),
        name="post",
    )(where, attended, hidden, front, up, down, vec, sel)


def norm_back(incoming, normed, factor, gain):
    scaled = incoming * gain
    return factor * (
        scaled
        - jnp.mean(scaled, axis=-1, keepdims=True)
        - normed * jnp.mean(scaled * normed, axis=-1, keepdims=True)
    )


def column_sum(value):
    return jnp.sum(value, axis=0, keepdims=True)


def post_back_kernel(
    e_ref, n1_ref, t1_ref, n2_ref, t2_ref, slope_ref, wo_ref, up_ref, down_ref, vec_ref,
    all_out, do_out, dr_out, sums_out,
    r_ref, y_ref,
):
    step = pl.program_id(0)

    @pl.when(step == 0)
    def _():
        incoming = wide(e_ref[...])
        normed = n2_ref[...]
        resid = norm_back(incoming, normed, t2_ref[...], vec_ref[6:7, :])
        r_ref[...] = resid
        rounded = low(resid)
        all_out[4] = rounded
        sums_out[0:2, :] = jnp.zeros((2, sums_out.shape[1]), jnp.float32)
        sums_out[5:6, :] = column_sum(wide(rounded))
        sums_out[6:7, :] = column_sum(incoming * normed)
        sums_out[7:8, :] = column_sum(incoming)

    steep = low(nt(all_out[4], down_ref[...]) * wide(slope_ref[...]))
    all_out[step] = steep
    sums_out[pl.ds(8 + step, 1), :] = column_sum(wide(steep))
    part = nt(steep, up_ref[...])

    @pl.when(step == 0)
    def _():
        y_ref[...] = part

    @pl.when(step > 0)
    def _():
        y_ref[...] += part

    @pl.when(step == 3)
    def _():
        incoming = r_ref[...] + y_ref[...]
        normed = n1_ref[...]
        resid = norm_back(incoming, normed, t1_ref[...], vec_ref[3:4, :])
        dr_out[...] = resid
        rounded = low(resid)
        all_out[5] = rounded
        do_out[...] = low(nt(rounded, wo_ref[...]))
        sums_out[2:3, :] = column_sum(wide(rounded))
        sums_out[3:4, :] = column_sum(incoming * normed)
        sums_out[4:5, :] = column_sum(incoming)


def post_back(upstream, n1, t1, n2, t2, slope, front, up, down, vec, spend):
    rows, width = upstream.shape
    full = fixed(rows, width)
    thin = fixed(rows, 1)
    return pl.pallas_call(
        post_back_kernel,
        grid=(4,),
        in_specs=[
            full, full, thin, full, thin, column_spec(rows, width),
            unit_spec(width, 3), step_spec(width), step_spec(width), fixed(12, width),
        ],
        out_specs=[fixed(6, rows, width), full, full, fixed(12, width)],
        out_shape=[
            shaped((6, rows, width)),
            shaped((rows, width)),
            shaped((rows, width), jnp.float32),
            shaped((12, width), jnp.float32),
        ],
        scratch_shapes=[
            pltpu.VMEM((rows, width), jnp.float32),
            pltpu.VMEM((rows, width), jnp.float32),
        ],
        compiler_params=LIMIT,
        cost_estimate=cost(spend),
        name="post_back",
    )(upstream, n1, t1, n2, t2, slope, front, up, down, vec)


def project_back_kernel(
    dq_ref, own_ref, got_ref, w_ref, dr_ref, dm_out, dx_out, dxl_out, sums_out
):
    unit = pl.program_id(0)

    @pl.when(unit == 0)
    def _():
        dm_out[...] = dq_ref[...]

    @pl.when(unit > 0)
    def _():
        dm_out[...] = low(own_ref[...] + wide(got_ref[...]))

    grad = dm_out[...]
    part = nt(grad, w_ref[...])
    total = column_sum(wide(grad))

    @pl.when(unit == 0)
    def _():
        dx_out[...] = dr_ref[...] + part
        sums_out[0:1, :] = total

    @pl.when(unit > 0)
    def _():
        dx_out[...] += part
        sums_out[1:2, :] = total

    @pl.when(unit == 2)
    def _():
        dxl_out[...] = low(dx_out[...])


def project_back(dq, own, got, front, dr, spend):
    rows, width = dq.shape
    full = fixed(rows, width)
    late = pl.BlockSpec((None, rows, width), lambda unit: (jnp.maximum(unit - 1, 0), 0, 0))
    return pl.pallas_call(
        project_back_kernel,
        grid=(3,),
        in_specs=[full, late, late, step_spec(width), full],
        out_specs=[
            pl.BlockSpec((None, rows, width), lambda unit: (unit, 0, 0)),
            full, full, fixed(2, width),
        ],
        out_shape=[
            shaped((3, rows, width)),
            shaped((rows, width), jnp.float32),
            shaped((rows, width)),
            shaped((2, width), jnp.float32),
        ],
        compiler_params=LIMIT,
        cost_estimate=cost(spend),
        name="project_back",
    )(dq, own, got, front, dr)


def tn(left, right):
    return nn(left.T, right)


def split_store(keep_ref, give_ref, bit, x_first, piece_of, store):
    for other in range(2):
        pair = []
        for side in range(2):
            rep = (other * 2 + side) if x_first else (side * 2 + other)
            pair.append(low(piece_of(rep)))
        store(keep_ref, other, jnp.where(bit == 0, pair[0], pair[1]))
        store(give_ref, other, jnp.where(bit == 0, pair[1], pair[0]))


def column_store(ref_pair, bit, x_first, product, unit):
    keep_ref, give_ref = ref_pair
    for level in range(4):
        base = level * 4 * UNIT

        def piece_of(rep):
            return product[base + rep * UNIT : base + (rep + 1) * UNIT, :]

        def store(ref, other, value):
            ref[level, other, unit] = value

        split_store(keep_ref, give_ref, bit, x_first, piece_of, store)


def front_grad_kernel(
    bit_ref, xm_ref, xt_ref, om_ref, ot_ref, dm_ref, dmt_ref, da_ref, dat_ref,
    keep_x, give_x, keep_y, give_y,
):
    unit = pl.program_id(0)

    def store(product, index, x_first):
        pair = (keep_x, give_x) if x_first else (keep_y, give_y)
        column_store(pair, bit_ref[0 if x_first else 1], x_first, product, index)

    @pl.when(unit < 2)
    def _():
        store(tn(xm_ref[...], dm_ref[...]) + tn(xt_ref[...], dmt_ref[...]), unit, True)

    @pl.when(unit == 2)
    def _():
        store(tn(xm_ref[...], dm_ref[...]) + tn(xt_ref[...], dmt_ref[...]), 0, False)

    @pl.when(unit == 3)
    def _():
        store(tn(om_ref[...], da_ref[...]) + tn(ot_ref[...], dat_ref[...]), 1, False)


def block_spec(rows, width, index):
    return pl.BlockSpec((None, rows, width), lambda step: (index, 0, 0))


def front_grad(bits, xm, xt, mine, theirs, dm, dmt, da, dat, spend):
    rows, half = xm.shape
    width = da.shape[2]
    late = pl.BlockSpec((None, rows, width), lambda unit: (jnp.minimum(unit, 2), 0, 0))
    shape = (4, 2, 2, UNIT, width)
    return pl.pallas_call(
        front_grad_kernel,
        grid=(4,),
        in_specs=[SMEM, fixed(rows, half), fixed(rows, half)]
        + [block_spec(rows, half, 5)] * 2
        + [late, late]
        + [block_spec(rows, width, 5)] * 2,
        out_specs=[fixed(*shape)] * 4,
        out_shape=[shaped(shape)] * 4,
        compiler_params=LIMIT,
        cost_estimate=cost(spend),
        name="front_grad",
    )(bits, xm, xt, mine, theirs, dm, dmt, da, dat)


def feed_grad_kernel(
    x_first, bit_ref, ym_ref, yt_ref, gm_ref, gt_ref, dz_ref, dzt_ref, df_ref, dft_ref,
    keep_up, give_up, keep_down, give_down,
):
    step = pl.program_id(0)
    up_bit = bit_ref[0 if x_first else 1]
    down_bit = bit_ref[1 if x_first else 0]

    @pl.when(step < 4)
    def _():
        product = tn(ym_ref[...], dz_ref[...]) + tn(yt_ref[...], dzt_ref[...])
        column_store((keep_up, give_up), up_bit, x_first, product, step)

    @pl.when(step >= 4)
    def _():
        product = tn(gm_ref[...], df_ref[...]) + tn(gt_ref[...], dft_ref[...])
        for sub in range(4):

            def piece_of(rep):
                base = (rep * 4 + sub) * UNIT
                return product[base : base + UNIT, :]

            def store(ref, other, value):
                ref[step - 4, other, sub] = value

            split_store(keep_down, give_down, down_bit, not x_first, piece_of, store)


def feed_grad(x_first, bits, mine, theirs, slopes, slopes_twin, spend):
    rows, half = mine.shape[1:]
    width = slopes.shape[2]
    early = pl.BlockSpec((None, rows, width), lambda step: (jnp.minimum(step, 3), 0, 0))
    late = pl.BlockSpec((None, rows, half), lambda step: (jnp.maximum(step - 4, 0), 0, 0))
    shape = (4, 2, 4, UNIT, width)
    return pl.pallas_call(
        functools.partial(feed_grad_kernel, x_first),
        grid=(8,),
        in_specs=[SMEM]
        + [block_spec(rows, half, 4)] * 2
        + [late, late, early, early]
        + [block_spec(rows, width, 4)] * 2,
        out_specs=[fixed(*shape)] * 4,
        out_shape=[shaped(shape)] * 4,
        compiler_params=LIMIT,
        cost_estimate=cost(spend),
        name="feed_grad",
    )(bits, mine, theirs, mine, theirs, slopes, slopes_twin, slopes, slopes_twin)


def halve_kernel(low_ref, keep_x, got_x, keep_y, got_y, keep_out, give_out):
    start = jnp.where(low_ref[0] == 1, 0, 2)
    for index, (keep, got) in enumerate(((keep_x, got_x), (keep_y, got_y))):
        for out, begin in ((keep_out, start), (give_out, 2 - start)):
            for level in range(2):
                out[index, level] = low(wide(keep[begin + level]) + wide(got[begin + level]))


def halve_sum(is_low, keeps, gots, spend):
    count, width = keeps[0].shape[2], keeps[0].shape[4]
    whole = pl.BlockSpec((4, None, count, UNIT, width), lambda other: (0, other, 0, 0, 0))
    half = pl.BlockSpec((2, 2, None, count, UNIT, width), lambda other: (0, 0, other, 0, 0, 0))
    return pl.pallas_call(
        halve_kernel,
        grid=(2,),
        in_specs=[SMEM] + [whole] * 4,
        out_specs=[half] * 2,
        out_shape=[shaped((2, 2, 2, count, UNIT, width))] * 2,
        compiler_params=LIMIT,
        cost_estimate=cost(spend),
        name="halve_sum",
    )(is_low.astype(jnp.int32).reshape(1), keeps[0], gots[0], keeps[1], gots[1])


class Reduction:
    def __init__(self, pairs, bits, is_low, is_core):
        self.keeps = [pair[0] for pair in pairs]
        self.firsts = [pair[2] for pair in pairs]
        self.bits, self.is_low, self.is_core = bits, is_low, is_core
        self.got = [send(pair[1], TO_X if pair[2] else TO_Y) for pair in pairs]

    def across(self, spend, *others):
        got = after(self.got, *others)
        self.keep, give = halve_sum(self.is_low, self.keeps, got, spend)
        self.mid = send(give, TO_MID)
        return give

    def join(self, other):
        self.keep = jnp.concatenate([self.keep, other.keep], axis=3)
        self.mid = jnp.concatenate([self.mid, other.mid], axis=3)

    def outward(self, *others):
        mid = after([self.mid], *others)[0]
        stage = low(wide(self.keep) + wide(mid))
        outer = jnp.where(self.is_low, stage[:, 0], stage[:, 1])
        self.inner = jnp.where(self.is_low, stage[:, 1], stage[:, 0])
        self.side = send(outer, TO_SIDE)
        return outer

    def turn(self, *others):
        side = after([self.side], *others)[0]
        stage = jnp.where(self.is_core, self.inner, side)
        self.pieces = [stage[index] for index in range(len(self.firsts))]
        self.over = [
            send(piece, TO_Y if first else TO_X)
            for piece, first in zip(self.pieces, self.firsts)
        ]
        return stage

    def share(self, *others):
        over = after(self.over, *others)
        self.sums = [low(wide(piece) + wide(item)) for piece, item in zip(self.pieces, over)]
        self.got = [
            send(piece, TO_X if first else TO_Y) for piece, first in zip(self.sums, self.firsts)
        ]
        return self.sums[0]

    def finish(self, *others):
        return list(zip(self.sums, after(self.got, *others)))


def unpack_kernel(plan, bit_ref, *refs):
    outs = refs[-4:]
    width = outs[1].shape[1]
    for index, (x_first, units) in enumerate(plan):
        piece, got = refs[2 * index], refs[2 * index + 1]
        bit = bit_ref[0 if x_first else 1]
        for other in range(2):
            for side in range(2):
                rep = (other * 2 + side) if x_first else (side * 2 + other)
                for unit, (target, place) in enumerate(units):
                    value = wide(jnp.where(bit == side, piece[other, unit], got[other, unit]))
                    if target < 3:
                        rows = slice(rep * UNIT, (rep + 1) * UNIT)
                        outs[target][rows, place * width : (place + 1) * width] = value
                    else:
                        base = (rep * 4 + place) * UNIT
                        outs[target][base : base + UNIT, :] = value


def unpack(bits, pairs, plan, layer, layers, before):
    width = pairs[0][0].shape[3]
    shapes = [(4 * UNIT, 3 * width), (4 * UNIT, width), (4 * UNIT, 4 * width), (16 * UNIT, width)]
    arrays = [item for pair in pairs for item in pair]
    first = 1 + len(arrays)
    return pl.pallas_call(
        functools.partial(unpack_kernel, plan),
        grid=(1,),
        in_specs=[SMEM]
        + [fixed(*item.shape) for item in arrays]
        + [pl.BlockSpec(memory_space=pl.ANY) for _ in before],
        out_specs=[pl.BlockSpec((None,) + shape, lambda step: (layer, 0, 0)) for shape in shapes],
        out_shape=[shaped((layers,) + shape, jnp.float32) for shape in shapes],
        input_output_aliases={first + index: index for index in range(len(before))},
        compiler_params=LIMIT,
        cost_estimate=cost(3),
        name="unpack",
    )(bits, *arrays, *before)


def body_fast(
    inputs, cotangent, lengths, dealing, key_mask,
    entry_weight, exit_weight, expand_weight, shrink_weight, vectors,
):
    rows, width = inputs.shape
    layers = entry_weight.shape[0]
    group_rows = 8 * rows
    half_rows = group_rows // 2
    core_rows = half_rows // 2
    rep = lax.axis_index("rep")
    shard = lax.axis_index("shard")
    depth, twin = shard // 2, shard % 2
    is_low = depth <= 1
    is_core = (depth == 1) | (depth == 2)
    where = jnp.stack([depth, rep, twin]).astype(jnp.int32)
    bits = (rep & 1, rep >> 1)
    bit_words = jnp.stack(bits).astype(jnp.int32)

    def order(four):
        own, near, middle, far = four
        return jnp.where(
            is_low, jnp.stack([near, own, middle, far]), jnp.stack([far, middle, own, near])
        )

    def absolute(mine, theirs):
        one, two = order(mine), order(theirs)
        return jnp.where(twin == 0, jnp.stack([one, two], 1), jnp.stack([two, one], 1))

    def own_piece(pack):
        piece = lax.dynamic_index_in_dim(pack, rep, 0, keepdims=False)
        return piece.reshape(-1, width)

    def units_of(item):
        return item.reshape(-1, UNIT, width)

    def pack_front(entry, leaving):
        return jnp.concatenate([by_columns(entry), by_columns(leaving)], axis=1)

    def pack_feed(expand, shrink):
        return jnp.concatenate([by_columns(expand), low(shrink).reshape(4, 4, UNIT, width)], axis=1)

    def by_columns(weight):
        count = weight.shape[1] // width
        return low(weight).reshape(4, UNIT, count, width).transpose(0, 2, 1, 3)

    extra = layers * vectors.shape[1] // width
    tail = low(vectors).reshape(extra, width)
    table = jnp.concatenate([dealing // 64, dealing % 64, key_mask], axis=0)
    table = low(table).reshape(1, width)
    filler = jnp.zeros((7 - extra, width), jnp.bfloat16)
    rows_in = jnp.concatenate([inputs, tail, table, filler], axis=0)

    def group(items, begin, end):
        return jnp.stack([units_of(item[begin:end]) for item in items])

    front_zero = pack_front(entry_weight[0], exit_weight[0])
    piece = own_piece(front_zero)
    near = send(piece, TO_SIDE)
    middle = send(piece, TO_MID)
    feed_zero = pack_feed(expand_weight[0], shrink_weight[0])
    in_rows = rows_in.shape[0]
    far = send(near, TO_MID)
    first = jnp.stack([units_of(item) for item in (near, middle, far)])
    front_spread = Spread(front_zero, first, False)
    rows_late, twin_late, lengths = after([rows_in, twin, lengths], first)
    second = jnp.concatenate([rows_late, own_piece(feed_zero)], axis=0)
    second_near = send(second, TO_SIDE)
    second_middle = send(second, TO_MID)
    second_far = send(second_near, TO_MID)

    entry_late, exit_late, expand_late, shrink_late, cotangent_late = after(
        [entry_weight[1], exit_weight[1], expand_weight[1], shrink_weight[1], cotangent], first
    )
    front_one = pack_front(entry_late, exit_late)
    feed_one = pack_feed(expand_late, shrink_late)
    third = jnp.concatenate([own_piece(front_one), own_piece(feed_one), cotangent_late], axis=0)
    ready = front_spread.turn()

    second_middle, second_far = after([second_middle, second_far], ready)
    four = (second, second_near, second_middle, second_far)
    mine = jnp.stack([item[:in_rows] for item in four])
    theirs = send(mine, TO_TWIN)
    feed_spread = Spread(feed_zero, tie(group(four[1:], in_rows, in_rows + 8 * UNIT), ready), True)
    third = tie(third, ready)
    third_near = send(third, TO_SIDE)
    third_middle = send(third, TO_MID)
    fronts = [assemble(where, front_spread.parts(feed_spread.first, mine, third_near), 0, False)]

    header = absolute(tuple(mine[:, rows:]), tuple(theirs[:, rows:]))
    header = header.reshape(8, 8, width)
    vector_all = wide(header[:, :extra]).reshape(8, layers, vectors.shape[1])
    vector_all = jnp.transpose(vector_all, (1, 0, 2)).reshape(layers, 12, width)
    numbers = wide(header[:, extra]).reshape(8, 3, rows)
    dealt_all = (numbers[:, 0] * 64 + numbers[:, 1]).astype(jnp.int32).reshape(group_rows)
    mask_all = numbers[:, 2].reshape(group_rows)

    member, leading = sequence_ids(lengths[0], group_rows)
    usable = (mask_all == 1) | leading
    code = jnp.where(usable, member, -1)
    longest = jnp.argmax(lengths[0])
    begin = jnp.cumsum(lengths[0])[longest] - lengths[0][longest]
    spot = jnp.arange(half_rows, dtype=jnp.int32)

    def halve(values, low_side):
        inside = lax.dynamic_slice_in_dim(values, begin, half_rows, 0)
        outside = jnp.where(spot < begin, values[:half_rows], values[half_rows:])
        return jnp.where(low_side, inside, outside)

    def cores(values):
        own = lax.dynamic_slice_in_dim(values, twin * core_rows, core_rows, 0)
        other = lax.dynamic_slice_in_dim(values, (1 - twin) * core_rows, core_rows, 0)
        return own, other

    code_half = jnp.concatenate(cores(halve(code, is_low))).reshape(half_rows, 1)
    member_own = cores(halve(member, is_low))[0].reshape(1, core_rows)
    dealt_near = cores(halve(dealt_all, is_low))
    dealt_far = cores(halve(dealt_all, ~is_low))

    block = jnp.arange(width, dtype=jnp.int32)
    place = jnp.arange(width // 2, dtype=jnp.int32)
    chunk = 4 * UNIT
    source = (place // chunk) * (2 * chunk) + place % chunk
    cores_at = jnp.stack([twin_late, 1 - twin_late])
    sel = low(block[None, :, None] == (source[None, :] + cores_at[:, None] * chunk)[:, None, :])

    local = jnp.arange(rows, dtype=jnp.int32)
    bases = jnp.stack(
        [
            (depth ^ flip) * (2 * rows) + (twin ^ side) * rows
            for side in range(2)
            for flip in (0, 1, 3, 2)
        ]
    ).astype(jnp.int32)
    source_ids = (bases[:, None] + local[None, :]).reshape(8, 1, rows)
    want_in = dealt_near[0].reshape(core_rows, 1)
    theirs, third_near = after([theirs, third_near], fronts[0])
    third_far = send(third_near, TO_MID)
    hidden_low = gather_rows((mine, tie(theirs, third_near)), source_ids, want_in, 0.3)

    result_ids = jnp.stack([dealt_near[0], dealt_far[0], dealt_near[1], dealt_far[1]]).reshape(
        4, 1, core_rows
    )
    want_out = jnp.concatenate([source_ids[0, 0], source_ids[1, 0]]).reshape(2 * rows, 1)

    def deliver(pieces, spend):
        pieces = [piece[None] for piece in pieces]
        found = gather_rows(pieces, result_ids, want_out, spend)
        return found, send(found[rows:], TO_SIDE)

    saved = []
    def begin(layer):
        queries, kv, xm, xt = project(hidden_low, fronts[layer], vector_all[layer], sel)
        return queries, kv, send(kv, TO_TWIN), xm, send(xt, TO_TWIN)

    def attention(queries, kv, kv_twin):
        return attend_fast(queries, kv, kv_twin, code_half, member_own)

    def complete(layer, attended):
        results = post(
            where, attended, hidden, fronts[layer], ups[layer], downs[layer],
            vector_all[layer], sel,
        )
        return results, send(results[8], TO_TWIN)

    def record(start, middle, results, others):
        queries, kv, kv_twin, xm, xo = start
        saved.append(
            (queries, kv, kv_twin) + tuple(middle[1:]) + tuple(results[2:7])
            + (xm, xo, results[7], others)
        )

    hidden = hidden_low
    ready = feed_spread.turn(fronts[0])
    hidden_low, third_middle = after([hidden_low, third_middle], ready)
    hidden_low = tie(hidden_low, third_middle)
    start = begin(0)
    middle = attention(*start[:3])
    parts = feed_spread.parts(middle[0])
    third_far = tie(third_far, middle[0])
    four = (third, third_near, third_middle, third_far)
    split = 12 * UNIT
    front_spread = Spread(front_one, group(four[1:], 0, 4 * UNIT), True)
    cotangent_mine = jnp.stack([item[split:] for item in four])
    ups = [assemble(where, parts, 0, False)]
    downs = [assemble(where, parts, 4, True)]
    ready = front_spread.turn(ups[0], downs[0])
    feed_spread = Spread(feed_one, tie(group(four[1:], 4 * UNIT, split), ready), False)
    cotangent_theirs = send(cotangent_mine, TO_TWIN)
    held = [feed_spread.first, cotangent_theirs] + front_spread.twins + feed_spread.twins
    results, others = complete(0, tie(middle[0], ready, start[4], *held))
    hidden, hidden_low = results[:2]
    record(start, middle, results, others)
    ready = feed_spread.turn(hidden_low)
    fronts.append(assemble(where, front_spread.parts(ready), 0, False))
    start = begin(1)
    upstream = gather_rows(
        (cotangent_mine, tie(cotangent_theirs, start[0])), source_ids, want_in, 0.3
    )
    middle = attention(tie(start[0], upstream), start[1], start[2])
    parts = feed_spread.parts(middle[0])
    ups.append(assemble(where, parts, 0, False))
    downs.append(assemble(where, parts, 4, True))
    results, others = complete(1, middle[0])
    hidden, hidden_low = results[:2]
    record(start, middle, results, others)
    result_mid = send(hidden_low, TO_MID)
    result_twin = send(hidden_low, TO_TWIN)

    def start_back(layer, grad, spend):
        n1, t1, n2, t2, slope = saved[layer][5:10]
        slopes, do, dr, sums = post_back(
            grad, n1, t1, n2, t2, slope,
            fronts[layer], ups[layer], downs[layer], vector_all[layer], spend,
        )
        return slopes, send(slopes, TO_TWIN), do, dr, sums

    def attention_back(layer, do, spend):
        queries, kv, kv_twin, ot, lse = saved[layer][:5]
        return attend_back_fast(
            queries, do, kv, kv_twin, ot, lse, code_half, member_own, spend
        )

    def feed_part(layer, x_first, slopes, slopes_twin, spend):
        mine, others = saved[layer][12:14]
        keep_up, give_up, keep_down, give_down = feed_grad(
            x_first, bit_words, mine, others, slopes, slopes_twin, spend
        )
        work = Reduction(
            [(keep_up, give_up, x_first), (keep_down, give_down, not x_first)],
            bits, is_low, is_core,
        )
        return work, keep_up

    def front_part(layer, slopes, slopes_twin, dm, dm_twin, spend):
        xm, xo, mine, others = saved[layer][10:14]
        keep_x, give_x, keep_y, give_y = front_grad(
            bit_words, xm, xo, mine, others, dm, dm_twin, slopes, slopes_twin, spend
        )
        work = Reduction(
            [(keep_x, give_x, True), (keep_y, give_y, False)], bits, is_low, is_core
        )
        return work, keep_x

    upstream = tie(upstream, saved[0][11], saved[0][13])
    slopes_b, slopes_tb, do, dr, sums_b = start_back(1, upstream, 16)
    dq, own, give = attention_back(1, do, 21)
    got = send(give, TO_TWIN)
    feed_b, mark = feed_part(1, True, slopes_b, tie(slopes_tb, dq, saved[1][11], result_twin), 12)
    pair = (hidden_low, tie(result_mid, mark))
    pair += (result_twin, send(pair[1], TO_TWIN))
    dm_b, grad, _, head_b = project_back(dq, own, got, fronts[1], tie(dr, mark, pair[1]), 0.5)
    dm_tb = send(dm_b, TO_TWIN)
    found, output_side = deliver(after(pair, head_b), 0.5)
    slopes_a, slopes_ta, do, dr, sums_a = start_back(0, tie(grad, found), 0.5)
    ready = feed_b.across(3, do)
    dq, own, give = attention_back(0, tie(do, ready), 45)
    got = send(give, TO_TWIN)
    front_b, mark = front_part(1, slopes_b, slopes_tb, dm_b, tie(dm_tb, dq), 0.5)
    feed_a, mark = feed_part(0, False, slopes_a, tie(slopes_ta, mark, output_side, feed_b.mid), 12)
    ready = front_b.across(2, mark)
    dm_a, grad, grad_low, head_a = project_back(
        dq, own, got, fronts[0], tie(dr, ready), 0.5
    )
    dm_ta = send(dm_a, TO_TWIN)
    grad_mid = send(grad_low, TO_MID)
    grad_twin = send(grad_low, TO_TWIN)

    vectors_all = [
        jnp.concatenate([head_sums, sums[2:]], axis=0)
        for head_sums, sums in ((head_a, sums_a), (head_b, sums_b))
    ]
    joined = jnp.stack([item.reshape(-1) for item in vectors_all])
    joined = jnp.transpose(joined.reshape(layers, 4, 2, vectors.shape[1]), (1, 2, 0, 3))
    vector_keep = lax.dynamic_index_in_dim(joined, twin, 1, keepdims=False)
    vector_give = lax.dynamic_index_in_dim(joined, 1 - twin, 1, keepdims=False)
    vector_twin = send(vector_give, TO_TWIN)

    ready = feed_a.across(25, grad_low, front_b.mid)
    front_a, mark = front_part(0, slopes_a, slopes_ta, dm_a, tie(dm_ta, vector_give, ready, grad_twin), 0.5)

    feed_b.join(front_b)
    ready = feed_b.outward(mark)
    vector_stage = vector_keep + tie(vector_twin, ready)
    vector_over = send(vector_stage, TO_X)
    pair = (grad_low, tie(grad_mid, vector_stage), grad_twin)
    pair += (send(pair[1], TO_TWIN),)
    found_in, input_side = deliver(pair, 0.5)
    ready = feed_b.turn(found_in)
    vector_stage = vector_stage + tie(vector_over, ready)
    vector_over = send(vector_stage, TO_Y)

    ready = front_a.across(0.5, vector_stage)
    ready = feed_b.share(ready)
    vector_stage = vector_stage + tie(vector_over, ready)
    vector_give = jnp.where(is_low, vector_stage[2:4], vector_stage[0:2])
    vector_keep = jnp.where(is_low, vector_stage[0:2], vector_stage[2:4])
    vector_mid = send(vector_give, TO_MID)
    ready = feed_a.outward(vector_give)
    ups_at = tuple((2, place) for place in range(4))
    downs_at = tuple((3, place) for place in range(4))
    early_at, late_at = ((0, 0), (0, 1)), ((0, 2), (1, 0))
    plan = ((True, ups_at + early_at), (False, downs_at + late_at))

    ready = front_a.outward(ready)
    grads = unpack(bit_words, feed_b.finish(ready), plan, 1, layers, ())
    vector_stage = vector_keep + tie(vector_mid, ready)
    vector_outer = jnp.where(is_low, vector_stage[0], vector_stage[1])
    vector_inner = jnp.where(is_low, vector_stage[1], vector_stage[0])
    vector_side = send(vector_outer, TO_SIDE)
    ready = feed_a.turn(vector_outer, grads[1])
    output = jnp.where(is_core, found[:rows], output_side)
    input_grad = wide(jnp.where(is_core, found_in[:rows], tie(input_side, ready)))

    ready = front_a.turn(ready)
    ready_two = feed_a.share(ready)
    ready = front_a.share(ready_two)
    pairs = feed_a.finish(ready) + front_a.finish(ready)
    plan = ((False, ups_at), (True, downs_at), (True, early_at), (False, late_at))
    entry_grad, exit_grad, expand_grad, shrink_grad = unpack(
        bit_words, pairs, plan, 0, layers, grads
    )
    vector_grad = jnp.where(is_core, vector_inner, tie(vector_side, ready))
    return (output, input_grad, entry_grad, exit_grad, expand_grad, shrink_grad, vector_grad)


def solution(mesh):
    placed = (
        P(("rep", "shard"), None),
        P(("rep", "shard"), None),
        P("rep", None),
        P("rep", "shard"),
        P("rep", "shard"),
        P(None, "shard", None),
        P(None, "shard", None),
        P(None, "shard", None),
        P(None, "shard", None),
        P(None, "shard"),
    )
    small = dict(mesh.shape) == {"rep": 4, "shard": 8}
    return jax.shard_map(
        body_fast if small else body,
        mesh=mesh,
        in_specs=placed,
        out_specs=(
            P(("rep", "shard"), None),
            P(("rep", "shard"), None),
            P(None, "shard", None),
            P(None, "shard", None),
            P(None, "shard", None),
            P(None, "shard", None),
            P(None, "shard"),
        ),
        check_vma=False,
    )
```
